32 devices in a mesh: dp: 8 (over z, x), seq: 4 (over y, core).
Axes of the slice: x: 2, y: 2, z: 4, core: 2. Of those that a mesh axis runs over, the one named last changes fastest.
Arguments:
- tokens: bfloat16 [4096, 2048], P(('dp', 'seq')), may hold values from -6 to 6
- cotangent: bfloat16 [4096, 2048], P(('dp', 'seq')), may hold values from -6 to 6
- first_layer_norm_gain: bfloat16 [2048], P('dp'), may hold values from 0.5 to 1.5
- first_layer_norm_bias: bfloat16 [2048], P('dp'), may hold values from -3 to 3
- w_qkv: bfloat16 [2048, 3072], P('dp')
- b_qkv: bfloat16 [3072], P('dp'), may hold values from -3 to 3
- w_out: bfloat16 [1024, 2048], P('dp'), may hold values from -0.75 to 0.75
- second_layer_norm_gain: bfloat16 [2048], P('dp'), may hold values from 0.5 to 1.5
- second_layer_norm_bias: bfloat16 [2048], P('dp'), may hold values from -3 to 3
- w_gate_up: bfloat16 [2048, 5632], P('dp'), may hold values from -0.125 to 0.125
- w_down: bfloat16 [2816, 2048], P('dp'), may hold values from -0.109375 to 0.109375
Outputs:
- block_out: bfloat16 [4096, 2048], P(('dp', 'seq'))
- input_grad: float32 [4096, 2048], P(('dp', 'seq'))
- g_ln1_gain: float32 [2048], P(('dp', 'seq'))
- g_ln1_bias: float32 [2048], P(('dp', 'seq'))
- g_w_qkv: float32 [2048, 3072], P(('dp', 'seq'))
- g_b_qkv: float32 [3072], P(('dp', 'seq'))
- g_w_out: float32 [1024, 2048], P(('dp', 'seq'))
- g_ln2_gain: float32 [2048], P(('dp', 'seq'))
- g_ln2_bias: float32 [2048], P(('dp', 'seq'))
- g_w_gate_up: float32 [2048, 5632], P(('dp', 'seq'))
- g_w_down: float32 [2816, 2048], P(('dp', 'seq'))
The draws below stay inside these ranges and needn't reach their ends.
All inputs are finite; a program needn't handle non-finite values.
Results may differ from the reference program's by a relative error of at most 0.014.
Values may be sent and summed in bfloat16 or wider, within the bound.
A program may use at most 320 MiB of HBM per device.

```python
import jax
import jax.numpy as jnp
from jax import lax

D = 2048
HEADS = 16
HEAD_DIM = 64
ROT = 16
FF = 2816
INNER = 1024
SEQ_LEN = 512
TOKENS = 4096
N_DP = 8


def draw_w_qkv(key, part):
    inner_width = HEADS * HEAD_DIM
    base = jax.random.normal(key, (D, 3 * inner_width), jnp.float32) * D ** (-0.5)
    return base.astype(jnp.bfloat16)


def raised(values, rng, source, target, blocks, factor):
    def block_of(position):
        return (jnp.arange(values.shape[position]) // (values.shape[position] // blocks)).reshape((-1,) + (1,) * (values.ndim - 1 - position))

    one_side = jax.random.permutation(rng, blocks)[block_of(target)]
    second = (block_of(target) + blocks // 2) % blocks
    return jnp.where((block_of(source) == one_side) | (block_of(source) == second), factor * values, values)


def shard_levels(stream_key, dims, shards, least, top_value):
    level = 1.0
    for dim, blocks in shards:
        heights = jax.random.uniform(jax.random.fold_in(jax.random.fold_in(stream_key, 6), dim), (blocks,), jnp.float32, least / len(shards), top_value / len(shards))
        level = level * jnp.repeat(jnp.exp(heights), dims[dim] // blocks).reshape((-1,) + (1,) * (len(dims) - 1 - dim))
    return level


def centred(stream_key, shape, spread, reach, pieces=(), kind=jnp.bfloat16):
    loudness = shard_levels(stream_key, shape, pieces, -0.22, 0.18) if pieces else 1.0
    drawn = jax.random.normal(stream_key, shape, jnp.float32) * spread * loudness
    return jnp.minimum(jnp.maximum(drawn, -reach), reach).astype(kind)


def gaussian_with(own_key, extent, deviation, reach, split, heavy, kind=jnp.bfloat16):
    values = deviation * jax.random.normal(own_key, extent, jnp.float32)
    if split:
        values = values * shard_levels(own_key, extent, split, -0.22, 0.18)
    return jnp.clip(raised(values, jax.random.fold_in(own_key, 3), *heavy), -reach, reach).astype(kind)


def setup_inputs(seed: int = 0) -> dict:
    splits = jax.random.split(jax.random.key(seed), 12)
    tokens = gaussian_with(splits[0], (TOKENS, D), 1.0, 6.0, ((0, 32),), (0, 1, 32, 2.75))
    cotangent = centred(splits[1], (TOKENS, D), 1.0, 6.0, ((0, 32),))
    first_layer_norm_gain = jnp.clip(1.0 + 0.1 * jax.random.normal(splits[2], (D,), jnp.float32), 0.5, 1.5).astype(jnp.bfloat16)
    first_layer_norm_bias = centred(splits[3], (D,), 0.5, 3.0, ((0, 8),))
    w_qkv = draw_w_qkv(jax.random.fold_in(splits[11], 71), 0)
    b_qkv = centred(splits[5], (3 * INNER,), 0.5, 3.0, ((0, 8),))
    w_out = centred(splits[6], (INNER, D), (INNER // 16) ** -0.5, 0.75, ((0, 8),))
    second_layer_norm_gain = jnp.clip(1.0 + 0.1 * jax.random.normal(splits[7], (D,), jnp.float32), 0.5, 1.5).astype(jnp.bfloat16)
    second_layer_norm_bias = centred(splits[8], (D,), 0.5, 3.0, ((0, 8),))
    w_gate_up = centred(splits[9], (D, 2 * FF), D ** -0.5, 0.125, ((0, 8),))
    w_down = centred(splits[10], (FF, D), FF ** -0.5, 0.109375, ((0, 8),))
    return dict(tokens=tokens, cotangent=cotangent, first_layer_norm_gain=first_layer_norm_gain, first_layer_norm_bias=first_layer_norm_bias, w_qkv=w_qkv, b_qkv=b_qkv, w_out=w_out, second_layer_norm_gain=second_layer_norm_gain, second_layer_norm_bias=second_layer_norm_bias, w_gate_up=w_gate_up, w_down=w_down)


EPS = 1e-05

def layer_norm_forward(value, gain, shift):
    center = value - lax.optimization_barrier(jnp.mean(value, axis=-1, keepdims=True))
    scale_inv = lax.rsqrt(lax.optimization_barrier(jnp.mean(center * center, axis=-1, keepdims=True)) + EPS)
    normed = center * scale_inv
    return (normed, scale_inv, normed * gain.astype(jnp.float32) + shift.astype(jnp.float32))

def layer_norm_backward(upstream, normed, scale_inv, gain):
    scaled = upstream * gain.astype(jnp.float32)
    inner = scaled - lax.optimization_barrier(jnp.mean(scaled, axis=-1, keepdims=True)) - normed * lax.optimization_barrier(jnp.mean(scaled * normed, axis=-1, keepdims=True))
    return (scale_inv * inner, lax.optimization_barrier(jnp.sum(upstream * normed, axis=0)), lax.optimization_barrier(jnp.sum(upstream, axis=0)))

def rotary_tables(positions):
    half = ROT // 2
    inverse = 10000.0 ** (-(jnp.arange(half, dtype=jnp.float32) * 2.0 / ROT))
    angles = positions.astype(jnp.float32)[:, None] * inverse[None, :]
    return (jnp.cos(angles)[:, None, :], jnp.sin(angles)[:, None, :])

def rotate(tensor, cosine, sine):
    half = ROT // 2
    first = tensor[..., :half]
    second = tensor[..., half:ROT]
    return jnp.concatenate([first * cosine - second * sine, second * cosine + first * sine, tensor[..., ROT:]], axis=-1)

def unrotate(tensor, cosine, sine):
    half = ROT // 2
    first = tensor[..., :half]
    second = tensor[..., half:ROT]
    return jnp.concatenate([first * cosine + second * sine, second * cosine - first * sine, tensor[..., ROT:]], axis=-1)

def masked_scores(queries, keys, positions):
    scale = HEAD_DIM ** (-0.5)
    scores = jnp.einsum('qhd,khd->hqk', queries.astype(jnp.float32), keys.astype(jnp.float32)) * scale
    allowed = positions[None, :] <= positions[:, None]
    return jnp.where(allowed[None], scores, -jnp.inf)

def one_sequence(params, x_b, dout_b):
    first_layer_norm_gain, first_layer_norm_bias, w_qkv, b_qkv, w_out, second_layer_norm_gain, second_layer_norm_bias, w_gate_up, w_down = params
    length = x_b.shape[0]
    width = HEADS * HEAD_DIM
    scale = HEAD_DIM ** (-0.5)
    positions = jnp.arange(length, dtype=jnp.int32)
    cosine, sine = rotary_tables(positions)
    input_state = x_b.astype(jnp.float32)
    first_centered_scaled, first_inverse_deviation, first_normalized = layer_norm_forward(input_state, first_layer_norm_gain, first_layer_norm_bias)
    normed1_b = first_normalized.astype(jnp.bfloat16)
    qkv = jnp.dot(normed1_b, w_qkv, preferred_element_type=jnp.float32) + b_qkv.astype(jnp.float32)
    queries = rotate(qkv[:, :width].reshape(length, HEADS, HEAD_DIM), cosine, sine).astype(jnp.bfloat16)
    keys = rotate(qkv[:, width:2 * width].reshape(length, HEADS, HEAD_DIM), cosine, sine).astype(jnp.bfloat16)
    values = qkv[:, 2 * width:].reshape(length, HEADS, HEAD_DIM).astype(jnp.bfloat16)
    scores = masked_scores(queries, keys, positions)
    top = lax.optimization_barrier(jnp.max(scores, axis=-1, keepdims=True))
    lse = top + jnp.log(lax.optimization_barrier(jnp.sum(jnp.exp(scores - top), axis=-1, keepdims=True)))
    probs_b = jnp.exp(scores - lse).astype(jnp.bfloat16)
    context = jnp.einsum('hqk,khd->qhd', probs_b.astype(jnp.float32), values.astype(jnp.float32)).astype(jnp.bfloat16)
    context_flat = context.reshape(length, width)
    middle_state = input_state + jnp.dot(context_flat, w_out, preferred_element_type=jnp.float32)
    second_centered_scaled, second_inverse_deviation, second_normalized = layer_norm_forward(middle_state, second_layer_norm_gain, second_layer_norm_bias)
    normed2_b = second_normalized.astype(jnp.bfloat16)
    gate_up = jnp.dot(normed2_b, w_gate_up, preferred_element_type=jnp.float32)
    gate = gate_up[:, :FF]
    up = gate_up[:, FF:]
    sigma = jax.nn.sigmoid(gate)
    silu = gate * sigma
    act = (silu * up).astype(jnp.bfloat16)
    out = (middle_state + jnp.dot(act, w_down, preferred_element_type=jnp.float32)).astype(jnp.bfloat16)
    g_down = jnp.dot(act.T, dout_b, preferred_element_type=jnp.float32)
    d_act = jnp.dot(dout_b, w_down.T, preferred_element_type=jnp.float32)
    d_gate = d_act * up * (sigma * (1.0 + gate * (1.0 - sigma)))
    d_up = d_act * silu
    d_gate_up = jnp.concatenate([d_gate, d_up], axis=1).astype(jnp.bfloat16)
    g_gate_up = jnp.dot(normed2_b.T, d_gate_up, preferred_element_type=jnp.float32)
    second_normalized_gradient = jnp.dot(d_gate_up, w_gate_up.T, preferred_element_type=jnp.float32)
    middle_norm_gradient, second_gain_gradient, second_bias_gradient = layer_norm_backward(second_normalized_gradient, second_centered_scaled, second_inverse_deviation, second_layer_norm_gain)
    d_mid = dout_b.astype(jnp.float32) + middle_norm_gradient
    d_mid_b = d_mid.astype(jnp.bfloat16)
    g_out = jnp.dot(context_flat.T, d_mid_b, preferred_element_type=jnp.float32)
    d_context = jnp.dot(d_mid_b, w_out.T, preferred_element_type=jnp.float32).astype(jnp.bfloat16).reshape(length, HEADS, HEAD_DIM)
    probs = jnp.exp(masked_scores(queries, keys, positions) - lse)
    probs_r = probs.astype(jnp.bfloat16)
    d_probs = jnp.einsum('qhd,khd->hqk', d_context.astype(jnp.float32), values.astype(jnp.float32))
    delta = jnp.einsum('qhd,qhd->hq', d_context.astype(jnp.float32), context.astype(jnp.float32))[..., None]
    d_scores = (probs * (d_probs - delta) * scale).astype(jnp.bfloat16).astype(jnp.float32)
    d_queries = jnp.einsum('hqk,khd->qhd', d_scores, keys.astype(jnp.float32))
    d_keys = jnp.einsum('hqk,qhd->khd', d_scores, queries.astype(jnp.float32))
    d_values = jnp.einsum('hqk,qhd->khd', probs_r.astype(jnp.float32), d_context.astype(jnp.float32))
    d_queries = unrotate(d_queries, cosine, sine).reshape(length, width)
    d_keys = unrotate(d_keys, cosine, sine).reshape(length, width)
    d_qkv = jnp.concatenate([d_queries, d_keys, d_values.reshape(length, width)], axis=1)
    g_bias_qkv = lax.optimization_barrier(jnp.sum(d_qkv, axis=0))
    d_qkv_b = d_qkv.astype(jnp.bfloat16)
    g_qkv = jnp.dot(normed1_b.T, d_qkv_b, preferred_element_type=jnp.float32)
    first_normalized_gradient = jnp.dot(d_qkv_b, w_qkv.T, preferred_element_type=jnp.float32)
    input_norm_gradient, first_gain_gradient, first_bias_gradient = layer_norm_backward(first_normalized_gradient, first_centered_scaled, first_inverse_deviation, first_layer_norm_gain)
    d_x = d_mid + input_norm_gradient
    grads = (first_gain_gradient, first_bias_gradient, g_qkv, g_bias_qkv, g_out, second_gain_gradient, second_bias_gradient, g_gate_up, g_down)
    return (out, d_x, grads)

def reference(tokens, cotangent, first_layer_norm_gain, first_layer_norm_bias, w_qkv, b_qkv, w_out, second_layer_norm_gain, second_layer_norm_bias, w_gate_up, w_down):
    params = (first_layer_norm_gain, first_layer_norm_bias, w_qkv, b_qkv, w_out, second_layer_norm_gain, second_layer_norm_bias, w_gate_up, w_down)
    inner_width = HEADS * HEAD_DIM
    shapes = [(D,), (D,), (D, 3 * inner_width), (3 * inner_width,), (inner_width, D), (D,), (D,), (D, 2 * FF), (FF, D)]
    start = tuple((jnp.zeros(shape, jnp.float32) for shape in shapes))
    sequences = tokens.reshape(N_DP, SEQ_LEN, D)
    upstream = cotangent.reshape(N_DP, SEQ_LEN, D)

    def step(carry, inputs):
        out, d_x, grads = one_sequence(params, inputs[0], inputs[1])
        return (tuple((a + b for a, b in zip(carry, grads))), (out, d_x))
    totals, (outs, d_xs) = lax.scan(step, start, (sequences, upstream))
    return (outs.reshape(TOKENS, D), d_xs.reshape(TOKENS, D), totals[0], totals[1], totals[2], totals[3], totals[4], totals[5], totals[6], totals[7], totals[8])
```

```python
import functools

import jax
import jax.numpy as jnp
from jax import lax
from jax.experimental import pallas as pl
from jax.experimental.pallas import tpu as pltpu
from jax.sharding import PartitionSpec as P

HEAD_DIM = 64
ROT = 16
EPS = 1e-05
F32 = jnp.float32
BF16 = jnp.bfloat16


def ring_order(n):
    return list(range(0, n, 2)) + list(range(n - 1, 0, -2))


def dot(a, b):
    return jnp.dot(a, b, preferred_element_type=F32)


def dot_rows(a, b):
    return lax.dot_general(a, b, (((0,), (0,)), ((), ())), preferred_element_type=F32)


def dot_cols(a, b):
    return lax.dot_general(a, b, (((1,), (1,)), ((), ())), preferred_element_type=F32)


class Ring:
    def __init__(self):
        n = lax.axis_size("dp")
        order = ring_order(n)
        place = [order.index(i) for i in range(n)]
        self.n, self.half = n, n // 2
        self.right = [(order[i], order[(i + 1) % n]) for i in range(n)]
        self.left = [(b, a) for a, b in self.right]
        self.order = jnp.array(order, jnp.int32)
        self.place = jnp.array(place, jnp.int32)[lax.axis_index("dp")]

    def owner(self, offset):
        return self.order[lax.rem(self.place + offset + self.n, self.n)]

    def go_right(self, value):
        return lax.ppermute(value, "dp", self.right)

    def go_left(self, value):
        return lax.ppermute(value, "dp", self.left)

    def gather(self, piece):
        rows = piece.shape[0]
        cut = rows // 2
        from_left = from_right = piece
        whole = jnp.zeros((self.n,) + piece.shape, piece.dtype)

        def put(whole, offset, chunk):
            return lax.dynamic_update_slice(
                whole, chunk[None], (self.owner(offset),) + (0,) * piece.ndim
            )

        whole = put(whole, 0, piece)
        for k in range(1, self.half):
            from_left = self.go_right(from_left)
            from_right = self.go_left(from_right)
            whole = put(put(whole, -k, from_left), k, from_right)
        upper = self.go_right(from_left[:cut])
        lower = self.go_left(from_right[cut:])
        return put(whole, self.half, jnp.concatenate([upper, lower]))

    def scatter(self, parts):
        rows = parts.shape[1]
        cut = rows // 2

        def mine(offset):
            start = (self.owner(offset),) + (0,) * (parts.ndim - 1)
            return lax.dynamic_slice(parts, start, (1,) + parts.shape[1:])[0]

        def add(a, b):
            return a.astype(F32) + b.astype(F32)

        far = mine(self.half)
        upper = self.go_right(far[:cut])
        lower = self.go_left(far[cut:])
        from_left, from_right = mine(self.half - 1), mine(1 - self.half)
        from_left = jnp.concatenate(
            [add(from_left[:cut], upper).astype(BF16), from_left[cut:]]
        )
        from_right = jnp.concatenate(
            [from_right[:cut], add(from_right[cut:], lower).astype(BF16)]
        )
        for k in range(self.half - 2, -1, -1):
            from_left = self.go_right(from_left)
            from_right = self.go_left(from_right)
            if k:
                from_left = add(from_left, mine(k)).astype(BF16)
                from_right = add(from_right, mine(-k)).astype(BF16)
        return add(mine(0), from_left) + from_right.astype(F32)


class Group:
    def __init__(self):
        self.m = lax.axis_size("seq")
        self.s = lax.axis_index("seq")
        self.bits = []
        bit = self.m // 2
        while bit:
            self.bits.append(bit)
            bit //= 2
        self.offsets = [0]
        for bit in self.bits:
            self.offsets += [o ^ bit for o in self.offsets]

    def swap(self, value, mask):
        return lax.ppermute(value, "seq", [(i, i ^ mask) for i in range(self.m)])

    def gather(self, value):
        for bit in self.bits:
            value = jnp.concatenate([value, self.swap(value, bit)])
        return value

    def scatter(self, value):
        for bit in reversed(self.bits):
            half = value.shape[0] // 2
            got = self.swap(value[half:].astype(BF16), bit)
            value = value[:half] + got.astype(F32)
        return value

    def exchange(self, blocks):
        got = []
        for mask in range(self.m):
            block = lax.dynamic_index_in_dim(blocks, self.s ^ mask, 0, keepdims=False)
            got.append(self.swap(block, mask) if mask else block)
        stacked = jnp.stack(got)
        return jnp.take(stacked, self.s ^ jnp.arange(self.m), axis=0)


def norm(value):
    center = value - jnp.mean(value, axis=-1, keepdims=True)
    rstd = lax.rsqrt(jnp.mean(center * center, axis=-1, keepdims=True) + EPS)
    return center * rstd, rstd


def norm_back(upstream, xhat, rstd, gain):
    e = upstream * gain
    inner = (
        e
        - jnp.mean(e, axis=-1, keepdims=True)
        - xhat * jnp.mean(e * xhat, axis=-1, keepdims=True)
    )
    return rstd * inner


def rotary_tables(positions):
    half = ROT // 2
    inverse = 10000.0 ** (-(jnp.arange(half, dtype=F32) * 2.0 / ROT))
    angles = positions.astype(F32)[:, None] * inverse[None, :]
    return jnp.cos(angles)[:, None, :], jnp.sin(angles)[:, None, :]


def rotate(tensor, cosine, sine):
    half = ROT // 2
    a, b = tensor[..., :half], tensor[..., half:ROT]
    return jnp.concatenate([a * cosine - b * sine, b * cosine + a * sine, tensor[..., ROT:]], axis=-1)


def shards_plain(tokens, cotangent, gain1, bias1, w_qkv, b_qkv, w_out, gain2, bias2, w_gate_up, w_down):
    ring, group = Ring(), Group()
    n, m, s = ring.n, group.m, group.s
    rows, width = tokens.shape
    slab = gain1.shape[0]
    inner = w_out.shape[0] * n
    hidden = w_down.shape[0] * n
    part, ff = inner // m, hidden // m
    heads = part // HEAD_DIM
    scale = HEAD_DIM ** (-0.5)

    both = jnp.stack([tokens, cotangent], axis=1)
    everything = group.gather(both)
    tokens_all, cot_all = everything[:, 0], everything[:, 1]

    qkv_piece = jnp.concatenate(
        [lax.dynamic_slice(w_qkv, (0, i * inner + s * part), (slab, part)) for i in range(3)], axis=1
    )
    small = jnp.concatenate([gain1, bias1, gain2, bias2, b_qkv])
    extra = -(-small.shape[0] // (3 * part))
    small = jnp.pad(small, (0, extra * 3 * part - small.shape[0])).reshape(extra, 3 * part)
    first = ring.gather(jnp.concatenate([qkv_piece, small]))
    wqkv = first[:, :slab].reshape(width, 3 * part)
    vectors = first[:, slab:].reshape(n, -1)

    def vector(at, size):
        return vectors[:, at : at + size].reshape(-1).astype(F32)

    g1, b1, g2, b2 = (vector(i * slab, slab) for i in range(4))
    bias_all = vector(4 * slab, b_qkv.shape[0]).reshape(3, m, part)
    bias_qkv = lax.dynamic_index_in_dim(bias_all, s, 1, keepdims=False).reshape(3 * part)

    turn = [(g, (g % n) * m + g // n) for g in range(n * m)]
    back = [(b, a) for a, b in turn]

    def quarter(weight):
        count = weight.shape[0] // m
        mine = lax.dynamic_slice(weight, (0, 0), weight.shape)
        return mine.reshape(m, count, weight.shape[1])[s]

    out_rows, down_rows = w_out.shape[0] // m, w_down.shape[0] // m
    moved = lax.ppermute(
        jnp.concatenate([quarter(w_out), quarter(w_down)]), ("dp", "seq"), turn
    )
    wout = ring.gather(moved[:out_rows]).reshape(part, width)
    gu_piece = jnp.concatenate(
        [lax.dynamic_slice(w_gate_up, (0, i * hidden + s * ff), (slab, ff)) for i in range(2)], axis=1
    )
    wgu = ring.gather(gu_piece).reshape(width, 2 * ff)
    wdown = ring.gather(moved[out_rows:]).reshape(ff, width)

    places = jnp.concatenate([(s ^ o) * rows + jnp.arange(rows, dtype=jnp.int32) for o in group.offsets])
    cosine, sine = rotary_tables(places)
    count = rows * m
    xhat1, rstd1 = norm(tokens_all.astype(F32))
    normed1 = (xhat1 * g1 + b1).astype(BF16)
    qkv = (dot(normed1, wqkv) + bias_qkv).reshape(count, 3, heads, HEAD_DIM)
    queries = rotate(qkv[:, 0], cosine, sine).astype(BF16)
    keys = rotate(qkv[:, 1], cosine, sine).astype(BF16)
    values = qkv[:, 2].astype(BF16)
    scores = jnp.einsum("qhd,khd->hqk", queries, keys, preferred_element_type=F32) * scale
    scores = jnp.where((places[None, :] <= places[:, None])[None], scores, -jnp.inf)
    top = jnp.max(scores, axis=-1, keepdims=True)
    lse = top + jnp.log(jnp.sum(jnp.exp(scores - top), axis=-1, keepdims=True))
    probs = jnp.exp(scores - lse)
    probs_r = probs.astype(BF16)
    context = jnp.einsum("hqk,khd->qhd", probs_r, values, preferred_element_type=F32).astype(BF16)
    context_flat = context.reshape(count, part)
    x_own = tokens.astype(F32)
    mid = x_own + group.scatter(dot(context_flat, wout))
    xhat2, rstd2 = norm(mid)
    normed2 = group.gather((xhat2 * g2 + b2).astype(BF16))
    gate_up = dot(normed2, wgu)
    gate, up = gate_up[:, :ff], gate_up[:, ff:]
    sigma = jax.nn.sigmoid(gate)
    silu = gate * sigma
    act = (silu * up).astype(BF16)
    d_act = dot_cols(cot_all, wdown)
    d_gate = d_act * up * (sigma * (1.0 + gate * (1.0 - sigma)))
    d_gate_up = jnp.concatenate([d_gate, d_act * silu], axis=1).astype(BF16)

    d_normed2 = group.scatter(dot_cols(d_gate_up, wgu))
    sum_down = ring.scatter(dot_rows(act, cot_all).astype(BF16).reshape(n, ff // n, width))
    sum_gu = ring.scatter(dot_rows(normed2, d_gate_up).astype(BF16).reshape(n, slab, 2 * ff))
    block_out = (mid + group.scatter(dot(act, wdown))).astype(BF16)
    d_mid = cotangent.astype(F32) + norm_back(d_normed2, xhat2, rstd2, g2)
    d_mid_r = group.gather(d_mid.astype(BF16))

    d_context = dot_cols(d_mid_r, wout).astype(BF16).reshape(count, heads, HEAD_DIM)
    sum_out = ring.scatter(dot_rows(context_flat, d_mid_r).astype(BF16).reshape(n, part // n, width))
    d_probs = jnp.einsum("qhd,khd->hqk", d_context, values, preferred_element_type=F32)
    delta = jnp.einsum("qhd,qhd->hq", d_context.astype(F32), context.astype(F32))[..., None]
    d_scores = (probs * (d_probs - delta) * scale).astype(BF16)
    d_queries = jnp.einsum("hqk,khd->qhd", d_scores, keys, preferred_element_type=F32)
    d_keys = jnp.einsum("hqk,qhd->khd", d_scores, queries, preferred_element_type=F32)
    d_values = jnp.einsum("hqk,qhd->khd", probs_r, d_context, preferred_element_type=F32)
    d_qkv = jnp.stack(
        [rotate(d_queries, cosine, -sine), rotate(d_keys, cosine, -sine), d_values], axis=1
    ).reshape(count, 3 * part)
    d_qkv_r = d_qkv.astype(BF16)
    d_normed1_part = dot_cols(d_qkv_r, wqkv)
    d_normed1 = group.scatter(d_normed1_part)
    own = (slice(0, rows),)
    input_grad = d_mid + norm_back(d_normed1, xhat1[own], rstd1[own], g1)

    bias_part = jnp.zeros((3, m, part), F32)
    bias_part = lax.dynamic_update_slice(bias_part, jnp.sum(d_qkv, axis=0).reshape(3, 1, part), (0, s, 0))
    vector_parts = [
        jnp.sum(d_normed1_part * xhat1, axis=0),
        jnp.sum(d_normed1_part, axis=0),
        jnp.sum(d_normed2 * xhat2, axis=0),
        jnp.sum(d_normed2, axis=0),
        bias_part.reshape(-1),
    ]
    line = jnp.concatenate([v.reshape(n, m, -1) for v in vector_parts], axis=-1)
    lines = -(-line.shape[-1] // (3 * part))
    line = jnp.pad(line, ((0, 0), (0, 0), (0, lines * 3 * part - line.shape[-1])))
    line = line.reshape(n, m, lines, 3 * part).astype(BF16)
    part_qkv = dot_rows(normed1, d_qkv_r).astype(BF16).reshape(n, m, slab // m, 3 * part)
    packed = jnp.concatenate([part_qkv, line], axis=2)
    packed_rows = packed.shape[2]
    sum_qkv = ring.scatter(packed.reshape(n, m * packed_rows, 3 * part))

    def owners(total):
        return group.exchange(total.astype(BF16).reshape((m, -1) + total.shape[1:])).astype(F32)

    last = owners(sum_qkv)
    g_qkv = last[:, : slab // m].reshape(m, slab // m, 3, part).transpose(1, 2, 0, 3)
    g_qkv = g_qkv.reshape(slab // m, 3 * inner)
    line = jnp.sum(last[:, slab // m :], axis=0).reshape(-1)
    sizes = [slab // m] * 4 + [b_qkv.shape[0] // m]
    vectors_out, at = [], 0
    for size in sizes:
        vectors_out.append(line[at : at + size])
        at += size
    g_gu = owners(sum_gu).reshape(m, slab // m, 2, ff).transpose(1, 2, 0, 3).reshape(slab // m, 2 * hidden)
    g_down = lax.ppermute(sum_down.astype(BF16), ("dp", "seq"), back).astype(F32)
    g_out = lax.ppermute(sum_out.astype(BF16), ("dp", "seq"), back).astype(F32)
    return (
        block_out,
        input_grad,
        vectors_out[0],
        vectors_out[1],
        g_qkv,
        vectors_out[4],
        g_out,
        vectors_out[2],
        vectors_out[3],
        g_gu,
        g_down,
    )


LOGICAL = pl.DeviceIdType.LOGICAL
MEAN, RSTD, SPOT, LSE = 0, 1, 2, 8
LANES = 128
TILE = 16
VMEM_BYTES = 67_043_328


def vmem(shape, dtype=BF16):
    return pltpu.VMEM(shape, dtype)


class Place:
    def __init__(self, n, m):
        self.n, self.m, self.half = n, m, n // 2
        self.d, self.s = lax.axis_index("dp"), lax.axis_index("seq")
        pair = lax.div(self.d, 2)
        odd = self.d - 2 * pair
        place = pair + odd * (n - 1 - 2 * pair)
        self.owners = []
        for offset in range(n):
            spot = lax.rem(place + offset, n)
            back = lax.div(spot, self.half)
            self.owners.append(2 * spot + back * (2 * n - 1 - 4 * spot))
        self.partners = []
        for mask in range(m):
            out, bit = self.s, 1
            while bit < m:
                if mask & bit:
                    out = out + bit - 2 * bit * lax.rem(lax.div(self.s, bit), 2)
                bit *= 2
            self.partners.append(out)
        self.rings = {1: self.owners[1] * m + self.s, -1: self.owners[n - 1] * m + self.s}
        self.seqs = [self.d * m + out for out in self.partners]
        g = self.d * m + self.s
        h = self.s * n + self.d
        self.there = lax.rem(g, n)
        self.target = self.there * m + lax.div(g, n)
        self.source = h
        self.moves = (self.target - g) * (self.target - g) > 0

    def owner(self, offset):
        return self.owners[offset % self.n]

    def partner(self, mask):
        return self.partners[mask]

    def bits(self):
        out, bit = [], self.m // 2
        while bit:
            out.append(bit)
            bit //= 2
        return out


class Sender:
    def __init__(self, sends, recvs):
        self.sends, self.recvs = sends, recvs
        self.used = 0
        self.open = []

    def slot(self):
        self.used += 1
        return self.used - 1

    def copy(self, slot, src, dst, device):
        return pltpu.make_async_remote_copy(
            src_ref=src,
            dst_ref=dst,
            send_sem=self.sends.at[slot],
            recv_sem=self.recvs.at[slot],
            device_id=device,
            device_id_type=LOGICAL,
        )

    def start(self, slot, src, dst, device):
        copy = self.copy(slot, src, dst, device)
        copy.start()
        self.open.append(copy)
        return copy

    def finish(self):
        for copy in self.open:
            copy.wait_send()
        self.open = []


class Gather:
    def __init__(self, place, sender, buf, rows):
        self.place, self.sender, self.buf, self.rows = place, sender, buf, rows
        self.slots = [[sender.slot() for _ in range(place.half)] for _ in range(2)]
        self.right, self.left = place.rings[1], place.rings[-1]

    def at(self, index, part=None):
        rows = self.rows
        start = index * rows
        if part is not None:
            rows = rows // 2
            start = start + part * rows
        return self.buf.at[pl.ds(pl.multiple_of(start, rows), rows)]

    def send(self, k):
        last = k == self.place.half - 1
        for way, device in ((0, self.right), (1, self.left)):
            index = self.place.owner(k if way else -k)
            ref = self.at(index, way if last else None)
            self.sender.start(self.slots[way][k], ref, ref, device)

    def pump(self, k):
        last = k == self.place.half
        for way, device in ((0, self.right), (1, self.left)):
            index = self.place.owner(k if way else -k)
            ref = self.at(index, way if last else None)
            self.sender.copy(self.slots[way][k - 1], ref, ref, device).wait_recv()
        if not last:
            self.send(k)


def greet(place, extra_seq=()):
    barrier = pltpu.get_barrier_semaphore()

    def hello(device):
        pl.semaphore_signal(barrier, inc=1, device_id=device, device_id_type=LOGICAL)

    near = [place.rings[1], place.rings[-1]] + [place.seqs[mask] for mask in tuple(place.bits()) + tuple(extra_seq)]
    for device in near:
        hello(device)

    @pl.when(place.moves)
    def _():
        hello(place.target)
        hello(place.source)
        pl.semaphore_wait(barrier, len(near) + 2)

    @pl.when(jnp.logical_not(place.moves))
    def _():
        pl.semaphore_wait(barrier, len(near))


def forward_kernel(
    dims,
    tok, cot, piece_qkv, piece_gu, piece_out, piece_down, piece_vec, rot_c, rot_a, rot_b, pos_q, pos_k,
    o_wqkv, o_wout, o_wgu, o_far, o_near, o_rows, o_tok, o_cot, o_n1, o_qkv, o_stat, o_ctx, o_mid, o_n2, o_act, o_dgu,
    wqkv, wout, wgu, wdown, vec, tok_all, cot_all, n1, qkv, stat, ctx, mid, n2, act, dgu,
    rows_v, bias_v, own, send1, send2, recv1, recv2,
    sends, recvs, locals_, outs,
):
    n, m, rows, width, slab, part, ffp, b_units = dims
    count = rows * m
    place = Place(n, m)
    sender = Sender(sends, recvs)
    moves = place.moves
    greet(place)
    d, s = place.d, place.s
    bits = place.bits()
    out_rows, down_rows, vec_rows = part // n, ffp // n, piece_vec.shape[0]

    def local(i, src, dst):
        copy = pltpu.make_async_copy(src, dst, locals_.at[i])
        copy.start()
        return copy

    ring_a = Gather(place, sender, wqkv, slab)
    ring_v = Gather(place, sender, vec, vec_rows)
    ring_b = Gather(place, sender, wout, out_rows)
    ring_c = Gather(place, sender, wgu, slab)
    ring_d = Gather(place, sender, wdown, down_rows)
    placed = [
        local(0, piece_qkv, ring_a.at(d)),
        local(1, piece_vec, ring_v.at(d)),
        local(2, piece_gu, ring_c.at(d)),
        local(3, tok, tok_all.at[pl.ds(0, rows)]),
        local(4, cot, cot_all.at[pl.ds(0, rows)]),
    ]

    class Spread:
        def __init__(self, buf):
            self.buf = buf
            self.slots = [sender.slot() for _ in bits]

        def ref(self, i, part):
            size = rows << i
            return self.buf.at[pl.ds(part * size, size)]

        def send(self, i):
            sender.start(self.slots[i], self.ref(i, 0), self.ref(i, 1), place.seqs[bits[i]])

        def wait(self, i):
            sender.copy(self.slots[i], self.ref(i, 0), self.ref(i, 1), place.seqs[bits[i]]).wait_recv()

    toks, cots, n2s = Spread(tok_all), Spread(cot_all), Spread(n2)
    turn_slots = [sender.slot(), sender.slot()]

    placed[0].wait()
    placed[1].wait()
    ring_a.send(0)
    ring_v.send(0)
    placed[3].wait()
    toks.send(0)

    turns = [(piece_out, ring_b, turn_slots[0], 5), (piece_down, ring_d, turn_slots[1], 6)]

    @pl.when(moves)
    def _():
        for piece, ring, slot, _ in turns:
            sender.copy(slot, piece, ring.at(place.there), place.target).start()

    @pl.when(jnp.logical_not(moves))
    def _():
        for piece, ring, _, i in turns:
            local(i, piece, ring.at(d)).wait()

    placed[4].wait()
    cots.send(0)

    lane = lax.broadcasted_iota(jnp.int32, (1, LANES), 1)

    def stats(j):
        span = pl.ds(pl.multiple_of(j * rows, rows), rows)
        x = tok_all[span, :].astype(F32)
        mu = jnp.mean(x, axis=-1, keepdims=True)
        c = x - mu
        r = lax.rsqrt(jnp.mean(c * c, axis=-1, keepdims=True) + EPS)
        stat[span, :] = jnp.where(lane == MEAN, mu, jnp.where(lane == RSTD, r, pos_q[span, :]))

    stats(0)
    size = 1
    for i in range(len(bits)):
        toks.wait(i)
        if i + 1 < len(bits):
            toks.send(i + 1)
        cots.wait(i)
        if i + 1 < len(bits):
            cots.send(i + 1)
        if i == 0:
            ring_v.pump(1)
            ring_a.pump(1)

            @pl.when(moves)
            def _():
                for piece, ring, slot, _ in turns:
                    sender.copy(slot, piece, ring.at(d), place.source).wait_recv()

            ring_b.send(0)
        if i == 1:
            ring_v.pump(2)
            ring_a.pump(2)
            ring_d.send(0)
            ring_b.pump(1)
        lax.fori_loop(size, 2 * size, lambda j, c: (stats(j), c)[1], 0)
        size *= 2
    ring_v.pump(3)
    ring_a.pump(3)
    placed[2].wait()
    ring_c.send(0)
    ring_b.pump(2)
    ring_v.pump(4)
    for c in range(n):
        for r in range(4):
            for u in range(slab // LANES):
                at = c * slab + u * LANES
                row = c * vec_rows + r * (slab // LANES) + u
                rows_v[r : r + 1, at : at + LANES] = vec[row : row + 1, :]
    head_row = 4 * (slab // LANES)
    for i in range(3):
        for u in range(part // LANES):
            unit = i * (m * part // LANES) + s * (part // LANES) + u
            row = lax.div(unit, b_units) * vec_rows + head_row + lax.rem(unit, b_units)
            at = i * part + u * LANES
            bias_v[0:1, at : at + LANES] = vec[pl.ds(row, 1), :]

    def normalize(j, carry):
        block = 64
        span = pl.ds(pl.multiple_of(j * block, block), block)
        x = tok_all[span, :].astype(F32)
        xhat = (x - stat[span, MEAN : MEAN + 1]) * stat[span, RSTD : RSTD + 1]
        n1[span, :] = (xhat * rows_v[0:1, :] + rows_v[1:2, :]).astype(BF16)
        return carry

    lax.fori_loop(0, count // 64, normalize, 0)
    ring_d.pump(1)
    ring_a.pump(4)

    def project(j, carry):
        span = pl.ds(pl.multiple_of(j * LANES, LANES), LANES)
        for i in range(3):
            cols = slice(i * part, (i + 1) * part)
            y = jnp.dot(n1[span, :], wqkv[:, cols], preferred_element_type=F32) + bias_v[0:1, cols]
            if i < 2:
                pieces = []
                for u in range(part // LANES):
                    z = y[:, u * LANES : (u + 1) * LANES]
                    pieces.append(
                        z * rot_c[span, :]
                        + pltpu.roll(z, LANES - ROT // 2, 1) * rot_a[span, :]
                        + pltpu.roll(z, ROT // 2, 1) * rot_b[span, :]
                    )
                y = jnp.concatenate(pieces, axis=1)
            qkv[span, cols] = y.astype(BF16)
        return carry

    lax.fori_loop(0, count // LANES, project, 0)
    ring_b.pump(3)
    ring_d.pump(2)
    scale = HEAD_DIM ** (-0.5)
    per = LANES // HEAD_DIM

    def attend(i, carry):
        pair, block = lax.div(i, m), lax.rem(i, m)
        span = pl.ds(pl.multiple_of(block * rows, rows), rows)
        at = pl.multiple_of(pair * LANES, LANES)
        q = qkv[span, pl.ds(at, LANES)]
        k = qkv[:, pl.ds(pl.multiple_of(part + at, LANES), LANES)]
        v = qkv[:, pl.ds(pl.multiple_of(2 * part + at, LANES), LANES)]
        allowed = pos_k[0:1, :] <= pos_q[span, 0:1]
        total = jnp.zeros((rows, LANES), F32)
        for h in range(per):
            mine = (lane // HEAD_DIM == h).astype(BF16)
            scores = dot_cols(q * mine, k) * scale
            scores = jnp.where(allowed, scores, -jnp.inf)
            top = jnp.max(scores, axis=-1, keepdims=True)
            weight = jnp.exp(scores - top)
            norm_ = jnp.sum(weight, axis=-1, keepdims=True)
            found = top + jnp.log(norm_)
            probs = jnp.exp(scores - found).astype(BF16)
            total = total + jnp.dot(probs, v * mine, preferred_element_type=F32)
            stat[span, :] = jnp.where(lane == LSE + pair * per + h, found, stat[span, :])
        ctx[span, pl.ds(at, LANES)] = total.astype(BF16)
        return carry

    lax.fori_loop(0, (part // LANES) * m, attend, 0)
    ring_b.pump(4)
    ring_c.pump(1)
    ring_d.pump(3)

    step = 512
    half = count // 2
    scatter_slots = [sender.slot(), sender.slot()]

    def far_part(j, carry):
        cols = pl.ds(pl.multiple_of(j * step, step), step)
        send1[:, cols] = jnp.dot(ctx[half:, :], wout[:, cols], preferred_element_type=F32).astype(BF16)
        return carry

    lax.fori_loop(0, width // step, far_part, 0)
    first = sender.start(scatter_slots[0], send1, recv1, place.seqs[bits[1]])

    def near_part(j, carry):
        cols = pl.ds(pl.multiple_of(j * step, step), step)
        own[:, cols] = jnp.dot(ctx[:half, :], wout[:, cols], preferred_element_type=F32)
        return carry

    lax.fori_loop(0, width // step, near_part, 0)
    first.wait_recv()
    send2[...] = (own[rows:, :] + recv1[rows:, :].astype(F32)).astype(BF16)
    second = sender.start(scatter_slots[1], send2, recv2, place.seqs[bits[0]])
    second.wait_recv()
    value = tok[...].astype(F32) + own[:rows, :] + recv1[:rows, :].astype(F32) + recv2[...].astype(F32)
    mid[...] = value
    c = value - jnp.mean(value, axis=-1, keepdims=True)
    r = lax.rsqrt(jnp.mean(c * c, axis=-1, keepdims=True) + EPS)
    n2[:rows, :] = (c * r * rows_v[2:3, :] + rows_v[3:4, :]).astype(BF16)
    n2s.send(0)
    ring_c.pump(2)
    n2s.wait(0)
    n2s.send(1)
    ring_d.pump(4)
    ring_c.pump(3)
    n2s.wait(1)
    ring_c.pump(4)

    block = 256

    def expand(j, carry):
        cols = pl.ds(pl.multiple_of(j * block, block), block)
        more = pl.ds(pl.multiple_of(ffp + j * block, block), block)
        gate = jnp.dot(n2[...], wgu[:, cols], preferred_element_type=F32)
        up = jnp.dot(n2[...], wgu[:, more], preferred_element_type=F32)
        d_act = dot_cols(cot_all[...], wdown[cols, :])
        sigma = jax.nn.sigmoid(gate)
        silu = gate * sigma
        act[:, cols] = (silu * up).astype(BF16)
        dgu[:, cols] = (d_act * up * (sigma * (1.0 + gate * (1.0 - sigma)))).astype(BF16)
        dgu[:, more] = (d_act * silu).astype(BF16)
        return carry

    lax.fori_loop(0, ffp // block, expand, 0)
    sender.finish()

    def down_far(j, carry):
        cols = pl.ds(pl.multiple_of(j * step, step), step)
        send1[:, cols] = jnp.dot(act[half:, :], wdown[:, cols], preferred_element_type=F32).astype(BF16)
        own[:, cols] = jnp.dot(act[:half, :], wdown[:, cols], preferred_element_type=F32)
        return carry

    lax.fori_loop(0, width // step, down_far, 0)
    written = []
    pairs = [
        (wqkv, o_wqkv), (wout, o_wout), (wgu, o_wgu), (send1, o_far), (own, o_near), (rows_v, o_rows), (tok_all, o_tok),
        (cot_all, o_cot), (n1, o_n1), (qkv, o_qkv), (stat, o_stat), (ctx, o_ctx), (mid, o_mid), (n2, o_n2),
        (act, o_act), (dgu, o_dgu),
    ]
    for i, (src, dst) in enumerate(pairs):
        copy = pltpu.make_async_copy(src, dst, outs.at[i])
        copy.start()
        written.append(copy)
    for copy in written:
        copy.wait()
    sender.finish()

    @pl.when(moves)
    def _():
        for piece, ring, slot, _ in turns:
            sender.copy(slot, piece, ring.at(place.there), place.target).wait_send()


def run_forward(n, m, dims, args):
    n, m, rows, width, slab, part, ffp, b_units = dims
    count = rows * m
    vec_rows = args[6].shape[0]
    arrays = [
        ((width, 3 * part), BF16), ((part, width), BF16), ((width, 2 * ffp), BF16), ((count // 2, width), BF16),
        ((count // 2, width), F32), ((8, width), F32), ((count, width), BF16), ((count, width), BF16), ((count, width), BF16),
        ((count, 3 * part), BF16), ((count, LANES), F32), ((count, part), BF16), ((rows, width), F32),
        ((count, width), BF16), ((count, ffp), BF16), ((count, 2 * ffp), BF16),
    ]
    scratch = [vmem(*a) for a in arrays]
    rows_v = scratch.pop(5)
    scratch[3:5] = [vmem((ffp, width)), vmem((n * vec_rows, LANES), F32)]
    half = n // 2
    slots = 5 * 2 * half + 3 * 2 + 2 + 2
    return pl.pallas_call(
        functools.partial(forward_kernel, dims),
        out_shape=[jax.ShapeDtypeStruct(*a) for a in arrays],
        in_specs=[pl.BlockSpec(memory_space=pltpu.VMEM)] * len(args),
        out_specs=[pl.BlockSpec(memory_space=pl.ANY)] * len(arrays),
        scratch_shapes=scratch
        + [
            rows_v,
            vmem((8, 3 * part), F32),
            vmem((count // 2, width), F32),
            vmem((count // 2, width)),
            vmem((rows, width)),
            vmem((count // 2, width)),
            vmem((rows, width)),
            pltpu.SemaphoreType.DMA((slots,)),
            pltpu.SemaphoreType.DMA((slots,)),
            pltpu.SemaphoreType.DMA((7,)),
            pltpu.SemaphoreType.DMA((len(arrays),)),
        ],
        compiler_params=pltpu.CompilerParams(
            collective_id=0, has_side_effects=True, vmem_limit_bytes=VMEM_BYTES
        ),
        name="forward",
    )(*args)


class Reduce:
    def __init__(self, place, sender, buf, inbox, rows):
        self.place, self.sender, self.buf, self.inbox, self.rows = place, sender, buf, inbox, rows
        self.slots = [[sender.slot() for _ in range(place.half)] for _ in range(2)]
        self.devices = (place.rings[1], place.rings[-1])

    def span(self, index, part=None):
        rows = self.rows
        start = index * rows
        if part is not None:
            rows = rows // 2
            start = start + part * rows
        return pl.multiple_of(start, rows), rows

    def landing(self, way, j):
        rows, half = self.rows, self.place.half
        base = way * ((half - 1) * rows + rows // 2)
        if j == 1:
            return base + (half - 1) * rows, rows // 2
        return base + (j - 2) * rows, rows

    def copy(self, way, j):
        offset = self.place.half - j + 1
        start, rows = self.span(self.place.owner(-offset if way else offset), way if j == 1 else None)
        at, _ = self.landing(way, j)
        return (
            self.slots[way][j - 1],
            self.buf.at[pl.ds(start, rows)],
            self.inbox.at[pl.ds(at, rows)],
        )

    def send(self, j, way):
        self.sender.start(*self.copy(way, j), self.devices[way])

    def begin(self):
        self.send(1, 0)
        self.send(1, 1)

    def add(self, start, rows, *froms):
        to = pl.ds(start, rows)
        value = self.buf[to, :].astype(F32)
        for at in froms:
            value = value + self.inbox[at : at + rows, :].astype(F32)
        self.buf[to, :] = value.astype(self.buf.dtype)

    def pump(self, j):
        half = self.place.half
        for way in range(2):
            self.sender.copy(*self.copy(way, j), self.devices[way]).wait_recv()
            if j < half:
                offset = half - j
                start, rows = self.span(self.place.owner(-offset if way else offset), way if j == 1 else None)
                self.add(start, rows, self.landing(way, j)[0])
                self.send(j + 1, way)
        if j == half:
            start, rows = self.span(self.place.d)
            self.add(start, rows, self.landing(0, j)[0], self.landing(1, j)[0])


def flip(value):
    size = value.shape[1]
    here = lax.broadcasted_iota(jnp.int32, (size, size), 0) == lax.broadcasted_iota(jnp.int32, (size, size), 1)
    return dot_cols(here.astype(F32).astype(BF16), value).astype(BF16)


def backward_kernel(
    dims,
    h_wqkv, h_wout, h_wgu, h_far, h_near, h_rows, h_tok, h_cot, h_n1, h_qkv, h_stat, h_ctx, h_mid, h_n2, h_act, h_dgu,
    h_rc, h_ra, h_rb, h_pk,
    o_block, o_input, o_gu, o_qkv, o_down, o_out, o_vec,
    wout, wgu, wqkv, rows_v, wide_a, wide_b, qkv, stat, ctx, mid, act, dgu, rot_c, rot_a, rot_b, pos_k,
    sum_a, sum_b, sum_c, sum_d, sum_v, in_a, in_b, in_c, in_d, in_v,
    own, send1, send2, recv1, recv2, dm_all, d_mid, cot, dctx, dqkv, dk, dv, sums_v, bias_v,
    x_gu, x_qkv, x_down, x_out, x_vec,
    sends, recvs, loads, outs,
):
    n, m, rows, width, slab, part, ffp, b_units = dims
    count = rows * m
    half = count // 2
    place = Place(n, m)
    sender = Sender(sends, recvs)
    waiting = {}

    def load(name, src, dst):
        copy = pltpu.make_async_copy(src, dst, loads.at[len(waiting)])
        copy.start()
        waiting[name] = copy

    load("act", h_act, act)
    load("cot", h_cot, wide_a)
    load("n2", h_n2, wide_b)
    load("dgu", h_dgu, dgu)
    load("wgu", h_wgu, wgu)
    load("own", h_cot.at[pl.ds(0, dims[2])], cot)
    load("mid", h_mid, mid)
    load("rows", h_rows, rows_v)
    load("wqkv", h_wqkv, wqkv)
    load("wout", h_wout, wout)
    load("ctx", h_ctx, ctx)
    load("qkv", h_qkv, qkv)
    load("stat", h_stat, stat)
    load("rc", h_rc, rot_c)
    load("ra", h_ra, rot_a)
    load("rb", h_rb, rot_b)
    load("pk", h_pk, pos_k)
    bits = place.bits()
    others = [mask for mask in range(1, m) if mask not in bits]
    moves = place.moves
    greet(place, others)
    d, s = place.d, place.s
    out_rows, down_rows, vec_rows = part // n, ffp // n, sum_v.shape[0] // n
    ring_a = Reduce(place, sender, sum_a, in_a, slab)
    ring_b = Reduce(place, sender, sum_b, in_b, out_rows)
    ring_c = Reduce(place, sender, sum_c, in_c, slab)
    ring_d = Reduce(place, sender, sum_d, in_d, down_rows)
    ring_v = Reduce(place, sender, sum_v, in_v, vec_rows)
    block = 256

    def outer(dst, left, right, size):
        def step(j, carry):
            cols = pl.ds(pl.multiple_of(j * block, block), block)
            dst[cols, :] = dot(flip(left[:, cols]), right[...]).astype(BF16)
            return carry

        lax.fori_loop(0, size // block, step, 0)

    class Halving:
        def __init__(self, at):
            self.slots = [sender.slot(), sender.slot()]
            self.at = at
            self.open = []

        def first(self, far):
            far()
            self.open.append(sender.start(self.slots[0], send1, recv1.at[pl.ds(self.at * half, half)], place.seqs[bits[1]]))

        def second(self):
            self.open[0].wait_recv()
            send2[...] = (own[rows:, :] + recv1[self.at * half + rows : (self.at + 1) * half, :].astype(F32)).astype(BF16)
            self.open.append(sender.start(self.slots[1], send2, recv2.at[pl.ds(self.at * rows, rows)], place.seqs[bits[0]]))

        def total(self):
            self.open[1].wait_recv()
            return own[:rows, :] + recv1[self.at * half : self.at * half + rows, :].astype(F32) + recv2[
                self.at * rows : (self.at + 1) * rows, :
            ].astype(F32)

        def sent(self):
            for copy in self.open:
                copy.wait_send()
            sender.open = [c for c in sender.open if all(c is not o for o in self.open)]

    waiting["act"].wait()
    waiting["cot"].wait()
    outer(sum_d, act, wide_a, ffp)
    ring_d.begin()
    waiting["n2"].wait()
    waiting["dgu"].wait()
    waiting["wgu"].wait()

    normed2 = Halving(0)

    def back_step(left, lo, hi, weight, to):
        def step(j, carry):
            cols = pl.ds(pl.multiple_of(j * block, block), block)
            to(cols, dot_cols(left[lo:hi, :], weight[cols, :]))
            return carry

        lax.fori_loop(0, width // block, step, 0)

    def to_send(cols, value):
        send1[:, cols] = value.astype(BF16)

    def to_own(cols, value):
        own[:, cols] = value

    normed2.first(lambda: back_step(dgu, half, count, wgu, to_send))
    back_step(dgu, 0, half, wgu, to_own)
    normed2.second()
    outer(sum_c, wide_b, dgu, width)
    ring_c.begin()
    load("n1", h_n1, wide_b)
    load("tok", h_tok, wide_a)
    ring_d.pump(1)

    waiting["mid"].wait()
    waiting["rows"].wait()
    waiting["own"].wait()

    def deviation(value):
        c = value - jnp.mean(value, axis=-1, keepdims=True)
        r = lax.rsqrt(jnp.mean(c * c, axis=-1, keepdims=True) + EPS)
        return c * r, r

    xhat, r = deviation(mid[...])
    up = normed2.total()
    sums_v[2:3, :] = jnp.sum(up * xhat, axis=0, keepdims=True)
    sums_v[3:4, :] = jnp.sum(up, axis=0, keepdims=True)
    d_mid[...] = cot[...].astype(F32) + norm_back(up, xhat, r, rows_v[2:3, :])
    dm_all[:rows, :] = d_mid[...].astype(BF16)
    spread = [sender.slot() for _ in bits]

    def spread_copy(i):
        size = rows << i
        return (spread[i], dm_all.at[pl.ds(0, size)], dm_all.at[pl.ds(size, size)])

    def spread_send(i):
        sender.start(*spread_copy(i), place.seqs[bits[i]])

    def spread_wait(i):
        sender.copy(*spread_copy(i), place.seqs[bits[i]]).wait_recv()

    spread_send(0)
    normed2.sent()

    load("far", h_far, send1)
    load("near", h_near, own)
    output = Halving(1)

    output.first(waiting["far"].wait)
    waiting["near"].wait()
    ring_d.pump(2)
    spread_wait(0)
    spread_send(1)
    output.second()
    ring_c.pump(1)
    spread_wait(1)

    waiting["wout"].wait()
    waiting["ctx"].wait()
    dctx[...] = dot_cols(dm_all[...], wout[...]).astype(BF16)
    outer(sum_b, ctx, dm_all, part)
    ring_b.begin()
    cot[...] = (mid[...] + output.total()).astype(BF16)
    output.sent()
    ring_d.pump(3)

    for name in ("qkv", "stat", "rc", "ra", "rb", "pk"):
        waiting[name].wait()
    scale = HEAD_DIM ** (-0.5)
    per = LANES // HEAD_DIM
    lane = lax.broadcasted_iota(jnp.int32, (1, LANES), 1) // HEAD_DIM

    def turned(z, span):
        return (
            z * rot_c[span, :]
            - pltpu.roll(z, LANES - ROT // 2, 1) * rot_a[span, :]
            - pltpu.roll(z, ROT // 2, 1) * rot_b[span, :]
        )

    bias_v[...] = jnp.zeros_like(bias_v)
    for pair in range(part // LANES):
        at = pair * LANES
        dk[...] = jnp.zeros_like(dk)
        dv[...] = jnp.zeros_like(dv)

        def attend(i, carry, pair=pair, at=at):
            span = pl.ds(pl.multiple_of(i * rows, rows), rows)
            q = qkv[span, at : at + LANES]
            k = qkv[:, part + at : part + at + LANES]
            v = qkv[:, 2 * part + at : 2 * part + at + LANES]
            dc = dctx[span, at : at + LANES]
            both = dc.astype(F32) * ctx[span, at : at + LANES].astype(F32)
            allowed = pos_k[0:1, :] <= stat[span, SPOT : SPOT + 1]
            dq = jnp.zeros((rows, LANES), F32)
            for h in range(per):
                pick = lane == h
                mine = pick.astype(BF16)
                qm, dcm = q * mine, dc * mine
                scores = dot_cols(qm, k) * scale
                at_lse = LSE + pair * per + h
                probs = jnp.exp(jnp.where(allowed, scores, -jnp.inf) - stat[span, at_lse : at_lse + 1])
                delta = jnp.sum(jnp.where(pick, both, 0.0), axis=-1, keepdims=True)
                ds = (probs * (dot_cols(dcm, v) - delta) * scale).astype(BF16)
                dq = dq + jnp.dot(ds, k * mine, preferred_element_type=F32)
                dk[...] += dot(flip(ds), qm)
                dv[...] += dot(flip(probs.astype(BF16)), dcm)
            dq = turned(dq, span)
            bias_v[0:1, at : at + LANES] += jnp.sum(dq, axis=0, keepdims=True)
            dqkv[span, at : at + LANES] = dq.astype(BF16)
            return carry

        lax.fori_loop(0, m, attend, 0)

        def settle(i, carry, at=at):
            span = pl.ds(pl.multiple_of(i * rows, rows), rows)
            key, value = turned(dk[span, :], span), dv[span, :]
            bias_v[0:1, part + at : part + at + LANES] += jnp.sum(key, axis=0, keepdims=True)
            bias_v[0:1, 2 * part + at : 2 * part + at + LANES] += jnp.sum(value, axis=0, keepdims=True)
            dqkv[span, part + at : part + at + LANES] = key.astype(BF16)
            dqkv[span, 2 * part + at : 2 * part + at + LANES] = value.astype(BF16)
            return carry

        lax.fori_loop(0, m, settle, 0)
        if pair == 0:
            ring_b.pump(1)
            ring_c.pump(2)

    ring_d.pump(4)
    ring_b.pump(2)
    waiting["n1"].wait()
    outer(sum_a, wide_b, dqkv, width)
    ring_a.begin()
    waiting["wqkv"].wait()
    waiting["tok"].wait()
    normed1 = Halving(2)

    def gains(cols, value, lo, hi):
        xh = (wide_a[lo:hi, cols].astype(F32) - stat[lo:hi, MEAN : MEAN + 1]) * stat[lo:hi, RSTD : RSTD + 1]
        return jnp.sum(value * xh, axis=0, keepdims=True), jnp.sum(value, axis=0, keepdims=True)

    def far_last(cols, value):
        send1[:, cols] = value.astype(BF16)
        sums_v[0:1, cols], sums_v[1:2, cols] = gains(cols, value, half, count)

    def near_last(cols, value):
        own[:, cols] = value
        gain, total = gains(cols, value, 0, half)
        sums_v[0:1, cols] += gain
        sums_v[1:2, cols] += total

    normed1.first(lambda: back_step(dqkv, half, count, wqkv, far_last))
    back_step(dqkv, 0, half, wqkv, near_last)

    sum_v[...] = jnp.zeros_like(sum_v)
    units = slab // LANES

    def lay(c, carry):
        for i in range(4):
            for u in range(units):
                at = pl.multiple_of(c * slab + u * LANES, LANES)
                sum_v[pl.ds(c * vec_rows + i * units + u, 1), :] = sums_v[i : i + 1, pl.ds(at, LANES)]
        return carry

    lax.fori_loop(0, n, lay, 0)
    for i in range(3):
        for u in range(part // LANES):
            unit = i * (m * part // LANES) + s * (part // LANES) + u
            row = lax.div(unit, b_units) * vec_rows + 4 * units + lax.rem(unit, b_units)
            at = i * part + u * LANES
            sum_v[pl.ds(row, 1), :] = bias_v[0:1, at : at + LANES]
    ring_v.begin()
    normed1.second()
    ring_a.pump(1)
    ring_v.pump(1)
    ring_b.pump(3)
    ring_c.pump(3)
    ring_v.pump(2)
    ring_a.pump(2)
    up = normed1.total()
    rstd = stat[:rows, RSTD : RSTD + 1]
    xhat = (wide_a[:rows, :].astype(F32) - stat[:rows, MEAN : MEAN + 1]) * rstd
    own[:rows, :] = d_mid[...] + norm_back(up, xhat, rstd, rows_v[0:1, :])
    ring_b.pump(4)
    ring_v.pump(3)

    written = []

    def store(src, dst):
        copy = pltpu.make_async_copy(src, dst, outs.at[len(written)])
        copy.start()
        written.append(copy)

    store(cot, o_block)
    store(own.at[pl.ds(0, rows)], o_input)
    turns = [(sum_d, down_rows, x_down, sender.slot()), (sum_b, out_rows, x_out, sender.slot())]

    def mine(buf, size):
        return buf.at[pl.ds(pl.multiple_of(d * size, size), size)]

    @pl.when(moves)
    def _():
        for buf, size, landing, slot in turns:
            sender.copy(slot, mine(buf, size), landing, place.source).start()

    @pl.when(jnp.logical_not(moves))
    def _():
        for i, (buf, size, landing, _) in enumerate(turns):
            copy = pltpu.make_async_copy(mine(buf, size), landing, loads.at[len(waiting) + i])
            copy.start()
            copy.wait()

    def deal(buf, size, landing, whole=False):
        share = size if whole else size // m
        got = []
        for mask in range(1, m):
            other = place.partner(mask)
            start = d * size + (0 if whole else other * share)
            src = buf.at[pl.ds(pl.multiple_of(start, share), share)]
            to = landing.at[pl.ds(pl.multiple_of(s * share, share), share)]
            got.append(sender.start(sender.slot(), src, to, place.seqs[mask]))
        start = d * size + (0 if whole else s * share)
        to = pl.ds(pl.multiple_of(s * share, share), share)
        landing[to, :] = buf[pl.ds(pl.multiple_of(start, share), share), :]
        return got

    ring_c.pump(4)
    got_gu = deal(sum_c, slab, x_gu)
    ring_a.pump(3)
    ring_v.pump(4)
    got_vec = deal(sum_v, vec_rows, x_vec, whole=True)
    ring_a.pump(4)
    got_qkv = deal(sum_a, slab, x_qkv)
    for copy in got_gu:
        copy.wait_recv()
    store(x_gu, o_gu)

    @pl.when(moves)
    def _():
        for buf, size, landing, slot in turns:
            sender.copy(slot, mine(buf, size), landing, place.target).wait_recv()

    store(x_down, o_down)
    store(x_out, o_out)
    for copy in got_vec:
        copy.wait_recv()
    store(x_vec, o_vec)
    for copy in got_qkv:
        copy.wait_recv()
    store(x_qkv, o_qkv)
    for copy in written:
        copy.wait()
    sender.finish()

    @pl.when(moves)
    def _():
        for buf, size, landing, slot in turns:
            sender.copy(slot, mine(buf, size), landing, place.source).wait_send()


def run_backward(dims, args):
    n, m, rows, width, slab, part, ffp, b_units = dims
    count = rows * m
    vec_rows = -(-(4 * (slab // LANES) + b_units) // TILE) * TILE
    half = n // 2
    out_rows, down_rows = part // n, ffp // n

    def inbox(size, cols, dtype=BF16):
        return vmem((2 * ((half - 1) * size + size // 2), cols), dtype)

    outputs = [
        ((rows, width), BF16), ((rows, width), F32), ((slab, 2 * ffp), BF16), ((slab, 3 * part), BF16),
        ((down_rows, width), BF16), ((out_rows, width), BF16), ((m * vec_rows, LANES), F32),
    ]
    scratch = [
        vmem((part, width)), vmem((width, 2 * ffp)), vmem((width, 3 * part)), vmem((8, width), F32),
        vmem((count, width)), vmem((count, width)), vmem((count, 3 * part)), vmem((count, LANES), F32),
        vmem((count, part)), vmem((rows, width), F32), vmem((count, ffp)), vmem((count, 2 * ffp)),
        vmem((count, LANES), F32), vmem((count, LANES), F32), vmem((count, LANES), F32), vmem((8, count), F32),
        vmem((n * slab, 3 * part)), vmem((part, width)), vmem((n * slab, 2 * ffp)), vmem((ffp, width)),
        vmem((n * vec_rows, LANES), F32),
        inbox(slab, 3 * part), inbox(out_rows, width), inbox(slab, 2 * ffp), inbox(down_rows, width),
        inbox(vec_rows, LANES, F32),
        vmem((count // 2, width), F32), vmem((count // 2, width)), vmem((rows, width)),
        vmem((3 * count // 2, width)), vmem((3 * rows, width)),
        vmem((count, width)), vmem((rows, width), F32), vmem((rows, width)), vmem((count, part)), vmem((count, 3 * part)),
        vmem((count, LANES), F32), vmem((count, LANES), F32), vmem((8, width), F32), vmem((8, 3 * part), F32),
        vmem((slab, 2 * ffp)), vmem((slab, 3 * part)), vmem((down_rows, width)), vmem((out_rows, width)),
        vmem((m * vec_rows, LANES), F32),
    ]
    slots = 5 * 2 * half + 3 * 2 + 2 + 2 + 3 * (m - 1)
    return pl.pallas_call(
        functools.partial(backward_kernel, dims),
        out_shape=[jax.ShapeDtypeStruct(*a) for a in outputs],
        in_specs=[pl.BlockSpec(memory_space=pl.ANY)] * len(args),
        out_specs=[pl.BlockSpec(memory_space=pl.ANY)] * len(outputs),
        scratch_shapes=scratch
        + [
            pltpu.SemaphoreType.DMA((slots,)),
            pltpu.SemaphoreType.DMA((slots,)),
            pltpu.SemaphoreType.DMA((len(args) + 6,)),
            pltpu.SemaphoreType.DMA((len(outputs),)),
        ],
        compiler_params=pltpu.CompilerParams(
            collective_id=1, has_side_effects=True, vmem_limit_bytes=VMEM_BYTES
        ),
        name="backward",
    )(*args)


def prepare(place_s, n, m, tokens, cotangent, gain1, bias1, w_qkv, b_qkv, w_out, gain2, bias2, w_gate_up, w_down, offsets):
    s = place_s
    rows, width = tokens.shape
    slab = gain1.shape[0]
    inner, hidden = w_out.shape[0] * n, w_down.shape[0] * n
    part, ff = inner // m, hidden // m
    down = w_down.shape[0] // m
    down_p = -(-down // TILE) * TILE
    ffp = n * down_p
    piece_qkv = jnp.concatenate(
        [lax.dynamic_slice(w_qkv, (0, i * inner + s * part), (slab, part)) for i in range(3)], axis=1
    )

    def spread(i):
        cols = lax.dynamic_slice(w_gate_up, (0, i * hidden + s * ff), (slab, ff))
        return jnp.pad(cols.reshape(slab, n, down), ((0, 0), (0, 0), (0, down_p - down))).reshape(slab, ffp)

    piece_gu = jnp.concatenate([spread(0), spread(1)], axis=1)
    out_rows = w_out.shape[0] // m
    piece_out = lax.dynamic_slice(w_out, (s * out_rows, 0), (out_rows, width))
    piece_down = jnp.pad(lax.dynamic_slice(w_down, (s * down, 0), (down, width)), ((0, down_p - down), (0, 0)))
    vec = jnp.concatenate([gain1, bias1, gain2, bias2, b_qkv]).astype(F32).reshape(-1, LANES)
    vec = jnp.pad(vec, ((0, -vec.shape[0] % TILE), (0, 0)))
    places = jnp.concatenate([(s ^ o) * rows + jnp.arange(rows, dtype=jnp.int32) for o in offsets])
    half = ROT // 2
    lane = jnp.arange(LANES) % HEAD_DIM
    inverse = 10000.0 ** (-((lane % half).astype(F32) * 2.0 / ROT))
    angles = places.astype(F32)[:, None] * inverse[None, :]
    cosine, sine = jnp.cos(angles), jnp.sin(angles)
    rot_c = jnp.where(lane < ROT, cosine, 1.0)
    rot_a = jnp.where(lane < half, -sine, 0.0)
    rot_b = jnp.where((lane >= half) & (lane < ROT), sine, 0.0)
    spots = places.astype(F32)
    pos_q = jnp.broadcast_to(spots[:, None], (spots.shape[0], LANES))
    pos_k = jnp.broadcast_to(spots[None, :], (8, spots.shape[0]))
    dims = (n, m, rows, width, slab, part, ffp, b_qkv.shape[0] // LANES)
    args = (tokens, cotangent, piece_qkv, piece_gu, piece_out, piece_down, vec, rot_c, rot_a, rot_b, pos_q, pos_k)
    return dims, args


def shards(tokens, cotangent, gain1, bias1, w_qkv, b_qkv, w_out, gain2, bias2, w_gate_up, w_down):
    group = Group()
    n, m = lax.axis_size("dp"), group.m
    slab = gain1.shape[0]
    inner, hidden = w_out.shape[0] * n, w_down.shape[0] * n
    part, ff = inner // m, hidden // m
    dims, args = prepare(
        group.s, n, m, tokens, cotangent, gain1, bias1, w_qkv, b_qkv, w_out, gain2, bias2, w_gate_up, w_down,
        group.offsets,
    )
    ffp = dims[6]
    kept = run_forward(n, m, dims, args)
    block_out, input_grad, gu, qkv, down_sum, out_sum, lines = run_backward(dims, tuple(kept) + args[7:10] + args[11:])
    down = w_down.shape[0] // m
    g_gu = gu.reshape(m, slab // m, 2, n, ffp // n)[..., :down].reshape(m, slab // m, 2, ff)
    g_gu = g_gu.transpose(1, 2, 0, 3).reshape(slab // m, 2 * hidden).astype(F32)
    g_qkv = qkv.reshape(m, slab // m, 3, part).transpose(1, 2, 0, 3).reshape(slab // m, 3 * inner).astype(F32)
    line = jnp.sum(lines.reshape(m, -1), axis=0)
    vectors, at = [], 0
    for size in [slab] * 4 + [b_qkv.shape[0]]:
        vectors.append(lax.dynamic_slice(line, (at + group.s * (size // m),), (size // m,)))
        at += size
    return (
        block_out,
        input_grad,
        vectors[0],
        vectors[1],
        g_qkv,
        vectors[4],
        out_sum.astype(F32),
        vectors[2],
        vectors[3],
        g_gu,
        down_sum[:down].astype(F32),
    )


def fits(mesh, shapes):
    n, m = mesh.shape["dp"], mesh.shape["seq"]
    rows, slab = shapes[0][0], shapes[2][0]
    part = shapes[6][0] * n // m
    return (
        m == 4
        and n % 2 == 0
        and rows % LANES == 0
        and slab % LANES == 0
        and shapes[5][0] % LANES == 0
        and part % 256 == 0
        and (part // n) % (2 * TILE) == 0
        and (n * (-(-(shapes[10][0] // m) // TILE) * TILE)) % 256 == 0
        and (-(-(shapes[10][0] // m) // TILE) * TILE) % (2 * TILE) == 0
    )


def solution(mesh):
    rows, cols, vec = P(("dp", "seq"), None), P("dp", None), P("dp")
    flat = P(("dp", "seq"))
    def step(*args):
        body = shards if fits(mesh, [a.shape for a in args]) else shards_plain
        return body(*args)

    return jax.shard_map(
        step,
        mesh=mesh,
        in_specs=(rows, rows, vec, vec, cols, vec, cols, vec, vec, cols, cols),
        out_specs=(rows, rows, flat, flat, rows, flat, rows, flat, flat, rows, rows),
        check_vma=False,
    )
```

```python
import functools

import jax
import jax.numpy as jnp
import numpy as np
from jax import lax
from jax.experimental import pallas as pl
from jax.experimental.pallas import tpu as pltpu
from jax.sharding import PartitionSpec as P

HEAD_DIM = 64
ROT = 16
EPS = 1e-05
F32 = jnp.float32
BF16 = jnp.bfloat16


def ring_order(n):
    return list(range(0, n, 2)) + list(range(n - 1, 0, -2))


def dot(a, b):
    return jnp.dot(a, b, preferred_element_type=F32)


def dot_rows(a, b):
    return lax.dot_general(a, b, (((0,), (0,)), ((), ())), preferred_element_type=F32)


def dot_cols(a, b):
    return lax.dot_general(a, b, (((1,), (1,)), ((), ())), preferred_element_type=F32)


class Ring:
    def __init__(self):
        n = lax.axis_size("dp")
        order = ring_order(n)
        place = [order.index(i) for i in range(n)]
        self.n, self.half = n, n // 2
        self.right = [(order[i], order[(i + 1) % n]) for i in range(n)]
        self.left = [(b, a) for a, b in self.right]
        self.order = jnp.array(order, jnp.int32)
        self.place = jnp.array(place, jnp.int32)[lax.axis_index("dp")]

    def owner(self, offset):
        return self.order[lax.rem(self.place + offset + self.n, self.n)]

    def go_right(self, value):
        return lax.ppermute(value, "dp", self.right)

    def go_left(self, value):
        return lax.ppermute(value, "dp", self.left)

    def gather(self, piece):
        rows = piece.shape[0]
        cut = rows // 2
        from_left = from_right = piece
        whole = jnp.zeros((self.n,) + piece.shape, piece.dtype)

        def put(whole, offset, chunk):
            return lax.dynamic_update_slice(
                whole, chunk[None], (self.owner(offset),) + (0,) * piece.ndim
            )

        whole = put(whole, 0, piece)
        for k in range(1, self.half):
            from_left = self.go_right(from_left)
            from_right = self.go_left(from_right)
            whole = put(put(whole, -k, from_left), k, from_right)
        upper = self.go_right(from_left[:cut])
        lower = self.go_left(from_right[cut:])
        return put(whole, self.half, jnp.concatenate([upper, lower]))

    def scatter(self, parts):
        rows = parts.shape[1]
        cut = rows // 2

        def mine(offset):
            start = (self.owner(offset),) + (0,) * (parts.ndim - 1)
            return lax.dynamic_slice(parts, start, (1,) + parts.shape[1:])[0]

        def add(a, b):
            return a.astype(F32) + b.astype(F32)

        far = mine(self.half)
        upper = self.go_right(far[:cut])
        lower = self.go_left(far[cut:])
        from_left, from_right = mine(self.half - 1), mine(1 - self.half)
        from_left = jnp.concatenate(
            [add(from_left[:cut], upper).astype(BF16), from_left[cut:]]
        )
        from_right = jnp.concatenate(
            [from_right[:cut], add(from_right[cut:], lower).astype(BF16)]
        )
        for k in range(self.half - 2, -1, -1):
            from_left = self.go_right(from_left)
            from_right = self.go_left(from_right)
            if k:
                from_left = add(from_left, mine(k)).astype(BF16)
                from_right = add(from_right, mine(-k)).astype(BF16)
        return add(mine(0), from_left) + from_right.astype(F32)


class Group:
    def __init__(self):
        self.m = lax.axis_size("seq")
        self.s = lax.axis_index("seq")
        self.bits = []
        bit = self.m // 2
        while bit:
            self.bits.append(bit)
            bit //= 2
        self.offsets = [0]
        for bit in self.bits:
            self.offsets += [o ^ bit for o in self.offsets]

    def swap(self, value, mask):
        return lax.ppermute(value, "seq", [(i, i ^ mask) for i in range(self.m)])

    def gather(self, value):
        for bit in self.bits:
            value = jnp.concatenate([value, self.swap(value, bit)])
        return value

    def scatter(self, value):
        for bit in reversed(self.bits):
            half = value.shape[0] // 2
            got = self.swap(value[half:].astype(BF16), bit)
            value = value[:half] + got.astype(F32)
        return value

    def exchange(self, blocks):
        got = []
        for mask in range(self.m):
            block = lax.dynamic_index_in_dim(blocks, self.s ^ mask, 0, keepdims=False)
            got.append(self.swap(block, mask) if mask else block)
        stacked = jnp.stack(got)
        return jnp.take(stacked, self.s ^ jnp.arange(self.m), axis=0)


def norm(value):
    center = value - jnp.mean(value, axis=-1, keepdims=True)
    rstd = lax.rsqrt(jnp.mean(center * center, axis=-1, keepdims=True) + EPS)
    return center * rstd, rstd


def norm_back(upstream, xhat, rstd, gain):
    e = upstream * gain
    inner = (
        e
        - jnp.mean(e, axis=-1, keepdims=True)
        - xhat * jnp.mean(e * xhat, axis=-1, keepdims=True)
    )
    return rstd * inner


def rotary_tables(positions):
    half = ROT // 2
    inverse = 10000.0 ** (-(jnp.arange(half, dtype=F32) * 2.0 / ROT))
    angles = positions.astype(F32)[:, None] * inverse[None, :]
    return jnp.cos(angles)[:, None, :], jnp.sin(angles)[:, None, :]


def rotate(tensor, cosine, sine):
    half = ROT // 2
    a, b = tensor[..., :half], tensor[..., half:ROT]
    return jnp.concatenate([a * cosine - b * sine, b * cosine + a * sine, tensor[..., ROT:]], axis=-1)


def shards_plain(tokens, cotangent, gain1, bias1, w_qkv, b_qkv, w_out, gain2, bias2, w_gate_up, w_down):
    ring, group = Ring(), Group()
    n, m, s = ring.n, group.m, group.s
    rows, width = tokens.shape
    slab = gain1.shape[0]
    inner = w_out.shape[0] * n
    hidden = w_down.shape[0] * n
    part, ff = inner // m, hidden // m
    heads = part // HEAD_DIM
    scale = HEAD_DIM ** (-0.5)

    both = jnp.stack([tokens, cotangent], axis=1)
    everything = group.gather(both)
    tokens_all, cot_all = everything[:, 0], everything[:, 1]

    qkv_piece = jnp.concatenate(
        [lax.dynamic_slice(w_qkv, (0, i * inner + s * part), (slab, part)) for i in range(3)], axis=1
    )
    small = jnp.concatenate([gain1, bias1, gain2, bias2, b_qkv])
    extra = -(-small.shape[0] // (3 * part))
    small = jnp.pad(small, (0, extra * 3 * part - small.shape[0])).reshape(extra, 3 * part)
    first = ring.gather(jnp.concatenate([qkv_piece, small]))
    wqkv = first[:, :slab].reshape(width, 3 * part)
    vectors = first[:, slab:].reshape(n, -1)

    def vector(at, size):
        return vectors[:, at : at + size].reshape(-1).astype(F32)

    g1, b1, g2, b2 = (vector(i * slab, slab) for i in range(4))
    bias_all = vector(4 * slab, b_qkv.shape[0]).reshape(3, m, part)
    bias_qkv = lax.dynamic_index_in_dim(bias_all, s, 1, keepdims=False).reshape(3 * part)

    turn = [(g, (g % n) * m + g // n) for g in range(n * m)]
    back = [(b, a) for a, b in turn]

    def quarter(weight):
        count = weight.shape[0] // m
        mine = lax.dynamic_slice(weight, (0, 0), weight.shape)
        return mine.reshape(m, count, weight.shape[1])[s]

    out_rows, down_rows = w_out.shape[0] // m, w_down.shape[0] // m
    moved = lax.ppermute(
        jnp.concatenate([quarter(w_out), quarter(w_down)]), ("dp", "seq"), turn
    )
    wout = ring.gather(moved[:out_rows]).reshape(part, width)
    gu_piece = jnp.concatenate(
        [lax.dynamic_slice(w_gate_up, (0, i * hidden + s * ff), (slab, ff)) for i in range(2)], axis=1
    )
    wgu = ring.gather(gu_piece).reshape(width, 2 * ff)
    wdown = ring.gather(moved[out_rows:]).reshape(ff, width)

    places = jnp.concatenate([(s ^ o) * rows + jnp.arange(rows, dtype=jnp.int32) for o in group.offsets])
    cosine, sine = rotary_tables(places)
    count = rows * m
    xhat1, rstd1 = norm(tokens_all.astype(F32))
    normed1 = (xhat1 * g1 + b1).astype(BF16)
    qkv = (dot(normed1, wqkv) + bias_qkv).reshape(count, 3, heads, HEAD_DIM)
    queries = rotate(qkv[:, 0], cosine, sine).astype(BF16)
    keys = rotate(qkv[:, 1], cosine, sine).astype(BF16)
    values = qkv[:, 2].astype(BF16)
    scores = jnp.einsum("qhd,khd->hqk", queries, keys, preferred_element_type=F32) * scale
    scores = jnp.where((places[None, :] <= places[:, None])[None], scores, -jnp.inf)
    top = jnp.max(scores, axis=-1, keepdims=True)
    lse = top + jnp.log(jnp.sum(jnp.exp(scores - top), axis=-1, keepdims=True))
    probs = jnp.exp(scores - lse)
    probs_r = probs.astype(BF16)
    context = jnp.einsum("hqk,khd->qhd", probs_r, values, preferred_element_type=F32).astype(BF16)
    context_flat = context.reshape(count, part)
    x_own = tokens.astype(F32)
    mid = x_own + group.scatter(dot(context_flat, wout))
    xhat2, rstd2 = norm(mid)
    normed2 = group.gather((xhat2 * g2 + b2).astype(BF16))
    gate_up = dot(normed2, wgu)
    gate, up = gate_up[:, :ff], gate_up[:, ff:]
    sigma = jax.nn.sigmoid(gate)
    silu = gate * sigma
    act = (silu * up).astype(BF16)
    d_act = dot_cols(cot_all, wdown)
    d_gate = d_act * up * (sigma * (1.0 + gate * (1.0 - sigma)))
    d_gate_up = jnp.concatenate([d_gate, d_act * silu], axis=1).astype(BF16)

    d_normed2 = group.scatter(dot_cols(d_gate_up, wgu))
    sum_down = ring.scatter(dot_rows(act, cot_all).astype(BF16).reshape(n, ff // n, width))
    sum_gu = ring.scatter(dot_rows(normed2, d_gate_up).astype(BF16).reshape(n, slab, 2 * ff))
    block_out = (mid + group.scatter(dot(act, wdown))).astype(BF16)
    d_mid = cotangent.astype(F32) + norm_back(d_normed2, xhat2, rstd2, g2)
    d_mid_r = group.gather(d_mid.astype(BF16))

    d_context = dot_cols(d_mid_r, wout).astype(BF16).reshape(count, heads, HEAD_DIM)
    sum_out = ring.scatter(dot_rows(context_flat, d_mid_r).astype(BF16).reshape(n, part // n, width))
    d_probs = jnp.einsum("qhd,khd->hqk", d_context, values, preferred_element_type=F32)
    delta = jnp.einsum("qhd,qhd->hq", d_context.astype(F32), context.astype(F32))[..., None]
    d_scores = (probs * (d_probs - delta) * scale).astype(BF16)
    d_queries = jnp.einsum("hqk,khd->qhd", d_scores, keys, preferred_element_type=F32)
    d_keys = jnp.einsum("hqk,qhd->khd", d_scores, queries, preferred_element_type=F32)
    d_values = jnp.einsum("hqk,qhd->khd", probs_r, d_context, preferred_element_type=F32)
    d_qkv = jnp.stack(
        [rotate(d_queries, cosine, -sine), rotate(d_keys, cosine, -sine), d_values], axis=1
    ).reshape(count, 3 * part)
    d_qkv_r = d_qkv.astype(BF16)
    d_normed1_part = dot_cols(d_qkv_r, wqkv)
    d_normed1 = group.scatter(d_normed1_part)
    own = (slice(0, rows),)
    input_grad = d_mid + norm_back(d_normed1, xhat1[own], rstd1[own], g1)

    bias_part = jnp.zeros((3, m, part), F32)
    bias_part = lax.dynamic_update_slice(bias_part, jnp.sum(d_qkv, axis=0).reshape(3, 1, part), (0, s, 0))
    vector_parts = [
        jnp.sum(d_normed1_part * xhat1, axis=0),
        jnp.sum(d_normed1_part, axis=0),
        jnp.sum(d_normed2 * xhat2, axis=0),
        jnp.sum(d_normed2, axis=0),
        bias_part.reshape(-1),
    ]
    line = jnp.concatenate([v.reshape(n, m, -1) for v in vector_parts], axis=-1)
    lines = -(-line.shape[-1] // (3 * part))
    line = jnp.pad(line, ((0, 0), (0, 0), (0, lines * 3 * part - line.shape[-1])))
    line = line.reshape(n, m, lines, 3 * part).astype(BF16)
    part_qkv = dot_rows(normed1, d_qkv_r).astype(BF16).reshape(n, m, slab // m, 3 * part)
    packed = jnp.concatenate([part_qkv, line], axis=2)
    packed_rows = packed.shape[2]
    sum_qkv = ring.scatter(packed.reshape(n, m * packed_rows, 3 * part))

    def owners(total):
        return group.exchange(total.astype(BF16).reshape((m, -1) + total.shape[1:])).astype(F32)

    last = owners(sum_qkv)
    g_qkv = last[:, : slab // m].reshape(m, slab // m, 3, part).transpose(1, 2, 0, 3)
    g_qkv = g_qkv.reshape(slab // m, 3 * inner)
    line = jnp.sum(last[:, slab // m :], axis=0).reshape(-1)
    sizes = [slab // m] * 4 + [b_qkv.shape[0] // m]
    vectors_out, at = [], 0
    for size in sizes:
        vectors_out.append(line[at : at + size])
        at += size
    g_gu = owners(sum_gu).reshape(m, slab // m, 2, ff).transpose(1, 2, 0, 3).reshape(slab // m, 2 * hidden)
    g_down = lax.ppermute(sum_down.astype(BF16), ("dp", "seq"), back).astype(F32)
    g_out = lax.ppermute(sum_out.astype(BF16), ("dp", "seq"), back).astype(F32)
    return (
        block_out,
        input_grad,
        vectors_out[0],
        vectors_out[1],
        g_qkv,
        vectors_out[4],
        g_out,
        vectors_out[2],
        vectors_out[3],
        g_gu,
        g_down,
    )


LOGICAL = pl.DeviceIdType.LOGICAL
MEAN, RSTD, SPOT, LSE = 0, 1, 2, 8
LANES = 128
TILE = 16
VMEM_BYTES = 67_043_328


def vmem(shape, dtype=BF16):
    return pltpu.VMEM(shape, dtype)


class Place:
    def __init__(self, n, m):
        self.n, self.m, self.half = n, m, n // 2
        self.d, self.s = lax.axis_index("dp"), lax.axis_index("seq")
        pair = lax.div(self.d, 2)
        odd = self.d - 2 * pair
        place = pair + odd * (n - 1 - 2 * pair)
        self.owners = []
        for offset in range(n):
            spot = lax.rem(place + offset, n)
            back = lax.div(spot, self.half)
            self.owners.append(2 * spot + back * (2 * n - 1 - 4 * spot))
        self.partners = []
        for mask in range(m):
            out, bit = self.s, 1
            while bit < m:
                if mask & bit:
                    out = out + bit - 2 * bit * lax.rem(lax.div(self.s, bit), 2)
                bit *= 2
            self.partners.append(out)
        self.rings = {1: self.owners[1] * m + self.s, -1: self.owners[n - 1] * m + self.s}
        self.seqs = [self.d * m + out for out in self.partners]
        g = self.d * m + self.s
        h = self.s * n + self.d
        self.there = lax.rem(g, n)
        self.target = self.there * m + lax.div(g, n)
        self.source = h
        self.moves = (self.target - g) * (self.target - g) > 0

        offsets = [0]
        for bit in self.bits():
            offsets += [o ^ bit for o in offsets]
        self.homes = [self.partners[o] for o in offsets]

    def owner(self, offset):
        return self.owners[offset % self.n]

    def partner(self, mask):
        return self.partners[mask]

    def bits(self):
        out, bit = [], self.m // 2
        while bit:
            out.append(bit)
            bit //= 2
        return out


class Sender:
    def __init__(self, sends, recvs):
        self.sends, self.recvs = sends, recvs
        self.used = 0
        self.open = []

    def slot(self):
        self.used += 1
        return self.used - 1

    def copy(self, slot, src, dst, device):
        return pltpu.make_async_remote_copy(
            src_ref=src,
            dst_ref=dst,
            send_sem=self.sends.at[slot],
            recv_sem=self.recvs.at[slot],
            device_id=device,
            device_id_type=LOGICAL,
        )

    def start(self, slot, src, dst, device):
        copy = self.copy(slot, src, dst, device)
        copy.start()
        self.open.append(copy)
        return copy

    def finish(self):
        for copy in self.open:
            copy.wait_send()
        self.open = []


def greet(place, extra_seq=()):
    barrier = pltpu.get_barrier_semaphore()

    def hello(device):
        pl.semaphore_signal(barrier, inc=1, device_id=device, device_id_type=LOGICAL)

    near = [place.rings[1], place.rings[-1]] + [place.seqs[mask] for mask in tuple(place.bits()) + tuple(extra_seq)]
    for device in near:
        hello(device)

    @pl.when(place.moves)
    def _():
        hello(place.target)
        hello(place.source)
        pl.semaphore_wait(barrier, len(near) + 2)

    @pl.when(jnp.logical_not(place.moves))
    def _():
        pl.semaphore_wait(barrier, len(near))


class RowSlots:
    def __init__(self, rows, cols, lo=0):
        self.rows, self.cols, self.lo = rows, cols, lo

    def where(self, index, part=None):
        rows, start = self.rows, index * self.rows
        if part is not None:
            rows = rows // 2
            start = start + part * rows
        return pl.ds(pl.multiple_of(start, rows), rows), pl.ds(self.lo, self.cols)

    def landing(self, way, j, half):
        base = way * ((half - 1) * self.rows + self.rows // 2)
        at, rows = (base + (half - 1) * self.rows, self.rows // 2) if j == 1 else (base + (j - 2) * self.rows, self.rows)
        return pl.ds(at, rows), pl.ds(0, self.cols)

    def inbox(self, half):
        return 2 * ((half - 1) * self.rows + self.rows // 2), self.cols


class TileSlots:
    def __init__(self, rows, cols):
        self.rows, self.cols = rows, cols

    def where(self, index, part=None):
        row = lax.div(index, 2)
        cols, start = self.cols, (index - 2 * row) * self.cols
        if part is not None:
            cols = cols // 2
            start = start + part * cols
        return pl.ds(pl.multiple_of(row * self.rows, self.rows), self.rows), pl.ds(pl.multiple_of(start, cols), cols)

    def landing(self, way, j, half):
        at, cols = ((half - 1) * self.cols, self.cols // 2) if j == 1 else ((j - 2) * self.cols, self.cols)
        return pl.ds(way * self.rows, self.rows), pl.ds(at, cols)

    def inbox(self, half):
        return 2 * self.rows, (half - 1) * self.cols + self.cols // 2


class Gather:
    def __init__(self, place, sender, buf, slots):
        self.place, self.sender, self.buf, self.slots = place, sender, buf, slots
        self.sems = [[sender.slot() for _ in range(place.half)] for _ in range(2)]
        self.devices = (place.rings[1], place.rings[-1])

    def own(self):
        return self.buf.at[self.slots.where(self.place.d)]

    def send(self, k, way):
        index = self.place.owner(k if way else -k)
        ref = self.buf.at[self.slots.where(index, way if k == self.place.half - 1 else None)]
        self.sender.start(self.sems[way][k], ref, ref, self.devices[way])

    def begin(self):
        self.send(0, 0)
        self.send(0, 1)

    def pump(self, k):
        last = k == self.place.half
        for way in range(2):
            index = self.place.owner(k if way else -k)
            ref = self.buf.at[self.slots.where(index, way if last else None)]
            self.sender.copy(self.sems[way][k - 1], ref, ref, self.devices[way]).wait_recv()
            if not last:
                self.send(k, way)


class Reduce:
    def __init__(self, place, sender, buf, inbox, slots):
        self.place, self.sender, self.buf, self.inbox, self.slots = place, sender, buf, inbox, slots
        self.sems = [[sender.slot() for _ in range(place.half)] for _ in range(2)]
        self.devices = (place.rings[1], place.rings[-1])

    def target(self, way, j):
        offset = self.place.half - j
        return self.slots.where(self.place.owner(-offset if way else offset), way if j == 1 else None)

    def copy(self, way, j):
        offset = self.place.half - j + 1
        src = self.slots.where(self.place.owner(-offset if way else offset), way if j == 1 else None)
        return self.sems[way][j - 1], self.buf.at[src], self.inbox.at[self.slots.landing(way, j, self.place.half)]

    def send(self, j, way):
        self.sender.start(*self.copy(way, j), self.devices[way])

    def begin(self):
        self.send(1, 0)
        self.send(1, 1)

    def add(self, to, *froms):
        value = self.buf[to].astype(F32)
        for at in froms:
            value = value + self.inbox[at].astype(F32)
        self.buf[to] = value.astype(self.buf.dtype)

    def pump(self, j):
        half = self.place.half
        for way in range(2):
            self.sender.copy(*self.copy(way, j), self.devices[way]).wait_recv()
            if j < half:
                self.add(self.target(way, j), self.slots.landing(way, j, half))
                self.send(j + 1, way)
        if j == half:
            self.add(self.slots.where(self.place.d), *(self.slots.landing(way, j, half) for way in range(2)))

    def mine(self):
        return self.buf.at[self.slots.where(self.place.d)]


def blocks_of(ff):
    return [(at, min(256, ff - at), 2 * at) for at in range(0, ff, 256)]


def key_spots(place, pos_k, rows):
    lane = lax.broadcasted_iota(jnp.int32, (8, rows), 1)
    for i, home in enumerate(place.homes):
        pos_k[:, i * rows : (i + 1) * rows] = (home * rows + lane).astype(F32)


def load_rotary(place, h_rot, rot, rows, sems, first):
    copies = []
    for i, home in enumerate(place.homes):
        src = h_rot.at[pl.ds(pl.multiple_of(home * rows, rows), rows)]
        copies.append(pltpu.make_async_copy(src, rot.at[pl.ds(i * rows, rows)], sems.at[first + i]))
        copies[-1].start()
    return copies


def forward_kernel(
    dims,
    tok, cot, h_wqkv, piece_gu, h_wout, h_wdown, piece_vec, h_rot,
    o_wqkv, o_wout, o_wgu, o_wdown, o_rows, o_tok, o_cot, o_n1, o_qkv, o_stat, o_ctx, o_mid, o_n2, o_act, o_dgu,
    wqkv, wout, wgu, wdown, vec, tok_all, cot_all, n1, qkv, stat, ctx, mid, n2, act, dgu,
    rows_v, bias_v, rot, pos_k, own, send1, send2, recv1, recv2,
    sends, recvs, locals_, outs,
):
    n, m, rows, width, slab, part, ff, b_units = dims
    count = rows * m
    half = count // 2
    inner = part * m
    place = Place(n, m)
    sender = Sender(sends, recvs)
    d, s = place.d, place.s
    bits = place.bits()
    out_rows, vec_rows = part // n, piece_vec.shape[0]
    down_rows, down_cols = 2 * ff // n, width // 2
    blocks = blocks_of(ff)

    ring_a = Gather(place, sender, wqkv, RowSlots(slab, 3 * part))
    ring_v = Gather(place, sender, vec, RowSlots(vec_rows, LANES))
    ring_b = Gather(place, sender, wout, RowSlots(out_rows, width))
    ring_c = [Gather(place, sender, wgu, RowSlots(slab, 2 * units, lane)) for _, units, lane in blocks]
    ring_d = Gather(place, sender, wdown, TileSlots(down_rows, down_cols))

    def local(i, src, dst):
        copy = pltpu.make_async_copy(src, dst, locals_.at[i])
        copy.start()
        return copy

    own_rows = pl.ds(pl.multiple_of(d * slab, slab), slab)
    placed_qkv = [
        local(
            i,
            h_wqkv.at[:, pl.ds(pl.multiple_of(i * inner + s * part, part), part)],
            wqkv.at[own_rows, pl.ds(i * part, part)],
        )
        for i in range(3)
    ]
    placed_vec = local(3, piece_vec, ring_v.own())
    placed_tok = local(4, tok, tok_all.at[pl.ds(0, rows)])
    placed_gu = local(5, piece_gu, wgu.at[own_rows])
    placed_cot = local(6, cot, cot_all.at[pl.ds(0, rows)])
    placed_rot = load_rotary(place, h_rot, rot, rows, locals_, 9)
    greet(place)
    moves = place.moves

    class Spread:
        def __init__(self, buf):
            self.buf = buf
            self.sems = [sender.slot() for _ in bits]

        def copy(self, i):
            size = rows << i
            return self.sems[i], self.buf.at[pl.ds(0, size)], self.buf.at[pl.ds(size, size)], place.seqs[bits[i]]

        def send(self, i):
            sender.start(*self.copy(i))

        def wait(self, i):
            sender.copy(*self.copy(i)).wait_recv()

    toks, cots, n2s = Spread(tok_all), Spread(cot_all), Spread(n2)
    written = []

    def write(src, dst):
        copy = pltpu.make_async_copy(src, dst, outs.at[len(written)])
        copy.start()
        written.append(copy)

    for copy in placed_qkv:
        copy.wait()
    ring_a.begin()
    placed_vec.wait()
    ring_v.begin()
    placed_tok.wait()
    toks.send(0)

    src_out = h_wout.at[pl.ds(pl.multiple_of(s * out_rows, out_rows), out_rows)]
    up = lax.div(s, 2)
    src_down = h_wdown.at[
        pl.ds(pl.multiple_of(up * down_rows, down_rows), down_rows),
        pl.ds(pl.multiple_of((s - 2 * up) * down_cols, down_cols), down_cols),
    ]
    turns = [(src_out, ring_b, sender.slot(), 7), (src_down, ring_d, sender.slot(), 8)]

    def turn(ring, index):
        return ring.buf.at[ring.slots.where(index)]

    @pl.when(moves)
    def _():
        for src, ring, slot, _ in turns:
            sender.copy(slot, src, turn(ring, place.there), place.target).start()

    @pl.when(jnp.logical_not(moves))
    def _():
        for src, ring, _, i in turns:
            local(i, src, ring.own()).wait()

    placed_gu.wait()
    ring_c[0].begin()
    placed_cot.wait()
    cots.send(0)
    wdown[ff:, :] = jnp.zeros((wdown.shape[0] - ff, width), BF16)
    key_spots(place, pos_k, rows)
    lane = lax.broadcasted_iota(jnp.int32, (1, LANES), 1)
    line = lax.broadcasted_iota(jnp.int32, (rows, 1), 0)

    def stats(i):
        span = slice(i * rows, (i + 1) * rows)
        x = tok_all[span, :].astype(F32)
        mu = jnp.mean(x, axis=-1, keepdims=True)
        c = x - mu
        r = lax.rsqrt(jnp.mean(c * c, axis=-1, keepdims=True) + EPS)
        spot = (place.homes[i] * rows + line).astype(F32)
        stat[span, :] = jnp.where(lane == MEAN, mu, jnp.where(lane == RSTD, r, spot))

    stats(0)
    ring_v.pump(1)
    ring_a.pump(1)

    @pl.when(moves)
    def _():
        for src, ring, slot, _ in turns:
            sender.copy(slot, src, ring.own(), place.source).wait_recv()

    ring_b.begin()
    toks.wait(0)
    toks.send(1)
    stats(1)
    ring_v.pump(2)
    ring_a.pump(2)
    ring_d.begin()
    ring_b.pump(1)
    toks.wait(1)
    write(tok_all, o_tok)
    stats(2)
    stats(3)
    cots.wait(0)
    cots.send(1)
    ring_v.pump(3)
    ring_a.pump(3)
    ring_c[1].begin()
    ring_b.pump(2)
    ring_c[0].pump(1)
    ring_v.pump(4)
    units = slab // LANES
    for c in range(n):
        for r in range(4):
            for u in range(units):
                at = c * slab + u * LANES
                row = c * vec_rows + r * units + u
                rows_v[r : r + 1, at : at + LANES] = vec[row : row + 1, :]
    for i in range(3):
        for u in range(part // LANES):
            unit = i * (inner // LANES) + s * (part // LANES) + u
            row = lax.div(unit, b_units) * vec_rows + 4 * units + lax.rem(unit, b_units)
            at = i * part + u * LANES
            bias_v[0:1, at : at + LANES] = vec[pl.ds(row, 1), :]
    write(rows_v, o_rows)

    def normalize(j, carry):
        size = 64
        span = pl.ds(pl.multiple_of(j * size, size), size)
        x = tok_all[span, :].astype(F32)
        xhat = (x - stat[span, MEAN : MEAN + 1]) * stat[span, RSTD : RSTD + 1]
        n1[span, :] = (xhat * rows_v[0:1, :] + rows_v[1:2, :]).astype(BF16)
        return carry

    lax.fori_loop(0, count // 64, normalize, 0)
    write(n1, o_n1)
    ring_d.pump(1)
    ring_c[2].begin()
    cots.wait(1)
    write(cot_all, o_cot)
    ring_a.pump(4)
    write(wqkv, o_wqkv)
    for copy in placed_rot:
        copy.wait()

    def project(j, carry):
        size = 256
        span = pl.ds(pl.multiple_of(j * size, size), size)
        for i in range(3):
            cols = slice(i * part, (i + 1) * part)
            y = dot(n1[span, :], wqkv[:, cols]) + bias_v[0:1, cols]
            if i < 2:
                pieces = []
                for u in range(part // LANES):
                    z = y[:, u * LANES : (u + 1) * LANES]
                    pieces.append(
                        z * rot[span, :LANES]
                        + pltpu.roll(z, LANES - ROT // 2, 1) * rot[span, LANES : 2 * LANES]
                        + pltpu.roll(z, ROT // 2, 1) * rot[span, 2 * LANES :]
                    )
                y = jnp.concatenate(pieces, axis=1)
            qkv[span, cols] = y.astype(BF16)
        return carry

    lax.fori_loop(0, count // 256, project, 0)
    write(qkv, o_qkv)
    ring_b.pump(3)
    ring_c[1].pump(1)
    ring_c[0].pump(2)
    scale = HEAD_DIM ** (-0.5)
    per = LANES // HEAD_DIM

    def attend(i, carry):
        pair, block = lax.div(i, m), lax.rem(i, m)
        span = pl.ds(pl.multiple_of(block * rows, rows), rows)
        at = pl.multiple_of(pair * LANES, LANES)
        q = qkv[span, pl.ds(at, LANES)]
        k = qkv[:, pl.ds(pl.multiple_of(part + at, LANES), LANES)]
        v = qkv[:, pl.ds(pl.multiple_of(2 * part + at, LANES), LANES)]
        allowed = pos_k[0:1, :] <= stat[span, SPOT : SPOT + 1]
        total = jnp.zeros((rows, LANES), F32)
        for h in range(per):
            mine = (lane // HEAD_DIM == h).astype(BF16)
            scores = dot_cols(q * mine, k) * scale
            scores = jnp.where(allowed, scores, -jnp.inf)
            top = jnp.max(scores, axis=-1, keepdims=True)
            found = top + jnp.log(jnp.sum(jnp.exp(scores - top), axis=-1, keepdims=True))
            probs = jnp.exp(scores - found).astype(BF16)
            total = total + dot(probs, v * mine)
            stat[span, :] = jnp.where(lane == LSE + pair * per + h, found, stat[span, :])
        ctx[span, pl.ds(at, LANES)] = total.astype(BF16)
        return carry

    lax.fori_loop(0, (part // LANES) * m, attend, 0)
    write(stat, o_stat)
    write(ctx, o_ctx)
    ring_d.pump(2)
    ring_c[2].pump(1)
    ring_b.pump(4)
    write(wout, o_wout)

    step = 512
    scatter = [sender.slot(), sender.slot()]

    def far_part(j, carry):
        cols = pl.ds(pl.multiple_of(j * step, step), step)
        send1[:, cols] = dot(ctx[half:, :], wout[:, cols]).astype(BF16)
        return carry

    lax.fori_loop(0, width // step, far_part, 0)
    first = sender.start(scatter[0], send1, recv1, place.seqs[bits[1]])

    def near_part(j, carry):
        cols = pl.ds(pl.multiple_of(j * step, step), step)
        own[:, cols] = dot(ctx[:half, :], wout[:, cols])
        return carry

    lax.fori_loop(0, width // step, near_part, 0)
    ring_c[1].pump(2)
    first.wait_recv()
    send2[...] = (own[rows:, :] + recv1[rows:, :].astype(F32)).astype(BF16)
    second = sender.start(scatter[1], send2, recv2, place.seqs[bits[0]])
    ring_c[0].pump(3)
    second.wait_recv()
    value = tok_all[:rows, :].astype(F32) + own[:rows, :] + recv1[:rows, :].astype(F32) + recv2[...].astype(F32)
    mid[...] = value
    c = value - jnp.mean(value, axis=-1, keepdims=True)
    r = lax.rsqrt(jnp.mean(c * c, axis=-1, keepdims=True) + EPS)
    n2[:rows, :] = (c * r * rows_v[2:3, :] + rows_v[3:4, :]).astype(BF16)
    n2s.send(0)
    write(mid, o_mid)
    ring_d.pump(3)
    ring_c[2].pump(2)
    ring_c[1].pump(3)
    n2s.wait(0)
    n2s.send(1)
    ring_c[0].pump(4)
    ring_d.pump(4)
    write(wdown, o_wdown)
    n2s.wait(1)
    write(n2, o_n2)
    ring_c[2].pump(3)

    def expand(first_unit, units, base):
        even = units // LANES * LANES
        y = dot(n2[...], wgu[:, base : base + 2 * units])
        d_act = dot_cols(cot_all[...], wdown[first_unit : first_unit + 256, :])
        if even == units:
            gate, up = y[:, :units], y[:, units:]
        else:
            gate = y[:, : even + LANES]
            up = jnp.concatenate([y[:, even + LANES :], pltpu.roll(gate[:, even:], LANES // 2, 1)], axis=1)
        sigma = jax.nn.sigmoid(gate)
        silu = gate * sigma
        value = silu * up
        d_gate = d_act * up * (sigma * (1.0 + gate * (1.0 - sigma)))
        d_up = d_act * silu
        if even == units:
            dgu[:, base : base + units] = d_gate.astype(BF16)
            dgu[:, base + units : base + 2 * units] = d_up.astype(BF16)
        else:
            value = jnp.where(lax.broadcasted_iota(jnp.int32, (1, 256), 1) < units, value, 0.0)
            mixed = jnp.where(lane < LANES // 2, d_gate[:, even:], pltpu.roll(d_up[:, even:], LANES // 2, 1))
            dgu[:, base : base + even] = d_gate[:, :even].astype(BF16)
            dgu[:, base + even : base + even + LANES] = mixed.astype(BF16)
            dgu[:, base + even + LANES : base + 2 * units] = d_up[:, :even].astype(BF16)
        act[:, first_unit : first_unit + 256] = value.astype(BF16)

    expand(*blocks[0])
    ring_c[1].pump(4)
    expand(*blocks[1])
    ring_c[2].pump(4)
    write(wgu, o_wgu)
    expand(*blocks[2])
    write(act, o_act)
    write(dgu, o_dgu)
    for copy in written:
        copy.wait()
    sender.finish()

    @pl.when(moves)
    def _():
        for src, ring, slot, _ in turns:
            sender.copy(slot, src, turn(ring, place.there), place.target).wait_send()


def run_forward(dims, args):
    n, m, rows, width, slab, part, ff, b_units = dims
    count = rows * m
    ffp = -(-ff // 256) * 256
    vec_rows = args[6].shape[0]
    arrays = [
        ((width, 3 * part), BF16), ((part, width), BF16), ((width, 2 * ff), BF16), ((ffp, width), BF16),
        ((8, width), F32), ((count, width), BF16), ((count, width), BF16), ((count, width), BF16),
        ((count, 3 * part), BF16), ((count, LANES), F32), ((count, part), BF16), ((rows, width), F32),
        ((count, width), BF16), ((count, ffp), BF16), ((count, 2 * ff), BF16),
    ]
    scratch = [vmem(*a) for a in arrays]
    rows_v, scratch[4] = scratch[4], vmem((n * vec_rows, LANES), F32)
    slots = (4 + len(blocks_of(ff))) * 2 * (n // 2) + 3 * 2 + 2 + 2
    return pl.pallas_call(
        functools.partial(forward_kernel, dims),
        out_shape=[jax.ShapeDtypeStruct(*a) for a in arrays],
        in_specs=[pl.BlockSpec(memory_space=pl.ANY)] * len(args),
        out_specs=[pl.BlockSpec(memory_space=pl.ANY)] * len(arrays),
        scratch_shapes=scratch
        + [
            rows_v,
            vmem((8, 3 * part), F32),
            vmem((count, 3 * LANES), F32),
            vmem((8, count), F32),
            vmem((count // 2, width), F32),
            vmem((count // 2, width)),
            vmem((rows, width)),
            vmem((count // 2, width)),
            vmem((rows, width)),
            pltpu.SemaphoreType.DMA((slots,)),
            pltpu.SemaphoreType.DMA((slots,)),
            pltpu.SemaphoreType.DMA((9 + m,)),
            pltpu.SemaphoreType.DMA((len(arrays),)),
        ],
        compiler_params=pltpu.CompilerParams(
            collective_id=0, has_side_effects=True, vmem_limit_bytes=VMEM_BYTES
        ),
        name="forward",
    )(*args)


def flip(value):
    size = value.shape[1]
    here = lax.broadcasted_iota(jnp.int32, (size, size), 0) == lax.broadcasted_iota(jnp.int32, (size, size), 1)
    return dot_cols(here.astype(F32).astype(BF16), value).astype(BF16)


def backward_kernel(
    dims,
    h_wqkv, h_wout, h_wgu, h_wdown, h_rows, h_tok, h_cot, h_n1, h_qkv, h_stat, h_ctx, h_mid, h_n2, h_act, h_dgu,
    h_rot,
    o_block, o_input, o_gu, o_qkv, o_down, o_out, o_vec,
    wout, wgu, wqkv, rows_v, wide_a, wide_b, qkv, stat, ctx, mid, act, dgu, rot, pos_k,
    sum_a, sum_b, sum_c, sum_d, sum_v, in_a, in_b, in_c, in_d, in_v,
    own, send1, send2, recv1, recv2, dm_all, d_mid, cot, dctx, dqkv, dk, dv, sums_v, bias_v,
    x_gu, x_qkv, x_down, x_half, x_out, x_vec, y_qkv, y_down,
    sends, recvs, loads, outs,
):
    n, m, rows, width, slab, part, ff, b_units = dims
    ffp = act.shape[1]
    inner = part * m
    count = rows * m
    half = count // 2
    place = Place(n, m)
    sender = Sender(sends, recvs)
    waiting = {}

    def load(name, src, dst):
        copy = pltpu.make_async_copy(src, dst, loads.at[len(waiting)])
        copy.start()
        waiting[name] = copy

    load("act", h_act, act)
    load("cot", h_cot, wide_a)
    load("n2", h_n2, wide_b)
    load("dgu", h_dgu, dgu)
    load("wgu", h_wgu, wgu)
    load("own", h_cot.at[pl.ds(0, dims[2])], cot)
    load("mid", h_mid, mid)
    load("rows", h_rows, rows_v)
    load("wqkv", h_wqkv, wqkv)
    load("wout", h_wout, wout)
    load("ctx", h_ctx, ctx)
    load("qkv", h_qkv, qkv)
    load("stat", h_stat, stat)
    spare = loads.shape[0] - 2
    rotary = load_rotary(place, h_rot, rot, rows, loads, spare - m)
    bits = place.bits()
    others = [mask for mask in range(1, m) if mask not in bits]
    moves = place.moves
    greet(place, others)
    d, s = place.d, place.s
    out_rows, vec_rows = part // n, sum_v.shape[0] // n
    down_rows, down_cols = 2 * ff // n, width // 2
    ring_a = Reduce(place, sender, sum_a, in_a, RowSlots(slab, 3 * part))
    ring_b = Reduce(place, sender, sum_b, in_b, RowSlots(out_rows, width))
    ring_c = Reduce(place, sender, sum_c, in_c, RowSlots(slab, 2 * ff))
    ring_d = Reduce(place, sender, sum_d, in_d, TileSlots(down_rows, down_cols))
    ring_v = Reduce(place, sender, sum_v, in_v, RowSlots(vec_rows, LANES))
    key_spots(place, pos_k, rows)
    block = 256

    def outer(dst, left, right, size):
        def step(j, carry):
            cols = pl.ds(pl.multiple_of(j * block, block), block)
            dst[cols, :] = dot(flip(left[:, cols]), right[...]).astype(BF16)
            return carry

        lax.fori_loop(0, size // block, step, 0)

    class Halving:
        def __init__(self, at):
            self.slots = [sender.slot(), sender.slot()]
            self.at = at
            self.open = []

        def first(self, far):
            far()
            self.open.append(sender.start(self.slots[0], send1, recv1.at[pl.ds(self.at * half, half)], place.seqs[bits[1]]))

        def second(self):
            self.open[0].wait_recv()
            send2[...] = (own[rows:, :] + recv1[self.at * half + rows : (self.at + 1) * half, :].astype(F32)).astype(BF16)
            self.open.append(sender.start(self.slots[1], send2, recv2.at[pl.ds(self.at * rows, rows)], place.seqs[bits[0]]))

        def total(self):
            self.open[1].wait_recv()
            return own[:rows, :] + recv1[self.at * half : self.at * half + rows, :].astype(F32) + recv2[
                self.at * rows : (self.at + 1) * rows, :
            ].astype(F32)

        def sent(self):
            for copy in self.open:
                copy.wait_send()
            sender.open = [c for c in sender.open if all(c is not o for o in self.open)]

    waiting["act"].wait()
    waiting["cot"].wait()
    outer(sum_d, act, wide_a, ffp)
    ring_d.begin()
    waiting["n2"].wait()
    waiting["dgu"].wait()

    def slab_of(index):
        cols = pl.ds(pl.multiple_of(index * slab, slab), slab)
        sum_c[cols, :] = dot(flip(wide_b[:, cols]), dgu[...]).astype(BF16)

    slab_of(place.owner(place.half))
    ring_c.begin()
    waiting["wgu"].wait()
    normed2 = Halving(0)

    def back_step(left, lo, hi, weight, to):
        def step(j, carry):
            cols = pl.ds(pl.multiple_of(j * block, block), block)
            to(cols, dot_cols(left[lo:hi, :], weight[cols, :]))
            return carry

        lax.fori_loop(0, width // block, step, 0)

    def to_send(cols, value):
        send1[:, cols] = value.astype(BF16)

    def to_own(cols, value):
        own[:, cols] = value

    normed2.first(lambda: back_step(dgu, half, count, wgu, to_send))
    back_step(dgu, 0, half, wgu, to_own)
    lanes = 2 * ff
    load("down_lo", h_wdown.at[:, pl.ds(0, lanes)], wgu.at[pl.ds(0, ffp)])
    load("down_hi", h_wdown.at[:, pl.ds(lanes, width - lanes)], wgu.at[pl.ds(ffp, ffp), pl.ds(0, width - lanes)])
    normed2.second()
    ring_d.pump(1)

    def other_slabs(i, carry):
        slab_of(lax.rem(place.owner(place.half) + i, n))
        return carry

    lax.fori_loop(1, n, other_slabs, 0)
    load("n1", h_n1, wide_b)
    load("tok", h_tok, wide_a)
    ring_c.pump(1)
    ring_d.pump(2)

    waiting["mid"].wait()
    waiting["rows"].wait()
    waiting["own"].wait()

    def deviation(value):
        c = value - jnp.mean(value, axis=-1, keepdims=True)
        r = lax.rsqrt(jnp.mean(c * c, axis=-1, keepdims=True) + EPS)
        return c * r, r

    xhat, r = deviation(mid[...])
    up = normed2.total()
    sums_v[2:3, :] = jnp.sum(up * xhat, axis=0, keepdims=True)
    sums_v[3:4, :] = jnp.sum(up, axis=0, keepdims=True)
    d_mid[...] = cot[...].astype(F32) + norm_back(up, xhat, r, rows_v[2:3, :])
    dm_all[:rows, :] = d_mid[...].astype(BF16)
    spread = [sender.slot() for _ in bits]

    def spread_copy(i):
        size = rows << i
        return (spread[i], dm_all.at[pl.ds(0, size)], dm_all.at[pl.ds(size, size)])

    def spread_send(i):
        sender.start(*spread_copy(i), place.seqs[bits[i]])

    def spread_wait(i):
        sender.copy(*spread_copy(i), place.seqs[bits[i]]).wait_recv()

    spread_send(0)
    normed2.sent()

    waiting["down_lo"].wait()
    waiting["down_hi"].wait()

    def down_step(lo, hi, to):
        def low(j, carry):
            cols = pl.ds(pl.multiple_of(j * LANES, LANES), LANES)
            to(cols, dot(act[lo:hi, :], wgu[:ffp, cols]))
            return carry

        def high(j, carry):
            cols = pl.ds(pl.multiple_of(j * LANES, LANES), LANES)
            to(pl.ds(pl.multiple_of(lanes + j * LANES, LANES), LANES), dot(act[lo:hi, :], wgu[ffp : 2 * ffp, cols]))
            return carry

        lax.fori_loop(0, lanes // LANES, low, 0)
        lax.fori_loop(0, (width - lanes) // LANES, high, 0)

    output = Halving(1)

    output.first(lambda: down_step(half, count, to_send))
    down_step(0, half, to_own)
    spread_wait(0)
    spread_send(1)
    output.second()
    ring_c.pump(2)
    spread_wait(1)

    waiting["wout"].wait()
    waiting["ctx"].wait()
    dctx[...] = dot_cols(dm_all[...], wout[...]).astype(BF16)
    outer(sum_b, ctx, dm_all, part)
    ring_b.begin()
    cot[...] = (mid[...] + output.total()).astype(BF16)
    output.sent()
    ring_d.pump(3)

    for name in ("qkv", "stat"):
        waiting[name].wait()
    for copy in rotary:
        copy.wait()
    scale = HEAD_DIM ** (-0.5)
    per = LANES // HEAD_DIM
    lane = lax.broadcasted_iota(jnp.int32, (1, LANES), 1) // HEAD_DIM

    def turned(z, span):
        return (
            z * rot[span, :LANES]
            - pltpu.roll(z, LANES - ROT // 2, 1) * rot[span, LANES : 2 * LANES]
            - pltpu.roll(z, ROT // 2, 1) * rot[span, 2 * LANES :]
        )

    bias_v[...] = jnp.zeros_like(bias_v)
    for pair in range(part // LANES):
        at = pair * LANES
        dk[...] = jnp.zeros_like(dk)
        dv[...] = jnp.zeros_like(dv)

        def attend(i, carry, pair=pair, at=at):
            span = pl.ds(pl.multiple_of(i * rows, rows), rows)
            q = qkv[span, at : at + LANES]
            k = qkv[:, part + at : part + at + LANES]
            v = qkv[:, 2 * part + at : 2 * part + at + LANES]
            dc = dctx[span, at : at + LANES]
            both = dc.astype(F32) * ctx[span, at : at + LANES].astype(F32)
            allowed = pos_k[0:1, :] <= stat[span, SPOT : SPOT + 1]
            dq = jnp.zeros((rows, LANES), F32)
            for h in range(per):
                pick = lane == h
                mine = pick.astype(BF16)
                qm, dcm = q * mine, dc * mine
                scores = dot_cols(qm, k) * scale
                at_lse = LSE + pair * per + h
                probs = jnp.exp(jnp.where(allowed, scores, -jnp.inf) - stat[span, at_lse : at_lse + 1])
                delta = jnp.sum(jnp.where(pick, both, 0.0), axis=-1, keepdims=True)
                ds = (probs * (dot_cols(dcm, v) - delta) * scale).astype(BF16)
                dq = dq + jnp.dot(ds, k * mine, preferred_element_type=F32)
                dk[...] += dot(flip(ds), qm)
                dv[...] += dot(flip(probs.astype(BF16)), dcm)
            dq = turned(dq, span)
            bias_v[0:1, at : at + LANES] += jnp.sum(dq, axis=0, keepdims=True)
            dqkv[span, at : at + LANES] = dq.astype(BF16)
            return carry

        lax.fori_loop(0, m, attend, 0)

        def settle(i, carry, at=at):
            span = pl.ds(pl.multiple_of(i * rows, rows), rows)
            key, value = turned(dk[span, :], span), dv[span, :]
            bias_v[0:1, part + at : part + at + LANES] += jnp.sum(key, axis=0, keepdims=True)
            bias_v[0:1, 2 * part + at : 2 * part + at + LANES] += jnp.sum(value, axis=0, keepdims=True)
            dqkv[span, part + at : part + at + LANES] = key.astype(BF16)
            dqkv[span, 2 * part + at : 2 * part + at + LANES] = value.astype(BF16)
            return carry

        lax.fori_loop(0, m, settle, 0)
        if pair == 0:
            ring_b.pump(1)

    waiting["n1"].wait()
    outer(sum_a, wide_b, dqkv, width)
    ring_a.begin()
    ring_c.pump(3)
    ring_b.pump(2)
    waiting["wqkv"].wait()
    waiting["tok"].wait()
    normed1 = Halving(2)

    def gains(cols, value, lo, hi):
        xh = (wide_a[lo:hi, cols].astype(F32) - stat[lo:hi, MEAN : MEAN + 1]) * stat[lo:hi, RSTD : RSTD + 1]
        return jnp.sum(value * xh, axis=0, keepdims=True), jnp.sum(value, axis=0, keepdims=True)

    def far_last(cols, value):
        send1[:, cols] = value.astype(BF16)
        sums_v[0:1, cols], sums_v[1:2, cols] = gains(cols, value, half, count)

    def near_last(cols, value):
        own[:, cols] = value
        gain, total = gains(cols, value, 0, half)
        sums_v[0:1, cols] += gain
        sums_v[1:2, cols] += total

    normed1.first(lambda: back_step(dqkv, half, count, wqkv, far_last))
    back_step(dqkv, 0, half, wqkv, near_last)

    sum_v[...] = jnp.zeros_like(sum_v)
    units = slab // LANES

    def lay(c, carry):
        for i in range(4):
            for u in range(units):
                at = pl.multiple_of(c * slab + u * LANES, LANES)
                sum_v[pl.ds(c * vec_rows + i * units + u, 1), :] = sums_v[i : i + 1, pl.ds(at, LANES)]
        return carry

    lax.fori_loop(0, n, lay, 0)
    for i in range(3):
        for u in range(part // LANES):
            unit = i * (m * part // LANES) + s * (part // LANES) + u
            row = lax.div(unit, b_units) * vec_rows + 4 * units + lax.rem(unit, b_units)
            at = i * part + u * LANES
            sum_v[pl.ds(row, 1), :] = bias_v[0:1, at : at + LANES]
    ring_v.begin()
    normed1.second()
    ring_d.pump(4)
    ring_b.pump(3)
    ring_a.pump(1)
    ring_v.pump(1)
    ring_a.pump(2)
    ring_v.pump(2)
    up = normed1.total()
    rstd = stat[:rows, RSTD : RSTD + 1]
    xhat = (wide_a[:rows, :].astype(F32) - stat[:rows, MEAN : MEAN + 1]) * rstd
    own[:rows, :] = d_mid[...] + norm_back(up, xhat, rstd, rows_v[0:1, :])
    ring_b.pump(4)
    ring_v.pump(3)

    written = []

    def store(src, dst):
        copy = pltpu.make_async_copy(src, dst, outs.at[len(written)])
        copy.start()
        written.append(copy)

    store(cot, o_block)
    store(own.at[pl.ds(0, rows)], o_input)
    turns = [(ring_d, x_down, sender.slot()), (ring_b, x_out, sender.slot())]

    @pl.when(moves)
    def _():
        for ring, landing, slot in turns:
            sender.copy(slot, ring.mine(), landing, place.source).start()

    @pl.when(jnp.logical_not(moves))
    def _():
        for i, (ring, landing, _) in enumerate(turns):
            copy = pltpu.make_async_copy(ring.mine(), landing, loads.at[spare + i])
            copy.start()
            copy.wait()

    def deal(buf, size, landing, whole=False):
        share = size if whole else size // m
        got = []
        to = pl.ds(pl.multiple_of(s * share, share), share)
        for mask in range(1, m):
            start = d * size + (0 if whole else place.partner(mask) * share)
            src = buf.at[pl.ds(pl.multiple_of(start, share), share)]
            got.append(sender.start(sender.slot(), src, landing.at[to], place.seqs[mask]))
        start = d * size + (0 if whole else s * share)
        landing[to, :] = buf[pl.ds(pl.multiple_of(start, share), share), :]
        return got

    ring_c.pump(4)
    got_gu = deal(sum_c, slab, x_gu)
    ring_a.pump(3)

    @pl.when(moves)
    def _():
        for ring, landing, slot in turns:
            sender.copy(slot, ring.mine(), landing, place.target).wait_recv()

    x_half[...] = x_down[...].astype(F32)
    some = down_rows // 2
    column = lax.rem(s, 2)
    across = pl.ds(pl.multiple_of(column * down_cols, down_cols), down_cols)
    swap = sender.start(
        sender.slot(),
        x_half.at[pl.ds(pl.multiple_of((1 - column) * some, some), some)],
        y_down.at[:, across],
        place.seqs[1],
    )
    y_down[:, across] = x_half[pl.ds(pl.multiple_of(column * some, some), some), :]
    store(x_out, o_out)
    ring_v.pump(4)
    got_vec = deal(sum_v, vec_rows, x_vec, whole=True)
    ring_a.pump(4)
    got_qkv = deal(sum_a, slab, x_qkv)
    for copy in got_gu:
        copy.wait_recv()
    store(x_gu, o_gu)
    swap.wait_recv()
    store(y_down, o_down)
    for copy in got_vec:
        copy.wait_recv()
    total = x_vec[:vec_rows, :]
    for t in range(1, m):
        total = total + x_vec[t * vec_rows : (t + 1) * vec_rows, :]
    x_vec[:vec_rows, :] = total
    store(x_vec.at[pl.ds(0, vec_rows)], o_vec)
    for copy in got_qkv:
        copy.wait_recv()
    share = slab // m
    for t in range(m):
        for i in range(3):
            at = i * inner + t * part
            y_qkv[:, at : at + part] = x_qkv[t * share : (t + 1) * share, i * part : (i + 1) * part].astype(F32)
    store(y_qkv, o_qkv)
    for copy in written:
        copy.wait()
    sender.finish()

    @pl.when(moves)
    def _():
        for ring, landing, slot in turns:
            sender.copy(slot, ring.mine(), landing, place.source).wait_send()


def run_backward(dims, args):
    n, m, rows, width, slab, part, ff, b_units = dims
    count = rows * m
    ffp = -(-ff // 256) * 256
    vec_rows = -(-(4 * (slab // LANES) + b_units) // TILE) * TILE
    half = n // 2
    out_rows = part // n
    down_rows, down_cols = 2 * ff // n, width // 2
    share = slab // m

    def inbox(slots, dtype=BF16):
        return vmem(slots.inbox(half), dtype)

    outputs = [
        ((rows, width), BF16), ((rows, width), F32), ((slab, 2 * ff), BF16), ((share, 3 * part * m), F32),
        ((down_rows // 2, width), F32), ((out_rows, width), BF16), ((vec_rows, LANES), F32),
    ]
    scratch = [
        vmem((part, width)), vmem((width, 2 * ff)), vmem((width, 3 * part)), vmem((8, width), F32),
        vmem((count, width)), vmem((count, width)), vmem((count, 3 * part)), vmem((count, LANES), F32),
        vmem((count, part)), vmem((rows, width), F32), vmem((count, ffp)), vmem((count, 2 * ff)),
        vmem((count, 3 * LANES), F32), vmem((8, count), F32),
        vmem((n * slab, 3 * part)), vmem((part, width)), vmem((n * slab, 2 * ff)), vmem((ffp, width)),
        vmem((n * vec_rows, LANES), F32),
        inbox(RowSlots(slab, 3 * part)), inbox(RowSlots(out_rows, width)), inbox(RowSlots(slab, 2 * ff)),
        inbox(TileSlots(down_rows, down_cols)), inbox(RowSlots(vec_rows, LANES), F32),
        vmem((count // 2, width), F32), vmem((count // 2, width)), vmem((rows, width)),
        vmem((3 * count // 2, width)), vmem((3 * rows, width)),
        vmem((count, width)), vmem((rows, width), F32), vmem((rows, width)), vmem((count, part)), vmem((count, 3 * part)),
        vmem((count, LANES), F32), vmem((count, LANES), F32), vmem((8, width), F32), vmem((8, 3 * part), F32),
        vmem((slab, 2 * ff)), vmem((slab, 3 * part)), vmem((down_rows, down_cols)), vmem((down_rows, down_cols), F32),
        vmem((out_rows, width)), vmem((m * vec_rows, LANES), F32), vmem((share, 3 * part * m), F32),
        vmem((down_rows // 2, width), F32),
    ]
    slots = 5 * 2 * half + 3 * 2 + 2 + 2 + 3 * (m - 1) + 1
    return pl.pallas_call(
        functools.partial(backward_kernel, dims),
        out_shape=[jax.ShapeDtypeStruct(*a) for a in outputs],
        in_specs=[pl.BlockSpec(memory_space=pl.ANY)] * len(args),
        out_specs=[pl.BlockSpec(memory_space=pl.ANY)] * len(outputs),
        scratch_shapes=scratch
        + [
            pltpu.SemaphoreType.DMA((slots,)),
            pltpu.SemaphoreType.DMA((slots,)),
            pltpu.SemaphoreType.DMA((len(args) + 12,)),
            pltpu.SemaphoreType.DMA((len(outputs),)),
        ],
        compiler_params=pltpu.CompilerParams(
            collective_id=1, has_side_effects=True, vmem_limit_bytes=VMEM_BYTES
        ),
        name="backward",
    )(*args)


def rotary_lines(length):
    half = ROT // 2
    lane = np.arange(LANES) % HEAD_DIM
    angles = np.arange(length)[:, None] * (10000.0 ** (-(lane % half) * 2.0 / ROT))[None, :]
    cosine, sine = np.cos(angles), np.sin(angles)
    lines = [
        np.where(lane < ROT, cosine, 1.0),
        np.where(lane < half, -sine, 0.0),
        np.where((lane >= half) & (lane < ROT), sine, 0.0),
    ]
    return jnp.asarray(np.concatenate(lines, axis=1), F32)


def columns_of(ff):
    runs = []
    for at, units, _ in blocks_of(ff):
        even = units // LANES * LANES
        runs.append((0, at, even))
        if even < units:
            runs += [(0, at + even, units - even), (1, at + even, units - even)]
        runs.append((1, at, even))
    return runs


def shards(tokens, cotangent, gain1, bias1, w_qkv, b_qkv, w_out, gain2, bias2, w_gate_up, w_down):
    n, m, s = lax.axis_size("dp"), lax.axis_size("seq"), lax.axis_index("seq")
    rows, width = tokens.shape
    slab = gain1.shape[0]
    inner, hidden = w_out.shape[0] * n, w_down.shape[0] * n
    part, ff = inner // m, hidden // m
    dims = (n, m, rows, width, slab, part, ff, b_qkv.shape[0] // LANES)
    runs = columns_of(ff)
    halves = [lax.dynamic_slice(w_gate_up, (0, i * hidden + s * ff), (slab, ff)) for i in range(2)]
    piece_gu = jnp.concatenate([halves[i][:, at : at + units] for i, at, units in runs], axis=1)
    vec = jnp.concatenate([gain1, bias1, gain2, bias2, b_qkv]).astype(F32).reshape(-1, LANES)
    vec = jnp.pad(vec, ((0, -vec.shape[0] % TILE), (0, 0)))
    rot = rotary_lines(rows * m)
    kept = run_forward(dims, (tokens, cotangent, w_qkv, piece_gu, w_out, w_down, vec, rot))
    block_out, input_grad, gu, g_qkv, g_down, g_out, line = run_backward(dims, tuple(kept) + (rot,))
    share = slab // m
    starts, at = {}, 0
    for i, first, units in runs:
        starts[i, first] = (at, units)
        at += units
    order = sorted(starts)
    g_gu = jnp.concatenate(
        [
            gu[t * share : (t + 1) * share, starts[key][0] : starts[key][0] + starts[key][1]]
            for i in range(2)
            for t in range(m)
            for key in order
            if key[0] == i
        ],
        axis=1,
    ).astype(F32)
    line = line.reshape(-1)
    vectors, at = [], 0
    for size in [slab] * 4 + [b_qkv.shape[0]]:
        vectors.append(lax.dynamic_slice(line, (at + s * (size // m),), (size // m,)))
        at += size
    return (
        block_out,
        input_grad,
        vectors[0],
        vectors[1],
        g_qkv,
        vectors[4],
        g_out.astype(F32),
        vectors[2],
        vectors[3],
        g_gu,
        g_down,
    )


def fits(mesh, shapes):
    n, m = mesh.shape["dp"], mesh.shape["seq"]
    (rows, width), slab = shapes[0], shapes[2][0]
    part, ff = shapes[6][0] * n // m, shapes[10][0] * n // m
    return (
        m == 4
        and n == 8
        and rows % LANES == 0
        and slab == 256
        and width % 512 == 0
        and shapes[5][0] % LANES == 0
        and part == 256
        and 512 < ff <= 768
        and ff % 64 == 0
        and (2 * ff // n) % TILE == 0
        and 2 * ff <= width <= 4 * ff
        and 2 * 768 <= width
    )


def solution(mesh):
    rows, cols, vec = P(("dp", "seq"), None), P("dp", None), P("dp")
    flat = P(("dp", "seq"))
    def step(*args):
        body = shards if fits(mesh, [a.shape for a in args]) else shards_plain
        return body(*args)

    return jax.shard_map(
        step,
        mesh=mesh,
        in_specs=(rows, rows, vec, vec, cols, vec, cols, vec, vec, cols, cols),
        out_specs=(rows, rows, flat, flat, rows, flat, rows, flat, flat, rows, rows),
        check_vma=False,
    )
```

```python
import functools

import jax
import jax.numpy as jnp
import numpy as np
from jax import lax
from jax.experimental import pallas as pl
from jax.experimental.pallas import tpu as pltpu
from jax.sharding import PartitionSpec as P

HEAD_DIM = 64
ROT = 16
EPS = 1e-05
F32 = jnp.float32
BF16 = jnp.bfloat16


def ring_order(n):
    return list(range(0, n, 2)) + list(range(n - 1, 0, -2))


def dot(a, b):
    return jnp.dot(a, b, preferred_element_type=F32)


def dot_rows(a, b):
    return lax.dot_general(a, b, (((0,), (0,)), ((), ())), preferred_element_type=F32)


def dot_cols(a, b):
    return lax.dot_general(a, b, (((1,), (1,)), ((), ())), preferred_element_type=F32)


class Ring:
    def __init__(self):
        n = lax.axis_size("dp")
        order = ring_order(n)
        place = [order.index(i) for i in range(n)]
        self.n, self.half = n, n // 2
        self.right = [(order[i], order[(i + 1) % n]) for i in range(n)]
        self.left = [(b, a) for a, b in self.right]
        self.order = jnp.array(order, jnp.int32)
        self.place = jnp.array(place, jnp.int32)[lax.axis_index("dp")]

    def owner(self, offset):
        return self.order[lax.rem(self.place + offset + self.n, self.n)]

    def go_right(self, value):
        return lax.ppermute(value, "dp", self.right)

    def go_left(self, value):
        return lax.ppermute(value, "dp", self.left)

    def gather(self, piece):
        rows = piece.shape[0]
        cut = rows // 2
        from_left = from_right = piece
        whole = jnp.zeros((self.n,) + piece.shape, piece.dtype)

        def put(whole, offset, chunk):
            return lax.dynamic_update_slice(
                whole, chunk[None], (self.owner(offset),) + (0,) * piece.ndim
            )

        whole = put(whole, 0, piece)
        for k in range(1, self.half):
            from_left = self.go_right(from_left)
            from_right = self.go_left(from_right)
            whole = put(put(whole, -k, from_left), k, from_right)
        upper = self.go_right(from_left[:cut])
        lower = self.go_left(from_right[cut:])
        return put(whole, self.half, jnp.concatenate([upper, lower]))

    def scatter(self, parts):
        rows = parts.shape[1]
        cut = rows // 2

        def mine(offset):
            start = (self.owner(offset),) + (0,) * (parts.ndim - 1)
            return lax.dynamic_slice(parts, start, (1,) + parts.shape[1:])[0]

        def add(a, b):
            return a.astype(F32) + b.astype(F32)

        far = mine(self.half)
        upper = self.go_right(far[:cut])
        lower = self.go_left(far[cut:])
        from_left, from_right = mine(self.half - 1), mine(1 - self.half)
        from_left = jnp.concatenate(
            [add(from_left[:cut], upper).astype(BF16), from_left[cut:]]
        )
        from_right = jnp.concatenate(
            [from_right[:cut], add(from_right[cut:], lower).astype(BF16)]
        )
        for k in range(self.half - 2, -1, -1):
            from_left = self.go_right(from_left)
            from_right = self.go_left(from_right)
            if k:
                from_left = add(from_left, mine(k)).astype(BF16)
                from_right = add(from_right, mine(-k)).astype(BF16)
        return add(mine(0), from_left) + from_right.astype(F32)


class Group:
    def __init__(self):
        self.m = lax.axis_size("seq")
        self.s = lax.axis_index("seq")
        self.bits = []
        bit = self.m // 2
        while bit:
            self.bits.append(bit)
            bit //= 2
        self.offsets = [0]
        for bit in self.bits:
            self.offsets += [o ^ bit for o in self.offsets]

    def swap(self, value, mask):
        return lax.ppermute(value, "seq", [(i, i ^ mask) for i in range(self.m)])

    def gather(self, value):
        for bit in self.bits:
            value = jnp.concatenate([value, self.swap(value, bit)])
        return value

    def scatter(self, value):
        for bit in reversed(self.bits):
            half = value.shape[0] // 2
            got = self.swap(value[half:].astype(BF16), bit)
            value = value[:half] + got.astype(F32)
        return value

    def exchange(self, blocks):
        got = []
        for mask in range(self.m):
            block = lax.dynamic_index_in_dim(blocks, self.s ^ mask, 0, keepdims=False)
            got.append(self.swap(block, mask) if mask else block)
        stacked = jnp.stack(got)
        return jnp.take(stacked, self.s ^ jnp.arange(self.m), axis=0)


def norm(value):
    center = value - jnp.mean(value, axis=-1, keepdims=True)
    rstd = lax.rsqrt(jnp.mean(center * center, axis=-1, keepdims=True) + EPS)
    return center * rstd, rstd


def norm_back(upstream, xhat, rstd, gain):
    e = upstream * gain
    inner = (
        e
        - jnp.mean(e, axis=-1, keepdims=True)
        - xhat * jnp.mean(e * xhat, axis=-1, keepdims=True)
    )
    return rstd * inner


def rotary_tables(positions):
    half = ROT // 2
    inverse = 10000.0 ** (-(jnp.arange(half, dtype=F32) * 2.0 / ROT))
    angles = positions.astype(F32)[:, None] * inverse[None, :]
    return jnp.cos(angles)[:, None, :], jnp.sin(angles)[:, None, :]


def rotate(tensor, cosine, sine):
    half = ROT // 2
    a, b = tensor[..., :half], tensor[..., half:ROT]
    return jnp.concatenate([a * cosine - b * sine, b * cosine + a * sine, tensor[..., ROT:]], axis=-1)


def shards_plain(tokens, cotangent, gain1, bias1, w_qkv, b_qkv, w_out, gain2, bias2, w_gate_up, w_down):
    ring, group = Ring(), Group()
    n, m, s = ring.n, group.m, group.s
    rows, width = tokens.shape
    slab = gain1.shape[0]
    inner = w_out.shape[0] * n
    hidden = w_down.shape[0] * n
    part, ff = inner // m, hidden // m
    heads = part // HEAD_DIM
    scale = HEAD_DIM ** (-0.5)

    both = jnp.stack([tokens, cotangent], axis=1)
    everything = group.gather(both)
    tokens_all, cot_all = everything[:, 0], everything[:, 1]

    qkv_piece = jnp.concatenate(
        [lax.dynamic_slice(w_qkv, (0, i * inner + s * part), (slab, part)) for i in range(3)], axis=1
    )
    small = jnp.concatenate([gain1, bias1, gain2, bias2, b_qkv])
    extra = -(-small.shape[0] // (3 * part))
    small = jnp.pad(small, (0, extra * 3 * part - small.shape[0])).reshape(extra, 3 * part)
    first = ring.gather(jnp.concatenate([qkv_piece, small]))
    wqkv = first[:, :slab].reshape(width, 3 * part)
    vectors = first[:, slab:].reshape(n, -1)

    def vector(at, size):
        return vectors[:, at : at + size].reshape(-1).astype(F32)

    g1, b1, g2, b2 = (vector(i * slab, slab) for i in range(4))
    bias_all = vector(4 * slab, b_qkv.shape[0]).reshape(3, m, part)
    bias_qkv = lax.dynamic_index_in_dim(bias_all, s, 1, keepdims=False).reshape(3 * part)

    turn = [(g, (g % n) * m + g // n) for g in range(n * m)]
    back = [(b, a) for a, b in turn]

    def quarter(weight):
        count = weight.shape[0] // m
        mine = lax.dynamic_slice(weight, (0, 0), weight.shape)
        return mine.reshape(m, count, weight.shape[1])[s]

    out_rows, down_rows = w_out.shape[0] // m, w_down.shape[0] // m
    moved = lax.ppermute(
        jnp.concatenate([quarter(w_out), quarter(w_down)]), ("dp", "seq"), turn
    )
    wout = ring.gather(moved[:out_rows]).reshape(part, width)
    gu_piece = jnp.concatenate(
        [lax.dynamic_slice(w_gate_up, (0, i * hidden + s * ff), (slab, ff)) for i in range(2)], axis=1
    )
    wgu = ring.gather(gu_piece).reshape(width, 2 * ff)
    wdown = ring.gather(moved[out_rows:]).reshape(ff, width)

    places = jnp.concatenate([(s ^ o) * rows + jnp.arange(rows, dtype=jnp.int32) for o in group.offsets])
    cosine, sine = rotary_tables(places)
    count = rows * m
    xhat1, rstd1 = norm(tokens_all.astype(F32))
    normed1 = (xhat1 * g1 + b1).astype(BF16)
    qkv = (dot(normed1, wqkv) + bias_qkv).reshape(count, 3, heads, HEAD_DIM)
    queries = rotate(qkv[:, 0], cosine, sine).astype(BF16)
    keys = rotate(qkv[:, 1], cosine, sine).astype(BF16)
    values = qkv[:, 2].astype(BF16)
    scores = jnp.einsum("qhd,khd->hqk", queries, keys, preferred_element_type=F32) * scale
    scores = jnp.where((places[None, :] <= places[:, None])[None], scores, -jnp.inf)
    top = jnp.max(scores, axis=-1, keepdims=True)
    lse = top + jnp.log(jnp.sum(jnp.exp(scores - top), axis=-1, keepdims=True))
    probs = jnp.exp(scores - lse)
    probs_r = probs.astype(BF16)
    context = jnp.einsum("hqk,khd->qhd", probs_r, values, preferred_element_type=F32).astype(BF16)
    context_flat = context.reshape(count, part)
    x_own = tokens.astype(F32)
    mid = x_own + group.scatter(dot(context_flat, wout))
    xhat2, rstd2 = norm(mid)
    normed2 = group.gather((xhat2 * g2 + b2).astype(BF16))
    gate_up = dot(normed2, wgu)
    gate, up = gate_up[:, :ff], gate_up[:, ff:]
    sigma = jax.nn.sigmoid(gate)
    silu = gate * sigma
    act = (silu * up).astype(BF16)
    d_act = dot_cols(cot_all, wdown)
    d_gate = d_act * up * (sigma * (1.0 + gate * (1.0 - sigma)))
    d_gate_up = jnp.concatenate([d_gate, d_act * silu], axis=1).astype(BF16)

    d_normed2 = group.scatter(dot_cols(d_gate_up, wgu))
    sum_down = ring.scatter(dot_rows(act, cot_all).astype(BF16).reshape(n, ff // n, width))
    sum_gu = ring.scatter(dot_rows(normed2, d_gate_up).astype(BF16).reshape(n, slab, 2 * ff))
    block_out = (mid + group.scatter(dot(act, wdown))).astype(BF16)
    d_mid = cotangent.astype(F32) + norm_back(d_normed2, xhat2, rstd2, g2)
    d_mid_r = group.gather(d_mid.astype(BF16))

    d_context = dot_cols(d_mid_r, wout).astype(BF16).reshape(count, heads, HEAD_DIM)
    sum_out = ring.scatter(dot_rows(context_flat, d_mid_r).astype(BF16).reshape(n, part // n, width))
    d_probs = jnp.einsum("qhd,khd->hqk", d_context, values, preferred_element_type=F32)
    delta = jnp.einsum("qhd,qhd->hq", d_context.astype(F32), context.astype(F32))[..., None]
    d_scores = (probs * (d_probs - delta) * scale).astype(BF16)
    d_queries = jnp.einsum("hqk,khd->qhd", d_scores, keys, preferred_element_type=F32)
    d_keys = jnp.einsum("hqk,qhd->khd", d_scores, queries, preferred_element_type=F32)
    d_values = jnp.einsum("hqk,qhd->khd", probs_r, d_context, preferred_element_type=F32)
    d_qkv = jnp.stack(
        [rotate(d_queries, cosine, -sine), rotate(d_keys, cosine, -sine), d_values], axis=1
    ).reshape(count, 3 * part)
    d_qkv_r = d_qkv.astype(BF16)
    d_normed1_part = dot_cols(d_qkv_r, wqkv)
    d_normed1 = group.scatter(d_normed1_part)
    own = (slice(0, rows),)
    input_grad = d_mid + norm_back(d_normed1, xhat1[own], rstd1[own], g1)

    bias_part = jnp.zeros((3, m, part), F32)
    bias_part = lax.dynamic_update_slice(bias_part, jnp.sum(d_qkv, axis=0).reshape(3, 1, part), (0, s, 0))
    vector_parts = [
        jnp.sum(d_normed1_part * xhat1, axis=0),
        jnp.sum(d_normed1_part, axis=0),
        jnp.sum(d_normed2 * xhat2, axis=0),
        jnp.sum(d_normed2, axis=0),
        bias_part.reshape(-1),
    ]
    line = jnp.concatenate([v.reshape(n, m, -1) for v in vector_parts], axis=-1)
    lines = -(-line.shape[-1] // (3 * part))
    line = jnp.pad(line, ((0, 0), (0, 0), (0, lines * 3 * part - line.shape[-1])))
    line = line.reshape(n, m, lines, 3 * part).astype(BF16)
    part_qkv = dot_rows(normed1, d_qkv_r).astype(BF16).reshape(n, m, slab // m, 3 * part)
    packed = jnp.concatenate([part_qkv, line], axis=2)
    packed_rows = packed.shape[2]
    sum_qkv = ring.scatter(packed.reshape(n, m * packed_rows, 3 * part))

    def owners(total):
        return group.exchange(total.astype(BF16).reshape((m, -1) + total.shape[1:])).astype(F32)

    last = owners(sum_qkv)
    g_qkv = last[:, : slab // m].reshape(m, slab // m, 3, part).transpose(1, 2, 0, 3)
    g_qkv = g_qkv.reshape(slab // m, 3 * inner)
    line = jnp.sum(last[:, slab // m :], axis=0).reshape(-1)
    sizes = [slab // m] * 4 + [b_qkv.shape[0] // m]
    vectors_out, at = [], 0
    for size in sizes:
        vectors_out.append(line[at : at + size])
        at += size
    g_gu = owners(sum_gu).reshape(m, slab // m, 2, ff).transpose(1, 2, 0, 3).reshape(slab // m, 2 * hidden)
    g_down = lax.ppermute(sum_down.astype(BF16), ("dp", "seq"), back).astype(F32)
    g_out = lax.ppermute(sum_out.astype(BF16), ("dp", "seq"), back).astype(F32)
    return (
        block_out,
        input_grad,
        vectors_out[0],
        vectors_out[1],
        g_qkv,
        vectors_out[4],
        g_out,
        vectors_out[2],
        vectors_out[3],
        g_gu,
        g_down,
    )


LOGICAL = pl.DeviceIdType.LOGICAL
MEAN, RSTD, SPOT, LSE = 0, 1, 2, 8
LANES = 128
TILE = 16
VMEM_BYTES = 67_043_328


def vmem(shape, dtype=BF16):
    return pltpu.VMEM(shape, dtype)


class Place:
    def __init__(self, n, m):
        self.n, self.m, self.half = n, m, n // 2
        self.d, self.s = lax.axis_index("dp"), lax.axis_index("seq")
        pair = lax.div(self.d, 2)
        odd = self.d - 2 * pair
        place = pair + odd * (n - 1 - 2 * pair)
        self.owners = []
        for offset in range(n):
            spot = lax.rem(place + offset, n)
            back = lax.div(spot, self.half)
            self.owners.append(2 * spot + back * (2 * n - 1 - 4 * spot))
        self.partners = []
        for mask in range(m):
            out, bit = self.s, 1
            while bit < m:
                if mask & bit:
                    out = out + bit - 2 * bit * lax.rem(lax.div(self.s, bit), 2)
                bit *= 2
            self.partners.append(out)
        self.rings = {1: self.owners[1] * m + self.s, -1: self.owners[n - 1] * m + self.s}
        self.seqs = [self.d * m + out for out in self.partners]
        inner_ = lax.rem(self.s, 2)
        side = lax.rem(lax.div(self.s, 2) + inner_, 2)
        self.shards = [2 * inner_ + side, n - 2 - 2 * inner_ + side]
        low = lax.div(self.d, m)
        self.source = (self.shards[0] + low * (self.shards[1] - self.shards[0])) * m + self.d - low * m
        across = lax.rem(lax.div(pair + 1, 2), 2)
        self.there = lax.div(self.d, m) * m + self.s
        self.target = self.there * m + 2 * lax.rem(odd + across, 2) + across
        here = self.d * m + self.s
        self.moves = (self.target - here) * (self.target - here) > 0

        offsets = [0]
        for bit in self.bits():
            offsets += [o ^ bit for o in offsets]
        self.homes = [self.partners[o] for o in offsets]

    def owner(self, offset):
        return self.owners[offset % self.n]

    def partner(self, mask):
        return self.partners[mask]

    def bits(self):
        out, bit = [], self.m // 2
        while bit:
            out.append(bit)
            bit //= 2
        return out


class Sender:
    def __init__(self, sends, recvs):
        self.sends, self.recvs = sends, recvs
        self.used = 0
        self.open = []

    def slot(self):
        self.used += 1
        return self.used - 1

    def copy(self, slot, src, dst, device):
        return pltpu.make_async_remote_copy(
            src_ref=src,
            dst_ref=dst,
            send_sem=self.sends.at[slot],
            recv_sem=self.recvs.at[slot],
            device_id=device,
            device_id_type=LOGICAL,
        )

    def start(self, slot, src, dst, device):
        copy = self.copy(slot, src, dst, device)
        copy.start()
        self.open.append(copy)
        return copy

    def finish(self):
        for copy in self.open:
            copy.wait_send()
        self.open = []


def greet(place, extra_seq=()):
    barrier = pltpu.get_barrier_semaphore()

    def hello(device):
        pl.semaphore_signal(barrier, inc=1, device_id=device, device_id_type=LOGICAL)

    near = [place.rings[1], place.rings[-1]] + [place.seqs[mask] for mask in tuple(place.bits()) + tuple(extra_seq)]
    for device in near:
        hello(device)

    @pl.when(place.moves)
    def _():
        hello(place.target)
        hello(place.source)
        pl.semaphore_wait(barrier, len(near) + 2)

    @pl.when(jnp.logical_not(place.moves))
    def _():
        pl.semaphore_wait(barrier, len(near))


class RowSlots:
    def __init__(self, rows, cols, lo=0):
        self.rows, self.cols, self.lo = rows, cols, lo

    def where(self, index, part=None):
        rows, start = self.rows, index * self.rows
        if part is not None:
            rows = rows // 2
            start = start + part * rows
        return pl.ds(pl.multiple_of(start, rows), rows), pl.ds(self.lo, self.cols)

    def landing(self, way, j, half):
        base = way * ((half - 1) * self.rows + self.rows // 2)
        at, rows = (base + (half - 1) * self.rows, self.rows // 2) if j == 1 else (base + (j - 2) * self.rows, self.rows)
        return pl.ds(at, rows), pl.ds(0, self.cols)

    def inbox(self, half):
        return 2 * ((half - 1) * self.rows + self.rows // 2), self.cols


class TileSlots:
    def __init__(self, rows, cols):
        self.rows, self.cols = rows, cols

    def where(self, index, part=None):
        row = lax.div(index, 2)
        cols, start = self.cols, (index - 2 * row) * self.cols
        if part is not None:
            cols = cols // 2
            start = start + part * cols
        return pl.ds(pl.multiple_of(row * self.rows, self.rows), self.rows), pl.ds(pl.multiple_of(start, cols), cols)

    def landing(self, way, j, half):
        at, cols = ((half - 1) * self.cols, self.cols // 2) if j == 1 else ((j - 2) * self.cols, self.cols)
        return pl.ds(way * self.rows, self.rows), pl.ds(at, cols)

    def inbox(self, half):
        return 2 * self.rows, (half - 1) * self.cols + self.cols // 2


class Gather:
    def __init__(self, place, sender, buf, slots):
        self.place, self.sender, self.buf, self.slots = place, sender, buf, slots
        self.sems = [[sender.slot() for _ in range(place.half)] for _ in range(2)]
        self.devices = (place.rings[1], place.rings[-1])

    def own(self):
        return self.buf.at[self.slots.where(self.place.d)]

    def send(self, k, way):
        index = self.place.owner(k if way else -k)
        ref = self.buf.at[self.slots.where(index, way if k == self.place.half - 1 else None)]
        self.sender.start(self.sems[way][k], ref, ref, self.devices[way])

    def begin(self):
        self.send(0, 0)
        self.send(0, 1)

    def pump(self, k):
        last = k == self.place.half
        for way in range(2):
            index = self.place.owner(k if way else -k)
            ref = self.buf.at[self.slots.where(index, way if last else None)]
            self.sender.copy(self.sems[way][k - 1], ref, ref, self.devices[way]).wait_recv()
            if not last:
                self.send(k, way)


class Reduce:
    def __init__(self, place, sender, buf, inbox, slots):
        self.place, self.sender, self.buf, self.inbox, self.slots = place, sender, buf, inbox, slots
        self.sems = [[sender.slot() for _ in range(place.half)] for _ in range(2)]
        self.devices = (place.rings[1], place.rings[-1])

    def target(self, way, j):
        offset = self.place.half - j
        return self.slots.where(self.place.owner(-offset if way else offset), way if j == 1 else None)

    def copy(self, way, j):
        offset = self.place.half - j + 1
        src = self.slots.where(self.place.owner(-offset if way else offset), way if j == 1 else None)
        return self.sems[way][j - 1], self.buf.at[src], self.inbox.at[self.slots.landing(way, j, self.place.half)]

    def send(self, j, way):
        self.sender.start(*self.copy(way, j), self.devices[way])

    def begin(self):
        self.send(1, 0)
        self.send(1, 1)

    def add(self, to, *froms):
        value = self.buf[to].astype(F32)
        for at in froms:
            value = value + self.inbox[at].astype(F32)
        self.buf[to] = value.astype(self.buf.dtype)

    def pump(self, j):
        half = self.place.half
        for way in range(2):
            self.sender.copy(*self.copy(way, j), self.devices[way]).wait_recv()
            if j < half:
                self.add(self.target(way, j), self.slots.landing(way, j, half))
                self.send(j + 1, way)
        if j == half:
            self.add(self.slots.where(self.place.d), *(self.slots.landing(way, j, half) for way in range(2)))

    def mine(self):
        return self.buf.at[self.slots.where(self.place.d)]


def shards_of(s, n):
    inner = s % 2
    side = (s // 2 + inner) % 2
    return [2 * inner + side, n - 2 - 2 * inner + side]


def blocks_of(ff):
    return [(at, min(256, ff - at), 2 * at) for at in range(0, ff, 256)]


def key_spots(place, pos_k, rows):
    lane = lax.broadcasted_iota(jnp.int32, (8, rows), 1)
    for i, home in enumerate(place.homes):
        pos_k[:, i * rows : (i + 1) * rows] = (home * rows + lane).astype(F32)


def load_rotary(place, h_rot, rot, rows, sems, first):
    copies = []
    for i, home in enumerate(place.homes):
        src = h_rot.at[pl.ds(pl.multiple_of(home * rows, rows), rows)]
        copies.append(pltpu.make_async_copy(src, rot.at[pl.ds(i * rows, rows)], sems.at[first + i]))
        copies[-1].start()
    return copies


def forward_kernel(
    dims,
    tok, cot, h_wqkv, piece_gu, h_wout, h_wdown, piece_vec, h_rot,
    o_wqkv, o_wout, o_wgu, o_wdown, o_rows, o_tok, o_cot, o_n1, o_qkv, o_stat, o_ctx, o_mid, o_n2, o_act, o_dgu,
    wqkv, wout, wgu, wdown, vec, tok_all, cot_all, n1, qkv, stat, ctx, mid, n2, act, dgu,
    rows_v, bias_v, rot, pos_k, own, send1, send2, recv1, recv2,
    sends, recvs, locals_, outs,
):
    n, m, rows, width, slab, part, ff, b_units = dims
    count = rows * m
    half = count // 2
    inner = part * m
    place = Place(n, m)
    sender = Sender(sends, recvs)
    d, s = place.d, place.s
    bits = place.bits()
    out_rows, vec_rows = part // n, piece_vec.shape[0]
    down_rows, down_cols = 2 * ff // n, width // 2
    blocks = blocks_of(ff)

    ring_a = Gather(place, sender, wqkv, RowSlots(slab, 3 * part))
    ring_v = Gather(place, sender, vec, RowSlots(vec_rows, LANES))
    ring_b = Gather(place, sender, wout, RowSlots(out_rows, width))
    ring_c = [Gather(place, sender, wgu, RowSlots(slab, 2 * units, lane)) for _, units, lane in blocks]
    ring_d = Gather(place, sender, wdown, TileSlots(down_rows, down_cols))

    def local(i, src, dst):
        copy = pltpu.make_async_copy(src, dst, locals_.at[i])
        copy.start()
        return copy

    own_rows = pl.ds(pl.multiple_of(d * slab, slab), slab)
    placed_qkv = [
        local(
            2 * i + u,
            h_wqkv.at[:, pl.ds(pl.multiple_of(i * inner + place.shards[u] * LANES, LANES), LANES)],
            wqkv.at[own_rows, pl.ds(i * part + u * LANES, LANES)],
        )
        for i in range(3)
        for u in range(2)
    ]
    placed_vec = local(6, piece_vec, ring_v.own())
    placed_tok = local(7, tok, tok_all.at[pl.ds(0, rows)])
    placed_gu = local(8, piece_gu, wgu.at[own_rows])
    placed_cot = local(9, cot, cot_all.at[pl.ds(0, rows)])
    placed_rot = load_rotary(place, h_rot, rot, rows, locals_, 12)
    greet(place)
    moves = place.moves

    class Spread:
        def __init__(self, buf):
            self.buf = buf
            self.sems = [sender.slot() for _ in bits]

        def copy(self, i):
            size = rows << i
            return self.sems[i], self.buf.at[pl.ds(0, size)], self.buf.at[pl.ds(size, size)], place.seqs[bits[i]]

        def send(self, i):
            sender.start(*self.copy(i))

        def wait(self, i):
            sender.copy(*self.copy(i)).wait_recv()

    toks, cots, n2s = Spread(tok_all), Spread(cot_all), Spread(n2)
    written = []

    def write(src, dst):
        copy = pltpu.make_async_copy(src, dst, outs.at[len(written)])
        copy.start()
        written.append(copy)

    for copy in placed_qkv:
        copy.wait()
    ring_a.begin()
    placed_vec.wait()
    ring_v.begin()
    placed_tok.wait()
    toks.send(0)

    src_out = h_wout.at[pl.ds(pl.multiple_of(s * out_rows, out_rows), out_rows)]
    up = lax.div(s, 2)
    src_down = h_wdown.at[
        pl.ds(pl.multiple_of(up * down_rows, down_rows), down_rows),
        pl.ds(pl.multiple_of((s - 2 * up) * down_cols, down_cols), down_cols),
    ]
    turns = [(src_out, ring_b, sender.slot(), 10), (src_down, ring_d, sender.slot(), 11)]

    def turn(ring, index):
        return ring.buf.at[ring.slots.where(index)]

    @pl.when(moves)
    def _():
        for src, ring, slot, _ in turns:
            sender.copy(slot, src, turn(ring, place.there), place.target).start()

    @pl.when(jnp.logical_not(moves))
    def _():
        for src, ring, _, i in turns:
            local(i, src, ring.own()).wait()

    placed_gu.wait()
    ring_c[0].begin()
    placed_cot.wait()
    cots.send(0)
    wdown[ff:, :] = jnp.zeros((wdown.shape[0] - ff, width), BF16)
    key_spots(place, pos_k, rows)
    lane = lax.broadcasted_iota(jnp.int32, (1, LANES), 1)
    line = lax.broadcasted_iota(jnp.int32, (rows, 1), 0)

    def stats(i):
        span = slice(i * rows, (i + 1) * rows)
        x = tok_all[span, :].astype(F32)
        mu = jnp.mean(x, axis=-1, keepdims=True)
        c = x - mu
        r = lax.rsqrt(jnp.mean(c * c, axis=-1, keepdims=True) + EPS)
        spot = (place.homes[i] * rows + line).astype(F32)
        stat[span, :] = jnp.where(lane == MEAN, mu, jnp.where(lane == RSTD, r, spot))

    stats(0)
    ring_v.pump(1)
    ring_a.pump(1)

    @pl.when(moves)
    def _():
        for src, ring, slot, _ in turns:
            sender.copy(slot, src, ring.own(), place.source).wait_recv()

    ring_b.begin()
    toks.wait(0)
    toks.send(1)
    stats(1)
    ring_v.pump(2)
    ring_a.pump(2)
    ring_d.begin()
    ring_b.pump(1)
    toks.wait(1)
    write(tok_all, o_tok)
    stats(2)
    stats(3)
    cots.wait(0)
    cots.send(1)
    ring_v.pump(3)
    ring_a.pump(3)
    ring_c[1].begin()
    ring_b.pump(2)
    ring_c[0].pump(1)
    ring_v.pump(4)
    units = slab // LANES
    for c in range(n):
        for r in range(4):
            for u in range(units):
                at = c * slab + u * LANES
                row = c * vec_rows + r * units + u
                rows_v[r : r + 1, at : at + LANES] = vec[row : row + 1, :]
    for i in range(3):
        for u in range(part // LANES):
            unit = i * (inner // LANES) + place.shards[u]
            row = lax.div(unit, b_units) * vec_rows + 4 * units + lax.rem(unit, b_units)
            at = i * part + u * LANES
            bias_v[0:1, at : at + LANES] = vec[pl.ds(row, 1), :]
    write(rows_v, o_rows)

    def normalize(j, carry):
        size = 64
        span = pl.ds(pl.multiple_of(j * size, size), size)
        x = tok_all[span, :].astype(F32)
        xhat = (x - stat[span, MEAN : MEAN + 1]) * stat[span, RSTD : RSTD + 1]
        n1[span, :] = (xhat * rows_v[0:1, :] + rows_v[1:2, :]).astype(BF16)
        return carry

    lax.fori_loop(0, count // 64, normalize, 0)
    write(n1, o_n1)
    ring_d.pump(1)
    ring_c[2].begin()
    cots.wait(1)
    write(cot_all, o_cot)
    ring_a.pump(4)
    write(wqkv, o_wqkv)
    for copy in placed_rot:
        copy.wait()

    def project(j, carry):
        size = 256
        span = pl.ds(pl.multiple_of(j * size, size), size)
        for i in range(3):
            cols = slice(i * part, (i + 1) * part)
            y = dot(n1[span, :], wqkv[:, cols]) + bias_v[0:1, cols]
            if i < 2:
                pieces = []
                for u in range(part // LANES):
                    z = y[:, u * LANES : (u + 1) * LANES]
                    pieces.append(
                        z * rot[span, :LANES]
                        + pltpu.roll(z, LANES - ROT // 2, 1) * rot[span, LANES : 2 * LANES]
                        + pltpu.roll(z, ROT // 2, 1) * rot[span, 2 * LANES :]
                    )
                y = jnp.concatenate(pieces, axis=1)
            qkv[span, cols] = y.astype(BF16)
        return carry

    lax.fori_loop(0, count // 256, project, 0)
    write(qkv, o_qkv)
    ring_b.pump(3)
    ring_c[1].pump(1)
    ring_c[0].pump(2)
    scale = HEAD_DIM ** (-0.5)
    per = LANES // HEAD_DIM

    def attend(i, carry):
        pair, block = lax.div(i, m), lax.rem(i, m)
        span = pl.ds(pl.multiple_of(block * rows, rows), rows)
        at = pl.multiple_of(pair * LANES, LANES)
        q = qkv[span, pl.ds(at, LANES)]
        k = qkv[:, pl.ds(pl.multiple_of(part + at, LANES), LANES)]
        v = qkv[:, pl.ds(pl.multiple_of(2 * part + at, LANES), LANES)]
        allowed = pos_k[0:1, :] <= stat[span, SPOT : SPOT + 1]
        total = jnp.zeros((rows, LANES), F32)
        for h in range(per):
            mine = (lane // HEAD_DIM == h).astype(BF16)
            scores = dot_cols(q * mine, k) * scale
            scores = jnp.where(allowed, scores, -jnp.inf)
            top = jnp.max(scores, axis=-1, keepdims=True)
            found = top + jnp.log(jnp.sum(jnp.exp(scores - top), axis=-1, keepdims=True))
            probs = jnp.exp(scores - found).astype(BF16)
            total = total + dot(probs, v * mine)
            stat[span, :] = jnp.where(lane == LSE + pair * per + h, found, stat[span, :])
        ctx[span, pl.ds(at, LANES)] = total.astype(BF16)
        return carry

    lax.fori_loop(0, (part // LANES) * m, attend, 0)
    write(stat, o_stat)
    write(ctx, o_ctx)
    ring_d.pump(2)
    ring_c[2].pump(1)
    ring_b.pump(4)
    write(wout, o_wout)

    step = 512
    scatter = [sender.slot(), sender.slot()]

    def far_part(j, carry):
        cols = pl.ds(pl.multiple_of(j * step, step), step)
        send1[:, cols] = dot(ctx[half:, :], wout[:, cols]).astype(BF16)
        return carry

    lax.fori_loop(0, width // step, far_part, 0)
    first = sender.start(scatter[0], send1, recv1, place.seqs[bits[1]])

    def near_part(j, carry):
        cols = pl.ds(pl.multiple_of(j * step, step), step)
        own[:, cols] = dot(ctx[:half, :], wout[:, cols])
        return carry

    lax.fori_loop(0, width // step, near_part, 0)
    ring_c[1].pump(2)
    first.wait_recv()
    send2[...] = (own[rows:, :] + recv1[rows:, :].astype(F32)).astype(BF16)
    second = sender.start(scatter[1], send2, recv2, place.seqs[bits[0]])
    ring_c[0].pump(3)
    second.wait_recv()
    value = tok_all[:rows, :].astype(F32) + own[:rows, :] + recv1[:rows, :].astype(F32) + recv2[...].astype(F32)
    mid[...] = value
    c = value - jnp.mean(value, axis=-1, keepdims=True)
    r = lax.rsqrt(jnp.mean(c * c, axis=-1, keepdims=True) + EPS)
    n2[:rows, :] = (c * r * rows_v[2:3, :] + rows_v[3:4, :]).astype(BF16)
    n2s.send(0)
    write(mid, o_mid)
    ring_d.pump(3)
    ring_c[2].pump(2)
    ring_c[1].pump(3)
    n2s.wait(0)
    n2s.send(1)
    ring_c[0].pump(4)
    ring_d.pump(4)
    write(wdown, o_wdown)
    n2s.wait(1)
    write(n2, o_n2)
    ring_c[2].pump(3)

    def expand(first_unit, units, base):
        even = units // LANES * LANES
        y = dot(n2[...], wgu[:, base : base + 2 * units])
        d_act = dot_cols(cot_all[...], wdown[first_unit : first_unit + 256, :])
        if even == units:
            gate, up = y[:, :units], y[:, units:]
        else:
            gate = y[:, : even + LANES]
            up = jnp.concatenate([y[:, even + LANES :], pltpu.roll(gate[:, even:], LANES // 2, 1)], axis=1)
        sigma = jax.nn.sigmoid(gate)
        silu = gate * sigma
        value = silu * up
        d_gate = d_act * up * (sigma * (1.0 + gate * (1.0 - sigma)))
        d_up = d_act * silu
        if even == units:
            dgu[:, base : base + units] = d_gate.astype(BF16)
            dgu[:, base + units : base + 2 * units] = d_up.astype(BF16)
        else:
            value = jnp.where(lax.broadcasted_iota(jnp.int32, (1, 256), 1) < units, value, 0.0)
            mixed = jnp.where(lane < LANES // 2, d_gate[:, even:], pltpu.roll(d_up[:, even:], LANES // 2, 1))
            dgu[:, base : base + even] = d_gate[:, :even].astype(BF16)
            dgu[:, base + even : base + even + LANES] = mixed.astype(BF16)
            dgu[:, base + even + LANES : base + 2 * units] = d_up[:, :even].astype(BF16)
        act[:, first_unit : first_unit + 256] = value.astype(BF16)

    expand(*blocks[0])
    ring_c[1].pump(4)
    expand(*blocks[1])
    ring_c[2].pump(4)
    write(wgu, o_wgu)
    expand(*blocks[2])
    write(act, o_act)
    write(dgu, o_dgu)
    for copy in written:
        copy.wait()
    sender.finish()

    @pl.when(moves)
    def _():
        for src, ring, slot, _ in turns:
            sender.copy(slot, src, turn(ring, place.there), place.target).wait_send()


def run_forward(dims, args):
    n, m, rows, width, slab, part, ff, b_units = dims
    count = rows * m
    ffp = -(-ff // 256) * 256
    vec_rows = args[6].shape[0]
    arrays = [
        ((width, 3 * part), BF16), ((part, width), BF16), ((width, 2 * ff), BF16), ((ffp, width), BF16),
        ((8, width), F32), ((count, width), BF16), ((count, width), BF16), ((count, width), BF16),
        ((count, 3 * part), BF16), ((count, LANES), F32), ((count, part), BF16), ((rows, width), F32),
        ((count, width), BF16), ((count, ffp), BF16), ((count, 2 * ff), BF16),
    ]
    scratch = [vmem(*a) for a in arrays]
    rows_v, scratch[4] = scratch[4], vmem((n * vec_rows, LANES), F32)
    slots = (4 + len(blocks_of(ff))) * 2 * (n // 2) + 3 * 2 + 2 + 2
    return pl.pallas_call(
        functools.partial(forward_kernel, dims),
        out_shape=[jax.ShapeDtypeStruct(*a) for a in arrays],
        in_specs=[pl.BlockSpec(memory_space=pl.ANY)] * len(args),
        out_specs=[pl.BlockSpec(memory_space=pl.ANY)] * len(arrays),
        scratch_shapes=scratch
        + [
            rows_v,
            vmem((8, 3 * part), F32),
            vmem((count, 3 * LANES), F32),
            vmem((8, count), F32),
            vmem((count // 2, width), F32),
            vmem((count // 2, width)),
            vmem((rows, width)),
            vmem((count // 2, width)),
            vmem((rows, width)),
            pltpu.SemaphoreType.DMA((slots,)),
            pltpu.SemaphoreType.DMA((slots,)),
            pltpu.SemaphoreType.DMA((12 + m,)),
            pltpu.SemaphoreType.DMA((len(arrays),)),
        ],
        compiler_params=pltpu.CompilerParams(
            collective_id=0, has_side_effects=True, vmem_limit_bytes=VMEM_BYTES
        ),
        name="forward",
    )(*args)


def flip(value):
    size = value.shape[1]
    here = lax.broadcasted_iota(jnp.int32, (size, size), 0) == lax.broadcasted_iota(jnp.int32, (size, size), 1)
    return dot_cols(here.astype(F32).astype(BF16), value).astype(BF16)


def backward_kernel(
    dims,
    h_wqkv, h_wout, h_wgu, h_wdown, h_rows, h_tok, h_cot, h_n1, h_qkv, h_stat, h_ctx, h_mid, h_n2, h_act, h_dgu,
    h_rot,
    o_block, o_input, o_gu, o_qkv, o_down, o_out, o_vec,
    wout, wgu, wqkv, rows_v, wide_a, wide_b, qkv, stat, ctx, mid, act, dgu, rot, pos_k,
    sum_a, sum_b, sum_c, sum_d, sum_v, in_a, in_b, in_c, in_d, in_v,
    own, send1, send2, recv1, recv2, dm_all, d_mid, cot, dctx, dqkv, dk, dv, sums_v, bias_v,
    x_gu, x_qkv, x_down, x_half, x_out, x_vec, y_qkv, y_down,
    sends, recvs, loads, outs,
):
    n, m, rows, width, slab, part, ff, b_units = dims
    ffp = act.shape[1]
    inner = part * m
    count = rows * m
    half = count // 2
    place = Place(n, m)
    sender = Sender(sends, recvs)
    waiting = {}

    def load(name, src, dst):
        copy = pltpu.make_async_copy(src, dst, loads.at[len(waiting)])
        copy.start()
        waiting[name] = copy

    load("act", h_act, act)
    load("cot", h_cot, wide_a)
    load("n2", h_n2, wide_b)
    load("dgu", h_dgu, dgu)
    load("wgu", h_wgu, wgu)
    load("own", h_cot.at[pl.ds(0, dims[2])], cot)
    load("mid", h_mid, mid)
    load("rows", h_rows, rows_v)
    load("wqkv", h_wqkv, wqkv)
    load("wout", h_wout, wout)
    load("ctx", h_ctx, ctx)
    load("qkv", h_qkv, qkv)
    load("stat", h_stat, stat)
    spare = loads.shape[0] - 2
    rotary = load_rotary(place, h_rot, rot, rows, loads, spare - m)
    bits = place.bits()
    others = [mask for mask in range(1, m) if mask not in bits]
    moves = place.moves
    greet(place, others)
    d, s = place.d, place.s
    out_rows, vec_rows = part // n, sum_v.shape[0] // n
    down_rows, down_cols = 2 * ff // n, width // 2
    ring_a = Reduce(place, sender, sum_a, in_a, RowSlots(slab, 3 * part))
    ring_b = Reduce(place, sender, sum_b, in_b, RowSlots(out_rows, width))
    ring_c = Reduce(place, sender, sum_c, in_c, RowSlots(slab, 2 * ff))
    ring_d = Reduce(place, sender, sum_d, in_d, TileSlots(down_rows, down_cols))
    ring_v = Reduce(place, sender, sum_v, in_v, RowSlots(vec_rows, LANES))
    key_spots(place, pos_k, rows)
    block = 256

    def outer(dst, left, right, size):
        def step(j, carry):
            cols = pl.ds(pl.multiple_of(j * block, block), block)
            dst[cols, :] = dot(flip(left[:, cols]), right[...]).astype(BF16)
            return carry

        lax.fori_loop(0, size // block, step, 0)

    class Halving:
        def __init__(self, at):
            self.slots = [sender.slot(), sender.slot()]
            self.at = at
            self.open = []

        def first(self, far):
            far()
            self.open.append(sender.start(self.slots[0], send1, recv1.at[pl.ds(self.at * half, half)], place.seqs[bits[1]]))

        def second(self):
            self.open[0].wait_recv()
            send2[...] = (own[rows:, :] + recv1[self.at * half + rows : (self.at + 1) * half, :].astype(F32)).astype(BF16)
            self.open.append(sender.start(self.slots[1], send2, recv2.at[pl.ds(self.at * rows, rows)], place.seqs[bits[0]]))

        def total(self):
            self.open[1].wait_recv()
            return own[:rows, :] + recv1[self.at * half : self.at * half + rows, :].astype(F32) + recv2[
                self.at * rows : (self.at + 1) * rows, :
            ].astype(F32)

        def sent(self):
            for copy in self.open:
                copy.wait_send()
            sender.open = [c for c in sender.open if all(c is not o for o in self.open)]

    waiting["act"].wait()
    waiting["cot"].wait()
    outer(sum_d, act, wide_a, ffp)
    ring_d.begin()
    waiting["n2"].wait()
    waiting["dgu"].wait()

    def slab_of(index):
        cols = pl.ds(pl.multiple_of(index * slab, slab), slab)
        sum_c[cols, :] = dot(flip(wide_b[:, cols]), dgu[...]).astype(BF16)

    slab_of(place.owner(place.half))
    ring_c.begin()
    waiting["wgu"].wait()
    normed2 = Halving(0)

    def back_step(left, lo, hi, weight, to):
        def step(j, carry):
            cols = pl.ds(pl.multiple_of(j * block, block), block)
            to(cols, dot_cols(left[lo:hi, :], weight[cols, :]))
            return carry

        lax.fori_loop(0, width // block, step, 0)

    def to_send(cols, value):
        send1[:, cols] = value.astype(BF16)

    def to_own(cols, value):
        own[:, cols] = value

    normed2.first(lambda: back_step(dgu, half, count, wgu, to_send))
    back_step(dgu, 0, half, wgu, to_own)
    lanes = 2 * ff
    load("down_lo", h_wdown.at[:, pl.ds(0, lanes)], wgu.at[pl.ds(0, ffp)])
    load("down_hi", h_wdown.at[:, pl.ds(lanes, width - lanes)], wgu.at[pl.ds(ffp, ffp), pl.ds(0, width - lanes)])
    normed2.second()
    ring_d.pump(1)

    def other_slabs(i, carry):
        slab_of(lax.rem(place.owner(place.half) + i, n))
        return carry

    lax.fori_loop(1, n, other_slabs, 0)
    load("n1", h_n1, wide_b)
    load("tok", h_tok, wide_a)
    ring_c.pump(1)
    ring_d.pump(2)

    waiting["mid"].wait()
    waiting["rows"].wait()
    waiting["own"].wait()

    def deviation(value):
        c = value - jnp.mean(value, axis=-1, keepdims=True)
        r = lax.rsqrt(jnp.mean(c * c, axis=-1, keepdims=True) + EPS)
        return c * r, r

    xhat, r = deviation(mid[...])
    up = normed2.total()
    sums_v[2:3, :] = jnp.sum(up * xhat, axis=0, keepdims=True)
    sums_v[3:4, :] = jnp.sum(up, axis=0, keepdims=True)
    d_mid[...] = cot[...].astype(F32) + norm_back(up, xhat, r, rows_v[2:3, :])
    dm_all[:rows, :] = d_mid[...].astype(BF16)
    spread = [sender.slot() for _ in bits]

    def spread_copy(i):
        size = rows << i
        return (spread[i], dm_all.at[pl.ds(0, size)], dm_all.at[pl.ds(size, size)])

    def spread_send(i):
        sender.start(*spread_copy(i), place.seqs[bits[i]])

    def spread_wait(i):
        sender.copy(*spread_copy(i), place.seqs[bits[i]]).wait_recv()

    spread_send(0)
    normed2.sent()

    waiting["down_lo"].wait()
    waiting["down_hi"].wait()

    def down_step(lo, hi, to):
        def low(j, carry):
            cols = pl.ds(pl.multiple_of(j * LANES, LANES), LANES)
            to(cols, dot(act[lo:hi, :], wgu[:ffp, cols]))
            return carry

        def high(j, carry):
            cols = pl.ds(pl.multiple_of(j * LANES, LANES), LANES)
            to(pl.ds(pl.multiple_of(lanes + j * LANES, LANES), LANES), dot(act[lo:hi, :], wgu[ffp : 2 * ffp, cols]))
            return carry

        lax.fori_loop(0, lanes // LANES, low, 0)
        lax.fori_loop(0, (width - lanes) // LANES, high, 0)

    output = Halving(1)

    output.first(lambda: down_step(half, count, to_send))
    down_step(0, half, to_own)
    spread_wait(0)
    spread_send(1)
    output.second()
    ring_c.pump(2)
    spread_wait(1)

    waiting["wout"].wait()
    waiting["ctx"].wait()
    dctx[...] = dot_cols(dm_all[...], wout[...]).astype(BF16)
    outer(sum_b, ctx, dm_all, part)
    ring_b.begin()
    cot[...] = (mid[...] + output.total()).astype(BF16)
    output.sent()
    ring_d.pump(3)

    for name in ("qkv", "stat"):
        waiting[name].wait()
    for copy in rotary:
        copy.wait()
    scale = HEAD_DIM ** (-0.5)
    per = LANES // HEAD_DIM
    lane = lax.broadcasted_iota(jnp.int32, (1, LANES), 1) // HEAD_DIM

    def turned(z, span):
        return (
            z * rot[span, :LANES]
            - pltpu.roll(z, LANES - ROT // 2, 1) * rot[span, LANES : 2 * LANES]
            - pltpu.roll(z, ROT // 2, 1) * rot[span, 2 * LANES :]
        )

    bias_v[...] = jnp.zeros_like(bias_v)
    for pair in range(part // LANES):
        at = pair * LANES
        dk[...] = jnp.zeros_like(dk)
        dv[...] = jnp.zeros_like(dv)

        def attend(i, carry, pair=pair, at=at):
            span = pl.ds(pl.multiple_of(i * rows, rows), rows)
            q = qkv[span, at : at + LANES]
            k = qkv[:, part + at : part + at + LANES]
            v = qkv[:, 2 * part + at : 2 * part + at + LANES]
            dc = dctx[span, at : at + LANES]
            both = dc.astype(F32) * ctx[span, at : at + LANES].astype(F32)
            allowed = pos_k[0:1, :] <= stat[span, SPOT : SPOT + 1]
            dq = jnp.zeros((rows, LANES), F32)
            for h in range(per):
                pick = lane == h
                mine = pick.astype(BF16)
                qm, dcm = q * mine, dc * mine
                scores = dot_cols(qm, k) * scale
                at_lse = LSE + pair * per + h
                probs = jnp.exp(jnp.where(allowed, scores, -jnp.inf) - stat[span, at_lse : at_lse + 1])
                delta = jnp.sum(jnp.where(pick, both, 0.0), axis=-1, keepdims=True)
                ds = (probs * (dot_cols(dcm, v) - delta) * scale).astype(BF16)
                dq = dq + jnp.dot(ds, k * mine, preferred_element_type=F32)
                dk[...] += dot(flip(ds), qm)
                dv[...] += dot(flip(probs.astype(BF16)), dcm)
            dq = turned(dq, span)
            bias_v[0:1, at : at + LANES] += jnp.sum(dq, axis=0, keepdims=True)
            dqkv[span, at : at + LANES] = dq.astype(BF16)
            return carry

        lax.fori_loop(0, m, attend, 0)

        def settle(i, carry, at=at):
            span = pl.ds(pl.multiple_of(i * rows, rows), rows)
            key, value = turned(dk[span, :], span), dv[span, :]
            bias_v[0:1, part + at : part + at + LANES] += jnp.sum(key, axis=0, keepdims=True)
            bias_v[0:1, 2 * part + at : 2 * part + at + LANES] += jnp.sum(value, axis=0, keepdims=True)
            dqkv[span, part + at : part + at + LANES] = key.astype(BF16)
            dqkv[span, 2 * part + at : 2 * part + at + LANES] = value.astype(BF16)
            return carry

        lax.fori_loop(0, m, settle, 0)
        if pair == 0:
            ring_b.pump(1)

    waiting["n1"].wait()
    outer(sum_a, wide_b, dqkv, width)
    ring_a.begin()
    ring_c.pump(3)
    ring_b.pump(2)
    waiting["wqkv"].wait()
    waiting["tok"].wait()
    normed1 = Halving(2)

    def gains(cols, value, lo, hi):
        xh = (wide_a[lo:hi, cols].astype(F32) - stat[lo:hi, MEAN : MEAN + 1]) * stat[lo:hi, RSTD : RSTD + 1]
        return jnp.sum(value * xh, axis=0, keepdims=True), jnp.sum(value, axis=0, keepdims=True)

    def far_last(cols, value):
        send1[:, cols] = value.astype(BF16)
        sums_v[0:1, cols], sums_v[1:2, cols] = gains(cols, value, half, count)

    def near_last(cols, value):
        own[:, cols] = value
        gain, total = gains(cols, value, 0, half)
        sums_v[0:1, cols] += gain
        sums_v[1:2, cols] += total

    normed1.first(lambda: back_step(dqkv, half, count, wqkv, far_last))
    back_step(dqkv, 0, half, wqkv, near_last)

    sum_v[...] = jnp.zeros_like(sum_v)
    units = slab // LANES

    def lay(c, carry):
        for i in range(4):
            for u in range(units):
                at = pl.multiple_of(c * slab + u * LANES, LANES)
                sum_v[pl.ds(c * vec_rows + i * units + u, 1), :] = sums_v[i : i + 1, pl.ds(at, LANES)]
        return carry

    lax.fori_loop(0, n, lay, 0)
    for i in range(3):
        for u in range(part // LANES):
            unit = i * (inner // LANES) + place.shards[u]
            row = lax.div(unit, b_units) * vec_rows + 4 * units + lax.rem(unit, b_units)
            at = i * part + u * LANES
            sum_v[pl.ds(row, 1), :] = bias_v[0:1, at : at + LANES]
    ring_v.begin()
    normed1.second()
    ring_d.pump(4)
    ring_b.pump(3)
    ring_a.pump(1)
    ring_v.pump(1)
    ring_a.pump(2)
    ring_v.pump(2)
    up = normed1.total()
    rstd = stat[:rows, RSTD : RSTD + 1]
    xhat = (wide_a[:rows, :].astype(F32) - stat[:rows, MEAN : MEAN + 1]) * rstd
    own[:rows, :] = d_mid[...] + norm_back(up, xhat, rstd, rows_v[0:1, :])
    ring_b.pump(4)
    ring_v.pump(3)

    written = []

    def store(src, dst):
        copy = pltpu.make_async_copy(src, dst, outs.at[len(written)])
        copy.start()
        written.append(copy)

    store(cot, o_block)
    store(own.at[pl.ds(0, rows)], o_input)
    turns = [(ring_d, x_down, sender.slot()), (ring_b, x_out, sender.slot())]

    @pl.when(moves)
    def _():
        for ring, landing, slot in turns:
            sender.copy(slot, ring.mine(), landing, place.source).start()

    @pl.when(jnp.logical_not(moves))
    def _():
        for i, (ring, landing, _) in enumerate(turns):
            copy = pltpu.make_async_copy(ring.mine(), landing, loads.at[spare + i])
            copy.start()
            copy.wait()

    def deal(buf, size, landing, whole=False):
        share = size if whole else size // m
        got = []
        to = pl.ds(pl.multiple_of(s * share, share), share)
        for mask in range(1, m):
            start = d * size + (0 if whole else place.partner(mask) * share)
            src = buf.at[pl.ds(pl.multiple_of(start, share), share)]
            got.append(sender.start(sender.slot(), src, landing.at[to], place.seqs[mask]))
        start = d * size + (0 if whole else s * share)
        landing[to, :] = buf[pl.ds(pl.multiple_of(start, share), share), :]
        return got

    ring_c.pump(4)
    got_gu = deal(sum_c, slab, x_gu)
    ring_a.pump(3)

    @pl.when(moves)
    def _():
        for ring, landing, slot in turns:
            sender.copy(slot, ring.mine(), landing, place.target).wait_recv()

    x_half[...] = x_down[...].astype(F32)
    some = down_rows // 2
    column = lax.rem(s, 2)
    across = pl.ds(pl.multiple_of(column * down_cols, down_cols), down_cols)
    swap = sender.start(
        sender.slot(),
        x_half.at[pl.ds(pl.multiple_of((1 - column) * some, some), some)],
        y_down.at[:, across],
        place.seqs[1],
    )
    y_down[:, across] = x_half[pl.ds(pl.multiple_of(column * some, some), some), :]
    store(x_out, o_out)
    ring_v.pump(4)
    got_vec = deal(sum_v, vec_rows, x_vec, whole=True)
    ring_a.pump(4)
    got_qkv = deal(sum_a, slab, x_qkv)
    for copy in got_gu:
        copy.wait_recv()
    store(x_gu, o_gu)
    swap.wait_recv()
    store(y_down, o_down)
    for copy in got_vec:
        copy.wait_recv()
    total = x_vec[:vec_rows, :]
    for t in range(1, m):
        total = total + x_vec[t * vec_rows : (t + 1) * vec_rows, :]
    x_vec[:vec_rows, :] = total
    store(x_vec.at[pl.ds(0, vec_rows)], o_vec)
    for copy in got_qkv:
        copy.wait_recv()
    share = slab // m
    for t in range(m):
        for i in range(3):
            for u, held in enumerate(shards_of(t, n)):
                at, come = i * inner + held * LANES, i * part + u * LANES
                y_qkv[:, at : at + LANES] = x_qkv[t * share : (t + 1) * share, come : come + LANES].astype(F32)
    store(y_qkv, o_qkv)
    for copy in written:
        copy.wait()
    sender.finish()

    @pl.when(moves)
    def _():
        for ring, landing, slot in turns:
            sender.copy(slot, ring.mine(), landing, place.source).wait_send()


def run_backward(dims, args):
    n, m, rows, width, slab, part, ff, b_units = dims
    count = rows * m
    ffp = -(-ff // 256) * 256
    vec_rows = -(-(4 * (slab // LANES) + b_units) // TILE) * TILE
    half = n // 2
    out_rows = part // n
    down_rows, down_cols = 2 * ff // n, width // 2
    share = slab // m

    def inbox(slots, dtype=BF16):
        return vmem(slots.inbox(half), dtype)

    outputs = [
        ((rows, width), BF16), ((rows, width), F32), ((slab, 2 * ff), BF16), ((share, 3 * part * m), F32),
        ((down_rows // 2, width), F32), ((out_rows, width), BF16), ((vec_rows, LANES), F32),
    ]
    scratch = [
        vmem((part, width)), vmem((width, 2 * ff)), vmem((width, 3 * part)), vmem((8, width), F32),
        vmem((count, width)), vmem((count, width)), vmem((count, 3 * part)), vmem((count, LANES), F32),
        vmem((count, part)), vmem((rows, width), F32), vmem((count, ffp)), vmem((count, 2 * ff)),
        vmem((count, 3 * LANES), F32), vmem((8, count), F32),
        vmem((n * slab, 3 * part)), vmem((part, width)), vmem((n * slab, 2 * ff)), vmem((ffp, width)),
        vmem((n * vec_rows, LANES), F32),
        inbox(RowSlots(slab, 3 * part)), inbox(RowSlots(out_rows, width)), inbox(RowSlots(slab, 2 * ff)),
        inbox(TileSlots(down_rows, down_cols)), inbox(RowSlots(vec_rows, LANES), F32),
        vmem((count // 2, width), F32), vmem((count // 2, width)), vmem((rows, width)),
        vmem((3 * count // 2, width)), vmem((3 * rows, width)),
        vmem((count, width)), vmem((rows, width), F32), vmem((rows, width)), vmem((count, part)), vmem((count, 3 * part)),
        vmem((count, LANES), F32), vmem((count, LANES), F32), vmem((8, width), F32), vmem((8, 3 * part), F32),
        vmem((slab, 2 * ff)), vmem((slab, 3 * part)), vmem((down_rows, down_cols)), vmem((down_rows, down_cols), F32),
        vmem((out_rows, width)), vmem((m * vec_rows, LANES), F32), vmem((share, 3 * part * m), F32),
        vmem((down_rows // 2, width), F32),
    ]
    slots = 5 * 2 * half + 3 * 2 + 2 + 2 + 3 * (m - 1) + 1
    return pl.pallas_call(
        functools.partial(backward_kernel, dims),
        out_shape=[jax.ShapeDtypeStruct(*a) for a in outputs],
        in_specs=[pl.BlockSpec(memory_space=pl.ANY)] * len(args),
        out_specs=[pl.BlockSpec(memory_space=pl.ANY)] * len(outputs),
        scratch_shapes=scratch
        + [
            pltpu.SemaphoreType.DMA((slots,)),
            pltpu.SemaphoreType.DMA((slots,)),
            pltpu.SemaphoreType.DMA((len(args) + 12,)),
            pltpu.SemaphoreType.DMA((len(outputs),)),
        ],
        compiler_params=pltpu.CompilerParams(
            collective_id=1, has_side_effects=True, vmem_limit_bytes=VMEM_BYTES
        ),
        name="backward",
    )(*args)


def rotary_lines(length):
    half = ROT // 2
    lane = np.arange(LANES) % HEAD_DIM
    angles = np.arange(length)[:, None] * (10000.0 ** (-(lane % half) * 2.0 / ROT))[None, :]
    cosine, sine = np.cos(angles), np.sin(angles)
    lines = [
        np.where(lane < ROT, cosine, 1.0),
        np.where(lane < half, -sine, 0.0),
        np.where((lane >= half) & (lane < ROT), sine, 0.0),
    ]
    return jnp.asarray(np.concatenate(lines, axis=1), F32)


def columns_of(ff):
    runs = []
    for at, units, _ in blocks_of(ff):
        even = units // LANES * LANES
        runs.append((0, at, even))
        if even < units:
            runs += [(0, at + even, units - even), (1, at + even, units - even)]
        runs.append((1, at, even))
    return runs


def shards(tokens, cotangent, gain1, bias1, w_qkv, b_qkv, w_out, gain2, bias2, w_gate_up, w_down):
    n, m, s = lax.axis_size("dp"), lax.axis_size("seq"), lax.axis_index("seq")
    rows, width = tokens.shape
    slab = gain1.shape[0]
    inner, hidden = w_out.shape[0] * n, w_down.shape[0] * n
    part, ff = inner // m, hidden // m
    dims = (n, m, rows, width, slab, part, ff, b_qkv.shape[0] // LANES)
    runs = columns_of(ff)
    shard = ff // 2
    held = jnp.array([shards_of(t, n) for t in range(m)], jnp.int32)[s]
    halves = [
        jnp.concatenate(
            [lax.dynamic_slice(w_gate_up, (0, i * hidden + held[u] * shard), (slab, shard)) for u in range(2)], axis=1
        )
        for i in range(2)
    ]
    piece_gu = jnp.concatenate([halves[i][:, at : at + units] for i, at, units in runs], axis=1)
    vec = jnp.concatenate([gain1, bias1, gain2, bias2, b_qkv]).astype(F32).reshape(-1, LANES)
    vec = jnp.pad(vec, ((0, -vec.shape[0] % TILE), (0, 0)))
    rot = rotary_lines(rows * m)
    kept = run_forward(dims, (tokens, cotangent, w_qkv, piece_gu, w_out, w_down, vec, rot))
    block_out, input_grad, gu, g_qkv, g_down, g_out, line = run_backward(dims, tuple(kept) + (rot,))
    share = slab // m
    starts, at = {}, 0
    for i, first, units in runs:
        starts[i, first] = (at, units)
        at += units

    def columns(i, t, first, last):
        found = []
        for (kind, at), (lane, units) in sorted(starts.items()):
            lo, hi = max(first, at), min(last, at + units)
            if kind == i and lo < hi:
                found.append(gu[t * share : (t + 1) * share, lane + lo - at : lane + hi - at])
        return found

    keeper = {held: (t, u) for t in range(m) for u, held in enumerate(shards_of(t, n))}
    pieces = []
    for i in range(2):
        for held in range(n):
            t, u = keeper[held]
            pieces += columns(i, t, u * shard, (u + 1) * shard)
    g_gu = jnp.concatenate(pieces, axis=1).astype(F32)
    line = line.reshape(-1)
    vectors, at = [], 0
    for size in [slab] * 4 + [b_qkv.shape[0]]:
        vectors.append(lax.dynamic_slice(line, (at + s * (size // m),), (size // m,)))
        at += size
    return (
        block_out,
        input_grad,
        vectors[0],
        vectors[1],
        g_qkv,
        vectors[4],
        g_out.astype(F32),
        vectors[2],
        vectors[3],
        g_gu,
        g_down,
    )


def fits(mesh, shapes):
    n, m = mesh.shape["dp"], mesh.shape["seq"]
    (rows, width), slab = shapes[0], shapes[2][0]
    part, ff = shapes[6][0] * n // m, shapes[10][0] * n // m
    return (
        m == 4
        and n == 2 * m
        and rows % LANES == 0
        and shapes[6][0] == LANES
        and slab == 256
        and width % 512 == 0
        and shapes[5][0] % LANES == 0
        and part == 256
        and 512 < ff <= 768
        and ff % 64 == 0
        and (2 * ff // n) % TILE == 0
        and 2 * ff <= width <= 4 * ff
        and 2 * 768 <= width
    )


def solution(mesh):
    rows, cols, vec = P(("dp", "seq"), None), P("dp", None), P("dp")
    flat = P(("dp", "seq"))
    def step(*args):
        body = shards if fits(mesh, [a.shape for a in args]) else shards_plain
        return body(*args)

    return jax.shard_map(
        step,
        mesh=mesh,
        in_specs=(rows, rows, vec, vec, cols, vec, cols, vec, vec, cols, cols),
        out_specs=(rows, rows, flat, flat, rows, flat, rows, flat, flat, rows, rows),
        check_vma=False,
    )
```

```python
import functools

import jax
import jax.numpy as jnp
import numpy as np
from jax import lax
from jax.experimental import pallas as pl
from jax.experimental.pallas import tpu as pltpu
from jax.sharding import PartitionSpec as P

HEAD_DIM = 64
ROT = 16
EPS = 1e-05
F32 = jnp.float32
BF16 = jnp.bfloat16


def ring_order(n):
    return list(range(0, n, 2)) + list(range(n - 1, 0, -2))


def dot(a, b):
    return jnp.dot(a, b, preferred_element_type=F32)


def dot_rows(a, b):
    return lax.dot_general(a, b, (((0,), (0,)), ((), ())), preferred_element_type=F32)


def dot_cols(a, b):
    return lax.dot_general(a, b, (((1,), (1,)), ((), ())), preferred_element_type=F32)


class Ring:
    def __init__(self):
        n = lax.axis_size("dp")
        order = ring_order(n)
        place = [order.index(i) for i in range(n)]
        self.n, self.half = n, n // 2
        self.right = [(order[i], order[(i + 1) % n]) for i in range(n)]
        self.left = [(b, a) for a, b in self.right]
        self.order = jnp.array(order, jnp.int32)
        self.place = jnp.array(place, jnp.int32)[lax.axis_index("dp")]

    def owner(self, offset):
        return self.order[lax.rem(self.place + offset + self.n, self.n)]

    def go_right(self, value):
        return lax.ppermute(value, "dp", self.right)

    def go_left(self, value):
        return lax.ppermute(value, "dp", self.left)

    def gather(self, piece):
        rows = piece.shape[0]
        cut = rows // 2
        from_left = from_right = piece
        whole = jnp.zeros((self.n,) + piece.shape, piece.dtype)

        def put(whole, offset, chunk):
            return lax.dynamic_update_slice(
                whole, chunk[None], (self.owner(offset),) + (0,) * piece.ndim
            )

        whole = put(whole, 0, piece)
        for k in range(1, self.half):
            from_left = self.go_right(from_left)
            from_right = self.go_left(from_right)
            whole = put(put(whole, -k, from_left), k, from_right)
        upper = self.go_right(from_left[:cut])
        lower = self.go_left(from_right[cut:])
        return put(whole, self.half, jnp.concatenate([upper, lower]))

    def scatter(self, parts):
        rows = parts.shape[1]
        cut = rows // 2

        def mine(offset):
            start = (self.owner(offset),) + (0,) * (parts.ndim - 1)
            return lax.dynamic_slice(parts, start, (1,) + parts.shape[1:])[0]

        def add(a, b):
            return a.astype(F32) + b.astype(F32)

        far = mine(self.half)
        upper = self.go_right(far[:cut])
        lower = self.go_left(far[cut:])
        from_left, from_right = mine(self.half - 1), mine(1 - self.half)
        from_left = jnp.concatenate(
            [add(from_left[:cut], upper).astype(BF16), from_left[cut:]]
        )
        from_right = jnp.concatenate(
            [from_right[:cut], add(from_right[cut:], lower).astype(BF16)]
        )
        for k in range(self.half - 2, -1, -1):
            from_left = self.go_right(from_left)
            from_right = self.go_left(from_right)
            if k:
                from_left = add(from_left, mine(k)).astype(BF16)
                from_right = add(from_right, mine(-k)).astype(BF16)
        return add(mine(0), from_left) + from_right.astype(F32)


class Group:
    def __init__(self):
        self.m = lax.axis_size("seq")
        self.s = lax.axis_index("seq")
        self.bits = []
        bit = self.m // 2
        while bit:
            self.bits.append(bit)
            bit //= 2
        self.offsets = [0]
        for bit in self.bits:
            self.offsets += [o ^ bit for o in self.offsets]

    def swap(self, value, mask):
        return lax.ppermute(value, "seq", [(i, i ^ mask) for i in range(self.m)])

    def gather(self, value):
        for bit in self.bits:
            value = jnp.concatenate([value, self.swap(value, bit)])
        return value

    def scatter(self, value):
        for bit in reversed(self.bits):
            half = value.shape[0] // 2
            got = self.swap(value[half:].astype(BF16), bit)
            value = value[:half] + got.astype(F32)
        return value

    def exchange(self, blocks):
        got = []
        for mask in range(self.m):
            block = lax.dynamic_index_in_dim(blocks, self.s ^ mask, 0, keepdims=False)
            got.append(self.swap(block, mask) if mask else block)
        stacked = jnp.stack(got)
        return jnp.take(stacked, self.s ^ jnp.arange(self.m), axis=0)


def norm(value):
    center = value - jnp.mean(value, axis=-1, keepdims=True)
    rstd = lax.rsqrt(jnp.mean(center * center, axis=-1, keepdims=True) + EPS)
    return center * rstd, rstd


def norm_back(upstream, xhat, rstd, gain):
    e = upstream * gain
    inner = (
        e
        - jnp.mean(e, axis=-1, keepdims=True)
        - xhat * jnp.mean(e * xhat, axis=-1, keepdims=True)
    )
    return rstd * inner


def rotary_tables(positions):
    half = ROT // 2
    inverse = 10000.0 ** (-(jnp.arange(half, dtype=F32) * 2.0 / ROT))
    angles = positions.astype(F32)[:, None] * inverse[None, :]
    return jnp.cos(angles)[:, None, :], jnp.sin(angles)[:, None, :]


def rotate(tensor, cosine, sine):
    half = ROT // 2
    a, b = tensor[..., :half], tensor[..., half:ROT]
    return jnp.concatenate([a * cosine - b * sine, b * cosine + a * sine, tensor[..., ROT:]], axis=-1)


def shards_plain(tokens, cotangent, gain1, bias1, w_qkv, b_qkv, w_out, gain2, bias2, w_gate_up, w_down):
    ring, group = Ring(), Group()
    n, m, s = ring.n, group.m, group.s
    rows, width = tokens.shape
    slab = gain1.shape[0]
    inner = w_out.shape[0] * n
    hidden = w_down.shape[0] * n
    part, ff = inner // m, hidden // m
    heads = part // HEAD_DIM
    scale = HEAD_DIM ** (-0.5)

    both = jnp.stack([tokens, cotangent], axis=1)
    everything = group.gather(both)
    tokens_all, cot_all = everything[:, 0], everything[:, 1]

    qkv_piece = jnp.concatenate(
        [lax.dynamic_slice(w_qkv, (0, i * inner + s * part), (slab, part)) for i in range(3)], axis=1
    )
    small = jnp.concatenate([gain1, bias1, gain2, bias2, b_qkv])
    extra = -(-small.shape[0] // (3 * part))
    small = jnp.pad(small, (0, extra * 3 * part - small.shape[0])).reshape(extra, 3 * part)
    first = ring.gather(jnp.concatenate([qkv_piece, small]))
    wqkv = first[:, :slab].reshape(width, 3 * part)
    vectors = first[:, slab:].reshape(n, -1)

    def vector(at, size):
        return vectors[:, at : at + size].reshape(-1).astype(F32)

    g1, b1, g2, b2 = (vector(i * slab, slab) for i in range(4))
    bias_all = vector(4 * slab, b_qkv.shape[0]).reshape(3, m, part)
    bias_qkv = lax.dynamic_index_in_dim(bias_all, s, 1, keepdims=False).reshape(3 * part)

    turn = [(g, (g % n) * m + g // n) for g in range(n * m)]
    back = [(b, a) for a, b in turn]

    def quarter(weight):
        count = weight.shape[0] // m
        mine = lax.dynamic_slice(weight, (0, 0), weight.shape)
        return mine.reshape(m, count, weight.shape[1])[s]

    out_rows, down_rows = w_out.shape[0] // m, w_down.shape[0] // m
    moved = lax.ppermute(
        jnp.concatenate([quarter(w_out), quarter(w_down)]), ("dp", "seq"), turn
    )
    wout = ring.gather(moved[:out_rows]).reshape(part, width)
    gu_piece = jnp.concatenate(
        [lax.dynamic_slice(w_gate_up, (0, i * hidden + s * ff), (slab, ff)) for i in range(2)], axis=1
    )
    wgu = ring.gather(gu_piece).reshape(width, 2 * ff)
    wdown = ring.gather(moved[out_rows:]).reshape(ff, width)

    places = jnp.concatenate([(s ^ o) * rows + jnp.arange(rows, dtype=jnp.int32) for o in group.offsets])
    cosine, sine = rotary_tables(places)
    count = rows * m
    xhat1, rstd1 = norm(tokens_all.astype(F32))
    normed1 = (xhat1 * g1 + b1).astype(BF16)
    qkv = (dot(normed1, wqkv) + bias_qkv).reshape(count, 3, heads, HEAD_DIM)
    queries = rotate(qkv[:, 0], cosine, sine).astype(BF16)
    keys = rotate(qkv[:, 1], cosine, sine).astype(BF16)
    values = qkv[:, 2].astype(BF16)
    scores = jnp.einsum("qhd,khd->hqk", queries, keys, preferred_element_type=F32) * scale
    scores = jnp.where((places[None, :] <= places[:, None])[None], scores, -jnp.inf)
    top = jnp.max(scores, axis=-1, keepdims=True)
    lse = top + jnp.log(jnp.sum(jnp.exp(scores - top), axis=-1, keepdims=True))
    probs = jnp.exp(scores - lse)
    probs_r = probs.astype(BF16)
    context = jnp.einsum("hqk,khd->qhd", probs_r, values, preferred_element_type=F32).astype(BF16)
    context_flat = context.reshape(count, part)
    x_own = tokens.astype(F32)
    mid = x_own + group.scatter(dot(context_flat, wout))
    xhat2, rstd2 = norm(mid)
    normed2 = group.gather((xhat2 * g2 + b2).astype(BF16))
    gate_up = dot(normed2, wgu)
    gate, up = gate_up[:, :ff], gate_up[:, ff:]
    sigma = jax.nn.sigmoid(gate)
    silu = gate * sigma
    act = (silu * up).astype(BF16)
    d_act = dot_cols(cot_all, wdown)
    d_gate = d_act * up * (sigma * (1.0 + gate * (1.0 - sigma)))
    d_gate_up = jnp.concatenate([d_gate, d_act * silu], axis=1).astype(BF16)

    d_normed2 = group.scatter(dot_cols(d_gate_up, wgu))
    sum_down = ring.scatter(dot_rows(act, cot_all).astype(BF16).reshape(n, ff // n, width))
    sum_gu = ring.scatter(dot_rows(normed2, d_gate_up).astype(BF16).reshape(n, slab, 2 * ff))
    block_out = (mid + group.scatter(dot(act, wdown))).astype(BF16)
    d_mid = cotangent.astype(F32) + norm_back(d_normed2, xhat2, rstd2, g2)
    d_mid_r = group.gather(d_mid.astype(BF16))

    d_context = dot_cols(d_mid_r, wout).astype(BF16).reshape(count, heads, HEAD_DIM)
    sum_out = ring.scatter(dot_rows(context_flat, d_mid_r).astype(BF16).reshape(n, part // n, width))
    d_probs = jnp.einsum("qhd,khd->hqk", d_context, values, preferred_element_type=F32)
    delta = jnp.einsum("qhd,qhd->hq", d_context.astype(F32), context.astype(F32))[..., None]
    d_scores = (probs * (d_probs - delta) * scale).astype(BF16)
    d_queries = jnp.einsum("hqk,khd->qhd", d_scores, keys, preferred_element_type=F32)
    d_keys = jnp.einsum("hqk,qhd->khd", d_scores, queries, preferred_element_type=F32)
    d_values = jnp.einsum("hqk,qhd->khd", probs_r, d_context, preferred_element_type=F32)
    d_qkv = jnp.stack(
        [rotate(d_queries, cosine, -sine), rotate(d_keys, cosine, -sine), d_values], axis=1
    ).reshape(count, 3 * part)
    d_qkv_r = d_qkv.astype(BF16)
    d_normed1_part = dot_cols(d_qkv_r, wqkv)
    d_normed1 = group.scatter(d_normed1_part)
    own = (slice(0, rows),)
    input_grad = d_mid + norm_back(d_normed1, xhat1[own], rstd1[own], g1)

    bias_part = jnp.zeros((3, m, part), F32)
    bias_part = lax.dynamic_update_slice(bias_part, jnp.sum(d_qkv, axis=0).reshape(3, 1, part), (0, s, 0))
    vector_parts = [
        jnp.sum(d_normed1_part * xhat1, axis=0),
        jnp.sum(d_normed1_part, axis=0),
        jnp.sum(d_normed2 * xhat2, axis=0),
        jnp.sum(d_normed2, axis=0),
        bias_part.reshape(-1),
    ]
    line = jnp.concatenate([v.reshape(n, m, -1) for v in vector_parts], axis=-1)
    lines = -(-line.shape[-1] // (3 * part))
    line = jnp.pad(line, ((0, 0), (0, 0), (0, lines * 3 * part - line.shape[-1])))
    line = line.reshape(n, m, lines, 3 * part).astype(BF16)
    part_qkv = dot_rows(normed1, d_qkv_r).astype(BF16).reshape(n, m, slab // m, 3 * part)
    packed = jnp.concatenate([part_qkv, line], axis=2)
    packed_rows = packed.shape[2]
    sum_qkv = ring.scatter(packed.reshape(n, m * packed_rows, 3 * part))

    def owners(total):
        return group.exchange(total.astype(BF16).reshape((m, -1) + total.shape[1:])).astype(F32)

    last = owners(sum_qkv)
    g_qkv = last[:, : slab // m].reshape(m, slab // m, 3, part).transpose(1, 2, 0, 3)
    g_qkv = g_qkv.reshape(slab // m, 3 * inner)
    line = jnp.sum(last[:, slab // m :], axis=0).reshape(-1)
    sizes = [slab // m] * 4 + [b_qkv.shape[0] // m]
    vectors_out, at = [], 0
    for size in sizes:
        vectors_out.append(line[at : at + size])
        at += size
    g_gu = owners(sum_gu).reshape(m, slab // m, 2, ff).transpose(1, 2, 0, 3).reshape(slab // m, 2 * hidden)
    g_down = lax.ppermute(sum_down.astype(BF16), ("dp", "seq"), back).astype(F32)
    g_out = lax.ppermute(sum_out.astype(BF16), ("dp", "seq"), back).astype(F32)
    return (
        block_out,
        input_grad,
        vectors_out[0],
        vectors_out[1],
        g_qkv,
        vectors_out[4],
        g_out,
        vectors_out[2],
        vectors_out[3],
        g_gu,
        g_down,
    )


LOGICAL = pl.DeviceIdType.LOGICAL
MEAN, RSTD, SPOT, LSE = 0, 1, 2, 8
LANES = 128
TILE = 16
WINDOW = 512
VMEM_BYTES = 67_043_328


def vmem(shape, dtype=BF16):
    return pltpu.VMEM(shape, dtype)


class Place:
    def __init__(self, n, m):
        self.n, self.m, self.half = n, m, n // 2
        self.d, self.s = lax.axis_index("dp"), lax.axis_index("seq")
        pair = lax.div(self.d, 2)
        odd = self.d - 2 * pair
        place = pair + odd * (n - 1 - 2 * pair)
        self.owners = []
        for offset in range(n):
            spot = lax.rem(place + offset, n)
            back = lax.div(spot, self.half)
            self.owners.append(2 * spot + back * (2 * n - 1 - 4 * spot))
        self.partners = []
        for mask in range(m):
            out, bit = self.s, 1
            while bit < m:
                if mask & bit:
                    out = out + bit - 2 * bit * lax.rem(lax.div(self.s, bit), 2)
                bit *= 2
            self.partners.append(out)
        self.rings = {1: self.owners[1] * m + self.s, -1: self.owners[n - 1] * m + self.s}
        self.seqs = [self.d * m + out for out in self.partners]
        inner_ = lax.rem(self.s, 2)
        side = lax.rem(lax.div(self.s, 2) + inner_, 2)
        self.shards = [2 * inner_ + side, n - 2 - 2 * inner_ + side]
        low = lax.div(self.d, m)
        self.source = (self.shards[0] + low * (self.shards[1] - self.shards[0])) * m + self.d - low * m
        across = lax.rem(lax.div(pair + 1, 2), 2)
        self.there = lax.div(self.d, m) * m + self.s
        self.target = self.there * m + 2 * lax.rem(odd + across, 2) + across
        here = self.d * m + self.s
        self.moves = (self.target - here) * (self.target - here) > 0

        offsets = [0]
        for bit in self.bits():
            offsets += [o ^ bit for o in offsets]
        self.homes = [self.partners[o] for o in offsets]

    def owner(self, offset):
        return self.owners[offset % self.n]

    def partner(self, mask):
        return self.partners[mask]

    def bits(self):
        out, bit = [], self.m // 2
        while bit:
            out.append(bit)
            bit //= 2
        return out


class Sender:
    def __init__(self, sends, recvs):
        self.sends, self.recvs = sends, recvs
        self.used = 0
        self.open = []

    def slot(self):
        self.used += 1
        return self.used - 1

    def copy(self, slot, src, dst, device):
        return pltpu.make_async_remote_copy(
            src_ref=src,
            dst_ref=dst,
            send_sem=self.sends.at[slot],
            recv_sem=self.recvs.at[slot],
            device_id=device,
            device_id_type=LOGICAL,
        )

    def start(self, slot, src, dst, device):
        copy = self.copy(slot, src, dst, device)
        copy.start()
        self.open.append(copy)
        return copy

    def finish(self):
        for copy in self.open:
            copy.wait_send()
        self.open = []


def greet(place, extra_seq=()):
    barrier = pltpu.get_barrier_semaphore()

    def hello(device):
        pl.semaphore_signal(barrier, inc=1, device_id=device, device_id_type=LOGICAL)

    near = [place.rings[1], place.rings[-1]] + [place.seqs[mask] for mask in tuple(place.bits()) + tuple(extra_seq)]
    for device in near:
        hello(device)

    @pl.when(place.moves)
    def _():
        hello(place.target)
        hello(place.source)
        pl.semaphore_wait(barrier, len(near) + 2)

    @pl.when(jnp.logical_not(place.moves))
    def _():
        pl.semaphore_wait(barrier, len(near))


class RowSlots:
    def __init__(self, rows, cols, lo=0):
        self.rows, self.cols, self.lo = rows, cols, lo

    def where(self, index, part=None):
        rows, start = self.rows, index * self.rows
        if part is not None:
            rows = rows // 2
            start = start + part * rows
        return pl.ds(pl.multiple_of(start, rows), rows), pl.ds(self.lo, self.cols)

    def landing(self, way, j, half):
        base = way * ((half - 1) * self.rows + self.rows // 2)
        at, rows = (base + (half - 1) * self.rows, self.rows // 2) if j == 1 else (base + (j - 2) * self.rows, self.rows)
        return pl.ds(at, rows), pl.ds(0, self.cols)

    def inbox(self, half):
        return 2 * ((half - 1) * self.rows + self.rows // 2), self.cols


class TileSlots:
    def __init__(self, rows, cols):
        self.rows, self.cols = rows, cols

    def where(self, index, part=None):
        row = lax.div(index, 2)
        cols, start = self.cols, (index - 2 * row) * self.cols
        if part is not None:
            cols = cols // 2
            start = start + part * cols
        return pl.ds(pl.multiple_of(row * self.rows, self.rows), self.rows), pl.ds(pl.multiple_of(start, cols), cols)

    def landing(self, way, j, half):
        at, cols = ((half - 1) * self.cols, self.cols // 2) if j == 1 else ((j - 2) * self.cols, self.cols)
        return pl.ds(way * self.rows, self.rows), pl.ds(at, cols)

    def inbox(self, half):
        return 2 * self.rows, (half - 1) * self.cols + self.cols // 2


class Gather:
    def __init__(self, place, sender, buf, slots):
        self.place, self.sender, self.buf, self.slots = place, sender, buf, slots
        self.sems = [[sender.slot() for _ in range(place.half)] for _ in range(2)]
        self.devices = (place.rings[1], place.rings[-1])

    def own(self):
        return self.buf.at[self.slots.where(self.place.d)]

    def send(self, k, way):
        index = self.place.owner(k if way else -k)
        ref = self.buf.at[self.slots.where(index, way if k == self.place.half - 1 else None)]
        self.sender.start(self.sems[way][k], ref, ref, self.devices[way])

    def begin(self):
        self.send(0, 0)
        self.send(0, 1)

    def pump(self, k):
        last = k == self.place.half
        for way in range(2):
            index = self.place.owner(k if way else -k)
            ref = self.buf.at[self.slots.where(index, way if last else None)]
            self.sender.copy(self.sems[way][k - 1], ref, ref, self.devices[way]).wait_recv()
            if not last:
                self.send(k, way)


class Reduce:
    def __init__(self, place, sender, buf, inbox, slots):
        self.place, self.sender, self.buf, self.inbox, self.slots = place, sender, buf, inbox, slots
        self.sems = [[sender.slot() for _ in range(place.half)] for _ in range(2)]
        self.devices = (place.rings[1], place.rings[-1])

    def target(self, way, j):
        offset = self.place.half - j
        return self.slots.where(self.place.owner(-offset if way else offset), way if j == 1 else None)

    def copy(self, way, j):
        offset = self.place.half - j + 1
        src = self.slots.where(self.place.owner(-offset if way else offset), way if j == 1 else None)
        return self.sems[way][j - 1], self.buf.at[src], self.inbox.at[self.slots.landing(way, j, self.place.half)]

    def send(self, j, way):
        self.sender.start(*self.copy(way, j), self.devices[way])

    def begin(self):
        self.send(1, 0)
        self.send(1, 1)

    def add(self, to, *froms):
        value = self.buf[to].astype(F32)
        for at in froms:
            value = value + self.inbox[at].astype(F32)
        self.buf[to] = value.astype(self.buf.dtype)

    def pump(self, j):
        half = self.place.half
        for way in range(2):
            self.sender.copy(*self.copy(way, j), self.devices[way]).wait_recv()
            if j < half:
                self.add(self.target(way, j), self.slots.landing(way, j, half))
                self.send(j + 1, way)
        if j == half:
            self.add(self.slots.where(self.place.d), *(self.slots.landing(way, j, half) for way in range(2)))

    def mine(self):
        return self.buf.at[self.slots.where(self.place.d)]


def shards_of(s, n):
    inner = s % 2
    side = (s // 2 + inner) % 2
    return [2 * inner + side, n - 2 - 2 * inner + side]


def blocks_of(ff):
    return [(at, min(256, ff - at), 2 * at) for at in range(0, ff, 256)]


def key_spots(place, pos_k, rows):
    lane = lax.broadcasted_iota(jnp.int32, (8, rows), 1)
    for i, home in enumerate(place.homes):
        pos_k[:, i * rows : (i + 1) * rows] = (home * rows + lane).astype(F32)


def load_rotary(place, h_rot, rot, rows, sems, first):
    copies = []
    for i, home in enumerate(place.homes):
        src = h_rot.at[pl.ds(pl.multiple_of(home * rows, rows), rows)]
        copies.append(pltpu.make_async_copy(src, rot.at[pl.ds(i * rows, rows)], sems.at[first + i]))
        copies[-1].start()
    return copies


def forward_kernel(
    dims,
    tok, cot, h_wqkv, h_wgu, h_wout, h_wdown, piece_vec, h_rot,
    o_wqkv, o_wout, o_wgu, o_wdown, o_rows, o_tok, o_cot, o_n1, o_qkv, o_stat, o_ctx, o_mid, o_n2, o_act, o_dgu,
    wqkv, wout, wgu, wdown, vec, tok_all, cot_all, n1, qkv, stat, ctx, mid, n2, act, dgu,
    rows_v, bias_v, rot, pos_k, raw, own, send1, send2, recv1, recv2,
    sends, recvs, locals_, outs,
):
    n, m, rows, width, slab, part, ff, b_units = dims
    count = rows * m
    half = count // 2
    inner = part * m
    place = Place(n, m)
    sender = Sender(sends, recvs)
    d, s = place.d, place.s
    bits = place.bits()
    out_rows, vec_rows = part // n, piece_vec.shape[0]
    down_rows, down_cols = 2 * ff // n, width // 2
    blocks = blocks_of(ff)

    ring_a = Gather(place, sender, wqkv, RowSlots(slab, 3 * part))
    ring_v = Gather(place, sender, vec, RowSlots(vec_rows, LANES))
    ring_b = Gather(place, sender, wout, RowSlots(out_rows, width))
    ring_c = [Gather(place, sender, wgu, RowSlots(slab, 2 * units, lane)) for _, units, lane in blocks]
    ring_d = Gather(place, sender, wdown, TileSlots(down_rows, down_cols))

    def local(i, src, dst):
        copy = pltpu.make_async_copy(src, dst, locals_.at[i])
        copy.start()
        return copy

    own_rows = pl.ds(pl.multiple_of(d * slab, slab), slab)
    placed_qkv = [
        local(
            2 * i + u,
            h_wqkv.at[:, pl.ds(pl.multiple_of(i * inner + place.shards[u] * LANES, LANES), LANES)],
            wqkv.at[own_rows, pl.ds(i * part + u * LANES, LANES)],
        )
        for i in range(3)
        for u in range(2)
    ]
    placed_vec = local(6, piece_vec, ring_v.own())
    placed_tok = local(7, tok, tok_all.at[pl.ds(0, rows)])
    shard, hidden = ff // 2, h_wgu.shape[1] // 2
    window = raw.shape[2]
    shifts, placed_gu = [], []
    for i in range(2):
        for u in range(2):
            col = place.shards[u] * shard
            first_tile = lax.div(col + (0 if i == 0 else shard + LANES - 1 + hidden - window), LANES)
            base = first_tile * LANES
            shifts.append(col - base + i * hidden)
            src = h_wgu.at[:, pl.ds(pl.multiple_of(base, LANES), window)]
            placed_gu.append(local((8, 12 + m, 13 + m, 14 + m)[2 * i + u], src, raw.at[2 * i + u]))
    placed_cot = local(9, cot, cot_all.at[pl.ds(0, rows)])
    placed_rot = load_rotary(place, h_rot, rot, rows, locals_, 12)
    greet(place)
    moves = place.moves

    class Spread:
        def __init__(self, buf):
            self.buf = buf
            self.sems = [sender.slot() for _ in bits]

        def copy(self, i):
            size = rows << i
            return self.sems[i], self.buf.at[pl.ds(0, size)], self.buf.at[pl.ds(size, size)], place.seqs[bits[i]]

        def send(self, i):
            sender.start(*self.copy(i))

        def wait(self, i):
            sender.copy(*self.copy(i)).wait_recv()

    toks, cots, n2s = Spread(tok_all), Spread(cot_all), Spread(n2)
    written = []

    def write(src, dst):
        copy = pltpu.make_async_copy(src, dst, outs.at[len(written)])
        copy.start()
        written.append(copy)

    for copy in placed_qkv:
        copy.wait()
    ring_a.begin()
    placed_vec.wait()
    ring_v.begin()
    placed_tok.wait()
    toks.send(0)

    src_out = h_wout.at[pl.ds(pl.multiple_of(s * out_rows, out_rows), out_rows)]
    up = lax.div(s, 2)
    src_down = h_wdown.at[
        pl.ds(pl.multiple_of(up * down_rows, down_rows), down_rows),
        pl.ds(pl.multiple_of((s - 2 * up) * down_cols, down_cols), down_cols),
    ]
    turns = [(src_out, ring_b, sender.slot(), 10), (src_down, ring_d, sender.slot(), 11)]

    def turn(ring, index):
        return ring.buf.at[ring.slots.where(index)]

    @pl.when(moves)
    def _():
        for src, ring, slot, _ in turns:
            sender.copy(slot, src, turn(ring, place.there), place.target).start()

    @pl.when(jnp.logical_not(moves))
    def _():
        for src, ring, _, i in turns:
            local(i, src, ring.own()).wait()

    for copy in placed_gu:
        copy.wait()
    lane = lax.broadcasted_iota(jnp.int32, (1, LANES), 1)
    whole, rest = shard // LANES, shard % LANES

    def cut(j, carry):
        size = 64
        span = pl.ds(pl.multiple_of(j * size, size), size)
        tiles = []
        for i in range(2):
            low = pltpu.roll(raw[2 * i, span, :].astype(F32), window - shifts[2 * i], 1)
            high = pltpu.roll(
                raw[2 * i + 1, span, :].astype(F32), lax.rem(window + rest - shifts[2 * i + 1] + window, window), 1
            )
            lows = [low[:, t * LANES : (t + 1) * LANES] for t in range(whole + 1)]
            highs = [high[:, t * LANES : (t + 1) * LANES] for t in range(window // LANES)]
            tiles.append(lows[:whole] + [jnp.where(lane < rest, lows[whole], highs[0])] + highs[1:])
        to = pl.ds(pl.multiple_of(d * slab + j * size, size), size)
        at = 0
        for first_unit, count_, _ in blocks:
            even = count_ // LANES
            t = first_unit // LANES
            line_ = tiles[0][t : t + even]
            if even * LANES < count_:
                line_.append(jnp.where(lane < LANES // 2, tiles[0][t + even], pltpu.roll(tiles[1][t + even], LANES // 2, 1)))
            for tile in line_ + tiles[1][t : t + even]:
                wgu[to, at : at + LANES] = tile.astype(BF16)
                at += LANES
        return carry

    lax.fori_loop(0, slab // 64, cut, 0)
    ring_c[0].begin()
    placed_cot.wait()
    cots.send(0)
    wdown[ff:, :] = jnp.zeros((wdown.shape[0] - ff, width), BF16)
    key_spots(place, pos_k, rows)
    line = lax.broadcasted_iota(jnp.int32, (rows, 1), 0)

    def stats(i):
        span = slice(i * rows, (i + 1) * rows)
        x = tok_all[span, :].astype(F32)
        mu = jnp.mean(x, axis=-1, keepdims=True)
        c = x - mu
        r = lax.rsqrt(jnp.mean(c * c, axis=-1, keepdims=True) + EPS)
        spot = (place.homes[i] * rows + line).astype(F32)
        stat[span, :] = jnp.where(lane == MEAN, mu, jnp.where(lane == RSTD, r, spot))

    stats(0)
    ring_v.pump(1)
    ring_a.pump(1)

    @pl.when(moves)
    def _():
        for src, ring, slot, _ in turns:
            sender.copy(slot, src, ring.own(), place.source).wait_recv()

    ring_b.begin()
    toks.wait(0)
    toks.send(1)
    stats(1)
    ring_v.pump(2)
    ring_a.pump(2)
    ring_d.begin()
    ring_b.pump(1)
    toks.wait(1)
    write(tok_all, o_tok)
    stats(2)
    stats(3)
    cots.wait(0)
    cots.send(1)
    ring_v.pump(3)
    ring_a.pump(3)
    ring_c[1].begin()
    ring_b.pump(2)
    ring_c[0].pump(1)
    ring_v.pump(4)
    units = slab // LANES
    for c in range(n):
        for r in range(4):
            for u in range(units):
                at = c * slab + u * LANES
                row = c * vec_rows + r * units + u
                rows_v[r : r + 1, at : at + LANES] = vec[row : row + 1, :]
    for i in range(3):
        for u in range(part // LANES):
            unit = i * (inner // LANES) + place.shards[u]
            row = lax.div(unit, b_units) * vec_rows + 4 * units + lax.rem(unit, b_units)
            at = i * part + u * LANES
            bias_v[0:1, at : at + LANES] = vec[pl.ds(row, 1), :]
    write(rows_v, o_rows)

    def normalize(j, carry):
        size = 64
        span = pl.ds(pl.multiple_of(j * size, size), size)
        x = tok_all[span, :].astype(F32)
        xhat = (x - stat[span, MEAN : MEAN + 1]) * stat[span, RSTD : RSTD + 1]
        n1[span, :] = (xhat * rows_v[0:1, :] + rows_v[1:2, :]).astype(BF16)
        return carry

    lax.fori_loop(0, count // 64, normalize, 0)
    write(n1, o_n1)
    ring_d.pump(1)
    ring_c[2].begin()
    cots.wait(1)
    write(cot_all, o_cot)
    ring_a.pump(4)
    write(wqkv, o_wqkv)
    for copy in placed_rot:
        copy.wait()

    def project(j, carry):
        size = 256
        span = pl.ds(pl.multiple_of(j * size, size), size)
        for i in range(3):
            cols = slice(i * part, (i + 1) * part)
            y = dot(n1[span, :], wqkv[:, cols]) + bias_v[0:1, cols]
            if i < 2:
                pieces = []
                for u in range(part // LANES):
                    z = y[:, u * LANES : (u + 1) * LANES]
                    pieces.append(
                        z * rot[span, :LANES]
                        + pltpu.roll(z, LANES - ROT // 2, 1) * rot[span, LANES : 2 * LANES]
                        + pltpu.roll(z, ROT // 2, 1) * rot[span, 2 * LANES :]
                    )
                y = jnp.concatenate(pieces, axis=1)
            qkv[span, cols] = y.astype(BF16)
        return carry

    lax.fori_loop(0, count // 256, project, 0)
    write(qkv, o_qkv)
    ring_b.pump(3)
    ring_c[1].pump(1)
    ring_c[0].pump(2)
    scale = HEAD_DIM ** (-0.5)
    per = LANES // HEAD_DIM

    def attend(i, carry):
        pair, block = lax.div(i, m), lax.rem(i, m)
        span = pl.ds(pl.multiple_of(block * rows, rows), rows)
        at = pl.multiple_of(pair * LANES, LANES)
        q = qkv[span, pl.ds(at, LANES)]
        k = qkv[:, pl.ds(pl.multiple_of(part + at, LANES), LANES)]
        v = qkv[:, pl.ds(pl.multiple_of(2 * part + at, LANES), LANES)]
        allowed = pos_k[0:1, :] <= stat[span, SPOT : SPOT + 1]
        total = jnp.zeros((rows, LANES), F32)
        for h in range(per):
            mine = (lane // HEAD_DIM == h).astype(BF16)
            scores = dot_cols(q * mine, k) * scale
            scores = jnp.where(allowed, scores, -jnp.inf)
            top = jnp.max(scores, axis=-1, keepdims=True)
            found = top + jnp.log(jnp.sum(jnp.exp(scores - top), axis=-1, keepdims=True))
            probs = jnp.exp(scores - found).astype(BF16)
            total = total + dot(probs, v * mine)
            stat[span, :] = jnp.where(lane == LSE + pair * per + h, found, stat[span, :])
        ctx[span, pl.ds(at, LANES)] = total.astype(BF16)
        return carry

    lax.fori_loop(0, (part // LANES) * m, attend, 0)
    write(stat, o_stat)
    write(ctx, o_ctx)
    ring_d.pump(2)
    ring_c[2].pump(1)
    ring_b.pump(4)
    write(wout, o_wout)

    step = 512
    scatter = [sender.slot(), sender.slot()]

    def far_part(j, carry):
        cols = pl.ds(pl.multiple_of(j * step, step), step)
        send1[:, cols] = dot(ctx[half:, :], wout[:, cols]).astype(BF16)
        return carry

    lax.fori_loop(0, width // step, far_part, 0)
    first = sender.start(scatter[0], send1, recv1, place.seqs[bits[1]])

    def near_part(j, carry):
        cols = pl.ds(pl.multiple_of(j * step, step), step)
        own[:, cols] = dot(ctx[:half, :], wout[:, cols])
        return carry

    lax.fori_loop(0, width // step, near_part, 0)
    ring_c[1].pump(2)
    first.wait_recv()
    send2[...] = (own[rows:, :] + recv1[rows:, :].astype(F32)).astype(BF16)
    second = sender.start(scatter[1], send2, recv2, place.seqs[bits[0]])
    ring_c[0].pump(3)
    second.wait_recv()
    value = tok_all[:rows, :].astype(F32) + own[:rows, :] + recv1[:rows, :].astype(F32) + recv2[...].astype(F32)
    mid[...] = value
    c = value - jnp.mean(value, axis=-1, keepdims=True)
    r = lax.rsqrt(jnp.mean(c * c, axis=-1, keepdims=True) + EPS)
    n2[:rows, :] = (c * r * rows_v[2:3, :] + rows_v[3:4, :]).astype(BF16)
    n2s.send(0)
    write(mid, o_mid)
    ring_d.pump(3)
    ring_c[2].pump(2)
    ring_c[1].pump(3)
    n2s.wait(0)
    n2s.send(1)
    ring_c[0].pump(4)
    ring_d.pump(4)
    write(wdown, o_wdown)
    n2s.wait(1)
    write(n2, o_n2)
    ring_c[2].pump(3)

    def expand(first_unit, units, base):
        even = units // LANES * LANES
        y = dot(n2[...], wgu[:, base : base + 2 * units])
        d_act = dot_cols(cot_all[...], wdown[first_unit : first_unit + 256, :])
        if even == units:
            gate, up = y[:, :units], y[:, units:]
        else:
            gate = y[:, : even + LANES]
            up = jnp.concatenate([y[:, even + LANES :], pltpu.roll(gate[:, even:], LANES // 2, 1)], axis=1)
        sigma = jax.nn.sigmoid(gate)
        silu = gate * sigma
        value = silu * up
        d_gate = d_act * up * (sigma * (1.0 + gate * (1.0 - sigma)))
        d_up = d_act * silu
        if even == units:
            dgu[:, base : base + units] = d_gate.astype(BF16)
            dgu[:, base + units : base + 2 * units] = d_up.astype(BF16)
        else:
            value = jnp.where(lax.broadcasted_iota(jnp.int32, (1, 256), 1) < units, value, 0.0)
            mixed = jnp.where(lane < LANES // 2, d_gate[:, even:], pltpu.roll(d_up[:, even:], LANES // 2, 1))
            dgu[:, base : base + even] = d_gate[:, :even].astype(BF16)
            dgu[:, base + even : base + even + LANES] = mixed.astype(BF16)
            dgu[:, base + even + LANES : base + 2 * units] = d_up[:, :even].astype(BF16)
        act[:, first_unit : first_unit + 256] = value.astype(BF16)

    expand(*blocks[0])
    ring_c[1].pump(4)
    expand(*blocks[1])
    ring_c[2].pump(4)
    write(wgu, o_wgu)
    expand(*blocks[2])
    write(act, o_act)
    write(dgu, o_dgu)
    for copy in written:
        copy.wait()
    sender.finish()

    @pl.when(moves)
    def _():
        for src, ring, slot, _ in turns:
            sender.copy(slot, src, turn(ring, place.there), place.target).wait_send()


def run_forward(dims, args):
    n, m, rows, width, slab, part, ff, b_units = dims
    count = rows * m
    ffp = -(-ff // 256) * 256
    vec_rows = args[6].shape[0]
    arrays = [
        ((width, 3 * part), BF16), ((part, width), BF16), ((width, 2 * ff), BF16), ((ffp, width), BF16),
        ((8, width), F32), ((count, width), BF16), ((count, width), BF16), ((count, width), BF16),
        ((count, 3 * part), BF16), ((count, LANES), F32), ((count, part), BF16), ((rows, width), F32),
        ((count, width), BF16), ((count, ffp), BF16), ((count, 2 * ff), BF16),
    ]
    scratch = [vmem(*a) for a in arrays]
    rows_v, scratch[4] = scratch[4], vmem((n * vec_rows, LANES), F32)
    slots = (4 + len(blocks_of(ff))) * 2 * (n // 2) + 3 * 2 + 2 + 2
    return pl.pallas_call(
        functools.partial(forward_kernel, dims),
        out_shape=[jax.ShapeDtypeStruct(*a) for a in arrays],
        in_specs=[pl.BlockSpec(memory_space=pl.ANY)] * len(args),
        out_specs=[pl.BlockSpec(memory_space=pl.ANY)] * len(arrays),
        scratch_shapes=scratch
        + [
            rows_v,
            vmem((8, 3 * part), F32),
            vmem((count, 3 * LANES), F32),
            vmem((8, count), F32),
            vmem((4, slab, WINDOW)),
            vmem((count // 2, width), F32),
            vmem((count // 2, width)),
            vmem((rows, width)),
            vmem((count // 2, width)),
            vmem((rows, width)),
            pltpu.SemaphoreType.DMA((slots,)),
            pltpu.SemaphoreType.DMA((slots,)),
            pltpu.SemaphoreType.DMA((15 + m,)),
            pltpu.SemaphoreType.DMA((len(arrays),)),
        ],
        compiler_params=pltpu.CompilerParams(
            collective_id=0, has_side_effects=True, vmem_limit_bytes=VMEM_BYTES
        ),
        name="forward",
    )(*args)


def flip(value):
    size = value.shape[1]
    here = lax.broadcasted_iota(jnp.int32, (size, size), 0) == lax.broadcasted_iota(jnp.int32, (size, size), 1)
    return dot_cols(here.astype(F32).astype(BF16), value).astype(BF16)


def backward_kernel(
    dims,
    h_wqkv, h_wout, h_wgu, h_wdown, h_rows, h_tok, h_cot, h_n1, h_qkv, h_stat, h_ctx, h_mid, h_n2, h_act, h_dgu,
    h_rot,
    o_block, o_input, o_gu, o_qkv, o_down, o_out, o_vec,
    wout, wgu, wqkv, rows_v, wide_a, wide_b, qkv, stat, ctx, mid, act, dgu, rot, pos_k,
    sum_a, sum_b, sum_c, sum_d, sum_v, in_a, in_b, in_c, in_d, in_v,
    own, send1, send2, recv1, recv2, dm_all, d_mid, cot, dctx, dqkv, dk, dv, sums_v, bias_v,
    x_gu, x_qkv, x_down, x_out, x_vec, y_qkv, y_down, y_gu,
    sends, recvs, loads, outs,
):
    n, m, rows, width, slab, part, ff, b_units = dims
    ffp = act.shape[1]
    inner = part * m
    count = rows * m
    half = count // 2
    place = Place(n, m)
    sender = Sender(sends, recvs)
    waiting = {}

    def load(name, src, dst):
        copy = pltpu.make_async_copy(src, dst, loads.at[len(waiting)])
        copy.start()
        waiting[name] = copy

    load("n2", h_n2, wide_b)
    load("dgu", h_dgu, dgu)
    load("act", h_act, act)
    load("cot", h_cot, wide_a)
    load("wgu", h_wgu, wgu)
    load("own", h_cot.at[pl.ds(0, dims[2])], cot)
    load("mid", h_mid, mid)
    load("rows", h_rows, rows_v)
    load("wqkv", h_wqkv, wqkv)
    load("wout", h_wout, wout)
    load("ctx", h_ctx, ctx)
    load("qkv", h_qkv, qkv)
    load("stat", h_stat, stat)
    spare = loads.shape[0] - 2
    rotary = load_rotary(place, h_rot, rot, rows, loads, spare - m)
    bits = place.bits()
    others = [mask for mask in range(1, m) if mask not in bits]
    moves = place.moves
    greet(place, others)
    d, s = place.d, place.s
    out_rows, vec_rows = part // n, sum_v.shape[0] // n
    down_rows, down_cols = 2 * ff // n, width // 2
    ring_a = Reduce(place, sender, sum_a, in_a, RowSlots(slab, 3 * part))
    ring_b = Reduce(place, sender, sum_b, in_b, RowSlots(out_rows, width))
    ring_c = Reduce(place, sender, sum_c, in_c, RowSlots(slab, 2 * ff))
    ring_d = Reduce(place, sender, sum_d, in_d, TileSlots(down_rows, down_cols))
    ring_v = Reduce(place, sender, sum_v, in_v, RowSlots(vec_rows, LANES))
    key_spots(place, pos_k, rows)
    block = 256

    def outer(dst, left, right, size):
        def step(j, carry):
            cols = pl.ds(pl.multiple_of(j * block, block), block)
            dst[cols, :] = dot(flip(left[:, cols]), right[...]).astype(BF16)
            return carry

        lax.fori_loop(0, size // block, step, 0)

    class Halving:
        def __init__(self, at):
            self.slots = [sender.slot(), sender.slot()]
            self.at = at
            self.open = []

        def first(self, far):
            far()
            self.open.append(sender.start(self.slots[0], send1, recv1.at[pl.ds(self.at * half, half)], place.seqs[bits[1]]))

        def second(self):
            self.open[0].wait_recv()
            send2[...] = (own[rows:, :] + recv1[self.at * half + rows : (self.at + 1) * half, :].astype(F32)).astype(BF16)
            self.open.append(sender.start(self.slots[1], send2, recv2.at[pl.ds(self.at * rows, rows)], place.seqs[bits[0]]))

        def total(self):
            self.open[1].wait_recv()
            return own[:rows, :] + recv1[self.at * half : self.at * half + rows, :].astype(F32) + recv2[
                self.at * rows : (self.at + 1) * rows, :
            ].astype(F32)

        def sent(self):
            for copy in self.open:
                copy.wait_send()
            sender.open = [c for c in sender.open if all(c is not o for o in self.open)]

    turns = [(ring_d, x_down, sender.slot()), (ring_b, x_out, sender.slot())]

    def turn_back(i):
        ring, landing, slot = turns[i]

        @pl.when(moves)
        def _():
            sender.copy(slot, ring.mine(), landing, place.source).start()

        @pl.when(jnp.logical_not(moves))
        def _():
            copy = pltpu.make_async_copy(ring.mine(), landing, loads.at[spare + i])
            copy.start()
            copy.wait()

    def turned_back(i):
        ring, landing, slot = turns[i]

        @pl.when(moves)
        def _():
            sender.copy(slot, ring.mine(), landing, place.target).wait_recv()

    def deal(buf, size, landing, whole=False):
        share = size if whole else size // m
        got = []
        to = pl.ds(pl.multiple_of(s * share, share), share)
        for mask in range(1, m):
            start = d * size + (0 if whole else place.partner(mask) * share)
            src = buf.at[pl.ds(pl.multiple_of(start, share), share)]
            got.append(sender.start(sender.slot(), src, landing.at[to], place.seqs[mask]))
        start = d * size + (0 if whole else s * share)
        landing[to, :] = buf[pl.ds(pl.multiple_of(start, share), share), :]
        return got

    waiting["n2"].wait()
    waiting["dgu"].wait()

    def slab_of(index):
        cols = pl.ds(pl.multiple_of(index * slab, slab), slab)
        sum_c[cols, :] = dot(flip(wide_b[:, cols]), dgu[...]).astype(BF16)

    slab_of(place.owner(place.half))
    ring_c.begin()
    waiting["act"].wait()
    waiting["cot"].wait()
    outer(sum_d, act, wide_a, ffp)
    ring_d.begin()
    waiting["wgu"].wait()
    normed2 = Halving(0)

    def back_step(left, lo, hi, weight, to):
        def step(j, carry):
            cols = pl.ds(pl.multiple_of(j * block, block), block)
            to(cols, dot_cols(left[lo:hi, :], weight[cols, :]))
            return carry

        lax.fori_loop(0, width // block, step, 0)

    def to_send(cols, value):
        send1[:, cols] = value.astype(BF16)

    def to_own(cols, value):
        own[:, cols] = value

    normed2.first(lambda: back_step(dgu, half, count, wgu, to_send))
    back_step(dgu, 0, half, wgu, to_own)
    lanes = 2 * ff
    load("down_lo", h_wdown.at[:, pl.ds(0, lanes)], wgu.at[pl.ds(0, ffp)])
    load("down_hi", h_wdown.at[:, pl.ds(lanes, width - lanes)], wgu.at[pl.ds(ffp, ffp), pl.ds(0, width - lanes)])
    normed2.second()

    def other_slabs(i, carry):
        slab_of(lax.rem(place.owner(place.half) + i, n))
        return carry

    lax.fori_loop(1, n, other_slabs, 0)
    load("n1", h_n1, wide_b)
    load("tok", h_tok, wide_a)
    ring_c.pump(1)
    ring_d.pump(1)

    waiting["mid"].wait()
    waiting["rows"].wait()
    waiting["own"].wait()

    def deviation(value):
        c = value - jnp.mean(value, axis=-1, keepdims=True)
        r = lax.rsqrt(jnp.mean(c * c, axis=-1, keepdims=True) + EPS)
        return c * r, r

    xhat, r = deviation(mid[...])
    up = normed2.total()
    sums_v[2:3, :] = jnp.sum(up * xhat, axis=0, keepdims=True)
    sums_v[3:4, :] = jnp.sum(up, axis=0, keepdims=True)
    d_mid[...] = cot[...].astype(F32) + norm_back(up, xhat, r, rows_v[2:3, :])
    dm_all[:rows, :] = d_mid[...].astype(BF16)
    spread = [sender.slot() for _ in bits]

    def spread_copy(i):
        size = rows << i
        return (spread[i], dm_all.at[pl.ds(0, size)], dm_all.at[pl.ds(size, size)])

    def spread_send(i):
        sender.start(*spread_copy(i), place.seqs[bits[i]])

    def spread_wait(i):
        sender.copy(*spread_copy(i), place.seqs[bits[i]]).wait_recv()

    spread_send(0)
    normed2.sent()

    waiting["down_lo"].wait()
    waiting["down_hi"].wait()

    def down_step(lo, hi, to):
        def low(j, carry):
            cols = pl.ds(pl.multiple_of(j * LANES, LANES), LANES)
            to(cols, dot(act[lo:hi, :], wgu[:ffp, cols]))
            return carry

        def high(j, carry):
            cols = pl.ds(pl.multiple_of(j * LANES, LANES), LANES)
            to(pl.ds(pl.multiple_of(lanes + j * LANES, LANES), LANES), dot(act[lo:hi, :], wgu[ffp : 2 * ffp, cols]))
            return carry

        lax.fori_loop(0, lanes // LANES, low, 0)
        lax.fori_loop(0, (width - lanes) // LANES, high, 0)

    output = Halving(1)

    output.first(lambda: down_step(half, count, to_send))
    down_step(0, half, to_own)
    spread_wait(0)
    spread_send(1)
    output.second()
    ring_c.pump(2)
    ring_d.pump(2)
    spread_wait(1)

    waiting["wout"].wait()
    waiting["ctx"].wait()
    dctx[...] = dot_cols(dm_all[...], wout[...]).astype(BF16)
    outer(sum_b, ctx, dm_all, part)
    ring_b.begin()
    cot[...] = (mid[...] + output.total()).astype(BF16)
    output.sent()

    for name in ("qkv", "stat"):
        waiting[name].wait()
    for copy in rotary:
        copy.wait()
    scale = HEAD_DIM ** (-0.5)
    per = LANES // HEAD_DIM
    lane = lax.broadcasted_iota(jnp.int32, (1, LANES), 1) // HEAD_DIM

    def turned(z, span):
        return (
            z * rot[span, :LANES]
            - pltpu.roll(z, LANES - ROT // 2, 1) * rot[span, LANES : 2 * LANES]
            - pltpu.roll(z, ROT // 2, 1) * rot[span, 2 * LANES :]
        )

    bias_v[...] = jnp.zeros_like(bias_v)
    for pair in range(part // LANES):
        at = pair * LANES
        dk[...] = jnp.zeros_like(dk)
        dv[...] = jnp.zeros_like(dv)

        def attend(i, carry, pair=pair, at=at):
            span = pl.ds(pl.multiple_of(i * rows, rows), rows)
            q = qkv[span, at : at + LANES]
            k = qkv[:, part + at : part + at + LANES]
            v = qkv[:, 2 * part + at : 2 * part + at + LANES]
            dc = dctx[span, at : at + LANES]
            both = dc.astype(F32) * ctx[span, at : at + LANES].astype(F32)
            allowed = pos_k[0:1, :] <= stat[span, SPOT : SPOT + 1]
            dq = jnp.zeros((rows, LANES), F32)
            for h in range(per):
                pick = lane == h
                mine = pick.astype(BF16)
                qm, dcm = q * mine, dc * mine
                scores = dot_cols(qm, k) * scale
                at_lse = LSE + pair * per + h
                probs = jnp.exp(jnp.where(allowed, scores, -jnp.inf) - stat[span, at_lse : at_lse + 1])
                delta = jnp.sum(jnp.where(pick, both, 0.0), axis=-1, keepdims=True)
                ds = (probs * (dot_cols(dcm, v) - delta) * scale).astype(BF16)
                dq = dq + jnp.dot(ds, k * mine, preferred_element_type=F32)
                dk[...] += dot(flip(ds), qm)
                dv[...] += dot(flip(probs.astype(BF16)), dcm)
            dq = turned(dq, span)
            bias_v[0:1, at : at + LANES] += jnp.sum(dq, axis=0, keepdims=True)
            dqkv[span, at : at + LANES] = dq.astype(BF16)
            return carry

        lax.fori_loop(0, m, attend, 0)

        def settle(i, carry, at=at):
            span = pl.ds(pl.multiple_of(i * rows, rows), rows)
            key, value = turned(dk[span, :], span), dv[span, :]
            bias_v[0:1, part + at : part + at + LANES] += jnp.sum(key, axis=0, keepdims=True)
            bias_v[0:1, 2 * part + at : 2 * part + at + LANES] += jnp.sum(value, axis=0, keepdims=True)
            dqkv[span, part + at : part + at + LANES] = key.astype(BF16)
            dqkv[span, 2 * part + at : 2 * part + at + LANES] = value.astype(BF16)
            return carry

        lax.fori_loop(0, m, settle, 0)
        if pair == 0:
            ring_c.pump(3)

    waiting["n1"].wait()
    outer(sum_a, wide_b, dqkv, width)
    ring_a.begin()
    ring_d.pump(3)
    ring_b.pump(1)
    waiting["wqkv"].wait()
    waiting["tok"].wait()
    normed1 = Halving(2)

    def gains(cols, value, lo, hi):
        xh = (wide_a[lo:hi, cols].astype(F32) - stat[lo:hi, MEAN : MEAN + 1]) * stat[lo:hi, RSTD : RSTD + 1]
        return jnp.sum(value * xh, axis=0, keepdims=True), jnp.sum(value, axis=0, keepdims=True)

    def far_last(cols, value):
        send1[:, cols] = value.astype(BF16)
        sums_v[0:1, cols], sums_v[1:2, cols] = gains(cols, value, half, count)

    def near_last(cols, value):
        own[:, cols] = value
        gain, total = gains(cols, value, 0, half)
        sums_v[0:1, cols] += gain
        sums_v[1:2, cols] += total

    normed1.first(lambda: back_step(dqkv, half, count, wqkv, far_last))
    back_step(dqkv, 0, half, wqkv, near_last)

    sum_v[...] = jnp.zeros_like(sum_v)
    units = slab // LANES

    def lay(c, carry):
        for i in range(4):
            for u in range(units):
                at = pl.multiple_of(c * slab + u * LANES, LANES)
                sum_v[pl.ds(c * vec_rows + i * units + u, 1), :] = sums_v[i : i + 1, pl.ds(at, LANES)]
        return carry

    lax.fori_loop(0, n, lay, 0)
    for i in range(3):
        for u in range(part // LANES):
            unit = i * (inner // LANES) + place.shards[u]
            row = lax.div(unit, b_units) * vec_rows + 4 * units + lax.rem(unit, b_units)
            at = i * part + u * LANES
            sum_v[pl.ds(row, 1), :] = bias_v[0:1, at : at + LANES]
    ring_v.begin()
    normed1.second()
    ring_b.pump(2)
    ring_a.pump(1)
    ring_v.pump(1)
    ring_c.pump(4)
    got_gu = deal(sum_c, slab, x_gu)
    ring_d.pump(4)
    turn_back(0)
    ring_b.pump(3)
    ring_a.pump(2)
    ring_v.pump(2)
    up = normed1.total()
    rstd = stat[:rows, RSTD : RSTD + 1]
    xhat = (wide_a[:rows, :].astype(F32) - stat[:rows, MEAN : MEAN + 1]) * rstd
    own[:rows, :] = d_mid[...] + norm_back(up, xhat, rstd, rows_v[0:1, :])
    ring_b.pump(4)
    ring_v.pump(3)

    written = []

    def store(src, dst):
        copy = pltpu.make_async_copy(src, dst, outs.at[len(written)])
        copy.start()
        written.append(copy)

    store(cot, o_block)
    store(own.at[pl.ds(0, rows)], o_input)
    turn_back(1)
    ring_a.pump(3)

    turned_back(0)
    lane128 = lax.broadcasted_iota(jnp.int32, (1, LANES), 1)

    def lay_out(got, to):
        share, shard, hidden = slab // m, ff // 2, ff * m
        found = {}
        for t in range(m):
            span = slice(t * share, (t + 1) * share)
            tiles = [[], []]
            at = 0
            for _, units_, _ in blocks_of(ff):
                even = units_ // LANES
                tiles[0] += [got[span, at + k * LANES : at + (k + 1) * LANES].astype(F32) for k in range(even)]
                at += even * LANES
                odd = []
                if even * LANES < units_:
                    mixed = got[span, at : at + LANES].astype(F32)
                    odd = [mixed, pltpu.roll(mixed, LANES // 2, 1)]
                    at += LANES
                tiles[1] += [got[span, at + k * LANES : at + (k + 1) * LANES].astype(F32) for k in range(even)]
                at += even * LANES
                if odd:
                    tiles[0].append(odd[0])
                    tiles[1].append(odd[1])
            for i in range(2):
                for u, held in enumerate(shards_of(t, n)):
                    start, first, end = u * shard, i * hidden + held * shard, i * hidden + (held + 1) * shard
                    shift = (first - start) % LANES
                    back = (first - start - shift) // LANES
                    for tile in range(first // LANES, (end - 1) // LANES + 1):
                        k = tile - back
                        parts_ = [tiles[i][q] if 0 <= q < len(tiles[i]) else None for q in (k, k - 1)]
                        if shift:
                            here, before = [None if p is None else pltpu.roll(p, shift, 1) for p in parts_]
                            if here is None or before is None:
                                value = before if here is None else here
                            else:
                                value = jnp.where(lane128 < shift, before, here)
                        else:
                            value = parts_[0]
                        lo, hi = max(first, tile * LANES), min(end, (tile + 1) * LANES)
                        found.setdefault(tile, []).append((lo - tile * LANES, hi - tile * LANES, value))
        for tile, parts_ in found.items():
            parts_.sort(key=lambda p: p[0])
            value = parts_[-1][2]
            for _, hi, other in reversed(parts_[:-1]):
                value = jnp.where(lane128 < hi, other, value)
            to[:, tile * LANES : (tile + 1) * LANES] = value.astype(BF16)

    some = down_rows // 2
    value = x_down[...].astype(F32)
    d_mid[:some, :down_cols] = value[:some, :]
    d_mid[:some, down_cols:] = value[some:, :]
    column = lax.rem(s, 2)
    across = pl.ds(pl.multiple_of(column * down_cols, down_cols), down_cols)
    swap = sender.start(
        sender.slot(),
        d_mid.at[pl.ds(0, some), pl.ds(pl.multiple_of((1 - column) * down_cols, down_cols), down_cols)],
        y_down.at[:, across],
        place.seqs[1],
    )
    y_down[:, across] = d_mid[:some, across]
    ring_v.pump(4)
    got_vec = deal(sum_v, vec_rows, x_vec, whole=True)
    for copy in got_gu:
        copy.wait_recv()
    lay_out(x_gu, y_gu)
    store(y_gu, o_gu)
    turned_back(1)
    store(x_out, o_out)
    swap.wait_recv()
    store(y_down, o_down)
    for copy in got_vec:
        copy.wait_recv()
    total = x_vec[:vec_rows, :]
    for t in range(1, m):
        total = total + x_vec[t * vec_rows : (t + 1) * vec_rows, :]
    x_vec[:vec_rows, :] = total
    some = slab // m
    sizes = [(i * units, some) for i in range(4)] + [(4 * units, b_units * LANES // m)]
    for i, (first_row, size) in enumerate(sizes):
        tile = lax.div(s * size, LANES)
        shift = s * size - tile * LANES
        low = x_vec[pl.ds(first_row + tile, 1), :]
        high = x_vec[pl.ds(first_row + tile + 1, 1), :]
        both = jnp.where(lane128 < shift, high, low)
        sums_v[i : i + 1, :LANES] = pltpu.roll(both, lax.rem(LANES - shift, LANES), 1)
    store(sums_v.at[:, pl.ds(0, LANES)], o_vec)
    ring_a.pump(4)
    got_qkv = deal(sum_a, slab, x_qkv)
    for copy in got_qkv:
        copy.wait_recv()
    share = slab // m
    for t in range(m):
        for i in range(3):
            for u, held in enumerate(shards_of(t, n)):
                at, come = i * inner + held * LANES, i * part + u * LANES
                y_qkv[:, at : at + LANES] = x_qkv[t * share : (t + 1) * share, come : come + LANES]
    store(y_qkv, o_qkv)
    for copy in written:
        copy.wait()
    sender.finish()

    @pl.when(moves)
    def _():
        for ring, landing, slot in turns:
            sender.copy(slot, ring.mine(), landing, place.source).wait_send()


def run_backward(dims, args):
    n, m, rows, width, slab, part, ff, b_units = dims
    count = rows * m
    ffp = -(-ff // 256) * 256
    vec_rows = -(-(4 * (slab // LANES) + b_units) // TILE) * TILE
    half = n // 2
    out_rows = part // n
    down_rows, down_cols = 2 * ff // n, width // 2
    share = slab // m

    def inbox(slots, dtype=BF16):
        return vmem(slots.inbox(half), dtype)

    outputs = [
        ((rows, width), BF16), ((rows, width), F32), ((share, 2 * ff * m), BF16), ((share, 3 * part * m), BF16),
        ((down_rows // 2, width), F32), ((out_rows, width), BF16), ((8, LANES), F32),
    ]
    scratch = [
        vmem((part, width)), vmem((width, 2 * ff)), vmem((width, 3 * part)), vmem((8, width), F32),
        vmem((count, width)), vmem((count, width)), vmem((count, 3 * part)), vmem((count, LANES), F32),
        vmem((count, part)), vmem((rows, width), F32), vmem((count, ffp)), vmem((count, 2 * ff)),
        vmem((count, 3 * LANES), F32), vmem((8, count), F32),
        vmem((n * slab, 3 * part)), vmem((part, width)), vmem((n * slab, 2 * ff)), vmem((ffp, width)),
        vmem((n * vec_rows, LANES), F32),
        inbox(RowSlots(slab, 3 * part)), inbox(RowSlots(out_rows, width)), inbox(RowSlots(slab, 2 * ff)),
        inbox(TileSlots(down_rows, down_cols)), inbox(RowSlots(vec_rows, LANES), F32),
        vmem((count // 2, width), F32), vmem((count // 2, width)), vmem((rows, width)),
        vmem((3 * count // 2, width)), vmem((3 * rows, width)),
        vmem((count, width)), vmem((rows, width), F32), vmem((rows, width)), vmem((count, part)), vmem((count, 3 * part)),
        vmem((count, LANES), F32), vmem((count, LANES), F32), vmem((8, width), F32), vmem((8, 3 * part), F32),
        vmem((slab, 2 * ff)), vmem((slab, 3 * part)), vmem((down_rows, down_cols)),
        vmem((out_rows, width)), vmem((m * vec_rows, LANES), F32), vmem((share, 3 * part * m)),
        vmem((down_rows // 2, width), F32), vmem((share, 2 * ff * m)),
    ]
    slots = 5 * 2 * half + 3 * 2 + 2 + 2 + 3 * (m - 1) + 1
    return pl.pallas_call(
        functools.partial(backward_kernel, dims),
        out_shape=[jax.ShapeDtypeStruct(*a) for a in outputs],
        in_specs=[pl.BlockSpec(memory_space=pl.ANY)] * len(args),
        out_specs=[pl.BlockSpec(memory_space=pl.ANY)] * len(outputs),
        scratch_shapes=scratch
        + [
            pltpu.SemaphoreType.DMA((slots,)),
            pltpu.SemaphoreType.DMA((slots,)),
            pltpu.SemaphoreType.DMA((len(args) + 12,)),
            pltpu.SemaphoreType.DMA((len(outputs),)),
        ],
        compiler_params=pltpu.CompilerParams(
            collective_id=1, has_side_effects=True, vmem_limit_bytes=VMEM_BYTES
        ),
        name="backward",
    )(*args)


def rotary_lines(length):
    half = ROT // 2
    lane = np.arange(LANES) % HEAD_DIM
    angles = np.arange(length)[:, None] * (10000.0 ** (-(lane % half) * 2.0 / ROT))[None, :]
    cosine, sine = np.cos(angles), np.sin(angles)
    lines = [
        np.where(lane < ROT, cosine, 1.0),
        np.where(lane < half, -sine, 0.0),
        np.where((lane >= half) & (lane < ROT), sine, 0.0),
    ]
    return jnp.asarray(np.concatenate(lines, axis=1), F32)


def shards(tokens, cotangent, gain1, bias1, w_qkv, b_qkv, w_out, gain2, bias2, w_gate_up, w_down):
    n, m, s = lax.axis_size("dp"), lax.axis_size("seq"), lax.axis_index("seq")
    rows, width = tokens.shape
    slab = gain1.shape[0]
    inner, hidden = w_out.shape[0] * n, w_down.shape[0] * n
    part, ff = inner // m, hidden // m
    dims = (n, m, rows, width, slab, part, ff, b_qkv.shape[0] // LANES)
    vec = jnp.concatenate([gain1, bias1, gain2, bias2, b_qkv]).astype(F32).reshape(-1, LANES)
    vec = jnp.pad(vec, ((0, -vec.shape[0] % TILE), (0, 0)))
    rot = rotary_lines(rows * m)
    kept = run_forward(dims, (tokens, cotangent, w_qkv, w_gate_up, w_out, w_down, vec, rot))
    block_out, input_grad, g_gu, g_qkv, g_down, g_out, line = run_backward(dims, tuple(kept) + (rot,))
    vectors = [line[i, : size // m] for i, size in enumerate([slab] * 4 + [b_qkv.shape[0]])]
    return (
        block_out,
        input_grad,
        vectors[0],
        vectors[1],
        g_qkv.astype(F32),
        vectors[4],
        g_out.astype(F32),
        vectors[2],
        vectors[3],
        g_gu.astype(F32),
        g_down,
    )


def fits(mesh, shapes):
    n, m = mesh.shape["dp"], mesh.shape["seq"]
    (rows, width), slab = shapes[0], shapes[2][0]
    part, ff = shapes[6][0] * n // m, shapes[10][0] * n // m
    return (
        m == 4
        and n == 2 * m
        and rows % LANES == 0
        and shapes[6][0] == LANES
        and slab == 256
        and width % 512 == 0
        and shapes[5][0] % LANES == 0
        and part == 256
        and (ff // 2) + LANES - 1 <= WINDOW
        and ff // 2 + (ff // 2) % LANES <= WINDOW
        and shapes[9][1] // 2 % LANES == 0
        and 512 < ff <= 768
        and ff % 64 == 0
        and (2 * ff // n) % TILE == 0
        and 2 * ff <= width <= 4 * ff
        and 2 * 768 <= width
    )


def solution(mesh):
    rows, cols, vec = P(("dp", "seq"), None), P("dp", None), P("dp")
    flat = P(("dp", "seq"))
    def step(*args):
        body = shards if fits(mesh, [a.shape for a in args]) else shards_plain
        return body(*args)

    return jax.shard_map(
        step,
        mesh=mesh,
        in_specs=(rows, rows, vec, vec, cols, vec, cols, vec, vec, cols, cols),
        out_specs=(rows, rows, flat, flat, rows, flat, rows, flat, flat, rows, rows),
        check_vma=False,
    )
```

```python
import functools

import jax
import jax.numpy as jnp
import numpy as np
from jax import lax
from jax.experimental import pallas as pl
from jax.experimental.pallas import tpu as pltpu
from jax.sharding import PartitionSpec as P

HEAD_DIM = 64
ROT = 16
EPS = 1e-05
F32 = jnp.float32
BF16 = jnp.bfloat16


def ring_order(n):
    return list(range(0, n, 2)) + list(range(n - 1, 0, -2))


def dot(a, b):
    return jnp.dot(a, b, preferred_element_type=F32)


def dot_rows(a, b):
    return lax.dot_general(a, b, (((0,), (0,)), ((), ())), preferred_element_type=F32)


def dot_cols(a, b):
    return lax.dot_general(a, b, (((1,), (1,)), ((), ())), preferred_element_type=F32)


class Ring:
    def __init__(self):
        n = lax.axis_size("dp")
        order = ring_order(n)
        place = [order.index(i) for i in range(n)]
        self.n, self.half = n, n // 2
        self.right = [(order[i], order[(i + 1) % n]) for i in range(n)]
        self.left = [(b, a) for a, b in self.right]
        self.order = jnp.array(order, jnp.int32)
        self.place = jnp.array(place, jnp.int32)[lax.axis_index("dp")]

    def owner(self, offset):
        return self.order[lax.rem(self.place + offset + self.n, self.n)]

    def go_right(self, value):
        return lax.ppermute(value, "dp", self.right)

    def go_left(self, value):
        return lax.ppermute(value, "dp", self.left)

    def gather(self, piece):
        rows = piece.shape[0]
        cut = rows // 2
        from_left = from_right = piece
        whole = jnp.zeros((self.n,) + piece.shape, piece.dtype)

        def put(whole, offset, chunk):
            return lax.dynamic_update_slice(
                whole, chunk[None], (self.owner(offset),) + (0,) * piece.ndim
            )

        whole = put(whole, 0, piece)
        for k in range(1, self.half):
            from_left = self.go_right(from_left)
            from_right = self.go_left(from_right)
            whole = put(put(whole, -k, from_left), k, from_right)
        upper = self.go_right(from_left[:cut])
        lower = self.go_left(from_right[cut:])
        return put(whole, self.half, jnp.concatenate([upper, lower]))

    def scatter(self, parts):
        rows = parts.shape[1]
        cut = rows // 2

        def mine(offset):
            start = (self.owner(offset),) + (0,) * (parts.ndim - 1)
            return lax.dynamic_slice(parts, start, (1,) + parts.shape[1:])[0]

        def add(a, b):
            return a.astype(F32) + b.astype(F32)

        far = mine(self.half)
        upper = self.go_right(far[:cut])
        lower = self.go_left(far[cut:])
        from_left, from_right = mine(self.half - 1), mine(1 - self.half)
        from_left = jnp.concatenate(
            [add(from_left[:cut], upper).astype(BF16), from_left[cut:]]
        )
        from_right = jnp.concatenate(
            [from_right[:cut], add(from_right[cut:], lower).astype(BF16)]
        )
        for k in range(self.half - 2, -1, -1):
            from_left = self.go_right(from_left)
            from_right = self.go_left(from_right)
            if k:
                from_left = add(from_left, mine(k)).astype(BF16)
                from_right = add(from_right, mine(-k)).astype(BF16)
        return add(mine(0), from_left) + from_right.astype(F32)


class Group:
    def __init__(self):
        self.m = lax.axis_size("seq")
        self.s = lax.axis_index("seq")
        self.bits = []
        bit = self.m // 2
        while bit:
            self.bits.append(bit)
            bit //= 2
        self.offsets = [0]
        for bit in self.bits:
            self.offsets += [o ^ bit for o in self.offsets]

    def swap(self, value, mask):
        return lax.ppermute(value, "seq", [(i, i ^ mask) for i in range(self.m)])

    def gather(self, value):
        for bit in self.bits:
            value = jnp.concatenate([value, self.swap(value, bit)])
        return value

    def scatter(self, value):
        for bit in reversed(self.bits):
            half = value.shape[0] // 2
            got = self.swap(value[half:].astype(BF16), bit)
            value = value[:half] + got.astype(F32)
        return value

    def exchange(self, blocks):
        got = []
        for mask in range(self.m):
            block = lax.dynamic_index_in_dim(blocks, self.s ^ mask, 0, keepdims=False)
            got.append(self.swap(block, mask) if mask else block)
        stacked = jnp.stack(got)
        return jnp.take(stacked, self.s ^ jnp.arange(self.m), axis=0)


def norm(value):
    center = value - jnp.mean(value, axis=-1, keepdims=True)
    rstd = lax.rsqrt(jnp.mean(center * center, axis=-1, keepdims=True) + EPS)
    return center * rstd, rstd


def norm_back(upstream, xhat, rstd, gain):
    e = upstream * gain
    inner = (
        e
        - jnp.mean(e, axis=-1, keepdims=True)
        - xhat * jnp.mean(e * xhat, axis=-1, keepdims=True)
    )
    return rstd * inner


def rotary_tables(positions):
    half = ROT // 2
    inverse = 10000.0 ** (-(jnp.arange(half, dtype=F32) * 2.0 / ROT))
    angles = positions.astype(F32)[:, None] * inverse[None, :]
    return jnp.cos(angles)[:, None, :], jnp.sin(angles)[:, None, :]


def rotate(tensor, cosine, sine):
    half = ROT // 2
    a, b = tensor[..., :half], tensor[..., half:ROT]
    return jnp.concatenate([a * cosine - b * sine, b * cosine + a * sine, tensor[..., ROT:]], axis=-1)


def shards_plain(tokens, cotangent, gain1, bias1, w_qkv, b_qkv, w_out, gain2, bias2, w_gate_up, w_down):
    ring, group = Ring(), Group()
    n, m, s = ring.n, group.m, group.s
    rows, width = tokens.shape
    slab = gain1.shape[0]
    inner = w_out.shape[0] * n
    hidden = w_down.shape[0] * n
    part, ff = inner // m, hidden // m
    heads = part // HEAD_DIM
    scale = HEAD_DIM ** (-0.5)

    both = jnp.stack([tokens, cotangent], axis=1)
    everything = group.gather(both)
    tokens_all, cot_all = everything[:, 0], everything[:, 1]

    qkv_piece = jnp.concatenate(
        [lax.dynamic_slice(w_qkv, (0, i * inner + s * part), (slab, part)) for i in range(3)], axis=1
    )
    small = jnp.concatenate([gain1, bias1, gain2, bias2, b_qkv])
    extra = -(-small.shape[0] // (3 * part))
    small = jnp.pad(small, (0, extra * 3 * part - small.shape[0])).reshape(extra, 3 * part)
    first = ring.gather(jnp.concatenate([qkv_piece, small]))
    wqkv = first[:, :slab].reshape(width, 3 * part)
    vectors = first[:, slab:].reshape(n, -1)

    def vector(at, size):
        return vectors[:, at : at + size].reshape(-1).astype(F32)

    g1, b1, g2, b2 = (vector(i * slab, slab) for i in range(4))
    bias_all = vector(4 * slab, b_qkv.shape[0]).reshape(3, m, part)
    bias_qkv = lax.dynamic_index_in_dim(bias_all, s, 1, keepdims=False).reshape(3 * part)

    turn = [(g, (g % n) * m + g // n) for g in range(n * m)]
    back = [(b, a) for a, b in turn]

    def quarter(weight):
        count = weight.shape[0] // m
        mine = lax.dynamic_slice(weight, (0, 0), weight.shape)
        return mine.reshape(m, count, weight.shape[1])[s]

    out_rows, down_rows = w_out.shape[0] // m, w_down.shape[0] // m
    moved = lax.ppermute(
        jnp.concatenate([quarter(w_out), quarter(w_down)]), ("dp", "seq"), turn
    )
    wout = ring.gather(moved[:out_rows]).reshape(part, width)
    gu_piece = jnp.concatenate(
        [lax.dynamic_slice(w_gate_up, (0, i * hidden + s * ff), (slab, ff)) for i in range(2)], axis=1
    )
    wgu = ring.gather(gu_piece).reshape(width, 2 * ff)
    wdown = ring.gather(moved[out_rows:]).reshape(ff, width)

    places = jnp.concatenate([(s ^ o) * rows + jnp.arange(rows, dtype=jnp.int32) for o in group.offsets])
    cosine, sine = rotary_tables(places)
    count = rows * m
    xhat1, rstd1 = norm(tokens_all.astype(F32))
    normed1 = (xhat1 * g1 + b1).astype(BF16)
    qkv = (dot(normed1, wqkv) + bias_qkv).reshape(count, 3, heads, HEAD_DIM)
    queries = rotate(qkv[:, 0], cosine, sine).astype(BF16)
    keys = rotate(qkv[:, 1], cosine, sine).astype(BF16)
    values = qkv[:, 2].astype(BF16)
    scores = jnp.einsum("qhd,khd->hqk", queries, keys, preferred_element_type=F32) * scale
    scores = jnp.where((places[None, :] <= places[:, None])[None], scores, -jnp.inf)
    top = jnp.max(scores, axis=-1, keepdims=True)
    lse = top + jnp.log(jnp.sum(jnp.exp(scores - top), axis=-1, keepdims=True))
    probs = jnp.exp(scores - lse)
    probs_r = probs.astype(BF16)
    context = jnp.einsum("hqk,khd->qhd", probs_r, values, preferred_element_type=F32).astype(BF16)
    context_flat = context.reshape(count, part)
    x_own = tokens.astype(F32)
    mid = x_own + group.scatter(dot(context_flat, wout))
    xhat2, rstd2 = norm(mid)
    normed2 = group.gather((xhat2 * g2 + b2).astype(BF16))
    gate_up = dot(normed2, wgu)
    gate, up = gate_up[:, :ff], gate_up[:, ff:]
    sigma = jax.nn.sigmoid(gate)
    silu = gate * sigma
    act = (silu * up).astype(BF16)
    d_act = dot_cols(cot_all, wdown)
    d_gate = d_act * up * (sigma * (1.0 + gate * (1.0 - sigma)))
    d_gate_up = jnp.concatenate([d_gate, d_act * silu], axis=1).astype(BF16)

    d_normed2 = group.scatter(dot_cols(d_gate_up, wgu))
    sum_down = ring.scatter(dot_rows(act, cot_all).astype(BF16).reshape(n, ff // n, width))
    sum_gu = ring.scatter(dot_rows(normed2, d_gate_up).astype(BF16).reshape(n, slab, 2 * ff))
    block_out = (mid + group.scatter(dot(act, wdown))).astype(BF16)
    d_mid = cotangent.astype(F32) + norm_back(d_normed2, xhat2, rstd2, g2)
    d_mid_r = group.gather(d_mid.astype(BF16))

    d_context = dot_cols(d_mid_r, wout).astype(BF16).reshape(count, heads, HEAD_DIM)
    sum_out = ring.scatter(dot_rows(context_flat, d_mid_r).astype(BF16).reshape(n, part // n, width))
    d_probs = jnp.einsum("qhd,khd->hqk", d_context, values, preferred_element_type=F32)
    delta = jnp.einsum("qhd,qhd->hq", d_context.astype(F32), context.astype(F32))[..., None]
    d_scores = (probs * (d_probs - delta) * scale).astype(BF16)
    d_queries = jnp.einsum("hqk,khd->qhd", d_scores, keys, preferred_element_type=F32)
    d_keys = jnp.einsum("hqk,qhd->khd", d_scores, queries, preferred_element_type=F32)
    d_values = jnp.einsum("hqk,qhd->khd", probs_r, d_context, preferred_element_type=F32)
    d_qkv = jnp.stack(
        [rotate(d_queries, cosine, -sine), rotate(d_keys, cosine, -sine), d_values], axis=1
    ).reshape(count, 3 * part)
    d_qkv_r = d_qkv.astype(BF16)
    d_normed1_part = dot_cols(d_qkv_r, wqkv)
    d_normed1 = group.scatter(d_normed1_part)
    own = (slice(0, rows),)
    input_grad = d_mid + norm_back(d_normed1, xhat1[own], rstd1[own], g1)

    bias_part = jnp.zeros((3, m, part), F32)
    bias_part = lax.dynamic_update_slice(bias_part, jnp.sum(d_qkv, axis=0).reshape(3, 1, part), (0, s, 0))
    vector_parts = [
        jnp.sum(d_normed1_part * xhat1, axis=0),
        jnp.sum(d_normed1_part, axis=0),
        jnp.sum(d_normed2 * xhat2, axis=0),
        jnp.sum(d_normed2, axis=0),
        bias_part.reshape(-1),
    ]
    line = jnp.concatenate([v.reshape(n, m, -1) for v in vector_parts], axis=-1)
    lines = -(-line.shape[-1] // (3 * part))
    line = jnp.pad(line, ((0, 0), (0, 0), (0, lines * 3 * part - line.shape[-1])))
    line = line.reshape(n, m, lines, 3 * part).astype(BF16)
    part_qkv = dot_rows(normed1, d_qkv_r).astype(BF16).reshape(n, m, slab // m, 3 * part)
    packed = jnp.concatenate([part_qkv, line], axis=2)
    packed_rows = packed.shape[2]
    sum_qkv = ring.scatter(packed.reshape(n, m * packed_rows, 3 * part))

    def owners(total):
        return group.exchange(total.astype(BF16).reshape((m, -1) + total.shape[1:])).astype(F32)

    last = owners(sum_qkv)
    g_qkv = last[:, : slab // m].reshape(m, slab // m, 3, part).transpose(1, 2, 0, 3)
    g_qkv = g_qkv.reshape(slab // m, 3 * inner)
    line = jnp.sum(last[:, slab // m :], axis=0).reshape(-1)
    sizes = [slab // m] * 4 + [b_qkv.shape[0] // m]
    vectors_out, at = [], 0
    for size in sizes:
        vectors_out.append(line[at : at + size])
        at += size
    g_gu = owners(sum_gu).reshape(m, slab // m, 2, ff).transpose(1, 2, 0, 3).reshape(slab // m, 2 * hidden)
    g_down = lax.ppermute(sum_down.astype(BF16), ("dp", "seq"), back).astype(F32)
    g_out = lax.ppermute(sum_out.astype(BF16), ("dp", "seq"), back).astype(F32)
    return (
        block_out,
        input_grad,
        vectors_out[0],
        vectors_out[1],
        g_qkv,
        vectors_out[4],
        g_out,
        vectors_out[2],
        vectors_out[3],
        g_gu,
        g_down,
    )


LOGICAL = pl.DeviceIdType.LOGICAL
MEAN, RSTD, SPOT, LSE = 0, 1, 2, 8
LANES = 128
TILE = 16
WINDOW = 512
VMEM_BYTES = 67_043_328


def vmem(shape, dtype=BF16):
    return pltpu.VMEM(shape, dtype)


class Place:
    def __init__(self, n, m):
        self.n, self.m, self.half = n, m, n // 2
        self.d, self.s = lax.axis_index("dp"), lax.axis_index("seq")
        pair = lax.div(self.d, 2)
        odd = self.d - 2 * pair
        place = pair + odd * (n - 1 - 2 * pair)
        self.owners = []
        for offset in range(n):
            spot = lax.rem(place + offset, n)
            back = lax.div(spot, self.half)
            self.owners.append(2 * spot + back * (2 * n - 1 - 4 * spot))
        self.partners = []
        for mask in range(m):
            out, bit = self.s, 1
            while bit < m:
                if mask & bit:
                    out = out + bit - 2 * bit * lax.rem(lax.div(self.s, bit), 2)
                bit *= 2
            self.partners.append(out)
        self.rings = {1: self.owners[1] * m + self.s, -1: self.owners[n - 1] * m + self.s}
        self.seqs = [self.d * m + out for out in self.partners]
        inner_ = lax.rem(self.s, 2)
        side = lax.rem(lax.div(self.s, 2) + inner_, 2)
        self.shards = [2 * inner_ + side, n - 2 - 2 * inner_ + side]
        low = lax.div(self.d, m)
        self.source = (self.shards[0] + low * (self.shards[1] - self.shards[0])) * m + self.d - low * m
        across = lax.rem(lax.div(pair + 1, 2), 2)
        self.there = lax.div(self.d, m) * m + self.s
        self.target = self.there * m + 2 * lax.rem(odd + across, 2) + across
        here = self.d * m + self.s
        self.moves = (self.target - here) * (self.target - here) > 0

        offsets = [0]
        for bit in self.bits():
            offsets += [o ^ bit for o in offsets]
        self.homes = [self.partners[o] for o in offsets]

    def owner(self, offset):
        return self.owners[offset % self.n]

    def partner(self, mask):
        return self.partners[mask]

    def bits(self):
        out, bit = [], self.m // 2
        while bit:
            out.append(bit)
            bit //= 2
        return out


class Sender:
    def __init__(self, sends, recvs):
        self.sends, self.recvs = sends, recvs
        self.used = 0
        self.open = []

    def slot(self):
        self.used += 1
        return self.used - 1

    def copy(self, slot, src, dst, device):
        return pltpu.make_async_remote_copy(
            src_ref=src,
            dst_ref=dst,
            send_sem=self.sends.at[slot],
            recv_sem=self.recvs.at[slot],
            device_id=device,
            device_id_type=LOGICAL,
        )

    def start(self, slot, src, dst, device):
        copy = self.copy(slot, src, dst, device)
        copy.start()
        self.open.append(copy)
        return copy

    def finish(self):
        for copy in self.open:
            copy.wait_send()
        self.open = []


def greet(place, extra_seq=()):
    barrier = pltpu.get_barrier_semaphore()

    def hello(device):
        pl.semaphore_signal(barrier, inc=1, device_id=device, device_id_type=LOGICAL)

    near = [place.rings[1], place.rings[-1]] + [place.seqs[mask] for mask in tuple(place.bits()) + tuple(extra_seq)]
    for device in near:
        hello(device)

    @pl.when(place.moves)
    def _():
        hello(place.target)
        hello(place.source)
        pl.semaphore_wait(barrier, len(near) + 2)

    @pl.when(jnp.logical_not(place.moves))
    def _():
        pl.semaphore_wait(barrier, len(near))


class RowSlots:
    def __init__(self, rows, cols, lo=0):
        self.rows, self.cols, self.lo = rows, cols, lo

    def where(self, index, part=None):
        rows, start = self.rows, index * self.rows
        if part is not None:
            rows = rows // 2
            start = start + part * rows
        return pl.ds(pl.multiple_of(start, rows), rows), pl.ds(self.lo, self.cols)

    def landing(self, way, j, half):
        base = way * ((half - 1) * self.rows + self.rows // 2)
        at, rows = (base + (half - 1) * self.rows, self.rows // 2) if j == 1 else (base + (j - 2) * self.rows, self.rows)
        return pl.ds(at, rows), pl.ds(0, self.cols)

    def inbox(self, half):
        return 2 * ((half - 1) * self.rows + self.rows // 2), self.cols


class TileSlots:
    def __init__(self, rows, cols):
        self.rows, self.cols = rows, cols

    def where(self, index, part=None):
        row = lax.div(index, 2)
        cols, start = self.cols, (index - 2 * row) * self.cols
        if part is not None:
            cols = cols // 2
            start = start + part * cols
        return pl.ds(pl.multiple_of(row * self.rows, self.rows), self.rows), pl.ds(pl.multiple_of(start, cols), cols)

    def landing(self, way, j, half):
        at, cols = ((half - 1) * self.cols, self.cols // 2) if j == 1 else ((j - 2) * self.cols, self.cols)
        return pl.ds(way * self.rows, self.rows), pl.ds(at, cols)

    def inbox(self, half):
        return 2 * self.rows, (half - 1) * self.cols + self.cols // 2


class Gather:
    def __init__(self, place, sender, buf, slots):
        self.place, self.sender, self.buf, self.slots = place, sender, buf, slots
        self.sems = [[sender.slot() for _ in range(place.half)] for _ in range(2)]
        self.devices = (place.rings[1], place.rings[-1])

    def own(self):
        return self.buf.at[self.slots.where(self.place.d)]

    def send(self, k, way):
        index = self.place.owner(k if way else -k)
        ref = self.buf.at[self.slots.where(index, way if k == self.place.half - 1 else None)]
        self.sender.start(self.sems[way][k], ref, ref, self.devices[way])

    def begin(self):
        self.send(0, 0)
        self.send(0, 1)

    def pump(self, k):
        last = k == self.place.half
        for way in range(2):
            index = self.place.owner(k if way else -k)
            ref = self.buf.at[self.slots.where(index, way if last else None)]
            self.sender.copy(self.sems[way][k - 1], ref, ref, self.devices[way]).wait_recv()
            if not last:
                self.send(k, way)


class Reduce:
    def __init__(self, place, sender, buf, inbox, slots):
        self.place, self.sender, self.buf, self.inbox, self.slots = place, sender, buf, inbox, slots
        self.sems = [[sender.slot() for _ in range(place.half)] for _ in range(2)]
        self.devices = (place.rings[1], place.rings[-1])

    def target(self, way, j):
        offset = self.place.half - j
        return self.slots.where(self.place.owner(-offset if way else offset), way if j == 1 else None)

    def copy(self, way, j):
        offset = self.place.half - j + 1
        src = self.slots.where(self.place.owner(-offset if way else offset), way if j == 1 else None)
        return self.sems[way][j - 1], self.buf.at[src], self.inbox.at[self.slots.landing(way, j, self.place.half)]

    def send(self, j, way):
        self.sender.start(*self.copy(way, j), self.devices[way])

    def begin(self):
        self.send(1, 0)
        self.send(1, 1)

    def add(self, to, *froms):
        value = self.buf[to].astype(F32)
        for at in froms:
            value = value + self.inbox[at].astype(F32)
        self.buf[to] = value.astype(self.buf.dtype)

    def pump(self, j):
        half = self.place.half
        for way in range(2):
            self.sender.copy(*self.copy(way, j), self.devices[way]).wait_recv()
            if j < half:
                self.add(self.target(way, j), self.slots.landing(way, j, half))
                self.send(j + 1, way)
        if j == half:
            self.add(self.slots.where(self.place.d), *(self.slots.landing(way, j, half) for way in range(2)))

    def mine(self):
        return self.buf.at[self.slots.where(self.place.d)]


def shards_of(s, n):
    inner = s % 2
    side = (s // 2 + inner) % 2
    return [2 * inner + side, n - 2 - 2 * inner + side]


def blocks_of(ff):
    return [(at, min(256, ff - at), 2 * at) for at in range(0, ff, 256)]


def key_spots(place, pos_k, rows):
    lane = lax.broadcasted_iota(jnp.int32, (8, rows), 1)
    for i, home in enumerate(place.homes):
        pos_k[:, i * rows : (i + 1) * rows] = (home * rows + lane).astype(F32)


def load_rotary(place, h_rot, rot, rows, sems, first):
    copies = []
    for i, home in enumerate(place.homes):
        src = h_rot.at[pl.ds(pl.multiple_of(home * rows, rows), rows)]
        copies.append(pltpu.make_async_copy(src, rot.at[pl.ds(i * rows, rows)], sems.at[first + i]))
        copies[-1].start()
    return copies


def forward_kernel(
    dims,
    tok, cot, h_wqkv, h_wgu, h_wout, h_wdown, piece_vec, h_rot,
    o_wqkv, o_wout, o_wgu, o_wdown, o_rows, o_tok, o_cot, o_n1, o_qkv, o_stat, o_ctx, o_mid, o_n2, o_act, o_dgu,
    wqkv, wout, wgu, wdown, vec, tok_all, cot_all, n1, qkv, stat, ctx, mid, n2, act, dgu,
    rows_v, bias_v, rot, pos_k, raw, own, send1, send2, recv1, recv2,
    sends, recvs, locals_, outs,
):
    n, m, rows, width, slab, part, ff, b_units = dims
    count = rows * m
    half = count // 2
    inner = part * m
    place = Place(n, m)
    sender = Sender(sends, recvs)
    d, s = place.d, place.s
    bits = place.bits()
    out_rows, vec_rows = part // n, piece_vec.shape[0]
    down_rows, down_cols = 2 * ff // n, width // 2
    blocks = blocks_of(ff)

    ring_a = Gather(place, sender, wqkv, RowSlots(slab, 3 * part))
    ring_v = Gather(place, sender, vec, RowSlots(vec_rows, LANES))
    ring_b = Gather(place, sender, wout, RowSlots(out_rows, width))
    ring_c = [Gather(place, sender, wgu, RowSlots(slab, 2 * units, lane)) for _, units, lane in blocks]
    ring_d = Gather(place, sender, wdown, TileSlots(down_rows, down_cols))

    def local(i, src, dst):
        copy = pltpu.make_async_copy(src, dst, locals_.at[i])
        copy.start()
        return copy

    own_rows = pl.ds(pl.multiple_of(d * slab, slab), slab)
    placed_qkv = [
        local(
            2 * i + u,
            h_wqkv.at[:, pl.ds(pl.multiple_of(i * inner + place.shards[u] * LANES, LANES), LANES)],
            wqkv.at[own_rows, pl.ds(i * part + u * LANES, LANES)],
        )
        for i in range(3)
        for u in range(2)
    ]
    placed_vec = local(6, piece_vec, ring_v.own())
    placed_tok = local(7, tok, tok_all.at[pl.ds(0, rows)])
    shard, hidden = ff // 2, h_wgu.shape[1] // 2
    window = raw.shape[2]
    shifts, placed_gu = [], []
    for i in range(2):
        for u in range(2):
            col = place.shards[u] * shard
            first_tile = lax.div(col + (0 if i == 0 else shard + LANES - 1 + hidden - window), LANES)
            base = first_tile * LANES
            shifts.append(col - base + i * hidden)
            src = h_wgu.at[:, pl.ds(pl.multiple_of(base, LANES), window)]
            placed_gu.append(local((8, 12 + m, 13 + m, 14 + m)[2 * i + u], src, raw.at[2 * i + u]))
    placed_cot = local(9, cot, cot_all.at[pl.ds(0, rows)])
    placed_rot = load_rotary(place, h_rot, rot, rows, locals_, 12)
    greet(place)
    moves = place.moves

    class Spread:
        def __init__(self, buf):
            self.buf = buf
            self.sems = [sender.slot() for _ in bits]

        def copy(self, i):
            size = rows << i
            return self.sems[i], self.buf.at[pl.ds(0, size)], self.buf.at[pl.ds(size, size)], place.seqs[bits[i]]

        def send(self, i):
            sender.start(*self.copy(i))

        def wait(self, i):
            sender.copy(*self.copy(i)).wait_recv()

    toks, cots, n2s = Spread(tok_all), Spread(cot_all), Spread(n2)
    written = []

    def write(src, dst):
        copy = pltpu.make_async_copy(src, dst, outs.at[len(written)])
        copy.start()
        written.append(copy)

    for copy in placed_qkv:
        copy.wait()
    ring_a.begin()
    placed_vec.wait()
    ring_v.begin()
    placed_tok.wait()
    toks.send(0)

    src_out = h_wout.at[pl.ds(pl.multiple_of(s * out_rows, out_rows), out_rows)]
    up = lax.div(s, 2)
    src_down = h_wdown.at[
        pl.ds(pl.multiple_of(up * down_rows, down_rows), down_rows),
        pl.ds(pl.multiple_of((s - 2 * up) * down_cols, down_cols), down_cols),
    ]
    turns = [(src_out, ring_b, sender.slot(), 10), (src_down, ring_d, sender.slot(), 11)]

    def turn(ring, index):
        return ring.buf.at[ring.slots.where(index)]

    @pl.when(moves)
    def _():
        for src, ring, slot, _ in turns:
            sender.copy(slot, src, turn(ring, place.there), place.target).start()

    @pl.when(jnp.logical_not(moves))
    def _():
        for src, ring, _, i in turns:
            local(i, src, ring.own()).wait()

    for copy in placed_gu:
        copy.wait()
    lane = lax.broadcasted_iota(jnp.int32, (1, LANES), 1)
    whole, rest = shard // LANES, shard % LANES

    def cut(j, carry):
        size = 64
        span = pl.ds(pl.multiple_of(j * size, size), size)
        tiles = []
        for i in range(2):
            low = pltpu.roll(raw[2 * i, span, :].astype(F32), window - shifts[2 * i], 1)
            high = pltpu.roll(
                raw[2 * i + 1, span, :].astype(F32), lax.rem(window + rest - shifts[2 * i + 1] + window, window), 1
            )
            lows = [low[:, t * LANES : (t + 1) * LANES] for t in range(whole + 1)]
            highs = [high[:, t * LANES : (t + 1) * LANES] for t in range(window // LANES)]
            tiles.append(lows[:whole] + [jnp.where(lane < rest, lows[whole], highs[0])] + highs[1:])
        to = pl.ds(pl.multiple_of(d * slab + j * size, size), size)
        at = 0
        for first_unit, count_, _ in blocks:
            even = count_ // LANES
            t = first_unit // LANES
            line_ = tiles[0][t : t + even]
            if even * LANES < count_:
                line_.append(jnp.where(lane < LANES // 2, tiles[0][t + even], pltpu.roll(tiles[1][t + even], LANES // 2, 1)))
            for tile in line_ + tiles[1][t : t + even]:
                wgu[to, at : at + LANES] = tile.astype(BF16)
                at += LANES
        return carry

    lax.fori_loop(0, slab // 64, cut, 0)
    ring_c[0].begin()
    placed_cot.wait()
    cots.send(0)
    wdown[ff:, :] = jnp.zeros((wdown.shape[0] - ff, width), BF16)
    key_spots(place, pos_k, rows)
    line = lax.broadcasted_iota(jnp.int32, (rows, 1), 0)

    def stats(i):
        span = slice(i * rows, (i + 1) * rows)
        x = tok_all[span, :].astype(F32)
        mu = jnp.mean(x, axis=-1, keepdims=True)
        c = x - mu
        r = lax.rsqrt(jnp.mean(c * c, axis=-1, keepdims=True) + EPS)
        spot = (place.homes[i] * rows + line).astype(F32)
        stat[span, :] = jnp.where(lane == MEAN, mu, jnp.where(lane == RSTD, r, spot))

    stats(0)
    ring_v.pump(1)
    ring_a.pump(1)

    @pl.when(moves)
    def _():
        for src, ring, slot, _ in turns:
            sender.copy(slot, src, ring.own(), place.source).wait_recv()

    ring_b.begin()
    toks.wait(0)
    toks.send(1)
    stats(1)
    ring_v.pump(2)
    ring_a.pump(2)
    ring_d.begin()
    ring_b.pump(1)
    toks.wait(1)
    write(tok_all, o_tok)
    stats(2)
    stats(3)
    cots.wait(0)
    cots.send(1)
    ring_v.pump(3)
    ring_a.pump(3)
    ring_c[1].begin()
    ring_b.pump(2)
    ring_c[0].pump(1)
    ring_v.pump(4)
    units = slab // LANES
    for c in range(n):
        for r in range(4):
            for u in range(units):
                at = c * slab + u * LANES
                row = c * vec_rows + r * units + u
                rows_v[r : r + 1, at : at + LANES] = vec[row : row + 1, :]
    for i in range(3):
        for u in range(part // LANES):
            unit = i * (inner // LANES) + place.shards[u]
            row = lax.div(unit, b_units) * vec_rows + 4 * units + lax.rem(unit, b_units)
            at = i * part + u * LANES
            bias_v[0:1, at : at + LANES] = vec[pl.ds(row, 1), :]
    write(rows_v, o_rows)

    def normalize(j, carry):
        size = 64
        span = pl.ds(pl.multiple_of(j * size, size), size)
        x = tok_all[span, :].astype(F32)
        xhat = (x - stat[span, MEAN : MEAN + 1]) * stat[span, RSTD : RSTD + 1]
        n1[span, :] = (xhat * rows_v[0:1, :] + rows_v[1:2, :]).astype(BF16)
        return carry

    lax.fori_loop(0, count // 64, normalize, 0)
    write(n1, o_n1)
    ring_d.pump(1)
    ring_c[2].begin()
    cots.wait(1)
    write(cot_all, o_cot)
    ring_a.pump(4)
    write(wqkv, o_wqkv)
    for copy in placed_rot:
        copy.wait()

    def project(j, carry):
        size = 256
        span = pl.ds(pl.multiple_of(j * size, size), size)
        for i in range(3):
            cols = slice(i * part, (i + 1) * part)
            y = dot(n1[span, :], wqkv[:, cols]) + bias_v[0:1, cols]
            if i < 2:
                pieces = []
                for u in range(part // LANES):
                    z = y[:, u * LANES : (u + 1) * LANES]
                    pieces.append(
                        z * rot[span, :LANES]
                        + pltpu.roll(z, LANES - ROT // 2, 1) * rot[span, LANES : 2 * LANES]
                        + pltpu.roll(z, ROT // 2, 1) * rot[span, 2 * LANES :]
                    )
                y = jnp.concatenate(pieces, axis=1)
            qkv[span, cols] = y.astype(BF16)
        return carry

    lax.fori_loop(0, count // 256, project, 0)
    write(qkv, o_qkv)
    ring_b.pump(3)
    ring_c[1].pump(1)
    ring_c[0].pump(2)
    scale = HEAD_DIM ** (-0.5)
    per = LANES // HEAD_DIM

    def attend(i, carry):
        pair, block = lax.div(i, m), lax.rem(i, m)
        span = pl.ds(pl.multiple_of(block * rows, rows), rows)
        at = pl.multiple_of(pair * LANES, LANES)
        q = qkv[span, pl.ds(at, LANES)]
        k = qkv[:, pl.ds(pl.multiple_of(part + at, LANES), LANES)]
        v = qkv[:, pl.ds(pl.multiple_of(2 * part + at, LANES), LANES)]
        allowed = pos_k[0:1, :] <= stat[span, SPOT : SPOT + 1]
        total = jnp.zeros((rows, LANES), F32)
        for h in range(per):
            mine = (lane // HEAD_DIM == h).astype(BF16)
            scores = dot_cols(q * mine, k) * scale
            scores = jnp.where(allowed, scores, -jnp.inf)
            top = jnp.max(scores, axis=-1, keepdims=True)
            found = top + jnp.log(jnp.sum(jnp.exp(scores - top), axis=-1, keepdims=True))
            probs = jnp.exp(scores - found).astype(BF16)
            total = total + dot(probs, v * mine)
            stat[span, :] = jnp.where(lane == LSE + pair * per + h, found, stat[span, :])
        ctx[span, pl.ds(at, LANES)] = total.astype(BF16)
        return carry

    lax.fori_loop(0, (part // LANES) * m, attend, 0)
    write(stat, o_stat)
    write(ctx, o_ctx)
    ring_d.pump(2)
    ring_c[2].pump(1)
    ring_b.pump(4)
    write(wout, o_wout)

    step = 512
    scatter = [sender.slot(), sender.slot()]

    def far_part(j, carry):
        cols = pl.ds(pl.multiple_of(j * step, step), step)
        send1[:, cols] = dot(ctx[half:, :], wout[:, cols]).astype(BF16)
        return carry

    lax.fori_loop(0, width // step, far_part, 0)
    first = sender.start(scatter[0], send1, recv1, place.seqs[bits[1]])

    def near_part(j, carry):
        cols = pl.ds(pl.multiple_of(j * step, step), step)
        own[:, cols] = dot(ctx[:half, :], wout[:, cols])
        return carry

    lax.fori_loop(0, width // step, near_part, 0)
    ring_c[1].pump(2)
    first.wait_recv()
    send2[...] = (own[rows:, :] + recv1[rows:, :].astype(F32)).astype(BF16)
    second = sender.start(scatter[1], send2, recv2, place.seqs[bits[0]])
    ring_c[0].pump(3)
    second.wait_recv()
    value = tok_all[:rows, :].astype(F32) + own[:rows, :] + recv1[:rows, :].astype(F32) + recv2[...].astype(F32)
    mid[...] = value
    c = value - jnp.mean(value, axis=-1, keepdims=True)
    r = lax.rsqrt(jnp.mean(c * c, axis=-1, keepdims=True) + EPS)
    n2[:rows, :] = (c * r * rows_v[2:3, :] + rows_v[3:4, :]).astype(BF16)
    n2s.send(0)
    write(mid, o_mid)
    ring_d.pump(3)
    ring_c[2].pump(2)
    ring_c[1].pump(3)
    n2s.wait(0)
    n2s.send(1)
    ring_c[0].pump(4)
    ring_d.pump(4)
    write(wdown, o_wdown)
    n2s.wait(1)
    write(n2, o_n2)
    ring_c[2].pump(3)

    def expand(first_unit, units, base):
        even = units // LANES * LANES
        y = dot(n2[...], wgu[:, base : base + 2 * units])
        d_act = dot_cols(cot_all[...], wdown[first_unit : first_unit + 256, :])
        if even == units:
            gate, up = y[:, :units], y[:, units:]
        else:
            gate = y[:, : even + LANES]
            up = jnp.concatenate([y[:, even + LANES :], pltpu.roll(gate[:, even:], LANES // 2, 1)], axis=1)
        sigma = jax.nn.sigmoid(gate)
        silu = gate * sigma
        value = silu * up
        d_gate = d_act * up * (sigma * (1.0 + gate * (1.0 - sigma)))
        d_up = d_act * silu
        if even == units:
            dgu[:, base : base + units] = d_gate.astype(BF16)
            dgu[:, base + units : base + 2 * units] = d_up.astype(BF16)
        else:
            value = jnp.where(lax.broadcasted_iota(jnp.int32, (1, 256), 1) < units, value, 0.0)
            mixed = jnp.where(lane < LANES // 2, d_gate[:, even:], pltpu.roll(d_up[:, even:], LANES // 2, 1))
            dgu[:, base : base + even] = d_gate[:, :even].astype(BF16)
            dgu[:, base + even : base + even + LANES] = mixed.astype(BF16)
            dgu[:, base + even + LANES : base + 2 * units] = d_up[:, :even].astype(BF16)
        act[:, first_unit : first_unit + 256] = value.astype(BF16)

    expand(*blocks[0])
    ring_c[1].pump(4)
    expand(*blocks[1])
    ring_c[2].pump(4)
    write(wgu, o_wgu)
    expand(*blocks[2])
    write(act, o_act)
    write(dgu, o_dgu)
    for copy in written:
        copy.wait()
    sender.finish()

    @pl.when(moves)
    def _():
        for src, ring, slot, _ in turns:
            sender.copy(slot, src, turn(ring, place.there), place.target).wait_send()


def run_forward(dims, args):
    n, m, rows, width, slab, part, ff, b_units = dims
    count = rows * m
    ffp = -(-ff // 256) * 256
    vec_rows = args[6].shape[0]
    arrays = [
        ((width, 3 * part), BF16), ((part, width), BF16), ((width, 2 * ff), BF16), ((ffp, width), BF16),
        ((8, width), F32), ((count, width), BF16), ((count, width), BF16), ((count, width), BF16),
        ((count, 3 * part), BF16), ((count, LANES), F32), ((count, part), BF16), ((rows, width), F32),
        ((count, width), BF16), ((count, ffp), BF16), ((count, 2 * ff), BF16),
    ]
    scratch = [vmem(*a) for a in arrays]
    rows_v, scratch[4] = scratch[4], vmem((n * vec_rows, LANES), F32)
    slots = (4 + len(blocks_of(ff))) * 2 * (n // 2) + 3 * 2 + 2 + 2
    return pl.pallas_call(
        functools.partial(forward_kernel, dims),
        out_shape=[jax.ShapeDtypeStruct(*a) for a in arrays],
        in_specs=[pl.BlockSpec(memory_space=pl.ANY)] * len(args),
        out_specs=[pl.BlockSpec(memory_space=pl.ANY)] * len(arrays),
        scratch_shapes=scratch
        + [
            rows_v,
            vmem((8, 3 * part), F32),
            vmem((count, 3 * LANES), F32),
            vmem((8, count), F32),
            vmem((4, slab, WINDOW)),
            vmem((count // 2, width), F32),
            vmem((count // 2, width)),
            vmem((rows, width)),
            vmem((count // 2, width)),
            vmem((rows, width)),
            pltpu.SemaphoreType.DMA((slots,)),
            pltpu.SemaphoreType.DMA((slots,)),
            pltpu.SemaphoreType.DMA((15 + m,)),
            pltpu.SemaphoreType.DMA((len(arrays),)),
        ],
        compiler_params=pltpu.CompilerParams(
            collective_id=0, has_side_effects=True, vmem_limit_bytes=VMEM_BYTES
        ),
        name="forward",
    )(*args)


def flip(value):
    size = value.shape[1]
    here = lax.broadcasted_iota(jnp.int32, (size, size), 0) == lax.broadcasted_iota(jnp.int32, (size, size), 1)
    return dot_cols(here.astype(F32).astype(BF16), value).astype(BF16)


def backward_kernel(
    dims,
    h_wqkv, h_wout, h_wgu, h_wdown, h_rows, h_tok, h_cot, h_n1, h_qkv, h_stat, h_ctx, h_mid, h_n2, h_act, h_dgu,
    h_rot,
    o_block, o_input, o_gu, o_qkv, o_down, o_out, o_vec,
    wout, wgu, wqkv, rows_v, wide_a, wide_b, qkv, stat, ctx, mid, act, dgu, rot, pos_k,
    sum_a, sum_b, sum_c, sum_d, sum_v, in_a, in_b, in_c0, in_c1, in_c2, in_d, in_v,
    own, send1, send2, recv1, recv2, dm_all, d_mid, cot, dctx, dqkv, dk, dv, sums_v, bias_v,
    x_gu, x_qkv, x_down, x_out, x_vec, y_qkv, y_down, y_gu,
    sends, recvs, loads, outs,
):
    n, m, rows, width, slab, part, ff, b_units = dims
    ffp = act.shape[1]
    inner = part * m
    count = rows * m
    half = count // 2
    place = Place(n, m)
    sender = Sender(sends, recvs)
    waiting = {}

    def load(name, src, dst):
        copy = pltpu.make_async_copy(src, dst, loads.at[len(waiting)])
        copy.start()
        waiting[name] = copy

    load("n2", h_n2, wide_b)
    load("dgu", h_dgu, dgu)
    load("act", h_act, act)
    load("cot", h_cot, wide_a)
    load("wgu", h_wgu, wgu)
    load("own", h_cot.at[pl.ds(0, dims[2])], cot)
    load("mid", h_mid, mid)
    load("rows", h_rows, rows_v)
    load("wqkv", h_wqkv, wqkv)
    load("wout", h_wout, wout)
    load("ctx", h_ctx, ctx)
    load("qkv", h_qkv, qkv)
    load("stat", h_stat, stat)
    spare = loads.shape[0] - 2
    rotary = load_rotary(place, h_rot, rot, rows, loads, spare - m)
    bits = place.bits()
    others = [mask for mask in range(1, m) if mask not in bits]
    moves = place.moves
    greet(place, others)
    d, s = place.d, place.s
    out_rows, vec_rows = part // n, sum_v.shape[0] // n
    down_rows, down_cols = 2 * ff // n, width // 2
    ring_a = Reduce(place, sender, sum_a, in_a, RowSlots(slab, 3 * part))
    ring_b = Reduce(place, sender, sum_b, in_b, RowSlots(out_rows, width))
    ring_c = [
        Reduce(place, sender, sum_c, inbox, RowSlots(slab, 2 * units_, lane_))
        for inbox, (_, units_, lane_) in zip((in_c0, in_c1, in_c2), blocks_of(ff))
    ]
    ring_d = Reduce(place, sender, sum_d, in_d, TileSlots(down_rows, down_cols))
    ring_v = Reduce(place, sender, sum_v, in_v, RowSlots(vec_rows, LANES))
    key_spots(place, pos_k, rows)
    block = 256

    def outer(dst, left, right, size):
        def step(j, carry):
            cols = pl.ds(pl.multiple_of(j * block, block), block)
            dst[cols, :] = dot(flip(left[:, cols]), right[...]).astype(BF16)
            return carry

        lax.fori_loop(0, size // block, step, 0)

    class Halving:
        def __init__(self, at):
            self.slots = [sender.slot(), sender.slot()]
            self.at = at
            self.open = []

        def first(self, far):
            far()
            self.open.append(sender.start(self.slots[0], send1, recv1.at[pl.ds(self.at * half, half)], place.seqs[bits[1]]))

        def second(self):
            self.open[0].wait_recv()
            send2[...] = (own[rows:, :] + recv1[self.at * half + rows : (self.at + 1) * half, :].astype(F32)).astype(BF16)
            self.open.append(sender.start(self.slots[1], send2, recv2.at[pl.ds(self.at * rows, rows)], place.seqs[bits[0]]))

        def total(self):
            self.open[1].wait_recv()
            return own[:rows, :] + recv1[self.at * half : self.at * half + rows, :].astype(F32) + recv2[
                self.at * rows : (self.at + 1) * rows, :
            ].astype(F32)

        def sent(self):
            for copy in self.open:
                copy.wait_send()
            sender.open = [c for c in sender.open if all(c is not o for o in self.open)]

    turns = [(ring_d, x_down, sender.slot()), (ring_b, x_out, sender.slot())]

    def turn_back(i):
        ring, landing, slot = turns[i]

        @pl.when(moves)
        def _():
            sender.copy(slot, ring.mine(), landing, place.source).start()

        @pl.when(jnp.logical_not(moves))
        def _():
            copy = pltpu.make_async_copy(ring.mine(), landing, loads.at[spare + i])
            copy.start()
            copy.wait()

    def turned_back(i):
        ring, landing, slot = turns[i]

        @pl.when(moves)
        def _():
            sender.copy(slot, ring.mine(), landing, place.target).wait_recv()

    def deal(buf, size, landing, whole=False):
        share = size if whole else size // m
        got = []
        to = pl.ds(pl.multiple_of(s * share, share), share)
        for mask in range(1, m):
            start = d * size + (0 if whole else place.partner(mask) * share)
            src = buf.at[pl.ds(pl.multiple_of(start, share), share)]
            got.append(sender.start(sender.slot(), src, landing.at[to], place.seqs[mask]))
        start = d * size + (0 if whole else s * share)
        landing[to, :] = buf[pl.ds(pl.multiple_of(start, share), share), :]
        return got

    waiting["n2"].wait()
    waiting["dgu"].wait()

    def slab_of(index):
        cols = pl.ds(pl.multiple_of(index * slab, slab), slab)
        sum_c[cols, :] = dot(flip(wide_b[:, cols]), dgu[...]).astype(BF16)

    slab_of(place.owner(place.half))
    for ring in ring_c:
        ring.begin()
    waiting["act"].wait()
    waiting["cot"].wait()
    outer(sum_d, act, wide_a, ffp)
    ring_d.begin()
    waiting["wgu"].wait()
    normed2 = Halving(0)

    def back_step(left, lo, hi, weight, to):
        def step(j, carry):
            cols = pl.ds(pl.multiple_of(j * block, block), block)
            to(cols, dot_cols(left[lo:hi, :], weight[cols, :]))
            return carry

        lax.fori_loop(0, width // block, step, 0)

    def to_send(cols, value):
        send1[:, cols] = value.astype(BF16)

    def to_own(cols, value):
        own[:, cols] = value

    normed2.first(lambda: back_step(dgu, half, count, wgu, to_send))
    back_step(dgu, 0, half, wgu, to_own)
    lanes = 2 * ff
    load("down_lo", h_wdown.at[:, pl.ds(0, lanes)], wgu.at[pl.ds(0, ffp)])
    load("down_hi", h_wdown.at[:, pl.ds(lanes, width - lanes)], wgu.at[pl.ds(ffp, ffp), pl.ds(0, width - lanes)])
    normed2.second()

    def other_slabs(i, carry):
        slab_of(lax.rem(place.owner(place.half) + i, n))
        return carry

    lax.fori_loop(1, n, other_slabs, 0)
    load("n1", h_n1, wide_b)
    load("tok", h_tok, wide_a)
    for ring in ring_c:
        ring.pump(1)
    ring_d.pump(1)

    waiting["mid"].wait()
    waiting["rows"].wait()
    waiting["own"].wait()

    def deviation(value):
        c = value - jnp.mean(value, axis=-1, keepdims=True)
        r = lax.rsqrt(jnp.mean(c * c, axis=-1, keepdims=True) + EPS)
        return c * r, r

    xhat, r = deviation(mid[...])
    up = normed2.total()
    sums_v[2:3, :] = jnp.sum(up * xhat, axis=0, keepdims=True)
    sums_v[3:4, :] = jnp.sum(up, axis=0, keepdims=True)
    d_mid[...] = cot[...].astype(F32) + norm_back(up, xhat, r, rows_v[2:3, :])
    dm_all[:rows, :] = d_mid[...].astype(BF16)
    spread = [sender.slot() for _ in bits]

    def spread_copy(i):
        size = rows << i
        return (spread[i], dm_all.at[pl.ds(0, size)], dm_all.at[pl.ds(size, size)])

    def spread_send(i):
        sender.start(*spread_copy(i), place.seqs[bits[i]])

    def spread_wait(i):
        sender.copy(*spread_copy(i), place.seqs[bits[i]]).wait_recv()

    spread_send(0)
    normed2.sent()
    ring_c[0].pump(2)
    ring_c[1].pump(2)

    waiting["down_lo"].wait()
    waiting["down_hi"].wait()

    def down_step(lo, hi, to):
        def low(j, carry):
            cols = pl.ds(pl.multiple_of(j * LANES, LANES), LANES)
            to(cols, dot(act[lo:hi, :], wgu[:ffp, cols]))
            return carry

        def high(j, carry):
            cols = pl.ds(pl.multiple_of(j * LANES, LANES), LANES)
            to(pl.ds(pl.multiple_of(lanes + j * LANES, LANES), LANES), dot(act[lo:hi, :], wgu[ffp : 2 * ffp, cols]))
            return carry

        lax.fori_loop(0, lanes // LANES, low, 0)
        lax.fori_loop(0, (width - lanes) // LANES, high, 0)

    output = Halving(1)

    output.first(lambda: down_step(half, count, to_send))
    down_step(0, half, to_own)
    spread_wait(0)
    spread_send(1)
    output.second()
    ring_c[2].pump(2)
    ring_d.pump(2)
    spread_wait(1)

    waiting["wout"].wait()
    waiting["ctx"].wait()
    dctx[...] = dot_cols(dm_all[...], wout[...]).astype(BF16)
    outer(sum_b, ctx, dm_all, part)
    ring_b.begin()
    cot[...] = (mid[...] + output.total()).astype(BF16)
    output.sent()

    for name in ("qkv", "stat"):
        waiting[name].wait()
    for copy in rotary:
        copy.wait()
    scale = HEAD_DIM ** (-0.5)
    per = LANES // HEAD_DIM
    lane = lax.broadcasted_iota(jnp.int32, (1, LANES), 1) // HEAD_DIM

    def turned(z, span):
        return (
            z * rot[span, :LANES]
            - pltpu.roll(z, LANES - ROT // 2, 1) * rot[span, LANES : 2 * LANES]
            - pltpu.roll(z, ROT // 2, 1) * rot[span, 2 * LANES :]
        )

    bias_v[...] = jnp.zeros_like(bias_v)
    for pair in range(part // LANES):
        at = pair * LANES
        dk[...] = jnp.zeros_like(dk)
        dv[...] = jnp.zeros_like(dv)

        def attend(i, carry, pair=pair, at=at):
            span = pl.ds(pl.multiple_of(i * rows, rows), rows)
            q = qkv[span, at : at + LANES]
            k = qkv[:, part + at : part + at + LANES]
            v = qkv[:, 2 * part + at : 2 * part + at + LANES]
            dc = dctx[span, at : at + LANES]
            both = dc.astype(F32) * ctx[span, at : at + LANES].astype(F32)
            allowed = pos_k[0:1, :] <= stat[span, SPOT : SPOT + 1]
            dq = jnp.zeros((rows, LANES), F32)
            for h in range(per):
                pick = lane == h
                mine = pick.astype(BF16)
                qm, dcm = q * mine, dc * mine
                scores = dot_cols(qm, k) * scale
                at_lse = LSE + pair * per + h
                probs = jnp.exp(jnp.where(allowed, scores, -jnp.inf) - stat[span, at_lse : at_lse + 1])
                delta = jnp.sum(jnp.where(pick, both, 0.0), axis=-1, keepdims=True)
                ds = (probs * (dot_cols(dcm, v) - delta) * scale).astype(BF16)
                dq = dq + jnp.dot(ds, k * mine, preferred_element_type=F32)
                dk[...] += dot(flip(ds), qm)
                dv[...] += dot(flip(probs.astype(BF16)), dcm)
            dq = turned(dq, span)
            bias_v[0:1, at : at + LANES] += jnp.sum(dq, axis=0, keepdims=True)
            dqkv[span, at : at + LANES] = dq.astype(BF16)
            return carry

        lax.fori_loop(0, m, attend, 0)

        def settle(i, carry, at=at):
            span = pl.ds(pl.multiple_of(i * rows, rows), rows)
            key, value = turned(dk[span, :], span), dv[span, :]
            bias_v[0:1, part + at : part + at + LANES] += jnp.sum(key, axis=0, keepdims=True)
            bias_v[0:1, 2 * part + at : 2 * part + at + LANES] += jnp.sum(value, axis=0, keepdims=True)
            dqkv[span, part + at : part + at + LANES] = key.astype(BF16)
            dqkv[span, 2 * part + at : 2 * part + at + LANES] = value.astype(BF16)
            return carry

        lax.fori_loop(0, m, settle, 0)
        if pair == 0:
            for ring in ring_c:
                ring.pump(3)

    waiting["n1"].wait()
    outer(sum_a, wide_b, dqkv, width)
    ring_a.begin()
    ring_d.pump(3)
    ring_b.pump(1)
    waiting["wqkv"].wait()
    waiting["tok"].wait()
    normed1 = Halving(2)

    def gains(cols, value, lo, hi):
        xh = (wide_a[lo:hi, cols].astype(F32) - stat[lo:hi, MEAN : MEAN + 1]) * stat[lo:hi, RSTD : RSTD + 1]
        return jnp.sum(value * xh, axis=0, keepdims=True), jnp.sum(value, axis=0, keepdims=True)

    def far_last(cols, value):
        send1[:, cols] = value.astype(BF16)
        sums_v[0:1, cols], sums_v[1:2, cols] = gains(cols, value, half, count)

    def near_last(cols, value):
        own[:, cols] = value
        gain, total = gains(cols, value, 0, half)
        sums_v[0:1, cols] += gain
        sums_v[1:2, cols] += total

    normed1.first(lambda: back_step(dqkv, half, count, wqkv, far_last))
    back_step(dqkv, 0, half, wqkv, near_last)

    sum_v[...] = jnp.zeros_like(sum_v)
    units = slab // LANES

    def lay(c, carry):
        for i in range(4):
            for u in range(units):
                at = pl.multiple_of(c * slab + u * LANES, LANES)
                sum_v[pl.ds(c * vec_rows + i * units + u, 1), :] = sums_v[i : i + 1, pl.ds(at, LANES)]
        return carry

    lax.fori_loop(0, n, lay, 0)
    for i in range(3):
        for u in range(part // LANES):
            unit = i * (inner // LANES) + place.shards[u]
            row = lax.div(unit, b_units) * vec_rows + 4 * units + lax.rem(unit, b_units)
            at = i * part + u * LANES
            sum_v[pl.ds(row, 1), :] = bias_v[0:1, at : at + LANES]
    ring_v.begin()
    normed1.second()
    ring_b.pump(2)
    ring_a.pump(1)
    ring_v.pump(1)
    for ring in ring_c:
        ring.pump(4)
    got_gu = deal(sum_c, slab, x_gu)
    ring_d.pump(4)
    turn_back(0)
    ring_b.pump(3)
    ring_a.pump(2)
    ring_v.pump(2)
    up = normed1.total()
    rstd = stat[:rows, RSTD : RSTD + 1]
    xhat = (wide_a[:rows, :].astype(F32) - stat[:rows, MEAN : MEAN + 1]) * rstd
    own[:rows, :] = d_mid[...] + norm_back(up, xhat, rstd, rows_v[0:1, :])
    ring_b.pump(4)
    ring_v.pump(3)

    written = []

    def store(src, dst):
        copy = pltpu.make_async_copy(src, dst, outs.at[len(written)])
        copy.start()
        written.append(copy)

    store(cot, o_block)
    store(own.at[pl.ds(0, rows)], o_input)
    turn_back(1)
    ring_a.pump(3)

    turned_back(0)
    lane128 = lax.broadcasted_iota(jnp.int32, (1, LANES), 1)

    def lay_out(got, to):
        share, shard, hidden = slab // m, ff // 2, ff * m
        found = {}
        for t in range(m):
            span = slice(t * share, (t + 1) * share)
            tiles = [[], []]
            at = 0
            for _, units_, _ in blocks_of(ff):
                even = units_ // LANES
                tiles[0] += [got[span, at + k * LANES : at + (k + 1) * LANES].astype(F32) for k in range(even)]
                at += even * LANES
                odd = []
                if even * LANES < units_:
                    mixed = got[span, at : at + LANES].astype(F32)
                    odd = [mixed, pltpu.roll(mixed, LANES // 2, 1)]
                    at += LANES
                tiles[1] += [got[span, at + k * LANES : at + (k + 1) * LANES].astype(F32) for k in range(even)]
                at += even * LANES
                if odd:
                    tiles[0].append(odd[0])
                    tiles[1].append(odd[1])
            for i in range(2):
                for u, held in enumerate(shards_of(t, n)):
                    start, first, end = u * shard, i * hidden + held * shard, i * hidden + (held + 1) * shard
                    shift = (first - start) % LANES
                    back = (first - start - shift) // LANES
                    for tile in range(first // LANES, (end - 1) // LANES + 1):
                        k = tile - back
                        parts_ = [tiles[i][q] if 0 <= q < len(tiles[i]) else None for q in (k, k - 1)]
                        if shift:
                            here, before = [None if p is None else pltpu.roll(p, shift, 1) for p in parts_]
                            if here is None or before is None:
                                value = before if here is None else here
                            else:
                                value = jnp.where(lane128 < shift, before, here)
                        else:
                            value = parts_[0]
                        lo, hi = max(first, tile * LANES), min(end, (tile + 1) * LANES)
                        found.setdefault(tile, []).append((lo - tile * LANES, hi - tile * LANES, value))
        for tile, parts_ in found.items():
            parts_.sort(key=lambda p: p[0])
            value = parts_[-1][2]
            for _, hi, other in reversed(parts_[:-1]):
                value = jnp.where(lane128 < hi, other, value)
            to[:, tile * LANES : (tile + 1) * LANES] = value.astype(BF16)

    some = down_rows // 2
    value = x_down[...].astype(F32)
    d_mid[:some, :down_cols] = value[:some, :]
    d_mid[:some, down_cols:] = value[some:, :]
    column = lax.rem(s, 2)
    across = pl.ds(pl.multiple_of(column * down_cols, down_cols), down_cols)
    swap = sender.start(
        sender.slot(),
        d_mid.at[pl.ds(0, some), pl.ds(pl.multiple_of((1 - column) * down_cols, down_cols), down_cols)],
        y_down.at[:, across],
        place.seqs[1],
    )
    y_down[:, across] = d_mid[:some, across]
    ring_v.pump(4)
    got_vec = deal(sum_v, vec_rows, x_vec, whole=True)
    for copy in got_gu:
        copy.wait_recv()
    lay_out(x_gu, y_gu)
    store(y_gu, o_gu)
    turned_back(1)
    store(x_out, o_out)
    swap.wait_recv()
    store(y_down, o_down)
    for copy in got_vec:
        copy.wait_recv()
    total = x_vec[:vec_rows, :]
    for t in range(1, m):
        total = total + x_vec[t * vec_rows : (t + 1) * vec_rows, :]
    x_vec[:vec_rows, :] = total
    some = slab // m
    sizes = [(i * units, some) for i in range(4)] + [(4 * units, b_units * LANES // m)]
    for i, (first_row, size) in enumerate(sizes):
        tile = lax.div(s * size, LANES)
        shift = s * size - tile * LANES
        low = x_vec[pl.ds(first_row + tile, 1), :]
        high = x_vec[pl.ds(first_row + tile + 1, 1), :]
        both = jnp.where(lane128 < shift, high, low)
        sums_v[i : i + 1, :LANES] = pltpu.roll(both, lax.rem(LANES - shift, LANES), 1)
    store(sums_v.at[:, pl.ds(0, LANES)], o_vec)
    ring_a.pump(4)
    got_qkv = deal(sum_a, slab, x_qkv)
    for copy in got_qkv:
        copy.wait_recv()
    share = slab // m
    for t in range(m):
        for i in range(3):
            for u, held in enumerate(shards_of(t, n)):
                at, come = i * inner + held * LANES, i * part + u * LANES
                y_qkv[:, at : at + LANES] = x_qkv[t * share : (t + 1) * share, come : come + LANES]
    store(y_qkv, o_qkv)
    for copy in written:
        copy.wait()
    sender.finish()

    @pl.when(moves)
    def _():
        for ring, landing, slot in turns:
            sender.copy(slot, ring.mine(), landing, place.source).wait_send()


def run_backward(dims, args):
    n, m, rows, width, slab, part, ff, b_units = dims
    count = rows * m
    ffp = -(-ff // 256) * 256
    vec_rows = -(-(4 * (slab // LANES) + b_units) // TILE) * TILE
    half = n // 2
    out_rows = part // n
    down_rows, down_cols = 2 * ff // n, width // 2
    share = slab // m

    def inbox(slots, dtype=BF16):
        return vmem(slots.inbox(half), dtype)

    outputs = [
        ((rows, width), BF16), ((rows, width), F32), ((share, 2 * ff * m), BF16), ((share, 3 * part * m), BF16),
        ((down_rows // 2, width), F32), ((out_rows, width), BF16), ((8, LANES), F32),
    ]
    scratch = [
        vmem((part, width)), vmem((width, 2 * ff)), vmem((width, 3 * part)), vmem((8, width), F32),
        vmem((count, width)), vmem((count, width)), vmem((count, 3 * part)), vmem((count, LANES), F32),
        vmem((count, part)), vmem((rows, width), F32), vmem((count, ffp)), vmem((count, 2 * ff)),
        vmem((count, 3 * LANES), F32), vmem((8, count), F32),
        vmem((n * slab, 3 * part)), vmem((part, width)), vmem((n * slab, 2 * ff)), vmem((ffp, width)),
        vmem((n * vec_rows, LANES), F32),
        inbox(RowSlots(slab, 3 * part)), inbox(RowSlots(out_rows, width)), *[inbox(RowSlots(slab, 2 * units)) for _, units, _ in blocks_of(ff)],
        inbox(TileSlots(down_rows, down_cols)), inbox(RowSlots(vec_rows, LANES), F32),
        vmem((count // 2, width), F32), vmem((count // 2, width)), vmem((rows, width)),
        vmem((3 * count // 2, width)), vmem((3 * rows, width)),
        vmem((count, width)), vmem((rows, width), F32), vmem((rows, width)), vmem((count, part)), vmem((count, 3 * part)),
        vmem((count, LANES), F32), vmem((count, LANES), F32), vmem((8, width), F32), vmem((8, 3 * part), F32),
        vmem((slab, 2 * ff)), vmem((slab, 3 * part)), vmem((down_rows, down_cols)),
        vmem((out_rows, width)), vmem((m * vec_rows, LANES), F32), vmem((share, 3 * part * m)),
        vmem((down_rows // 2, width), F32), vmem((share, 2 * ff * m)),
    ]
    slots = (4 + len(blocks_of(ff))) * 2 * half + 3 * 2 + 2 + 2 + 3 * (m - 1) + 1
    return pl.pallas_call(
        functools.partial(backward_kernel, dims),
        out_shape=[jax.ShapeDtypeStruct(*a) for a in outputs],
        in_specs=[pl.BlockSpec(memory_space=pl.ANY)] * len(args),
        out_specs=[pl.BlockSpec(memory_space=pl.ANY)] * len(outputs),
        scratch_shapes=scratch
        + [
            pltpu.SemaphoreType.DMA((slots,)),
            pltpu.SemaphoreType.DMA((slots,)),
            pltpu.SemaphoreType.DMA((len(args) + 12,)),
            pltpu.SemaphoreType.DMA((len(outputs),)),
        ],
        compiler_params=pltpu.CompilerParams(
            collective_id=1, has_side_effects=True, vmem_limit_bytes=VMEM_BYTES
        ),
        name="backward",
    )(*args)


def rotary_lines(length):
    half = ROT // 2
    lane = np.arange(LANES) % HEAD_DIM
    angles = np.arange(length)[:, None] * (10000.0 ** (-(lane % half) * 2.0 / ROT))[None, :]
    cosine, sine = np.cos(angles), np.sin(angles)
    lines = [
        np.where(lane < ROT, cosine, 1.0),
        np.where(lane < half, -sine, 0.0),
        np.where((lane >= half) & (lane < ROT), sine, 0.0),
    ]
    return jnp.asarray(np.concatenate(lines, axis=1), F32)


def shards(tokens, cotangent, gain1, bias1, w_qkv, b_qkv, w_out, gain2, bias2, w_gate_up, w_down):
    n, m, s = lax.axis_size("dp"), lax.axis_size("seq"), lax.axis_index("seq")
    rows, width = tokens.shape
    slab = gain1.shape[0]
    inner, hidden = w_out.shape[0] * n, w_down.shape[0] * n
    part, ff = inner // m, hidden // m
    dims = (n, m, rows, width, slab, part, ff, b_qkv.shape[0] // LANES)
    parts = [gain1, bias1, gain2, bias2, b_qkv]
    total = sum(p.shape[0] for p in parts)
    length = -(-total // (TILE * LANES)) * TILE * LANES
    vec, at = jnp.zeros((length,), F32), 0
    for p in parts:
        vec = vec + jnp.pad(p.astype(F32), (at, length - at - p.shape[0]))
        at += p.shape[0]
    vec = vec.reshape(-1, LANES)
    rot = rotary_lines(rows * m)
    kept = run_forward(dims, (tokens, cotangent, w_qkv, w_gate_up, w_out, w_down, vec, rot))
    block_out, input_grad, g_gu, g_qkv, g_down, g_out, line = run_backward(dims, tuple(kept) + (rot,))
    vectors = [line[i, : size // m] for i, size in enumerate([slab] * 4 + [b_qkv.shape[0]])]
    return (
        block_out,
        input_grad,
        vectors[0],
        vectors[1],
        g_qkv.astype(F32),
        vectors[4],
        g_out.astype(F32),
        vectors[2],
        vectors[3],
        g_gu.astype(F32),
        g_down,
    )


def fits(mesh, shapes):
    n, m = mesh.shape["dp"], mesh.shape["seq"]
    (rows, width), slab = shapes[0], shapes[2][0]
    part, ff = shapes[6][0] * n // m, shapes[10][0] * n // m
    return (
        m == 4
        and n == 2 * m
        and rows % LANES == 0
        and shapes[6][0] == LANES
        and slab == 256
        and width % 512 == 0
        and shapes[5][0] % LANES == 0
        and part == 256
        and (ff // 2) + LANES - 1 <= WINDOW
        and ff // 2 + (ff // 2) % LANES <= WINDOW
        and shapes[9][1] // 2 % LANES == 0
        and 512 < ff <= 768
        and ff % 64 == 0
        and (2 * ff // n) % TILE == 0
        and 2 * ff <= width <= 4 * ff
        and 2 * 768 <= width
    )


def solution(mesh):
    rows, cols, vec = P(("dp", "seq"), None), P("dp", None), P("dp")
    flat = P(("dp", "seq"))
    def step(*args):
        body = shards if fits(mesh, [a.shape for a in args]) else shards_plain
        return body(*args)

    return jax.shard_map(
        step,
        mesh=mesh,
        in_specs=(rows, rows, vec, vec, cols, vec, cols, vec, vec, cols, cols),
        out_specs=(rows, rows, flat, flat, rows, flat, rows, flat, flat, rows, rows),
        check_vma=False,
    )
```

```python
import functools

import jax
import jax.numpy as jnp
import numpy as np
from jax import lax
from jax.experimental import pallas as pl
from jax.experimental.pallas import tpu as pltpu
from jax.sharding import PartitionSpec as P

HEAD_DIM = 64
ROT = 16
EPS = 1e-05
F32 = jnp.float32
BF16 = jnp.bfloat16


def ring_order(n):
    return list(range(0, n, 2)) + list(range(n - 1, 0, -2))


def dot(a, b):
    return jnp.dot(a, b, preferred_element_type=F32)


def dot_rows(a, b):
    return lax.dot_general(a, b, (((0,), (0,)), ((), ())), preferred_element_type=F32)


def dot_cols(a, b):
    return lax.dot_general(a, b, (((1,), (1,)), ((), ())), preferred_element_type=F32)


class Ring:
    def __init__(self):
        n = lax.axis_size("dp")
        order = ring_order(n)
        place = [order.index(i) for i in range(n)]
        self.n, self.half = n, n // 2
        self.right = [(order[i], order[(i + 1) % n]) for i in range(n)]
        self.left = [(b, a) for a, b in self.right]
        self.order = jnp.array(order, jnp.int32)
        self.place = jnp.array(place, jnp.int32)[lax.axis_index("dp")]

    def owner(self, offset):
        return self.order[lax.rem(self.place + offset + self.n, self.n)]

    def go_right(self, value):
        return lax.ppermute(value, "dp", self.right)

    def go_left(self, value):
        return lax.ppermute(value, "dp", self.left)

    def gather(self, piece):
        rows = piece.shape[0]
        cut = rows // 2
        from_left = from_right = piece
        whole = jnp.zeros((self.n,) + piece.shape, piece.dtype)

        def put(whole, offset, chunk):
            return lax.dynamic_update_slice(
                whole, chunk[None], (self.owner(offset),) + (0,) * piece.ndim
            )

        whole = put(whole, 0, piece)
        for k in range(1, self.half):
            from_left = self.go_right(from_left)
            from_right = self.go_left(from_right)
            whole = put(put(whole, -k, from_left), k, from_right)
        upper = self.go_right(from_left[:cut])
        lower = self.go_left(from_right[cut:])
        return put(whole, self.half, jnp.concatenate([upper, lower]))

    def scatter(self, parts):
        rows = parts.shape[1]
        cut = rows // 2

        def mine(offset):
            start = (self.owner(offset),) + (0,) * (parts.ndim - 1)
            return lax.dynamic_slice(parts, start, (1,) + parts.shape[1:])[0]

        def add(a, b):
            return a.astype(F32) + b.astype(F32)

        far = mine(self.half)
        upper = self.go_right(far[:cut])
        lower = self.go_left(far[cut:])
        from_left, from_right = mine(self.half - 1), mine(1 - self.half)
        from_left = jnp.concatenate(
            [add(from_left[:cut], upper).astype(BF16), from_left[cut:]]
        )
        from_right = jnp.concatenate(
            [from_right[:cut], add(from_right[cut:], lower).astype(BF16)]
        )
        for k in range(self.half - 2, -1, -1):
            from_left = self.go_right(from_left)
            from_right = self.go_left(from_right)
            if k:
                from_left = add(from_left, mine(k)).astype(BF16)
                from_right = add(from_right, mine(-k)).astype(BF16)
        return add(mine(0), from_left) + from_right.astype(F32)


class Group:
    def __init__(self):
        self.m = lax.axis_size("seq")
        self.s = lax.axis_index("seq")
        self.bits = []
        bit = self.m // 2
        while bit:
            self.bits.append(bit)
            bit //= 2
        self.offsets = [0]
        for bit in self.bits:
            self.offsets += [o ^ bit for o in self.offsets]

    def swap(self, value, mask):
        return lax.ppermute(value, "seq", [(i, i ^ mask) for i in range(self.m)])

    def gather(self, value):
        for bit in self.bits:
            value = jnp.concatenate([value, self.swap(value, bit)])
        return value

    def scatter(self, value):
        for bit in reversed(self.bits):
            half = value.shape[0] // 2
            got = self.swap(value[half:].astype(BF16), bit)
            value = value[:half] + got.astype(F32)
        return value

    def exchange(self, blocks):
        got = []
        for mask in range(self.m):
            block = lax.dynamic_index_in_dim(blocks, self.s ^ mask, 0, keepdims=False)
            got.append(self.swap(block, mask) if mask else block)
        stacked = jnp.stack(got)
        return jnp.take(stacked, self.s ^ jnp.arange(self.m), axis=0)


def norm(value):
    center = value - jnp.mean(value, axis=-1, keepdims=True)
    rstd = lax.rsqrt(jnp.mean(center * center, axis=-1, keepdims=True) + EPS)
    return center * rstd, rstd


def norm_back(upstream, xhat, rstd, gain):
    e = upstream * gain
    inner = (
        e
        - jnp.mean(e, axis=-1, keepdims=True)
        - xhat * jnp.mean(e * xhat, axis=-1, keepdims=True)
    )
    return rstd * inner


def rotary_tables(positions):
    half = ROT // 2
    inverse = 10000.0 ** (-(jnp.arange(half, dtype=F32) * 2.0 / ROT))
    angles = positions.astype(F32)[:, None] * inverse[None, :]
    return jnp.cos(angles)[:, None, :], jnp.sin(angles)[:, None, :]


def rotate(tensor, cosine, sine):
    half = ROT // 2
    a, b = tensor[..., :half], tensor[..., half:ROT]
    return jnp.concatenate([a * cosine - b * sine, b * cosine + a * sine, tensor[..., ROT:]], axis=-1)


def shards_plain(tokens, cotangent, gain1, bias1, w_qkv, b_qkv, w_out, gain2, bias2, w_gate_up, w_down):
    ring, group = Ring(), Group()
    n, m, s = ring.n, group.m, group.s
    rows, width = tokens.shape
    slab = gain1.shape[0]
    inner = w_out.shape[0] * n
    hidden = w_down.shape[0] * n
    part, ff = inner // m, hidden // m
    heads = part // HEAD_DIM
    scale = HEAD_DIM ** (-0.5)

    both = jnp.stack([tokens, cotangent], axis=1)
    everything = group.gather(both)
    tokens_all, cot_all = everything[:, 0], everything[:, 1]

    qkv_piece = jnp.concatenate(
        [lax.dynamic_slice(w_qkv, (0, i * inner + s * part), (slab, part)) for i in range(3)], axis=1
    )
    small = jnp.concatenate([gain1, bias1, gain2, bias2, b_qkv])
    extra = -(-small.shape[0] // (3 * part))
    small = jnp.pad(small, (0, extra * 3 * part - small.shape[0])).reshape(extra, 3 * part)
    first = ring.gather(jnp.concatenate([qkv_piece, small]))
    wqkv = first[:, :slab].reshape(width, 3 * part)
    vectors = first[:, slab:].reshape(n, -1)

    def vector(at, size):
        return vectors[:, at : at + size].reshape(-1).astype(F32)

    g1, b1, g2, b2 = (vector(i * slab, slab) for i in range(4))
    bias_all = vector(4 * slab, b_qkv.shape[0]).reshape(3, m, part)
    bias_qkv = lax.dynamic_index_in_dim(bias_all, s, 1, keepdims=False).reshape(3 * part)

    turn = [(g, (g % n) * m + g // n) for g in range(n * m)]
    back = [(b, a) for a, b in turn]

    def quarter(weight):
        count = weight.shape[0] // m
        mine = lax.dynamic_slice(weight, (0, 0), weight.shape)
        return mine.reshape(m, count, weight.shape[1])[s]

    out_rows, down_rows = w_out.shape[0] // m, w_down.shape[0] // m
    moved = lax.ppermute(
        jnp.concatenate([quarter(w_out), quarter(w_down)]), ("dp", "seq"), turn
    )
    wout = ring.gather(moved[:out_rows]).reshape(part, width)
    gu_piece = jnp.concatenate(
        [lax.dynamic_slice(w_gate_up, (0, i * hidden + s * ff), (slab, ff)) for i in range(2)], axis=1
    )
    wgu = ring.gather(gu_piece).reshape(width, 2 * ff)
    wdown = ring.gather(moved[out_rows:]).reshape(ff, width)

    places = jnp.concatenate([(s ^ o) * rows + jnp.arange(rows, dtype=jnp.int32) for o in group.offsets])
    cosine, sine = rotary_tables(places)
    count = rows * m
    xhat1, rstd1 = norm(tokens_all.astype(F32))
    normed1 = (xhat1 * g1 + b1).astype(BF16)
    qkv = (dot(normed1, wqkv) + bias_qkv).reshape(count, 3, heads, HEAD_DIM)
    queries = rotate(qkv[:, 0], cosine, sine).astype(BF16)
    keys = rotate(qkv[:, 1], cosine, sine).astype(BF16)
    values = qkv[:, 2].astype(BF16)
    scores = jnp.einsum("qhd,khd->hqk", queries, keys, preferred_element_type=F32) * scale
    scores = jnp.where((places[None, :] <= places[:, None])[None], scores, -jnp.inf)
    top = jnp.max(scores, axis=-1, keepdims=True)
    lse = top + jnp.log(jnp.sum(jnp.exp(scores - top), axis=-1, keepdims=True))
    probs = jnp.exp(scores - lse)
    probs_r = probs.astype(BF16)
    context = jnp.einsum("hqk,khd->qhd", probs_r, values, preferred_element_type=F32).astype(BF16)
    context_flat = context.reshape(count, part)
    x_own = tokens.astype(F32)
    mid = x_own + group.scatter(dot(context_flat, wout))
    xhat2, rstd2 = norm(mid)
    normed2 = group.gather((xhat2 * g2 + b2).astype(BF16))
    gate_up = dot(normed2, wgu)
    gate, up = gate_up[:, :ff], gate_up[:, ff:]
    sigma = jax.nn.sigmoid(gate)
    silu = gate * sigma
    act = (silu * up).astype(BF16)
    d_act = dot_cols(cot_all, wdown)
    d_gate = d_act * up * (sigma * (1.0 + gate * (1.0 - sigma)))
    d_gate_up = jnp.concatenate([d_gate, d_act * silu], axis=1).astype(BF16)

    d_normed2 = group.scatter(dot_cols(d_gate_up, wgu))
    sum_down = ring.scatter(dot_rows(act, cot_all).astype(BF16).reshape(n, ff // n, width))
    sum_gu = ring.scatter(dot_rows(normed2, d_gate_up).astype(BF16).reshape(n, slab, 2 * ff))
    block_out = (mid + group.scatter(dot(act, wdown))).astype(BF16)
    d_mid = cotangent.astype(F32) + norm_back(d_normed2, xhat2, rstd2, g2)
    d_mid_r = group.gather(d_mid.astype(BF16))

    d_context = dot_cols(d_mid_r, wout).astype(BF16).reshape(count, heads, HEAD_DIM)
    sum_out = ring.scatter(dot_rows(context_flat, d_mid_r).astype(BF16).reshape(n, part // n, width))
    d_probs = jnp.einsum("qhd,khd->hqk", d_context, values, preferred_element_type=F32)
    delta = jnp.einsum("qhd,qhd->hq", d_context.astype(F32), context.astype(F32))[..., None]
    d_scores = (probs * (d_probs - delta) * scale).astype(BF16)
    d_queries = jnp.einsum("hqk,khd->qhd", d_scores, keys, preferred_element_type=F32)
    d_keys = jnp.einsum("hqk,qhd->khd", d_scores, queries, preferred_element_type=F32)
    d_values = jnp.einsum("hqk,qhd->khd", probs_r, d_context, preferred_element_type=F32)
    d_qkv = jnp.stack(
        [rotate(d_queries, cosine, -sine), rotate(d_keys, cosine, -sine), d_values], axis=1
    ).reshape(count, 3 * part)
    d_qkv_r = d_qkv.astype(BF16)
    d_normed1_part = dot_cols(d_qkv_r, wqkv)
    d_normed1 = group.scatter(d_normed1_part)
    own = (slice(0, rows),)
    input_grad = d_mid + norm_back(d_normed1, xhat1[own], rstd1[own], g1)

    bias_part = jnp.zeros((3, m, part), F32)
    bias_part = lax.dynamic_update_slice(bias_part, jnp.sum(d_qkv, axis=0).reshape(3, 1, part), (0, s, 0))
    vector_parts = [
        jnp.sum(d_normed1_part * xhat1, axis=0),
        jnp.sum(d_normed1_part, axis=0),
        jnp.sum(d_normed2 * xhat2, axis=0),
        jnp.sum(d_normed2, axis=0),
        bias_part.reshape(-1),
    ]
    line = jnp.concatenate([v.reshape(n, m, -1) for v in vector_parts], axis=-1)
    lines = -(-line.shape[-1] // (3 * part))
    line = jnp.pad(line, ((0, 0), (0, 0), (0, lines * 3 * part - line.shape[-1])))
    line = line.reshape(n, m, lines, 3 * part).astype(BF16)
    part_qkv = dot_rows(normed1, d_qkv_r).astype(BF16).reshape(n, m, slab // m, 3 * part)
    packed = jnp.concatenate([part_qkv, line], axis=2)
    packed_rows = packed.shape[2]
    sum_qkv = ring.scatter(packed.reshape(n, m * packed_rows, 3 * part))

    def owners(total):
        return group.exchange(total.astype(BF16).reshape((m, -1) + total.shape[1:])).astype(F32)

    last = owners(sum_qkv)
    g_qkv = last[:, : slab // m].reshape(m, slab // m, 3, part).transpose(1, 2, 0, 3)
    g_qkv = g_qkv.reshape(slab // m, 3 * inner)
    line = jnp.sum(last[:, slab // m :], axis=0).reshape(-1)
    sizes = [slab // m] * 4 + [b_qkv.shape[0] // m]
    vectors_out, at = [], 0
    for size in sizes:
        vectors_out.append(line[at : at + size])
        at += size
    g_gu = owners(sum_gu).reshape(m, slab // m, 2, ff).transpose(1, 2, 0, 3).reshape(slab // m, 2 * hidden)
    g_down = lax.ppermute(sum_down.astype(BF16), ("dp", "seq"), back).astype(F32)
    g_out = lax.ppermute(sum_out.astype(BF16), ("dp", "seq"), back).astype(F32)
    return (
        block_out,
        input_grad,
        vectors_out[0],
        vectors_out[1],
        g_qkv,
        vectors_out[4],
        g_out,
        vectors_out[2],
        vectors_out[3],
        g_gu,
        g_down,
    )


LOGICAL = pl.DeviceIdType.LOGICAL
MEAN, RSTD, SPOT, LSE = 0, 1, 2, 8
LANES = 128
TILE = 16
WINDOW = 512
VMEM_BYTES = 67_043_328


def vmem(shape, dtype=BF16):
    return pltpu.VMEM(shape, dtype)


class Place:
    def __init__(self, n, m):
        self.n, self.m, self.half = n, m, n // 2
        self.d, self.s = lax.axis_index("dp"), lax.axis_index("seq")
        pair = lax.div(self.d, 2)
        odd = self.d - 2 * pair
        place = pair + odd * (n - 1 - 2 * pair)
        self.owners = []
        for offset in range(n):
            spot = lax.rem(place + offset, n)
            back = lax.div(spot, self.half)
            self.owners.append(2 * spot + back * (2 * n - 1 - 4 * spot))
        self.partners = []
        for mask in range(m):
            out, bit = self.s, 1
            while bit < m:
                if mask & bit:
                    out = out + bit - 2 * bit * lax.rem(lax.div(self.s, bit), 2)
                bit *= 2
            self.partners.append(out)
        self.rings = {1: self.owners[1] * m + self.s, -1: self.owners[n - 1] * m + self.s}
        self.seqs = [self.d * m + out for out in self.partners]
        inner_ = lax.div(self.s, 2)
        side = self.s - 2 * inner_
        self.shards = [2 * inner_ + side, n - 2 - 2 * inner_ + side]
        self.shares = []
        for index in self.owners:
            low = lax.div(index, m)
            rest = index - low * m
            x = lax.rem(rest, 2)
            self.shares.append(low * m + 2 * x + lax.div(rest, 2))
        low = lax.div(self.d, m)
        self.source = (self.shards[0] + low * (self.shards[1] - self.shards[0])) * m + self.shares[0] - low * m
        across = lax.rem(lax.div(pair + 1, 2), 2)
        self.there = low * m + self.s
        outer_ = lax.div(self.s, 2)
        there_d = low * m + 2 * (self.s - 2 * outer_) + outer_
        self.target = there_d * m + 2 * across + odd
        here = self.d * m + self.s
        self.moves = (self.target - here) * (self.target - here) > 0

        offsets = [0]
        for bit in self.bits():
            offsets += [o ^ bit for o in offsets]
        self.homes = [self.partners[o] for o in offsets]

    def owner(self, offset, shares=False):
        return (self.shares if shares else self.owners)[offset % self.n]

    def partner(self, mask):
        return self.partners[mask]

    def bits(self):
        out, bit = [], self.m // 2
        while bit:
            out.append(bit)
            bit //= 2
        return out


class Sender:
    def __init__(self, sends, recvs):
        self.sends, self.recvs = sends, recvs
        self.used = 0
        self.open = []

    def slot(self):
        self.used += 1
        return self.used - 1

    def copy(self, slot, src, dst, device):
        return pltpu.make_async_remote_copy(
            src_ref=src,
            dst_ref=dst,
            send_sem=self.sends.at[slot],
            recv_sem=self.recvs.at[slot],
            device_id=device,
            device_id_type=LOGICAL,
        )

    def start(self, slot, src, dst, device):
        copy = self.copy(slot, src, dst, device)
        copy.start()
        self.open.append(copy)
        return copy

    def finish(self):
        for copy in self.open:
            copy.wait_send()
        self.open = []


def greet(place, extra_seq=()):
    barrier = pltpu.get_barrier_semaphore()

    def hello(device):
        pl.semaphore_signal(barrier, inc=1, device_id=device, device_id_type=LOGICAL)

    near = [place.rings[1], place.rings[-1]] + [place.seqs[mask] for mask in tuple(place.bits()) + tuple(extra_seq)]
    for device in near:
        hello(device)

    @pl.when(place.moves)
    def _():
        hello(place.target)
        hello(place.source)
        pl.semaphore_wait(barrier, len(near) + 2)

    @pl.when(jnp.logical_not(place.moves))
    def _():
        pl.semaphore_wait(barrier, len(near))


class RowSlots:
    def __init__(self, rows, cols, lo=0, shares=False):
        self.rows, self.cols, self.lo, self.shares = rows, cols, lo, shares

    def where(self, index, part=None):
        rows, start = self.rows, index * self.rows
        if part is not None:
            rows = rows // 2
            start = start + part * rows
        return pl.ds(pl.multiple_of(start, rows), rows), pl.ds(self.lo, self.cols)

    def landing(self, way, j, half):
        base = way * ((half - 1) * self.rows + self.rows // 2)
        at, rows = (base + (half - 1) * self.rows, self.rows // 2) if j == 1 else (base + (j - 2) * self.rows, self.rows)
        return pl.ds(at, rows), pl.ds(0, self.cols)

    def inbox(self, half):
        return 2 * ((half - 1) * self.rows + self.rows // 2), self.cols


class TileSlots:
    shares = True

    def __init__(self, rows, cols):
        self.rows, self.cols = rows, cols

    def where(self, index, part=None):
        row = lax.div(index, 2)
        cols, start = self.cols, (index - 2 * row) * self.cols
        if part is not None:
            cols = cols // 2
            start = start + part * cols
        return pl.ds(pl.multiple_of(row * self.rows, self.rows), self.rows), pl.ds(pl.multiple_of(start, cols), cols)

    def landing(self, way, j, half):
        at, cols = ((half - 1) * self.cols, self.cols // 2) if j == 1 else ((j - 2) * self.cols, self.cols)
        return pl.ds(way * self.rows, self.rows), pl.ds(at, cols)

    def inbox(self, half):
        return 2 * self.rows, (half - 1) * self.cols + self.cols // 2


class Gather:
    def __init__(self, place, sender, buf, slots):
        self.place, self.sender, self.buf, self.slots = place, sender, buf, slots
        self.sems = [[sender.slot() for _ in range(place.half)] for _ in range(2)]
        self.devices = (place.rings[1], place.rings[-1])

    def own(self):
        return self.buf.at[self.slots.where(self.place.owner(0, self.slots.shares))]

    def send(self, k, way):
        index = self.place.owner(k if way else -k, self.slots.shares)
        ref = self.buf.at[self.slots.where(index, way if k == self.place.half - 1 else None)]
        self.sender.start(self.sems[way][k], ref, ref, self.devices[way])

    def begin(self):
        self.send(0, 0)
        self.send(0, 1)

    def pump(self, k):
        last = k == self.place.half
        for way in range(2):
            index = self.place.owner(k if way else -k, self.slots.shares)
            ref = self.buf.at[self.slots.where(index, way if last else None)]
            self.sender.copy(self.sems[way][k - 1], ref, ref, self.devices[way]).wait_recv()
            if not last:
                self.send(k, way)


class Reduce:
    def __init__(self, place, sender, buf, inbox, slots):
        self.place, self.sender, self.buf, self.inbox, self.slots = place, sender, buf, inbox, slots
        self.sems = [[sender.slot() for _ in range(place.half)] for _ in range(2)]
        self.devices = (place.rings[1], place.rings[-1])

    def target(self, way, j):
        offset = self.place.half - j
        return self.slots.where(
            self.place.owner(-offset if way else offset, self.slots.shares), way if j == 1 else None
        )

    def copy(self, way, j):
        offset = self.place.half - j + 1
        src = self.slots.where(
            self.place.owner(-offset if way else offset, self.slots.shares), way if j == 1 else None
        )
        return self.sems[way][j - 1], self.buf.at[src], self.inbox.at[self.slots.landing(way, j, self.place.half)]

    def send(self, j, way):
        self.sender.start(*self.copy(way, j), self.devices[way])

    def begin(self):
        self.send(1, 0)
        self.send(1, 1)

    def add(self, to, *froms):
        value = self.buf[to].astype(F32)
        for at in froms:
            value = value + self.inbox[at].astype(F32)
        self.buf[to] = value.astype(self.buf.dtype)

    def pump(self, j):
        half = self.place.half
        for way in range(2):
            self.sender.copy(*self.copy(way, j), self.devices[way]).wait_recv()
            if j < half:
                self.add(self.target(way, j), self.slots.landing(way, j, half))
                self.send(j + 1, way)
        if j == half:
            self.add(self.slots.where(self.place.owner(0, self.slots.shares)), *(self.slots.landing(way, j, half) for way in range(2)))

    def mine(self):
        return self.buf.at[self.slots.where(self.place.owner(0, self.slots.shares))]


def shards_of(s, n):
    inner = s // 2
    side = s % 2
    return [2 * inner + side, n - 2 - 2 * inner + side]


def blocks_of(ff):
    return [(at, min(256, ff - at), 2 * at) for at in range(0, ff, 256)]


def key_spots(place, pos_k, rows):
    lane = lax.broadcasted_iota(jnp.int32, (8, rows), 1)
    for i, home in enumerate(place.homes):
        pos_k[:, i * rows : (i + 1) * rows] = (home * rows + lane).astype(F32)


def load_rotary(place, h_rot, rot, rows, sems, first):
    copies = []
    for i, home in enumerate(place.homes):
        src = h_rot.at[pl.ds(pl.multiple_of(home * rows, rows), rows)]
        copies.append(pltpu.make_async_copy(src, rot.at[pl.ds(i * rows, rows)], sems.at[first + i]))
        copies[-1].start()
    return copies


def forward_kernel(
    dims,
    tok, cot, h_wqkv, h_wgu, h_wout, h_wdown, piece_vec, h_rot,
    o_wqkv, o_wout, o_wgu, o_wdown, o_rows, o_tok, o_cot, o_n1, o_qkv, o_stat, o_ctx, o_mid, o_n2, o_act, o_dgu,
    wqkv, wout, wgu, wdown, vec, tok_all, cot_all, n1, qkv, stat, ctx, mid, n2, act, dgu,
    rows_v, bias_v, rot, pos_k, raw, own, send1, send2, recv1, recv2,
    sends, recvs, locals_, outs,
):
    n, m, rows, width, slab, part, ff, b_units = dims
    count = rows * m
    half = count // 2
    inner = part * m
    place = Place(n, m)
    sender = Sender(sends, recvs)
    d, s = place.d, place.s
    bits = place.bits()
    out_rows, vec_rows = part // n, piece_vec.shape[0]
    down_rows, down_cols = 2 * ff // n, width // 2
    blocks = blocks_of(ff)

    ring_a = Gather(place, sender, wqkv, RowSlots(slab, 3 * part))
    ring_v = Gather(place, sender, vec, RowSlots(vec_rows, LANES))
    ring_b = Gather(place, sender, wout, RowSlots(out_rows, width, shares=True))
    ring_c = [Gather(place, sender, wgu, RowSlots(slab, 2 * units, lane)) for _, units, lane in blocks]
    ring_d = Gather(place, sender, wdown, TileSlots(down_rows, down_cols))

    def local(i, src, dst):
        copy = pltpu.make_async_copy(src, dst, locals_.at[i])
        copy.start()
        return copy

    own_rows = pl.ds(pl.multiple_of(d * slab, slab), slab)
    placed_qkv = [
        local(
            2 * i + u,
            h_wqkv.at[:, pl.ds(pl.multiple_of(i * inner + place.shards[u] * LANES, LANES), LANES)],
            wqkv.at[own_rows, pl.ds(i * part + u * LANES, LANES)],
        )
        for i in range(3)
        for u in range(2)
    ]
    placed_vec = local(6, piece_vec, ring_v.own())
    placed_tok = local(7, tok, tok_all.at[pl.ds(0, rows)])
    shard, hidden = ff // 2, h_wgu.shape[1] // 2
    window = raw.shape[2]
    shifts, placed_gu = [], []
    for i in range(2):
        for u in range(2):
            col = place.shards[u] * shard
            first_tile = lax.div(col + (0 if i == 0 else shard + LANES - 1 + hidden - window), LANES)
            base = first_tile * LANES
            shifts.append(col - base + i * hidden)
            src = h_wgu.at[:, pl.ds(pl.multiple_of(base, LANES), window)]
            placed_gu.append(local((8, 12 + m, 13 + m, 14 + m)[2 * i + u], src, raw.at[2 * i + u]))
    placed_cot = local(9, cot, cot_all.at[pl.ds(0, rows)])
    placed_rot = load_rotary(place, h_rot, rot, rows, locals_, 12)
    greet(place)
    moves = place.moves

    class Spread:
        def __init__(self, buf):
            self.buf = buf
            self.sems = [sender.slot() for _ in bits]

        def copy(self, i):
            size = rows << i
            return self.sems[i], self.buf.at[pl.ds(0, size)], self.buf.at[pl.ds(size, size)], place.seqs[bits[i]]

        def send(self, i):
            sender.start(*self.copy(i))

        def wait(self, i):
            sender.copy(*self.copy(i)).wait_recv()

    toks, cots, n2s = Spread(tok_all), Spread(cot_all), Spread(n2)
    written = []

    def write(src, dst):
        copy = pltpu.make_async_copy(src, dst, outs.at[len(written)])
        copy.start()
        written.append(copy)

    for copy in placed_qkv:
        copy.wait()
    ring_a.begin()
    placed_vec.wait()
    ring_v.begin()
    placed_tok.wait()
    toks.send(0)

    src_out = h_wout.at[pl.ds(pl.multiple_of(s * out_rows, out_rows), out_rows)]
    up = lax.div(s, 2)
    src_down = h_wdown.at[
        pl.ds(pl.multiple_of(up * down_rows, down_rows), down_rows),
        pl.ds(pl.multiple_of((s - 2 * up) * down_cols, down_cols), down_cols),
    ]
    turns = [(src_out, ring_b, sender.slot(), 10), (src_down, ring_d, sender.slot(), 11)]

    def turn(ring, index):
        return ring.buf.at[ring.slots.where(index)]

    @pl.when(moves)
    def _():
        for src, ring, slot, _ in turns:
            sender.copy(slot, src, turn(ring, place.there), place.target).start()

    @pl.when(jnp.logical_not(moves))
    def _():
        for src, ring, _, i in turns:
            local(i, src, ring.own()).wait()

    for copy in placed_gu:
        copy.wait()
    lane = lax.broadcasted_iota(jnp.int32, (1, LANES), 1)
    whole, rest = shard // LANES, shard % LANES

    def cut(j, carry):
        size = 64
        span = pl.ds(pl.multiple_of(j * size, size), size)
        tiles = []
        for i in range(2):
            low = pltpu.roll(raw[2 * i, span, :].astype(F32), window - shifts[2 * i], 1)
            high = pltpu.roll(
                raw[2 * i + 1, span, :].astype(F32), lax.rem(window + rest - shifts[2 * i + 1] + window, window), 1
            )
            lows = [low[:, t * LANES : (t + 1) * LANES] for t in range(whole + 1)]
            highs = [high[:, t * LANES : (t + 1) * LANES] for t in range(window // LANES)]
            tiles.append(lows[:whole] + [jnp.where(lane < rest, lows[whole], highs[0])] + highs[1:])
        to = pl.ds(pl.multiple_of(d * slab + j * size, size), size)
        at = 0
        for first_unit, count_, _ in blocks:
            even = count_ // LANES
            t = first_unit // LANES
            line_ = tiles[0][t : t + even]
            if even * LANES < count_:
                line_.append(jnp.where(lane < LANES // 2, tiles[0][t + even], pltpu.roll(tiles[1][t + even], LANES // 2, 1)))
            for tile in line_ + tiles[1][t : t + even]:
                wgu[to, at : at + LANES] = tile.astype(BF16)
                at += LANES
        return carry

    lax.fori_loop(0, slab // 64, cut, 0)
    ring_c[0].begin()
    placed_cot.wait()
    cots.send(0)
    wdown[ff:, :] = jnp.zeros((wdown.shape[0] - ff, width), BF16)
    key_spots(place, pos_k, rows)
    line = lax.broadcasted_iota(jnp.int32, (rows, 1), 0)

    def stats(i):
        span = slice(i * rows, (i + 1) * rows)
        x = tok_all[span, :].astype(F32)
        mu = jnp.mean(x, axis=-1, keepdims=True)
        c = x - mu
        r = lax.rsqrt(jnp.mean(c * c, axis=-1, keepdims=True) + EPS)
        spot = (place.homes[i] * rows + line).astype(F32)
        stat[span, :] = jnp.where(lane == MEAN, mu, jnp.where(lane == RSTD, r, spot))

    stats(0)
    ring_v.pump(1)
    ring_a.pump(1)

    @pl.when(moves)
    def _():
        for src, ring, slot, _ in turns:
            sender.copy(slot, src, ring.own(), place.source).wait_recv()

    ring_b.begin()
    toks.wait(0)
    toks.send(1)
    stats(1)
    ring_v.pump(2)
    ring_a.pump(2)
    ring_d.begin()
    ring_b.pump(1)
    toks.wait(1)
    write(tok_all, o_tok)
    stats(2)
    stats(3)
    cots.wait(0)
    cots.send(1)
    ring_v.pump(3)
    ring_a.pump(3)
    ring_c[1].begin()
    ring_b.pump(2)
    ring_c[0].pump(1)
    ring_v.pump(4)
    units = slab // LANES
    for c in range(n):
        for r in range(4):
            for u in range(units):
                at = c * slab + u * LANES
                row = c * vec_rows + r * units + u
                rows_v[r : r + 1, at : at + LANES] = vec[row : row + 1, :]
    for i in range(3):
        for u in range(part // LANES):
            unit = i * (inner // LANES) + place.shards[u]
            row = lax.div(unit, b_units) * vec_rows + 4 * units + lax.rem(unit, b_units)
            at = i * part + u * LANES
            bias_v[0:1, at : at + LANES] = vec[pl.ds(row, 1), :]
    write(rows_v, o_rows)

    def normalize(j, carry):
        size = 64
        span = pl.ds(pl.multiple_of(j * size, size), size)
        x = tok_all[span, :].astype(F32)
        xhat = (x - stat[span, MEAN : MEAN + 1]) * stat[span, RSTD : RSTD + 1]
        n1[span, :] = (xhat * rows_v[0:1, :] + rows_v[1:2, :]).astype(BF16)
        return carry

    lax.fori_loop(0, count // 64, normalize, 0)
    write(n1, o_n1)
    ring_d.pump(1)
    ring_c[2].begin()
    cots.wait(1)
    write(cot_all, o_cot)
    ring_a.pump(4)
    write(wqkv, o_wqkv)
    for copy in placed_rot:
        copy.wait()

    def project(j, carry):
        size = 256
        span = pl.ds(pl.multiple_of(j * size, size), size)
        for i in range(3):
            cols = slice(i * part, (i + 1) * part)
            y = dot(n1[span, :], wqkv[:, cols]) + bias_v[0:1, cols]
            if i < 2:
                pieces = []
                for u in range(part // LANES):
                    z = y[:, u * LANES : (u + 1) * LANES]
                    pieces.append(
                        z * rot[span, :LANES]
                        + pltpu.roll(z, LANES - ROT // 2, 1) * rot[span, LANES : 2 * LANES]
                        + pltpu.roll(z, ROT // 2, 1) * rot[span, 2 * LANES :]
                    )
                y = jnp.concatenate(pieces, axis=1)
            qkv[span, cols] = y.astype(BF16)
        return carry

    lax.fori_loop(0, count // 256, project, 0)
    write(qkv, o_qkv)
    ring_b.pump(3)
    ring_c[1].pump(1)
    ring_c[0].pump(2)
    scale = HEAD_DIM ** (-0.5)
    per = LANES // HEAD_DIM

    def attend(i, carry):
        pair, block = lax.div(i, m), lax.rem(i, m)
        span = pl.ds(pl.multiple_of(block * rows, rows), rows)
        at = pl.multiple_of(pair * LANES, LANES)
        q = qkv[span, pl.ds(at, LANES)]
        k = qkv[:, pl.ds(pl.multiple_of(part + at, LANES), LANES)]
        v = qkv[:, pl.ds(pl.multiple_of(2 * part + at, LANES), LANES)]
        allowed = pos_k[0:1, :] <= stat[span, SPOT : SPOT + 1]
        total = jnp.zeros((rows, LANES), F32)
        for h in range(per):
            mine = (lane // HEAD_DIM == h).astype(BF16)
            scores = dot_cols(q * mine, k) * scale
            scores = jnp.where(allowed, scores, -jnp.inf)
            top = jnp.max(scores, axis=-1, keepdims=True)
            found = top + jnp.log(jnp.sum(jnp.exp(scores - top), axis=-1, keepdims=True))
            probs = jnp.exp(scores - found).astype(BF16)
            total = total + dot(probs, v * mine)
            stat[span, :] = jnp.where(lane == LSE + pair * per + h, found, stat[span, :])
        ctx[span, pl.ds(at, LANES)] = total.astype(BF16)
        return carry

    lax.fori_loop(0, (part // LANES) * m, attend, 0)
    write(stat, o_stat)
    write(ctx, o_ctx)
    ring_d.pump(2)
    ring_c[2].pump(1)
    ring_b.pump(4)
    write(wout, o_wout)

    step = 512
    scatter = [sender.slot(), sender.slot()]

    def far_part(j, carry):
        cols = pl.ds(pl.multiple_of(j * step, step), step)
        send1[:, cols] = dot(ctx[half:, :], wout[:, cols]).astype(BF16)
        return carry

    lax.fori_loop(0, width // step, far_part, 0)
    first = sender.start(scatter[0], send1, recv1, place.seqs[bits[1]])

    def near_part(j, carry):
        cols = pl.ds(pl.multiple_of(j * step, step), step)
        own[:, cols] = dot(ctx[:half, :], wout[:, cols])
        return carry

    lax.fori_loop(0, width // step, near_part, 0)
    ring_c[1].pump(2)
    first.wait_recv()
    send2[...] = (own[rows:, :] + recv1[rows:, :].astype(F32)).astype(BF16)
    second = sender.start(scatter[1], send2, recv2, place.seqs[bits[0]])
    ring_c[0].pump(3)
    second.wait_recv()
    value = tok_all[:rows, :].astype(F32) + own[:rows, :] + recv1[:rows, :].astype(F32) + recv2[...].astype(F32)
    mid[...] = value
    c = value - jnp.mean(value, axis=-1, keepdims=True)
    r = lax.rsqrt(jnp.mean(c * c, axis=-1, keepdims=True) + EPS)
    n2[:rows, :] = (c * r * rows_v[2:3, :] + rows_v[3:4, :]).astype(BF16)
    n2s.send(0)
    write(mid, o_mid)
    ring_d.pump(3)
    ring_c[2].pump(2)
    ring_c[1].pump(3)
    n2s.wait(0)
    n2s.send(1)
    ring_c[0].pump(4)
    ring_d.pump(4)
    write(wdown, o_wdown)
    n2s.wait(1)
    write(n2, o_n2)
    ring_c[2].pump(3)

    def expand(first_unit, units, base):
        even = units // LANES * LANES
        y = dot(n2[...], wgu[:, base : base + 2 * units])
        d_act = dot_cols(cot_all[...], wdown[first_unit : first_unit + 256, :])
        if even == units:
            gate, up = y[:, :units], y[:, units:]
        else:
            gate = y[:, : even + LANES]
            up = jnp.concatenate([y[:, even + LANES :], pltpu.roll(gate[:, even:], LANES // 2, 1)], axis=1)
        sigma = jax.nn.sigmoid(gate)
        silu = gate * sigma
        value = silu * up
        d_gate = d_act * up * (sigma * (1.0 + gate * (1.0 - sigma)))
        d_up = d_act * silu
        if even == units:
            dgu[:, base : base + units] = d_gate.astype(BF16)
            dgu[:, base + units : base + 2 * units] = d_up.astype(BF16)
        else:
            value = jnp.where(lax.broadcasted_iota(jnp.int32, (1, 256), 1) < units, value, 0.0)
            mixed = jnp.where(lane < LANES // 2, d_gate[:, even:], pltpu.roll(d_up[:, even:], LANES // 2, 1))
            dgu[:, base : base + even] = d_gate[:, :even].astype(BF16)
            dgu[:, base + even : base + even + LANES] = mixed.astype(BF16)
            dgu[:, base + even + LANES : base + 2 * units] = d_up[:, :even].astype(BF16)
        act[:, first_unit : first_unit + 256] = value.astype(BF16)

    expand(*blocks[0])
    ring_c[1].pump(4)
    expand(*blocks[1])
    ring_c[2].pump(4)
    write(wgu, o_wgu)
    expand(*blocks[2])
    write(act, o_act)
    write(dgu, o_dgu)
    for copy in written:
        copy.wait()
    sender.finish()

    @pl.when(moves)
    def _():
        for src, ring, slot, _ in turns:
            sender.copy(slot, src, turn(ring, place.there), place.target).wait_send()


def run_forward(dims, args):
    n, m, rows, width, slab, part, ff, b_units = dims
    count = rows * m
    ffp = -(-ff // 256) * 256
    vec_rows = args[6].shape[0]
    arrays = [
        ((width, 3 * part), BF16), ((part, width), BF16), ((width, 2 * ff), BF16), ((ffp, width), BF16),
        ((8, width), F32), ((count, width), BF16), ((count, width), BF16), ((count, width), BF16),
        ((count, 3 * part), BF16), ((count, LANES), F32), ((count, part), BF16), ((rows, width), F32),
        ((count, width), BF16), ((count, ffp), BF16), ((count, 2 * ff), BF16),
    ]
    scratch = [vmem(*a) for a in arrays]
    rows_v, scratch[4] = scratch[4], vmem((n * vec_rows, LANES), F32)
    slots = (4 + len(blocks_of(ff))) * 2 * (n // 2) + 3 * 2 + 2 + 2
    return pl.pallas_call(
        functools.partial(forward_kernel, dims),
        out_shape=[jax.ShapeDtypeStruct(*a) for a in arrays],
        in_specs=[pl.BlockSpec(memory_space=pl.ANY)] * len(args),
        out_specs=[pl.BlockSpec(memory_space=pl.ANY)] * len(arrays),
        scratch_shapes=scratch
        + [
            rows_v,
            vmem((8, 3 * part), F32),
            vmem((count, 3 * LANES), F32),
            vmem((8, count), F32),
            vmem((4, slab, WINDOW)),
            vmem((count // 2, width), F32),
            vmem((count // 2, width)),
            vmem((rows, width)),
            vmem((count // 2, width)),
            vmem((rows, width)),
            pltpu.SemaphoreType.DMA((slots,)),
            pltpu.SemaphoreType.DMA((slots,)),
            pltpu.SemaphoreType.DMA((15 + m,)),
            pltpu.SemaphoreType.DMA((len(arrays),)),
        ],
        compiler_params=pltpu.CompilerParams(
            collective_id=0, has_side_effects=True, vmem_limit_bytes=VMEM_BYTES
        ),
        name="forward",
    )(*args)


def flip(value):
    size = value.shape[1]
    here = lax.broadcasted_iota(jnp.int32, (size, size), 0) == lax.broadcasted_iota(jnp.int32, (size, size), 1)
    return dot_cols(here.astype(F32).astype(BF16), value).astype(BF16)


def backward_kernel(
    dims,
    h_wqkv, h_wout, h_wgu, h_wdown, h_rows, h_tok, h_cot, h_n1, h_qkv, h_stat, h_ctx, h_mid, h_n2, h_act, h_dgu,
    h_rot,
    o_block, o_input, o_gu, o_qkv, o_down, o_out, o_vec,
    wout, wgu, wqkv, rows_v, wide_a, wide_b, qkv, stat, ctx, mid, act, dgu, rot, pos_k,
    sum_a, sum_b, sum_c, sum_d, sum_v, in_a, in_b, in_c0, in_c1, in_c2, in_d, in_v,
    own, send1, send2, recv1, recv2, dm_all, d_mid, cot, dctx, dqkv, dk, dv, sums_v, bias_v,
    x_gu, x_qkv, x_down, x_out, x_vec, y_qkv, y_down, y_gu,
    sends, recvs, loads, outs,
):
    n, m, rows, width, slab, part, ff, b_units = dims
    ffp = act.shape[1]
    inner = part * m
    count = rows * m
    half = count // 2
    place = Place(n, m)
    sender = Sender(sends, recvs)
    waiting = {}

    def load(name, src, dst):
        copy = pltpu.make_async_copy(src, dst, loads.at[len(waiting)])
        copy.start()
        waiting[name] = copy

    load("n2", h_n2, wide_b)
    load("dgu", h_dgu, dgu)
    load("act", h_act, act)
    load("cot", h_cot, wide_a)
    load("wgu", h_wgu, wgu)
    load("own", h_cot.at[pl.ds(0, dims[2])], cot)
    load("mid", h_mid, mid)
    load("rows", h_rows, rows_v)
    load("wqkv", h_wqkv, wqkv)
    load("wout", h_wout, wout)
    load("ctx", h_ctx, ctx)
    load("qkv", h_qkv, qkv)
    load("stat", h_stat, stat)
    spare = loads.shape[0] - 2
    rotary = load_rotary(place, h_rot, rot, rows, loads, spare - m)
    bits = place.bits()
    others = [mask for mask in range(1, m) if mask not in bits]
    moves = place.moves
    greet(place, others)
    d, s = place.d, place.s
    out_rows, vec_rows = part // n, sum_v.shape[0] // n
    down_rows, down_cols = 2 * ff // n, width // 2
    ring_a = Reduce(place, sender, sum_a, in_a, RowSlots(slab, 3 * part))
    ring_b = Reduce(place, sender, sum_b, in_b, RowSlots(out_rows, width, shares=True))
    ring_c = [
        Reduce(place, sender, sum_c, inbox, RowSlots(slab, 2 * units_, lane_))
        for inbox, (_, units_, lane_) in zip((in_c0, in_c1, in_c2), blocks_of(ff))
    ]
    ring_d = Reduce(place, sender, sum_d, in_d, TileSlots(down_rows, down_cols))
    ring_v = Reduce(place, sender, sum_v, in_v, RowSlots(vec_rows, LANES))
    key_spots(place, pos_k, rows)
    block = 256

    def outer(dst, left, right, size):
        def step(j, carry):
            cols = pl.ds(pl.multiple_of(j * block, block), block)
            dst[cols, :] = dot(flip(left[:, cols]), right[...]).astype(BF16)
            return carry

        lax.fori_loop(0, size // block, step, 0)

    class Halving:
        def __init__(self, at):
            self.slots = [sender.slot(), sender.slot()]
            self.at = at
            self.open = []

        def first(self, far):
            far()
            self.open.append(sender.start(self.slots[0], send1, recv1.at[pl.ds(self.at * half, half)], place.seqs[bits[1]]))

        def second(self):
            self.open[0].wait_recv()
            send2[...] = (own[rows:, :] + recv1[self.at * half + rows : (self.at + 1) * half, :].astype(F32)).astype(BF16)
            self.open.append(sender.start(self.slots[1], send2, recv2.at[pl.ds(self.at * rows, rows)], place.seqs[bits[0]]))

        def total(self):
            self.open[1].wait_recv()
            return own[:rows, :] + recv1[self.at * half : self.at * half + rows, :].astype(F32) + recv2[
                self.at * rows : (self.at + 1) * rows, :
            ].astype(F32)

        def sent(self):
            for copy in self.open:
                copy.wait_send()
            sender.open = [c for c in sender.open if all(c is not o for o in self.open)]

    turns = [(ring_d, x_down, sender.slot()), (ring_b, x_out, sender.slot())]

    def turn_back(i):
        ring, landing, slot = turns[i]

        @pl.when(moves)
        def _():
            sender.copy(slot, ring.mine(), landing, place.source).start()

        @pl.when(jnp.logical_not(moves))
        def _():
            copy = pltpu.make_async_copy(ring.mine(), landing, loads.at[spare + i])
            copy.start()
            copy.wait()

    def turned_back(i):
        ring, landing, slot = turns[i]

        @pl.when(moves)
        def _():
            sender.copy(slot, ring.mine(), landing, place.target).wait_recv()

    def deal(buf, size, landing, whole=False):
        share = size if whole else size // m
        got = []
        to = pl.ds(pl.multiple_of(s * share, share), share)
        for mask in range(1, m):
            start = d * size + (0 if whole else place.partner(mask) * share)
            src = buf.at[pl.ds(pl.multiple_of(start, share), share)]
            got.append(sender.start(sender.slot(), src, landing.at[to], place.seqs[mask]))
        start = d * size + (0 if whole else s * share)
        landing[to, :] = buf[pl.ds(pl.multiple_of(start, share), share), :]
        return got

    waiting["n2"].wait()
    waiting["dgu"].wait()

    def slab_of(index):
        cols = pl.ds(pl.multiple_of(index * slab, slab), slab)
        sum_c[cols, :] = dot(flip(wide_b[:, cols]), dgu[...]).astype(BF16)

    slab_of(place.owner(place.half))
    for ring in ring_c:
        ring.begin()
    waiting["act"].wait()
    waiting["cot"].wait()
    outer(sum_d, act, wide_a, ffp)
    ring_d.begin()
    waiting["wgu"].wait()
    normed2 = Halving(0)

    def back_step(left, lo, hi, weight, to):
        def step(j, carry):
            cols = pl.ds(pl.multiple_of(j * block, block), block)
            to(cols, dot_cols(left[lo:hi, :], weight[cols, :]))
            return carry

        lax.fori_loop(0, width // block, step, 0)

    def to_send(cols, value):
        send1[:, cols] = value.astype(BF16)

    def to_own(cols, value):
        own[:, cols] = value

    normed2.first(lambda: back_step(dgu, half, count, wgu, to_send))
    back_step(dgu, 0, half, wgu, to_own)
    lanes = 2 * ff
    load("down_lo", h_wdown.at[:, pl.ds(0, lanes)], wgu.at[pl.ds(0, ffp)])
    load("down_hi", h_wdown.at[:, pl.ds(lanes, width - lanes)], wgu.at[pl.ds(ffp, ffp), pl.ds(0, width - lanes)])
    normed2.second()

    def other_slabs(i, carry):
        slab_of(lax.rem(place.owner(place.half) + i, n))
        return carry

    lax.fori_loop(1, n, other_slabs, 0)
    load("n1", h_n1, wide_b)
    load("tok", h_tok, wide_a)
    for ring in ring_c:
        ring.pump(1)
    ring_d.pump(1)

    waiting["mid"].wait()
    waiting["rows"].wait()
    waiting["own"].wait()

    def deviation(value):
        c = value - jnp.mean(value, axis=-1, keepdims=True)
        r = lax.rsqrt(jnp.mean(c * c, axis=-1, keepdims=True) + EPS)
        return c * r, r

    xhat, r = deviation(mid[...])
    up = normed2.total()
    sums_v[2:3, :] = jnp.sum(up * xhat, axis=0, keepdims=True)
    sums_v[3:4, :] = jnp.sum(up, axis=0, keepdims=True)
    d_mid[...] = cot[...].astype(F32) + norm_back(up, xhat, r, rows_v[2:3, :])
    dm_all[:rows, :] = d_mid[...].astype(BF16)
    spread = [sender.slot() for _ in bits]

    def spread_copy(i):
        size = rows << i
        return (spread[i], dm_all.at[pl.ds(0, size)], dm_all.at[pl.ds(size, size)])

    def spread_send(i):
        sender.start(*spread_copy(i), place.seqs[bits[i]])

    def spread_wait(i):
        sender.copy(*spread_copy(i), place.seqs[bits[i]]).wait_recv()

    spread_send(0)
    normed2.sent()
    ring_c[0].pump(2)
    ring_c[1].pump(2)

    waiting["down_lo"].wait()
    waiting["down_hi"].wait()

    def down_step(lo, hi, to):
        def low(j, carry):
            cols = pl.ds(pl.multiple_of(j * LANES, LANES), LANES)
            to(cols, dot(act[lo:hi, :], wgu[:ffp, cols]))
            return carry

        def high(j, carry):
            cols = pl.ds(pl.multiple_of(j * LANES, LANES), LANES)
            to(pl.ds(pl.multiple_of(lanes + j * LANES, LANES), LANES), dot(act[lo:hi, :], wgu[ffp : 2 * ffp, cols]))
            return carry

        lax.fori_loop(0, lanes // LANES, low, 0)
        lax.fori_loop(0, (width - lanes) // LANES, high, 0)

    output = Halving(1)

    output.first(lambda: down_step(half, count, to_send))
    down_step(0, half, to_own)
    spread_wait(0)
    spread_send(1)
    output.second()
    ring_c[2].pump(2)
    ring_d.pump(2)
    spread_wait(1)

    waiting["wout"].wait()
    waiting["ctx"].wait()
    dctx[...] = dot_cols(dm_all[...], wout[...]).astype(BF16)
    outer(sum_b, ctx, dm_all, part)
    ring_b.begin()
    cot[...] = (mid[...] + output.total()).astype(BF16)
    output.sent()

    for name in ("qkv", "stat"):
        waiting[name].wait()
    for copy in rotary:
        copy.wait()
    scale = HEAD_DIM ** (-0.5)
    per = LANES // HEAD_DIM
    lane = lax.broadcasted_iota(jnp.int32, (1, LANES), 1) // HEAD_DIM

    def turned(z, span):
        return (
            z * rot[span, :LANES]
            - pltpu.roll(z, LANES - ROT // 2, 1) * rot[span, LANES : 2 * LANES]
            - pltpu.roll(z, ROT // 2, 1) * rot[span, 2 * LANES :]
        )

    bias_v[...] = jnp.zeros_like(bias_v)
    for pair in range(part // LANES):
        at = pair * LANES
        dk[...] = jnp.zeros_like(dk)
        dv[...] = jnp.zeros_like(dv)

        def attend(i, carry, pair=pair, at=at):
            span = pl.ds(pl.multiple_of(i * rows, rows), rows)
            q = qkv[span, at : at + LANES]
            k = qkv[:, part + at : part + at + LANES]
            v = qkv[:, 2 * part + at : 2 * part + at + LANES]
            dc = dctx[span, at : at + LANES]
            both = dc.astype(F32) * ctx[span, at : at + LANES].astype(F32)
            allowed = pos_k[0:1, :] <= stat[span, SPOT : SPOT + 1]
            dq = jnp.zeros((rows, LANES), F32)
            for h in range(per):
                pick = lane == h
                mine = pick.astype(BF16)
                qm, dcm = q * mine, dc * mine
                scores = dot_cols(qm, k) * scale
                at_lse = LSE + pair * per + h
                probs = jnp.exp(jnp.where(allowed, scores, -jnp.inf) - stat[span, at_lse : at_lse + 1])
                delta = jnp.sum(jnp.where(pick, both, 0.0), axis=-1, keepdims=True)
                ds = (probs * (dot_cols(dcm, v) - delta) * scale).astype(BF16)
                dq = dq + jnp.dot(ds, k * mine, preferred_element_type=F32)
                dk[...] += dot(flip(ds), qm)
                dv[...] += dot(flip(probs.astype(BF16)), dcm)
            dq = turned(dq, span)
            bias_v[0:1, at : at + LANES] += jnp.sum(dq, axis=0, keepdims=True)
            dqkv[span, at : at + LANES] = dq.astype(BF16)
            return carry

        lax.fori_loop(0, m, attend, 0)

        def settle(i, carry, at=at):
            span = pl.ds(pl.multiple_of(i * rows, rows), rows)
            key, value = turned(dk[span, :], span), dv[span, :]
            bias_v[0:1, part + at : part + at + LANES] += jnp.sum(key, axis=0, keepdims=True)
            bias_v[0:1, 2 * part + at : 2 * part + at + LANES] += jnp.sum(value, axis=0, keepdims=True)
            dqkv[span, part + at : part + at + LANES] = key.astype(BF16)
            dqkv[span, 2 * part + at : 2 * part + at + LANES] = value.astype(BF16)
            return carry

        lax.fori_loop(0, m, settle, 0)
        if pair == 0:
            for ring in ring_c:
                ring.pump(3)

    waiting["n1"].wait()
    outer(sum_a, wide_b, dqkv, width)
    ring_a.begin()
    ring_d.pump(3)
    ring_b.pump(1)
    waiting["wqkv"].wait()
    waiting["tok"].wait()
    normed1 = Halving(2)

    def gains(cols, value, lo, hi):
        xh = (wide_a[lo:hi, cols].astype(F32) - stat[lo:hi, MEAN : MEAN + 1]) * stat[lo:hi, RSTD : RSTD + 1]
        return jnp.sum(value * xh, axis=0, keepdims=True), jnp.sum(value, axis=0, keepdims=True)

    def far_last(cols, value):
        send1[:, cols] = value.astype(BF16)
        sums_v[0:1, cols], sums_v[1:2, cols] = gains(cols, value, half, count)

    def near_last(cols, value):
        own[:, cols] = value
        gain, total = gains(cols, value, 0, half)
        sums_v[0:1, cols] += gain
        sums_v[1:2, cols] += total

    normed1.first(lambda: back_step(dqkv, half, count, wqkv, far_last))
    back_step(dqkv, 0, half, wqkv, near_last)

    sum_v[...] = jnp.zeros_like(sum_v)
    units = slab // LANES

    def lay(c, carry):
        for i in range(4):
            for u in range(units):
                at = pl.multiple_of(c * slab + u * LANES, LANES)
                sum_v[pl.ds(c * vec_rows + i * units + u, 1), :] = sums_v[i : i + 1, pl.ds(at, LANES)]
        return carry

    lax.fori_loop(0, n, lay, 0)
    for i in range(3):
        for u in range(part // LANES):
            unit = i * (inner // LANES) + place.shards[u]
            row = lax.div(unit, b_units) * vec_rows + 4 * units + lax.rem(unit, b_units)
            at = i * part + u * LANES
            sum_v[pl.ds(row, 1), :] = bias_v[0:1, at : at + LANES]
    ring_v.begin()
    normed1.second()
    ring_b.pump(2)
    ring_a.pump(1)
    ring_v.pump(1)
    for ring in ring_c:
        ring.pump(4)
    got_gu = deal(sum_c, slab, x_gu)
    ring_d.pump(4)
    ring_b.pump(3)
    ring_a.pump(2)
    ring_v.pump(2)
    ring_b.pump(4)
    up = normed1.total()
    rstd = stat[:rows, RSTD : RSTD + 1]
    xhat = (wide_a[:rows, :].astype(F32) - stat[:rows, MEAN : MEAN + 1]) * rstd
    own[:rows, :] = d_mid[...] + norm_back(up, xhat, rstd, rows_v[0:1, :])
    ring_v.pump(3)

    written = []

    def store(src, dst):
        copy = pltpu.make_async_copy(src, dst, outs.at[len(written)])
        copy.start()
        written.append(copy)

    store(cot, o_block)
    store(own.at[pl.ds(0, rows)], o_input)
    ring_a.pump(3)
    turn_back(0)
    turn_back(1)
    lane128 = lax.broadcasted_iota(jnp.int32, (1, LANES), 1)

    def lay_out(got, to):
        share, shard, hidden = slab // m, ff // 2, ff * m
        found = {}
        for t in range(m):
            span = slice(t * share, (t + 1) * share)
            tiles = [[], []]
            at = 0
            for _, units_, _ in blocks_of(ff):
                even = units_ // LANES
                tiles[0] += [got[span, at + k * LANES : at + (k + 1) * LANES].astype(F32) for k in range(even)]
                at += even * LANES
                odd = []
                if even * LANES < units_:
                    mixed = got[span, at : at + LANES].astype(F32)
                    odd = [mixed, pltpu.roll(mixed, LANES // 2, 1)]
                    at += LANES
                tiles[1] += [got[span, at + k * LANES : at + (k + 1) * LANES].astype(F32) for k in range(even)]
                at += even * LANES
                if odd:
                    tiles[0].append(odd[0])
                    tiles[1].append(odd[1])
            for i in range(2):
                for u, held in enumerate(shards_of(t, n)):
                    start, first, end = u * shard, i * hidden + held * shard, i * hidden + (held + 1) * shard
                    shift = (first - start) % LANES
                    back = (first - start - shift) // LANES
                    for tile in range(first // LANES, (end - 1) // LANES + 1):
                        k = tile - back
                        parts_ = [tiles[i][q] if 0 <= q < len(tiles[i]) else None for q in (k, k - 1)]
                        if shift:
                            here, before = [None if p is None else pltpu.roll(p, shift, 1) for p in parts_]
                            if here is None or before is None:
                                value = before if here is None else here
                            else:
                                value = jnp.where(lane128 < shift, before, here)
                        else:
                            value = parts_[0]
                        lo, hi = max(first, tile * LANES), min(end, (tile + 1) * LANES)
                        found.setdefault(tile, []).append((lo - tile * LANES, hi - tile * LANES, value))
        for tile, parts_ in found.items():
            parts_.sort(key=lambda p: p[0])
            value = parts_[-1][2]
            for _, hi, other in reversed(parts_[:-1]):
                value = jnp.where(lane128 < hi, other, value)
            to[:, tile * LANES : (tile + 1) * LANES] = value.astype(BF16)

    ring_v.pump(4)
    got_vec = deal(sum_v, vec_rows, x_vec, whole=True)
    for copy in got_gu:
        copy.wait_recv()
    lay_out(x_gu, y_gu)
    store(y_gu, o_gu)
    for copy in got_vec:
        copy.wait_recv()
    total = x_vec[:vec_rows, :]
    for t in range(1, m):
        total = total + x_vec[t * vec_rows : (t + 1) * vec_rows, :]
    x_vec[:vec_rows, :] = total
    some = slab // m
    sizes = [(i * units, some) for i in range(4)] + [(4 * units, b_units * LANES // m)]
    for i, (first_row, size) in enumerate(sizes):
        tile = lax.div(s * size, LANES)
        shift = s * size - tile * LANES
        low = x_vec[pl.ds(first_row + tile, 1), :]
        high = x_vec[pl.ds(first_row + tile + 1, 1), :]
        both = jnp.where(lane128 < shift, high, low)
        sums_v[i : i + 1, :LANES] = pltpu.roll(both, lax.rem(LANES - shift, LANES), 1)
    store(sums_v.at[:, pl.ds(0, LANES)], o_vec)
    ring_a.pump(4)
    got_qkv = deal(sum_a, slab, x_qkv)
    turned_back(0)
    some = down_rows // 2
    value = x_down[...].astype(F32)
    d_mid[:some, :down_cols] = value[:some, :]
    d_mid[:some, down_cols:] = value[some:, :]
    column = lax.rem(s, 2)
    across = pl.ds(pl.multiple_of(column * down_cols, down_cols), down_cols)
    swap = sender.start(
        sender.slot(),
        d_mid.at[pl.ds(0, some), pl.ds(pl.multiple_of((1 - column) * down_cols, down_cols), down_cols)],
        y_down.at[:, across],
        place.seqs[1],
    )
    y_down[:, across] = d_mid[:some, across]
    turned_back(1)
    store(x_out, o_out)
    swap.wait_recv()
    store(y_down, o_down)
    for copy in got_qkv:
        copy.wait_recv()
    share = slab // m
    for t in range(m):
        for i in range(3):
            for u, held in enumerate(shards_of(t, n)):
                at, come = i * inner + held * LANES, i * part + u * LANES
                y_qkv[:, at : at + LANES] = x_qkv[t * share : (t + 1) * share, come : come + LANES]
    store(y_qkv, o_qkv)
    for copy in written:
        copy.wait()
    sender.finish()

    @pl.when(moves)
    def _():
        for ring, landing, slot in turns:
            sender.copy(slot, ring.mine(), landing, place.source).wait_send()


def run_backward(dims, args):
    n, m, rows, width, slab, part, ff, b_units = dims
    count = rows * m
    ffp = -(-ff // 256) * 256
    vec_rows = -(-(4 * (slab // LANES) + b_units) // TILE) * TILE
    half = n // 2
    out_rows = part // n
    down_rows, down_cols = 2 * ff // n, width // 2
    share = slab // m

    def inbox(slots, dtype=BF16):
        return vmem(slots.inbox(half), dtype)

    outputs = [
        ((rows, width), BF16), ((rows, width), F32), ((share, 2 * ff * m), BF16), ((share, 3 * part * m), BF16),
        ((down_rows // 2, width), F32), ((out_rows, width), BF16), ((8, LANES), F32),
    ]
    scratch = [
        vmem((part, width)), vmem((width, 2 * ff)), vmem((width, 3 * part)), vmem((8, width), F32),
        vmem((count, width)), vmem((count, width)), vmem((count, 3 * part)), vmem((count, LANES), F32),
        vmem((count, part)), vmem((rows, width), F32), vmem((count, ffp)), vmem((count, 2 * ff)),
        vmem((count, 3 * LANES), F32), vmem((8, count), F32),
        vmem((n * slab, 3 * part)), vmem((part, width)), vmem((n * slab, 2 * ff)), vmem((ffp, width)),
        vmem((n * vec_rows, LANES), F32),
        inbox(RowSlots(slab, 3 * part)), inbox(RowSlots(out_rows, width, shares=True)), *[inbox(RowSlots(slab, 2 * units)) for _, units, _ in blocks_of(ff)],
        inbox(TileSlots(down_rows, down_cols)), inbox(RowSlots(vec_rows, LANES), F32),
        vmem((count // 2, width), F32), vmem((count // 2, width)), vmem((rows, width)),
        vmem((3 * count // 2, width)), vmem((3 * rows, width)),
        vmem((count, width)), vmem((rows, width), F32), vmem((rows, width)), vmem((count, part)), vmem((count, 3 * part)),
        vmem((count, LANES), F32), vmem((count, LANES), F32), vmem((8, width), F32), vmem((8, 3 * part), F32),
        vmem((slab, 2 * ff)), vmem((slab, 3 * part)), vmem((down_rows, down_cols)),
        vmem((out_rows, width)), vmem((m * vec_rows, LANES), F32), vmem((share, 3 * part * m)),
        vmem((down_rows // 2, width), F32), vmem((share, 2 * ff * m)),
    ]
    slots = (4 + len(blocks_of(ff))) * 2 * half + 3 * 2 + 2 + 2 + 3 * (m - 1) + 1
    return pl.pallas_call(
        functools.partial(backward_kernel, dims),
        out_shape=[jax.ShapeDtypeStruct(*a) for a in outputs],
        in_specs=[pl.BlockSpec(memory_space=pl.ANY)] * len(args),
        out_specs=[pl.BlockSpec(memory_space=pl.ANY)] * len(outputs),
        scratch_shapes=scratch
        + [
            pltpu.SemaphoreType.DMA((slots,)),
            pltpu.SemaphoreType.DMA((slots,)),
            pltpu.SemaphoreType.DMA((len(args) + 12,)),
            pltpu.SemaphoreType.DMA((len(outputs),)),
        ],
        compiler_params=pltpu.CompilerParams(
            collective_id=1, has_side_effects=True, vmem_limit_bytes=VMEM_BYTES
        ),
        name="backward",
    )(*args)


def rotary_lines(length):
    half = ROT // 2
    lane = np.arange(LANES) % HEAD_DIM
    angles = np.arange(length)[:, None] * (10000.0 ** (-(lane % half) * 2.0 / ROT))[None, :]
    cosine, sine = np.cos(angles), np.sin(angles)
    lines = [
        np.where(lane < ROT, cosine, 1.0),
        np.where(lane < half, -sine, 0.0),
        np.where((lane >= half) & (lane < ROT), sine, 0.0),
    ]
    return jnp.asarray(np.concatenate(lines, axis=1), F32)


def shards(tokens, cotangent, gain1, bias1, w_qkv, b_qkv, w_out, gain2, bias2, w_gate_up, w_down):
    n, m, s = lax.axis_size("dp"), lax.axis_size("seq"), lax.axis_index("seq")
    rows, width = tokens.shape
    slab = gain1.shape[0]
    inner, hidden = w_out.shape[0] * n, w_down.shape[0] * n
    part, ff = inner // m, hidden // m
    dims = (n, m, rows, width, slab, part, ff, b_qkv.shape[0] // LANES)
    parts = [gain1, bias1, gain2, bias2, b_qkv]
    total = sum(p.shape[0] for p in parts)
    length = -(-total // (TILE * LANES)) * TILE * LANES
    vec, at = jnp.zeros((length,), F32), 0
    for p in parts:
        vec = vec + jnp.pad(p.astype(F32), (at, length - at - p.shape[0]))
        at += p.shape[0]
    vec = vec.reshape(-1, LANES)
    rot = rotary_lines(rows * m)
    kept = run_forward(dims, (tokens, cotangent, w_qkv, w_gate_up, w_out, w_down, vec, rot))
    block_out, input_grad, g_gu, g_qkv, g_down, g_out, line = run_backward(dims, tuple(kept) + (rot,))
    vectors = [line[i, : size // m] for i, size in enumerate([slab] * 4 + [b_qkv.shape[0]])]
    return (
        block_out,
        input_grad,
        vectors[0],
        vectors[1],
        g_qkv.astype(F32),
        vectors[4],
        g_out.astype(F32),
        vectors[2],
        vectors[3],
        g_gu.astype(F32),
        g_down,
    )


def fits(mesh, shapes):
    n, m = mesh.shape["dp"], mesh.shape["seq"]
    (rows, width), slab = shapes[0], shapes[2][0]
    part, ff = shapes[6][0] * n // m, shapes[10][0] * n // m
    return (
        m == 4
        and n == 2 * m
        and rows % LANES == 0
        and shapes[6][0] == LANES
        and slab == 256
        and width % 512 == 0
        and shapes[5][0] % LANES == 0
        and part == 256
        and (ff // 2) + LANES - 1 <= WINDOW
        and ff // 2 + (ff // 2) % LANES <= WINDOW
        and shapes[9][1] // 2 % LANES == 0
        and 512 < ff <= 768
        and ff % 64 == 0
        and (2 * ff // n) % TILE == 0
        and 2 * ff <= width <= 4 * ff
        and 2 * 768 <= width
    )


def solution(mesh):
    rows, cols, vec = P(("dp", "seq"), None), P("dp", None), P("dp")
    flat = P(("dp", "seq"))
    def step(*args):
        body = shards if fits(mesh, [a.shape for a in args]) else shards_plain
        return body(*args)

    return jax.shard_map(
        step,
        mesh=mesh,
        in_specs=(rows, rows, vec, vec, cols, vec, cols, vec, vec, cols, cols),
        out_specs=(rows, rows, flat, flat, rows, flat, rows, flat, flat, rows, rows),
        check_vma=False,
    )
```

```python
import functools

import jax
import jax.numpy as jnp
import numpy as np
from jax import lax
from jax.experimental import pallas as pl
from jax.experimental.pallas import tpu as pltpu
from jax.sharding import PartitionSpec as P

HEAD_DIM = 64
ROT = 16
EPS = 1e-05
F32 = jnp.float32
BF16 = jnp.bfloat16


def ring_order(n):
    return list(range(0, n, 2)) + list(range(n - 1, 0, -2))


def dot(a, b):
    return jnp.dot(a, b, preferred_element_type=F32)


def dot_rows(a, b):
    return lax.dot_general(a, b, (((0,), (0,)), ((), ())), preferred_element_type=F32)


def dot_cols(a, b):
    return lax.dot_general(a, b, (((1,), (1,)), ((), ())), preferred_element_type=F32)


class Ring:
    def __init__(self):
        n = lax.axis_size("dp")
        order = ring_order(n)
        place = [order.index(i) for i in range(n)]
        self.n, self.half = n, n // 2
        self.right = [(order[i], order[(i + 1) % n]) for i in range(n)]
        self.left = [(b, a) for a, b in self.right]
        self.order = jnp.array(order, jnp.int32)
        self.place = jnp.array(place, jnp.int32)[lax.axis_index("dp")]

    def owner(self, offset):
        return self.order[lax.rem(self.place + offset + self.n, self.n)]

    def go_right(self, value):
        return lax.ppermute(value, "dp", self.right)

    def go_left(self, value):
        return lax.ppermute(value, "dp", self.left)

    def gather(self, piece):
        rows = piece.shape[0]
        cut = rows // 2
        from_left = from_right = piece
        whole = jnp.zeros((self.n,) + piece.shape, piece.dtype)

        def put(whole, offset, chunk):
            return lax.dynamic_update_slice(
                whole, chunk[None], (self.owner(offset),) + (0,) * piece.ndim
            )

        whole = put(whole, 0, piece)
        for k in range(1, self.half):
            from_left = self.go_right(from_left)
            from_right = self.go_left(from_right)
            whole = put(put(whole, -k, from_left), k, from_right)
        upper = self.go_right(from_left[:cut])
        lower = self.go_left(from_right[cut:])
        return put(whole, self.half, jnp.concatenate([upper, lower]))

    def scatter(self, parts):
        rows = parts.shape[1]
        cut = rows // 2

        def mine(offset):
            start = (self.owner(offset),) + (0,) * (parts.ndim - 1)
            return lax.dynamic_slice(parts, start, (1,) + parts.shape[1:])[0]

        def add(a, b):
            return a.astype(F32) + b.astype(F32)

        far = mine(self.half)
        upper = self.go_right(far[:cut])
        lower = self.go_left(far[cut:])
        from_left, from_right = mine(self.half - 1), mine(1 - self.half)
        from_left = jnp.concatenate(
            [add(from_left[:cut], upper).astype(BF16), from_left[cut:]]
        )
        from_right = jnp.concatenate(
            [from_right[:cut], add(from_right[cut:], lower).astype(BF16)]
        )
        for k in range(self.half - 2, -1, -1):
            from_left = self.go_right(from_left)
            from_right = self.go_left(from_right)
            if k:
                from_left = add(from_left, mine(k)).astype(BF16)
                from_right = add(from_right, mine(-k)).astype(BF16)
        return add(mine(0), from_left) + from_right.astype(F32)


class Group:
    def __init__(self):
        self.m = lax.axis_size("seq")
        self.s = lax.axis_index("seq")
        self.bits = []
        bit = self.m // 2
        while bit:
            self.bits.append(bit)
            bit //= 2
        self.offsets = [0]
        for bit in self.bits:
            self.offsets += [o ^ bit for o in self.offsets]

    def swap(self, value, mask):
        return lax.ppermute(value, "seq", [(i, i ^ mask) for i in range(self.m)])

    def gather(self, value):
        for bit in self.bits:
            value = jnp.concatenate([value, self.swap(value, bit)])
        return value

    def scatter(self, value):
        for bit in reversed(self.bits):
            half = value.shape[0] // 2
            got = self.swap(value[half:].astype(BF16), bit)
            value = value[:half] + got.astype(F32)
        return value

    def exchange(self, blocks):
        got = []
        for mask in range(self.m):
            block = lax.dynamic_index_in_dim(blocks, self.s ^ mask, 0, keepdims=False)
            got.append(self.swap(block, mask) if mask else block)
        stacked = jnp.stack(got)
        return jnp.take(stacked, self.s ^ jnp.arange(self.m), axis=0)


def norm(value):
    center = value - jnp.mean(value, axis=-1, keepdims=True)
    rstd = lax.rsqrt(jnp.mean(center * center, axis=-1, keepdims=True) + EPS)
    return center * rstd, rstd


def norm_back(upstream, xhat, rstd, gain):
    e = upstream * gain
    inner = (
        e
        - jnp.mean(e, axis=-1, keepdims=True)
        - xhat * jnp.mean(e * xhat, axis=-1, keepdims=True)
    )
    return rstd * inner


def rotary_tables(positions):
    half = ROT // 2
    inverse = 10000.0 ** (-(jnp.arange(half, dtype=F32) * 2.0 / ROT))
    angles = positions.astype(F32)[:, None] * inverse[None, :]
    return jnp.cos(angles)[:, None, :], jnp.sin(angles)[:, None, :]


def rotate(tensor, cosine, sine):
    half = ROT // 2
    a, b = tensor[..., :half], tensor[..., half:ROT]
    return jnp.concatenate([a * cosine - b * sine, b * cosine + a * sine, tensor[..., ROT:]], axis=-1)


def shards_plain(tokens, cotangent, gain1, bias1, w_qkv, b_qkv, w_out, gain2, bias2, w_gate_up, w_down):
    ring, group = Ring(), Group()
    n, m, s = ring.n, group.m, group.s
    rows, width = tokens.shape
    slab = gain1.shape[0]
    inner = w_out.shape[0] * n
    hidden = w_down.shape[0] * n
    part, ff = inner // m, hidden // m
    heads = part // HEAD_DIM
    scale = HEAD_DIM ** (-0.5)

    both = jnp.stack([tokens, cotangent], axis=1)
    everything = group.gather(both)
    tokens_all, cot_all = everything[:, 0], everything[:, 1]

    qkv_piece = jnp.concatenate(
        [lax.dynamic_slice(w_qkv, (0, i * inner + s * part), (slab, part)) for i in range(3)], axis=1
    )
    small = jnp.concatenate([gain1, bias1, gain2, bias2, b_qkv])
    extra = -(-small.shape[0] // (3 * part))
    small = jnp.pad(small, (0, extra * 3 * part - small.shape[0])).reshape(extra, 3 * part)
    first = ring.gather(jnp.concatenate([qkv_piece, small]))
    wqkv = first[:, :slab].reshape(width, 3 * part)
    vectors = first[:, slab:].reshape(n, -1)

    def vector(at, size):
        return vectors[:, at : at + size].reshape(-1).astype(F32)

    g1, b1, g2, b2 = (vector(i * slab, slab) for i in range(4))
    bias_all = vector(4 * slab, b_qkv.shape[0]).reshape(3, m, part)
    bias_qkv = lax.dynamic_index_in_dim(bias_all, s, 1, keepdims=False).reshape(3 * part)

    turn = [(g, (g % n) * m + g // n) for g in range(n * m)]
    back = [(b, a) for a, b in turn]

    def quarter(weight):
        count = weight.shape[0] // m
        mine = lax.dynamic_slice(weight, (0, 0), weight.shape)
        return mine.reshape(m, count, weight.shape[1])[s]

    out_rows, down_rows = w_out.shape[0] // m, w_down.shape[0] // m
    moved = lax.ppermute(
        jnp.concatenate([quarter(w_out), quarter(w_down)]), ("dp", "seq"), turn
    )
    wout = ring.gather(moved[:out_rows]).reshape(part, width)
    gu_piece = jnp.concatenate(
        [lax.dynamic_slice(w_gate_up, (0, i * hidden + s * ff), (slab, ff)) for i in range(2)], axis=1
    )
    wgu = ring.gather(gu_piece).reshape(width, 2 * ff)
    wdown = ring.gather(moved[out_rows:]).reshape(ff, width)

    places = jnp.concatenate([(s ^ o) * rows + jnp.arange(rows, dtype=jnp.int32) for o in group.offsets])
    cosine, sine = rotary_tables(places)
    count = rows * m
    xhat1, rstd1 = norm(tokens_all.astype(F32))
    normed1 = (xhat1 * g1 + b1).astype(BF16)
    qkv = (dot(normed1, wqkv) + bias_qkv).reshape(count, 3, heads, HEAD_DIM)
    queries = rotate(qkv[:, 0], cosine, sine).astype(BF16)
    keys = rotate(qkv[:, 1], cosine, sine).astype(BF16)
    values = qkv[:, 2].astype(BF16)
    scores = jnp.einsum("qhd,khd->hqk", queries, keys, preferred_element_type=F32) * scale
    scores = jnp.where((places[None, :] <= places[:, None])[None], scores, -jnp.inf)
    top = jnp.max(scores, axis=-1, keepdims=True)
    lse = top + jnp.log(jnp.sum(jnp.exp(scores - top), axis=-1, keepdims=True))
    probs = jnp.exp(scores - lse)
    probs_r = probs.astype(BF16)
    context = jnp.einsum("hqk,khd->qhd", probs_r, values, preferred_element_type=F32).astype(BF16)
    context_flat = context.reshape(count, part)
    x_own = tokens.astype(F32)
    mid = x_own + group.scatter(dot(context_flat, wout))
    xhat2, rstd2 = norm(mid)
    normed2 = group.gather((xhat2 * g2 + b2).astype(BF16))
    gate_up = dot(normed2, wgu)
    gate, up = gate_up[:, :ff], gate_up[:, ff:]
    sigma = jax.nn.sigmoid(gate)
    silu = gate * sigma
    act = (silu * up).astype(BF16)
    d_act = dot_cols(cot_all, wdown)
    d_gate = d_act * up * (sigma * (1.0 + gate * (1.0 - sigma)))
    d_gate_up = jnp.concatenate([d_gate, d_act * silu], axis=1).astype(BF16)

    d_normed2 = group.scatter(dot_cols(d_gate_up, wgu))
    sum_down = ring.scatter(dot_rows(act, cot_all).astype(BF16).reshape(n, ff // n, width))
    sum_gu = ring.scatter(dot_rows(normed2, d_gate_up).astype(BF16).reshape(n, slab, 2 * ff))
    block_out = (mid + group.scatter(dot(act, wdown))).astype(BF16)
    d_mid = cotangent.astype(F32) + norm_back(d_normed2, xhat2, rstd2, g2)
    d_mid_r = group.gather(d_mid.astype(BF16))

    d_context = dot_cols(d_mid_r, wout).astype(BF16).reshape(count, heads, HEAD_DIM)
    sum_out = ring.scatter(dot_rows(context_flat, d_mid_r).astype(BF16).reshape(n, part // n, width))
    d_probs = jnp.einsum("qhd,khd->hqk", d_context, values, preferred_element_type=F32)
    delta = jnp.einsum("qhd,qhd->hq", d_context.astype(F32), context.astype(F32))[..., None]
    d_scores = (probs * (d_probs - delta) * scale).astype(BF16)
    d_queries = jnp.einsum("hqk,khd->qhd", d_scores, keys, preferred_element_type=F32)
    d_keys = jnp.einsum("hqk,qhd->khd", d_scores, queries, preferred_element_type=F32)
    d_values = jnp.einsum("hqk,qhd->khd", probs_r, d_context, preferred_element_type=F32)
    d_qkv = jnp.stack(
        [rotate(d_queries, cosine, -sine), rotate(d_keys, cosine, -sine), d_values], axis=1
    ).reshape(count, 3 * part)
    d_qkv_r = d_qkv.astype(BF16)
    d_normed1_part = dot_cols(d_qkv_r, wqkv)
    d_normed1 = group.scatter(d_normed1_part)
    own = (slice(0, rows),)
    input_grad = d_mid + norm_back(d_normed1, xhat1[own], rstd1[own], g1)

    bias_part = jnp.zeros((3, m, part), F32)
    bias_part = lax.dynamic_update_slice(bias_part, jnp.sum(d_qkv, axis=0).reshape(3, 1, part), (0, s, 0))
    vector_parts = [
        jnp.sum(d_normed1_part * xhat1, axis=0),
        jnp.sum(d_normed1_part, axis=0),
        jnp.sum(d_normed2 * xhat2, axis=0),
        jnp.sum(d_normed2, axis=0),
        bias_part.reshape(-1),
    ]
    line = jnp.concatenate([v.reshape(n, m, -1) for v in vector_parts], axis=-1)
    lines = -(-line.shape[-1] // (3 * part))
    line = jnp.pad(line, ((0, 0), (0, 0), (0, lines * 3 * part - line.shape[-1])))
    line = line.reshape(n, m, lines, 3 * part).astype(BF16)
    part_qkv = dot_rows(normed1, d_qkv_r).astype(BF16).reshape(n, m, slab // m, 3 * part)
    packed = jnp.concatenate([part_qkv, line], axis=2)
    packed_rows = packed.shape[2]
    sum_qkv = ring.scatter(packed.reshape(n, m * packed_rows, 3 * part))

    def owners(total):
        return group.exchange(total.astype(BF16).reshape((m, -1) + total.shape[1:])).astype(F32)

    last = owners(sum_qkv)
    g_qkv = last[:, : slab // m].reshape(m, slab // m, 3, part).transpose(1, 2, 0, 3)
    g_qkv = g_qkv.reshape(slab // m, 3 * inner)
    line = jnp.sum(last[:, slab // m :], axis=0).reshape(-1)
    sizes = [slab // m] * 4 + [b_qkv.shape[0] // m]
    vectors_out, at = [], 0
    for size in sizes:
        vectors_out.append(line[at : at + size])
        at += size
    g_gu = owners(sum_gu).reshape(m, slab // m, 2, ff).transpose(1, 2, 0, 3).reshape(slab // m, 2 * hidden)
    g_down = lax.ppermute(sum_down.astype(BF16), ("dp", "seq"), back).astype(F32)
    g_out = lax.ppermute(sum_out.astype(BF16), ("dp", "seq"), back).astype(F32)
    return (
        block_out,
        input_grad,
        vectors_out[0],
        vectors_out[1],
        g_qkv,
        vectors_out[4],
        g_out,
        vectors_out[2],
        vectors_out[3],
        g_gu,
        g_down,
    )


LOGICAL = pl.DeviceIdType.LOGICAL
MEAN, RSTD, SPOT, LSE = 0, 1, 2, 8
LANES = 128
TILE = 16
WINDOW = 512
VMEM_BYTES = 67_043_328


def vmem(shape, dtype=BF16):
    return pltpu.VMEM(shape, dtype)


class Place:
    def __init__(self, n, m):
        self.n, self.m, self.half = n, m, n // 2
        self.d, self.s = lax.axis_index("dp"), lax.axis_index("seq")
        pair = lax.div(self.d, 2)
        odd = self.d - 2 * pair
        place = pair + odd * (n - 1 - 2 * pair)
        self.owners = []
        for offset in range(n):
            spot = lax.rem(place + offset, n)
            back = lax.div(spot, self.half)
            self.owners.append(2 * spot + back * (2 * n - 1 - 4 * spot))
        self.partners = []
        for mask in range(m):
            out, bit = self.s, 1
            while bit < m:
                if mask & bit:
                    out = out + bit - 2 * bit * lax.rem(lax.div(self.s, bit), 2)
                bit *= 2
            self.partners.append(out)
        self.rings = {1: self.owners[1] * m + self.s, -1: self.owners[n - 1] * m + self.s}
        self.seqs = [self.d * m + out for out in self.partners]
        inner_ = lax.div(self.s, 2)
        side = self.s - 2 * inner_
        self.shards = [2 * inner_ + side, n - 2 - 2 * inner_ + side]
        self.shares = []
        for index in self.owners:
            low = lax.div(index, m)
            rest = index - low * m
            x = lax.rem(rest, 2)
            self.shares.append(low * m + 2 * x + lax.div(rest, 2))
        low = lax.div(self.d, m)
        self.source = (self.shards[0] + low * (self.shards[1] - self.shards[0])) * m + self.shares[0] - low * m
        across = lax.rem(lax.div(pair + 1, 2), 2)
        self.there = low * m + self.s
        outer_ = lax.div(self.s, 2)
        there_d = low * m + 2 * (self.s - 2 * outer_) + outer_
        self.target = there_d * m + 2 * across + odd
        here = self.d * m + self.s
        self.moves = (self.target - here) * (self.target - here) > 0

        offsets = [0]
        for bit in self.bits():
            offsets += [o ^ bit for o in offsets]
        self.homes = [self.partners[o] for o in offsets]

    def owner(self, offset, shares=False):
        return (self.shares if shares else self.owners)[offset % self.n]

    def partner(self, mask):
        return self.partners[mask]

    def bits(self):
        out, bit = [], self.m // 2
        while bit:
            out.append(bit)
            bit //= 2
        return out


class Sender:
    def __init__(self, sends, recvs):
        self.sends, self.recvs = sends, recvs
        self.used = 0
        self.open = []

    def slot(self):
        self.used += 1
        return self.used - 1

    def copy(self, slot, src, dst, device):
        return pltpu.make_async_remote_copy(
            src_ref=src,
            dst_ref=dst,
            send_sem=self.sends.at[slot],
            recv_sem=self.recvs.at[slot],
            device_id=device,
            device_id_type=LOGICAL,
        )

    def start(self, slot, src, dst, device):
        copy = self.copy(slot, src, dst, device)
        copy.start()
        self.open.append(copy)
        return copy

    def finish(self):
        for copy in self.open:
            copy.wait_send()
        self.open = []


def greet(place, extra_seq=()):
    barrier = pltpu.get_barrier_semaphore()

    def hello(device):
        pl.semaphore_signal(barrier, inc=1, device_id=device, device_id_type=LOGICAL)

    near = [place.rings[1], place.rings[-1]] + [place.seqs[mask] for mask in tuple(place.bits()) + tuple(extra_seq)]
    for device in near:
        hello(device)

    @pl.when(place.moves)
    def _():
        hello(place.target)
        hello(place.source)
        pl.semaphore_wait(barrier, len(near) + 2)

    @pl.when(jnp.logical_not(place.moves))
    def _():
        pl.semaphore_wait(barrier, len(near))


class RowSlots:
    def __init__(self, rows, cols, lo=0, shares=False):
        self.rows, self.cols, self.lo, self.shares = rows, cols, lo, shares

    def where(self, index, part=None):
        rows, start = self.rows, index * self.rows
        if part is not None:
            rows = rows // 2
            start = start + part * rows
        return pl.ds(pl.multiple_of(start, rows), rows), pl.ds(self.lo, self.cols)

    def landing(self, way, j, half):
        base = way * ((half - 1) * self.rows + self.rows // 2)
        at, rows = (base + (half - 1) * self.rows, self.rows // 2) if j == 1 else (base + (j - 2) * self.rows, self.rows)
        return pl.ds(at, rows), pl.ds(0, self.cols)

    def inbox(self, half):
        return 2 * ((half - 1) * self.rows + self.rows // 2), self.cols


class TileSlots:
    shares = True

    def __init__(self, rows, cols):
        self.rows, self.cols = rows, cols

    def where(self, index, part=None):
        row = lax.div(index, 2)
        cols, start = self.cols, (index - 2 * row) * self.cols
        if part is not None:
            cols = cols // 2
            start = start + part * cols
        return pl.ds(pl.multiple_of(row * self.rows, self.rows), self.rows), pl.ds(pl.multiple_of(start, cols), cols)

    def landing(self, way, j, half):
        at, cols = ((half - 1) * self.cols, self.cols // 2) if j == 1 else ((j - 2) * self.cols, self.cols)
        return pl.ds(way * self.rows, self.rows), pl.ds(at, cols)

    def inbox(self, half):
        return 2 * self.rows, (half - 1) * self.cols + self.cols // 2


class Gather:
    def __init__(self, place, sender, buf, slots):
        self.place, self.sender, self.buf, self.slots = place, sender, buf, slots
        self.sems = [[sender.slot() for _ in range(place.half)] for _ in range(2)]
        self.devices = (place.rings[1], place.rings[-1])

    def own(self):
        return self.buf.at[self.slots.where(self.place.owner(0, self.slots.shares))]

    def send(self, k, way):
        index = self.place.owner(k if way else -k, self.slots.shares)
        ref = self.buf.at[self.slots.where(index, way if k == self.place.half - 1 else None)]
        self.sender.start(self.sems[way][k], ref, ref, self.devices[way])

    def begin(self):
        self.send(0, 0)
        self.send(0, 1)

    def pump(self, k):
        last = k == self.place.half
        for way in range(2):
            index = self.place.owner(k if way else -k, self.slots.shares)
            ref = self.buf.at[self.slots.where(index, way if last else None)]
            self.sender.copy(self.sems[way][k - 1], ref, ref, self.devices[way]).wait_recv()
            if not last:
                self.send(k, way)


class Reduce:
    def __init__(self, place, sender, buf, inbox, slots):
        self.place, self.sender, self.buf, self.inbox, self.slots = place, sender, buf, inbox, slots
        self.sems = [[sender.slot() for _ in range(place.half)] for _ in range(2)]
        self.devices = (place.rings[1], place.rings[-1])

    def target(self, way, j):
        offset = self.place.half - j
        return self.slots.where(
            self.place.owner(-offset if way else offset, self.slots.shares), way if j == 1 else None
        )

    def copy(self, way, j):
        offset = self.place.half - j + 1
        src = self.slots.where(
            self.place.owner(-offset if way else offset, self.slots.shares), way if j == 1 else None
        )
        return self.sems[way][j - 1], self.buf.at[src], self.inbox.at[self.slots.landing(way, j, self.place.half)]

    def send(self, j, way):
        self.sender.start(*self.copy(way, j), self.devices[way])

    def begin(self):
        self.send(1, 0)
        self.send(1, 1)

    def add(self, to, *froms):
        value = self.buf[to].astype(F32)
        for at in froms:
            value = value + self.inbox[at].astype(F32)
        self.buf[to] = value.astype(self.buf.dtype)

    def pump(self, j):
        half = self.place.half
        for way in range(2):
            self.sender.copy(*self.copy(way, j), self.devices[way]).wait_recv()
            if j < half:
                self.add(self.target(way, j), self.slots.landing(way, j, half))
                self.send(j + 1, way)
        if j == half:
            self.add(self.slots.where(self.place.owner(0, self.slots.shares)), *(self.slots.landing(way, j, half) for way in range(2)))

    def mine(self):
        return self.buf.at[self.slots.where(self.place.owner(0, self.slots.shares))]


def shards_of(s, n):
    inner = s // 2
    side = s % 2
    return [2 * inner + side, n - 2 - 2 * inner + side]


def blocks_of(ff):
    return [(at, min(256, ff - at), 2 * at) for at in range(0, ff, 256)]


def key_spots(place, pos_k, rows):
    lane = lax.broadcasted_iota(jnp.int32, (8, rows), 1)
    for i, home in enumerate(place.homes):
        pos_k[:, i * rows : (i + 1) * rows] = (home * rows + lane).astype(F32)


def load_rotary(place, h_rot, rot, rows, sems, first):
    copies = []
    for i, home in enumerate(place.homes):
        src = h_rot.at[pl.ds(pl.multiple_of(home * rows, rows), rows)]
        copies.append(pltpu.make_async_copy(src, rot.at[pl.ds(i * rows, rows)], sems.at[first + i]))
        copies[-1].start()
    return copies


def forward_kernel(
    dims,
    tok, cot, h_wqkv, h_wgu, h_wout, h_wdown, piece_vec, h_rot,
    o_wqkv, o_wout, o_wgu, o_wdown, o_rows, o_tok, o_cot, o_n1, o_qkv, o_stat, o_ctx, o_mid, o_n2, o_act, o_dgu,
    wqkv, wout, wgu, wdown, vec, tok_all, cot_all, n1, qkv, stat, ctx, mid, n2, act, dgu,
    rows_v, bias_v, rot, pos_k, raw, own, send1, send2, recv1, recv2,
    sends, recvs, locals_, outs,
):
    n, m, rows, width, slab, part, ff, b_units = dims
    count = rows * m
    half = count // 2
    inner = part * m
    place = Place(n, m)
    sender = Sender(sends, recvs)
    d, s = place.d, place.s
    bits = place.bits()
    out_rows, vec_rows = part // n, piece_vec.shape[0]
    down_rows, down_cols = 2 * ff // n, width // 2
    blocks = blocks_of(ff)

    ring_a = Gather(place, sender, wqkv, RowSlots(slab, 3 * part))
    ring_v = Gather(place, sender, vec, RowSlots(vec_rows, LANES))
    ring_b = Gather(place, sender, wout, RowSlots(out_rows, width, shares=True))
    ring_c = [Gather(place, sender, wgu, RowSlots(slab, 2 * units, lane)) for _, units, lane in blocks]
    ring_d = Gather(place, sender, wdown, TileSlots(down_rows, down_cols))

    def local(i, src, dst):
        copy = pltpu.make_async_copy(src, dst, locals_.at[i])
        copy.start()
        return copy

    own_rows = pl.ds(pl.multiple_of(d * slab, slab), slab)
    placed_qkv = [
        local(
            2 * i + u,
            h_wqkv.at[:, pl.ds(pl.multiple_of(i * inner + place.shards[u] * LANES, LANES), LANES)],
            wqkv.at[own_rows, pl.ds(i * part + u * LANES, LANES)],
        )
        for i in range(3)
        for u in range(2)
    ]
    placed_vec = local(6, piece_vec, ring_v.own())
    placed_tok = local(7, tok, tok_all.at[pl.ds(0, rows)])
    shard, hidden = ff // 2, h_wgu.shape[1] // 2
    window = raw.shape[2]
    shifts, placed_gu = [], []
    for i in range(2):
        for u in range(2):
            col = place.shards[u] * shard
            first_tile = lax.div(col + (0 if i == 0 else shard + LANES - 1 + hidden - window), LANES)
            base = first_tile * LANES
            shifts.append(col - base + i * hidden)
            src = h_wgu.at[:, pl.ds(pl.multiple_of(base, LANES), window)]
            placed_gu.append(local((8, 12 + m, 13 + m, 14 + m)[2 * i + u], src, raw.at[2 * i + u]))
    placed_cot = local(9, cot, cot_all.at[pl.ds(0, rows)])
    placed_rot = load_rotary(place, h_rot, rot, rows, locals_, 12)
    greet(place)
    moves = place.moves

    class Spread:
        def __init__(self, buf):
            self.buf = buf
            self.sems = [sender.slot() for _ in bits]

        def copy(self, i):
            size = rows << i
            return self.sems[i], self.buf.at[pl.ds(0, size)], self.buf.at[pl.ds(size, size)], place.seqs[bits[i]]

        def send(self, i):
            sender.start(*self.copy(i))

        def wait(self, i):
            sender.copy(*self.copy(i)).wait_recv()

    toks, cots, n2s = Spread(tok_all), Spread(cot_all), Spread(n2)
    written = []

    def write(src, dst):
        copy = pltpu.make_async_copy(src, dst, outs.at[len(written)])
        copy.start()
        written.append(copy)

    for copy in placed_qkv:
        copy.wait()
    ring_a.begin()
    placed_vec.wait()
    ring_v.begin()
    placed_tok.wait()
    toks.send(0)

    for copy in placed_gu:
        copy.wait()
    lane = lax.broadcasted_iota(jnp.int32, (1, LANES), 1)
    whole, rest = shard // LANES, shard % LANES

    def cut(j, carry):
        size = 64
        span = pl.ds(pl.multiple_of(j * size, size), size)
        tiles = []
        for i in range(2):
            low = pltpu.roll(raw[2 * i, span, :].astype(F32), window - shifts[2 * i], 1)
            high = pltpu.roll(
                raw[2 * i + 1, span, :].astype(F32), lax.rem(window + rest - shifts[2 * i + 1] + window, window), 1
            )
            lows = [low[:, t * LANES : (t + 1) * LANES] for t in range(whole + 1)]
            highs = [high[:, t * LANES : (t + 1) * LANES] for t in range(window // LANES)]
            tiles.append(lows[:whole] + [jnp.where(lane < rest, lows[whole], highs[0])] + highs[1:])
        to = pl.ds(pl.multiple_of(d * slab + j * size, size), size)
        at = 0
        for first_unit, count_, _ in blocks:
            even = count_ // LANES
            t = first_unit // LANES
            line_ = tiles[0][t : t + even]
            if even * LANES < count_:
                line_.append(jnp.where(lane < LANES // 2, tiles[0][t + even], pltpu.roll(tiles[1][t + even], LANES // 2, 1)))
            for tile in line_ + tiles[1][t : t + even]:
                wgu[to, at : at + LANES] = tile.astype(BF16)
                at += LANES
        return carry

    lax.fori_loop(0, slab // 64, cut, 0)
    ring_c[0].begin()
    placed_cot.wait()
    cots.send(0)
    wdown[ff:, :] = jnp.zeros((wdown.shape[0] - ff, width), BF16)
    key_spots(place, pos_k, rows)
    line = lax.broadcasted_iota(jnp.int32, (rows, 1), 0)

    def stats(i):
        span = slice(i * rows, (i + 1) * rows)
        x = tok_all[span, :].astype(F32)
        mu = jnp.mean(x, axis=-1, keepdims=True)
        c = x - mu
        r = lax.rsqrt(jnp.mean(c * c, axis=-1, keepdims=True) + EPS)
        spot = (place.homes[i] * rows + line).astype(F32)
        stat[span, :] = jnp.where(lane == MEAN, mu, jnp.where(lane == RSTD, r, spot))

    stats(0)
    ring_v.pump(1)
    ring_a.pump(1)
    src_out = h_wout.at[pl.ds(pl.multiple_of(s * out_rows, out_rows), out_rows)]
    up = lax.div(s, 2)
    src_down = h_wdown.at[
        pl.ds(pl.multiple_of(up * down_rows, down_rows), down_rows),
        pl.ds(pl.multiple_of((s - 2 * up) * down_cols, down_cols), down_cols),
    ]
    turns = [(src_out, ring_b, sender.slot(), 10), (src_down, ring_d, sender.slot(), 11)]

    def turn(ring, index):
        return ring.buf.at[ring.slots.where(index)]

    @pl.when(moves)
    def _():
        for src, ring, slot, _ in turns:
            sender.copy(slot, src, turn(ring, place.there), place.target).start()

    @pl.when(jnp.logical_not(moves))
    def _():
        for src, ring, _, i in turns:
            local(i, src, ring.own()).wait()


    toks.wait(0)
    toks.send(1)
    stats(1)
    ring_v.pump(2)
    ring_a.pump(2)
    @pl.when(moves)
    def _():
        for src, ring, slot, _ in turns:
            sender.copy(slot, src, ring.own(), place.source).wait_recv()

    ring_b.begin()
    ring_d.begin()
    toks.wait(1)
    write(tok_all, o_tok)
    stats(2)
    stats(3)
    cots.wait(0)
    cots.send(1)
    ring_v.pump(3)
    ring_a.pump(3)
    ring_b.pump(1)
    ring_c[1].begin()
    ring_b.pump(2)
    ring_c[0].pump(1)
    ring_v.pump(4)
    units = slab // LANES
    for c in range(n):
        for r in range(4):
            for u in range(units):
                at = c * slab + u * LANES
                row = c * vec_rows + r * units + u
                rows_v[r : r + 1, at : at + LANES] = vec[row : row + 1, :]
    for i in range(3):
        for u in range(part // LANES):
            unit = i * (inner // LANES) + place.shards[u]
            row = lax.div(unit, b_units) * vec_rows + 4 * units + lax.rem(unit, b_units)
            at = i * part + u * LANES
            bias_v[0:1, at : at + LANES] = vec[pl.ds(row, 1), :]
    write(rows_v, o_rows)

    def normalize(j, carry):
        size = 64
        span = pl.ds(pl.multiple_of(j * size, size), size)
        x = tok_all[span, :].astype(F32)
        xhat = (x - stat[span, MEAN : MEAN + 1]) * stat[span, RSTD : RSTD + 1]
        n1[span, :] = (xhat * rows_v[0:1, :] + rows_v[1:2, :]).astype(BF16)
        return carry

    lax.fori_loop(0, count // 64, normalize, 0)
    write(n1, o_n1)
    ring_d.pump(1)
    ring_c[2].begin()
    cots.wait(1)
    write(cot_all, o_cot)
    ring_a.pump(4)
    write(wqkv, o_wqkv)
    for copy in placed_rot:
        copy.wait()

    def project(j, carry):
        size = 256
        span = pl.ds(pl.multiple_of(j * size, size), size)
        for i in range(3):
            cols = slice(i * part, (i + 1) * part)
            y = dot(n1[span, :], wqkv[:, cols]) + bias_v[0:1, cols]
            if i < 2:
                pieces = []
                for u in range(part // LANES):
                    z = y[:, u * LANES : (u + 1) * LANES]
                    pieces.append(
                        z * rot[span, :LANES]
                        + pltpu.roll(z, LANES - ROT // 2, 1) * rot[span, LANES : 2 * LANES]
                        + pltpu.roll(z, ROT // 2, 1) * rot[span, 2 * LANES :]
                    )
                y = jnp.concatenate(pieces, axis=1)
            qkv[span, cols] = y.astype(BF16)
        return carry

    lax.fori_loop(0, count // 256, project, 0)
    write(qkv, o_qkv)
    ring_b.pump(3)
    ring_c[1].pump(1)
    ring_c[0].pump(2)
    scale = HEAD_DIM ** (-0.5)
    per = LANES // HEAD_DIM

    def attend(i, carry):
        pair, block = lax.div(i, m), lax.rem(i, m)
        span = pl.ds(pl.multiple_of(block * rows, rows), rows)
        at = pl.multiple_of(pair * LANES, LANES)
        q = qkv[span, pl.ds(at, LANES)]
        k = qkv[:, pl.ds(pl.multiple_of(part + at, LANES), LANES)]
        v = qkv[:, pl.ds(pl.multiple_of(2 * part + at, LANES), LANES)]
        allowed = pos_k[0:1, :] <= stat[span, SPOT : SPOT + 1]
        total = jnp.zeros((rows, LANES), F32)
        for h in range(per):
            mine = (lane // HEAD_DIM == h).astype(BF16)
            scores = dot_cols(q * mine, k) * scale
            scores = jnp.where(allowed, scores, -jnp.inf)
            top = jnp.max(scores, axis=-1, keepdims=True)
            found = top + jnp.log(jnp.sum(jnp.exp(scores - top), axis=-1, keepdims=True))
            probs = jnp.exp(scores - found).astype(BF16)
            total = total + dot(probs, v * mine)
            stat[span, :] = jnp.where(lane == LSE + pair * per + h, found, stat[span, :])
        ctx[span, pl.ds(at, LANES)] = total.astype(BF16)
        return carry

    lax.fori_loop(0, (part // LANES) * m, attend, 0)
    write(stat, o_stat)
    write(ctx, o_ctx)
    ring_d.pump(2)
    ring_c[2].pump(1)
    ring_b.pump(4)
    write(wout, o_wout)

    step = 512
    scatter = [sender.slot(), sender.slot()]

    def far_part(j, carry):
        cols = pl.ds(pl.multiple_of(j * step, step), step)
        send1[:, cols] = dot(ctx[half:, :], wout[:, cols]).astype(BF16)
        return carry

    lax.fori_loop(0, width // step, far_part, 0)
    first = sender.start(scatter[0], send1, recv1, place.seqs[bits[1]])

    def near_part(j, carry):
        cols = pl.ds(pl.multiple_of(j * step, step), step)
        own[:, cols] = dot(ctx[:half, :], wout[:, cols])
        return carry

    lax.fori_loop(0, width // step, near_part, 0)
    ring_c[1].pump(2)
    first.wait_recv()
    send2[...] = (own[rows:, :] + recv1[rows:, :].astype(F32)).astype(BF16)
    second = sender.start(scatter[1], send2, recv2, place.seqs[bits[0]])
    ring_c[0].pump(3)
    second.wait_recv()
    value = tok_all[:rows, :].astype(F32) + own[:rows, :] + recv1[:rows, :].astype(F32) + recv2[...].astype(F32)
    mid[...] = value
    c = value - jnp.mean(value, axis=-1, keepdims=True)
    r = lax.rsqrt(jnp.mean(c * c, axis=-1, keepdims=True) + EPS)
    n2[:rows, :] = (c * r * rows_v[2:3, :] + rows_v[3:4, :]).astype(BF16)
    n2s.send(0)
    write(mid, o_mid)
    ring_d.pump(3)
    ring_c[2].pump(2)
    ring_c[1].pump(3)
    n2s.wait(0)
    n2s.send(1)
    ring_c[0].pump(4)
    ring_d.pump(4)
    write(wdown, o_wdown)
    n2s.wait(1)
    write(n2, o_n2)
    ring_c[2].pump(3)

    def expand(first_unit, units, base):
        even = units // LANES * LANES
        y = dot(n2[...], wgu[:, base : base + 2 * units])
        d_act = dot_cols(cot_all[...], wdown[first_unit : first_unit + 256, :])
        if even == units:
            gate, up = y[:, :units], y[:, units:]
        else:
            gate = y[:, : even + LANES]
            up = jnp.concatenate([y[:, even + LANES :], pltpu.roll(gate[:, even:], LANES // 2, 1)], axis=1)
        sigma = jax.nn.sigmoid(gate)
        silu = gate * sigma
        value = silu * up
        d_gate = d_act * up * (sigma * (1.0 + gate * (1.0 - sigma)))
        d_up = d_act * silu
        if even == units:
            dgu[:, base : base + units] = d_gate.astype(BF16)
            dgu[:, base + units : base + 2 * units] = d_up.astype(BF16)
        else:
            value = jnp.where(lax.broadcasted_iota(jnp.int32, (1, 256), 1) < units, value, 0.0)
            mixed = jnp.where(lane < LANES // 2, d_gate[:, even:], pltpu.roll(d_up[:, even:], LANES // 2, 1))
            dgu[:, base : base + even] = d_gate[:, :even].astype(BF16)
            dgu[:, base + even : base + even + LANES] = mixed.astype(BF16)
            dgu[:, base + even + LANES : base + 2 * units] = d_up[:, :even].astype(BF16)
        act[:, first_unit : first_unit + 256] = value.astype(BF16)

    expand(*blocks[0])
    ring_c[1].pump(4)
    expand(*blocks[1])
    ring_c[2].pump(4)
    write(wgu, o_wgu)
    expand(*blocks[2])
    write(act, o_act)
    write(dgu, o_dgu)
    for copy in written:
        copy.wait()
    sender.finish()

    @pl.when(moves)
    def _():
        for src, ring, slot, _ in turns:
            sender.copy(slot, src, turn(ring, place.there), place.target).wait_send()


def run_forward(dims, args):
    n, m, rows, width, slab, part, ff, b_units = dims
    count = rows * m
    ffp = -(-ff // 256) * 256
    vec_rows = args[6].shape[0]
    arrays = [
        ((width, 3 * part), BF16), ((part, width), BF16), ((width, 2 * ff), BF16), ((ffp, width), BF16),
        ((8, width), F32), ((count, width), BF16), ((count, width), BF16), ((count, width), BF16),
        ((count, 3 * part), BF16), ((count, LANES), F32), ((count, part), BF16), ((rows, width), F32),
        ((count, width), BF16), ((count, ffp), BF16), ((count, 2 * ff), BF16),
    ]
    scratch = [vmem(*a) for a in arrays]
    rows_v, scratch[4] = scratch[4], vmem((n * vec_rows, LANES), F32)
    slots = (4 + len(blocks_of(ff))) * 2 * (n // 2) + 3 * 2 + 2 + 2
    return pl.pallas_call(
        functools.partial(forward_kernel, dims),
        out_shape=[jax.ShapeDtypeStruct(*a) for a in arrays],
        in_specs=[pl.BlockSpec(memory_space=pl.ANY)] * len(args),
        out_specs=[pl.BlockSpec(memory_space=pl.ANY)] * len(arrays),
        scratch_shapes=scratch
        + [
            rows_v,
            vmem((8, 3 * part), F32),
            vmem((count, 3 * LANES), F32),
            vmem((8, count), F32),
            vmem((4, slab, WINDOW)),
            vmem((count // 2, width), F32),
            vmem((count // 2, width)),
            vmem((rows, width)),
            vmem((count // 2, width)),
            vmem((rows, width)),
            pltpu.SemaphoreType.DMA((slots,)),
            pltpu.SemaphoreType.DMA((slots,)),
            pltpu.SemaphoreType.DMA((15 + m,)),
            pltpu.SemaphoreType.DMA((len(arrays),)),
        ],
        compiler_params=pltpu.CompilerParams(
            collective_id=0, has_side_effects=True, vmem_limit_bytes=VMEM_BYTES
        ),
        name="forward",
    )(*args)


def flip(value):
    size = value.shape[1]
    here = lax.broadcasted_iota(jnp.int32, (size, size), 0) == lax.broadcasted_iota(jnp.int32, (size, size), 1)
    return dot_cols(here.astype(F32).astype(BF16), value).astype(BF16)


def backward_kernel(
    dims,
    h_wqkv, h_wout, h_wgu, h_wdown, h_rows, h_tok, h_cot, h_n1, h_qkv, h_stat, h_ctx, h_mid, h_n2, h_act, h_dgu,
    h_rot,
    o_block, o_input, o_gu, o_qkv, o_down, o_out, o_vec,
    wout, wgu, wqkv, rows_v, wide_a, wide_b, qkv, stat, ctx, mid, act, dgu, rot, pos_k,
    sum_a, sum_b, sum_c, sum_d, sum_v, in_a, in_b, in_c0, in_c1, in_c2, in_d, in_v,
    own, send1, send2, recv1, recv2, dm_all, d_mid, cot, dctx, dqkv, dk, dv, sums_v, bias_v,
    x_gu, x_qkv, x_down, x_out, x_vec, y_qkv, y_down, y_gu,
    sends, recvs, loads, outs,
):
    n, m, rows, width, slab, part, ff, b_units = dims
    ffp = act.shape[1]
    inner = part * m
    count = rows * m
    half = count // 2
    place = Place(n, m)
    sender = Sender(sends, recvs)
    waiting = {}

    def load(name, src, dst):
        copy = pltpu.make_async_copy(src, dst, loads.at[len(waiting)])
        copy.start()
        waiting[name] = copy

    load("n2", h_n2, wide_b)
    load("dgu", h_dgu, dgu)
    load("act", h_act, act)
    load("cot", h_cot, wide_a)
    load("wgu", h_wgu, wgu)
    load("own", h_cot.at[pl.ds(0, dims[2])], cot)
    load("mid", h_mid, mid)
    load("rows", h_rows, rows_v)
    load("wqkv", h_wqkv, wqkv)
    load("wout", h_wout, wout)
    load("ctx", h_ctx, ctx)
    load("qkv", h_qkv, qkv)
    load("stat", h_stat, stat)
    spare = loads.shape[0] - 2
    rotary = load_rotary(place, h_rot, rot, rows, loads, spare - m)
    bits = place.bits()
    others = [mask for mask in range(1, m) if mask not in bits]
    moves = place.moves
    greet(place, others)
    d, s = place.d, place.s
    out_rows, vec_rows = part // n, sum_v.shape[0] // n
    down_rows, down_cols = 2 * ff // n, width // 2
    ring_a = Reduce(place, sender, sum_a, in_a, RowSlots(slab, 3 * part))
    ring_b = Reduce(place, sender, sum_b, in_b, RowSlots(out_rows, width, shares=True))
    ring_c = [
        Reduce(place, sender, sum_c, inbox, RowSlots(slab, 2 * units_, lane_))
        for inbox, (_, units_, lane_) in zip((in_c0, in_c1, in_c2), blocks_of(ff))
    ]
    ring_d = Reduce(place, sender, sum_d, in_d, TileSlots(down_rows, down_cols))
    ring_v = Reduce(place, sender, sum_v, in_v, RowSlots(vec_rows, LANES))
    key_spots(place, pos_k, rows)
    block = 256

    def outer(dst, left, right, size):
        def step(j, carry):
            cols = pl.ds(pl.multiple_of(j * block, block), block)
            dst[cols, :] = dot(flip(left[:, cols]), right[...]).astype(BF16)
            return carry

        lax.fori_loop(0, size // block, step, 0)

    class Halving:
        def __init__(self, at):
            self.slots = [sender.slot(), sender.slot()]
            self.at = at
            self.open = []

        def first(self, far):
            far()
            self.open.append(sender.start(self.slots[0], send1, recv1.at[pl.ds(self.at * half, half)], place.seqs[bits[1]]))

        def second(self):
            self.open[0].wait_recv()
            send2[...] = (own[rows:, :] + recv1[self.at * half + rows : (self.at + 1) * half, :].astype(F32)).astype(BF16)
            self.open.append(sender.start(self.slots[1], send2, recv2.at[pl.ds(self.at * rows, rows)], place.seqs[bits[0]]))

        def total(self):
            self.open[1].wait_recv()
            return own[:rows, :] + recv1[self.at * half : self.at * half + rows, :].astype(F32) + recv2[
                self.at * rows : (self.at + 1) * rows, :
            ].astype(F32)

        def sent(self):
            for copy in self.open:
                copy.wait_send()
            sender.open = [c for c in sender.open if all(c is not o for o in self.open)]

    turns = [(ring_d, x_down, sender.slot()), (ring_b, x_out, sender.slot())]

    def turn_back(i):
        ring, landing, slot = turns[i]

        @pl.when(moves)
        def _():
            sender.copy(slot, ring.mine(), landing, place.source).start()

        @pl.when(jnp.logical_not(moves))
        def _():
            copy = pltpu.make_async_copy(ring.mine(), landing, loads.at[spare + i])
            copy.start()
            copy.wait()

    def turned_back(i):
        ring, landing, slot = turns[i]

        @pl.when(moves)
        def _():
            sender.copy(slot, ring.mine(), landing, place.target).wait_recv()

    def deal(buf, size, landing, whole=False):
        share = size if whole else size // m
        got = []
        to = pl.ds(pl.multiple_of(s * share, share), share)
        for mask in range(1, m):
            start = d * size + (0 if whole else place.partner(mask) * share)
            src = buf.at[pl.ds(pl.multiple_of(start, share), share)]
            got.append(sender.start(sender.slot(), src, landing.at[to], place.seqs[mask]))
        start = d * size + (0 if whole else s * share)
        landing[to, :] = buf[pl.ds(pl.multiple_of(start, share), share), :]
        return got

    waiting["n2"].wait()
    waiting["dgu"].wait()

    def slab_of(index):
        cols = pl.ds(pl.multiple_of(index * slab, slab), slab)
        sum_c[cols, :] = dot(flip(wide_b[:, cols]), dgu[...]).astype(BF16)

    slab_of(place.owner(place.half))
    for ring in ring_c:
        ring.begin()
    waiting["act"].wait()
    waiting["cot"].wait()
    outer(sum_d, act, wide_a, ffp)
    ring_d.begin()
    waiting["wgu"].wait()
    normed2 = Halving(0)

    def back_step(left, lo, hi, weight, to):
        def step(j, carry):
            cols = pl.ds(pl.multiple_of(j * block, block), block)
            to(cols, dot_cols(left[lo:hi, :], weight[cols, :]))
            return carry

        lax.fori_loop(0, width // block, step, 0)

    def to_send(cols, value):
        send1[:, cols] = value.astype(BF16)

    def to_own(cols, value):
        own[:, cols] = value

    normed2.first(lambda: back_step(dgu, half, count, wgu, to_send))
    back_step(dgu, 0, half, wgu, to_own)
    lanes = 2 * ff
    load("down_lo", h_wdown.at[:, pl.ds(0, lanes)], wgu.at[pl.ds(0, ffp)])
    load("down_hi", h_wdown.at[:, pl.ds(lanes, width - lanes)], wgu.at[pl.ds(ffp, ffp), pl.ds(0, width - lanes)])
    normed2.second()

    def other_slabs(i, carry):
        slab_of(lax.rem(place.owner(place.half) + i, n))
        return carry

    lax.fori_loop(1, n, other_slabs, 0)
    load("n1", h_n1, wide_b)
    load("tok", h_tok, wide_a)
    for ring in ring_c:
        ring.pump(1)
    ring_d.pump(1)

    waiting["mid"].wait()
    waiting["rows"].wait()
    waiting["own"].wait()

    def deviation(value):
        c = value - jnp.mean(value, axis=-1, keepdims=True)
        r = lax.rsqrt(jnp.mean(c * c, axis=-1, keepdims=True) + EPS)
        return c * r, r

    xhat, r = deviation(mid[...])
    up = normed2.total()
    sums_v[2:3, :] = jnp.sum(up * xhat, axis=0, keepdims=True)
    sums_v[3:4, :] = jnp.sum(up, axis=0, keepdims=True)
    d_mid[...] = cot[...].astype(F32) + norm_back(up, xhat, r, rows_v[2:3, :])
    dm_all[:rows, :] = d_mid[...].astype(BF16)
    spread = [sender.slot() for _ in bits]

    def spread_copy(i):
        size = rows << i
        return (spread[i], dm_all.at[pl.ds(0, size)], dm_all.at[pl.ds(size, size)])

    def spread_send(i):
        sender.start(*spread_copy(i), place.seqs[bits[i]])

    def spread_wait(i):
        sender.copy(*spread_copy(i), place.seqs[bits[i]]).wait_recv()

    spread_send(0)
    normed2.sent()
    ring_c[0].pump(2)
    ring_c[1].pump(2)

    waiting["down_lo"].wait()
    waiting["down_hi"].wait()

    def down_step(lo, hi, to):
        def low(j, carry):
            cols = pl.ds(pl.multiple_of(j * LANES, LANES), LANES)
            to(cols, dot(act[lo:hi, :], wgu[:ffp, cols]))
            return carry

        def high(j, carry):
            cols = pl.ds(pl.multiple_of(j * LANES, LANES), LANES)
            to(pl.ds(pl.multiple_of(lanes + j * LANES, LANES), LANES), dot(act[lo:hi, :], wgu[ffp : 2 * ffp, cols]))
            return carry

        lax.fori_loop(0, lanes // LANES, low, 0)
        lax.fori_loop(0, (width - lanes) // LANES, high, 0)

    output = Halving(1)

    output.first(lambda: down_step(half, count, to_send))
    down_step(0, half, to_own)
    spread_wait(0)
    spread_send(1)
    output.second()
    ring_c[2].pump(2)
    ring_d.pump(2)
    spread_wait(1)

    waiting["wout"].wait()
    waiting["ctx"].wait()
    dctx[...] = dot_cols(dm_all[...], wout[...]).astype(BF16)
    outer(sum_b, ctx, dm_all, part)
    ring_b.begin()
    cot[...] = (mid[...] + output.total()).astype(BF16)
    output.sent()

    for name in ("qkv", "stat"):
        waiting[name].wait()
    for copy in rotary:
        copy.wait()
    scale = HEAD_DIM ** (-0.5)
    per = LANES // HEAD_DIM
    lane = lax.broadcasted_iota(jnp.int32, (1, LANES), 1) // HEAD_DIM

    def turned(z, span):
        return (
            z * rot[span, :LANES]
            - pltpu.roll(z, LANES - ROT // 2, 1) * rot[span, LANES : 2 * LANES]
            - pltpu.roll(z, ROT // 2, 1) * rot[span, 2 * LANES :]
        )

    bias_v[...] = jnp.zeros_like(bias_v)
    for pair in range(part // LANES):
        at = pair * LANES
        dk[...] = jnp.zeros_like(dk)
        dv[...] = jnp.zeros_like(dv)

        def attend(i, carry, pair=pair, at=at):
            span = pl.ds(pl.multiple_of(i * rows, rows), rows)
            q = qkv[span, at : at + LANES]
            k = qkv[:, part + at : part + at + LANES]
            v = qkv[:, 2 * part + at : 2 * part + at + LANES]
            dc = dctx[span, at : at + LANES]
            both = dc.astype(F32) * ctx[span, at : at + LANES].astype(F32)
            allowed = pos_k[0:1, :] <= stat[span, SPOT : SPOT + 1]
            dq = jnp.zeros((rows, LANES), F32)
            for h in range(per):
                pick = lane == h
                mine = pick.astype(BF16)
                qm, dcm = q * mine, dc * mine
                scores = dot_cols(qm, k) * scale
                at_lse = LSE + pair * per + h
                probs = jnp.exp(jnp.where(allowed, scores, -jnp.inf) - stat[span, at_lse : at_lse + 1])
                delta = jnp.sum(jnp.where(pick, both, 0.0), axis=-1, keepdims=True)
                ds = (probs * (dot_cols(dcm, v) - delta) * scale).astype(BF16)
                dq = dq + jnp.dot(ds, k * mine, preferred_element_type=F32)
                dk[...] += dot(flip(ds), qm)
                dv[...] += dot(flip(probs.astype(BF16)), dcm)
            dq = turned(dq, span)
            bias_v[0:1, at : at + LANES] += jnp.sum(dq, axis=0, keepdims=True)
            dqkv[span, at : at + LANES] = dq.astype(BF16)
            return carry

        lax.fori_loop(0, m, attend, 0)

        def settle(i, carry, at=at):
            span = pl.ds(pl.multiple_of(i * rows, rows), rows)
            key, value = turned(dk[span, :], span), dv[span, :]
            bias_v[0:1, part + at : part + at + LANES] += jnp.sum(key, axis=0, keepdims=True)
            bias_v[0:1, 2 * part + at : 2 * part + at + LANES] += jnp.sum(value, axis=0, keepdims=True)
            dqkv[span, part + at : part + at + LANES] = key.astype(BF16)
            dqkv[span, 2 * part + at : 2 * part + at + LANES] = value.astype(BF16)
            return carry

        lax.fori_loop(0, m, settle, 0)
        if pair == 0:
            for ring in ring_c:
                ring.pump(3)

    waiting["n1"].wait()
    outer(sum_a, wide_b, dqkv, width)
    ring_a.begin()
    ring_d.pump(3)
    ring_b.pump(1)
    waiting["wqkv"].wait()
    waiting["tok"].wait()
    normed1 = Halving(2)

    def gains(cols, value, lo, hi):
        xh = (wide_a[lo:hi, cols].astype(F32) - stat[lo:hi, MEAN : MEAN + 1]) * stat[lo:hi, RSTD : RSTD + 1]
        return jnp.sum(value * xh, axis=0, keepdims=True), jnp.sum(value, axis=0, keepdims=True)

    def far_last(cols, value):
        send1[:, cols] = value.astype(BF16)
        sums_v[0:1, cols], sums_v[1:2, cols] = gains(cols, value, half, count)

    def near_last(cols, value):
        own[:, cols] = value
        gain, total = gains(cols, value, 0, half)
        sums_v[0:1, cols] += gain
        sums_v[1:2, cols] += total

    normed1.first(lambda: back_step(dqkv, half, count, wqkv, far_last))
    back_step(dqkv, 0, half, wqkv, near_last)

    sum_v[...] = jnp.zeros_like(sum_v)
    units = slab // LANES

    def lay(c, carry):
        for i in range(4):
            for u in range(units):
                at = pl.multiple_of(c * slab + u * LANES, LANES)
                sum_v[pl.ds(c * vec_rows + i * units + u, 1), :] = sums_v[i : i + 1, pl.ds(at, LANES)]
        return carry

    lax.fori_loop(0, n, lay, 0)
    for i in range(3):
        for u in range(part // LANES):
            unit = i * (inner // LANES) + place.shards[u]
            row = lax.div(unit, b_units) * vec_rows + 4 * units + lax.rem(unit, b_units)
            at = i * part + u * LANES
            sum_v[pl.ds(row, 1), :] = bias_v[0:1, at : at + LANES]
    ring_v.begin()
    normed1.second()
    ring_b.pump(2)
    ring_a.pump(1)
    ring_v.pump(1)
    for ring in ring_c:
        ring.pump(4)
    got_gu = deal(sum_c, slab, x_gu)
    ring_d.pump(4)
    ring_b.pump(3)
    ring_a.pump(2)
    ring_v.pump(2)
    ring_b.pump(4)
    up = normed1.total()
    rstd = stat[:rows, RSTD : RSTD + 1]
    xhat = (wide_a[:rows, :].astype(F32) - stat[:rows, MEAN : MEAN + 1]) * rstd
    own[:rows, :] = d_mid[...] + norm_back(up, xhat, rstd, rows_v[0:1, :])
    ring_v.pump(3)

    written = []

    def store(src, dst):
        copy = pltpu.make_async_copy(src, dst, outs.at[len(written)])
        copy.start()
        written.append(copy)

    store(cot, o_block)
    store(own.at[pl.ds(0, rows)], o_input)
    ring_a.pump(3)
    turn_back(0)
    turn_back(1)
    lane128 = lax.broadcasted_iota(jnp.int32, (1, LANES), 1)

    def lay_out(got, to):
        share, shard, hidden = slab // m, ff // 2, ff * m
        found = {}
        for t in range(m):
            span = slice(t * share, (t + 1) * share)
            tiles = [[], []]
            at = 0
            for _, units_, _ in blocks_of(ff):
                even = units_ // LANES
                tiles[0] += [got[span, at + k * LANES : at + (k + 1) * LANES].astype(F32) for k in range(even)]
                at += even * LANES
                odd = []
                if even * LANES < units_:
                    mixed = got[span, at : at + LANES].astype(F32)
                    odd = [mixed, pltpu.roll(mixed, LANES // 2, 1)]
                    at += LANES
                tiles[1] += [got[span, at + k * LANES : at + (k + 1) * LANES].astype(F32) for k in range(even)]
                at += even * LANES
                if odd:
                    tiles[0].append(odd[0])
                    tiles[1].append(odd[1])
            for i in range(2):
                for u, held in enumerate(shards_of(t, n)):
                    start, first, end = u * shard, i * hidden + held * shard, i * hidden + (held + 1) * shard
                    shift = (first - start) % LANES
                    back = (first - start - shift) // LANES
                    for tile in range(first // LANES, (end - 1) // LANES + 1):
                        k = tile - back
                        parts_ = [tiles[i][q] if 0 <= q < len(tiles[i]) else None for q in (k, k - 1)]
                        if shift:
                            here, before = [None if p is None else pltpu.roll(p, shift, 1) for p in parts_]
                            if here is None or before is None:
                                value = before if here is None else here
                            else:
                                value = jnp.where(lane128 < shift, before, here)
                        else:
                            value = parts_[0]
                        lo, hi = max(first, tile * LANES), min(end, (tile + 1) * LANES)
                        found.setdefault(tile, []).append((lo - tile * LANES, hi - tile * LANES, value))
        for tile, parts_ in found.items():
            parts_.sort(key=lambda p: p[0])
            value = parts_[-1][2]
            for _, hi, other in reversed(parts_[:-1]):
                value = jnp.where(lane128 < hi, other, value)
            to[:, tile * LANES : (tile + 1) * LANES] = value.astype(BF16)

    ring_v.pump(4)
    got_vec = deal(sum_v, vec_rows, x_vec, whole=True)
    for copy in got_gu:
        copy.wait_recv()
    lay_out(x_gu, y_gu)
    store(y_gu, o_gu)
    for copy in got_vec:
        copy.wait_recv()
    total = x_vec[:vec_rows, :]
    for t in range(1, m):
        total = total + x_vec[t * vec_rows : (t + 1) * vec_rows, :]
    x_vec[:vec_rows, :] = total
    some = slab // m
    sizes = [(i * units, some) for i in range(4)] + [(4 * units, b_units * LANES // m)]
    for i, (first_row, size) in enumerate(sizes):
        tile = lax.div(s * size, LANES)
        shift = s * size - tile * LANES
        low = x_vec[pl.ds(first_row + tile, 1), :]
        high = x_vec[pl.ds(first_row + tile + 1, 1), :]
        both = jnp.where(lane128 < shift, high, low)
        sums_v[i : i + 1, :LANES] = pltpu.roll(both, lax.rem(LANES - shift, LANES), 1)
    store(sums_v.at[:, pl.ds(0, LANES)], o_vec)
    ring_a.pump(4)
    got_qkv = deal(sum_a, slab, x_qkv)
    turned_back(0)
    some = down_rows // 2
    value = x_down[...].astype(F32)
    d_mid[:some, :down_cols] = value[:some, :]
    d_mid[:some, down_cols:] = value[some:, :]
    column = lax.rem(s, 2)
    across = pl.ds(pl.multiple_of(column * down_cols, down_cols), down_cols)
    swap = sender.start(
        sender.slot(),
        d_mid.at[pl.ds(0, some), pl.ds(pl.multiple_of((1 - column) * down_cols, down_cols), down_cols)],
        y_down.at[:, across],
        place.seqs[1],
    )
    y_down[:, across] = d_mid[:some, across]
    turned_back(1)
    store(x_out, o_out)
    swap.wait_recv()
    store(y_down, o_down)
    for copy in got_qkv:
        copy.wait_recv()
    share = slab // m
    for t in range(m):
        for i in range(3):
            for u, held in enumerate(shards_of(t, n)):
                at, come = i * inner + held * LANES, i * part + u * LANES
                y_qkv[:, at : at + LANES] = x_qkv[t * share : (t + 1) * share, come : come + LANES]
    store(y_qkv, o_qkv)
    for copy in written:
        copy.wait()
    sender.finish()

    @pl.when(moves)
    def _():
        for ring, landing, slot in turns:
            sender.copy(slot, ring.mine(), landing, place.source).wait_send()


def run_backward(dims, args):
    n, m, rows, width, slab, part, ff, b_units = dims
    count = rows * m
    ffp = -(-ff // 256) * 256
    vec_rows = -(-(4 * (slab // LANES) + b_units) // TILE) * TILE
    half = n // 2
    out_rows = part // n
    down_rows, down_cols = 2 * ff // n, width // 2
    share = slab // m

    def inbox(slots, dtype=BF16):
        return vmem(slots.inbox(half), dtype)

    outputs = [
        ((rows, width), BF16), ((rows, width), F32), ((share, 2 * ff * m), BF16), ((share, 3 * part * m), BF16),
        ((down_rows // 2, width), F32), ((out_rows, width), BF16), ((8, LANES), F32),
    ]
    scratch = [
        vmem((part, width)), vmem((width, 2 * ff)), vmem((width, 3 * part)), vmem((8, width), F32),
        vmem((count, width)), vmem((count, width)), vmem((count, 3 * part)), vmem((count, LANES), F32),
        vmem((count, part)), vmem((rows, width), F32), vmem((count, ffp)), vmem((count, 2 * ff)),
        vmem((count, 3 * LANES), F32), vmem((8, count), F32),
        vmem((n * slab, 3 * part)), vmem((part, width)), vmem((n * slab, 2 * ff)), vmem((ffp, width)),
        vmem((n * vec_rows, LANES), F32),
        inbox(RowSlots(slab, 3 * part)), inbox(RowSlots(out_rows, width, shares=True)), *[inbox(RowSlots(slab, 2 * units)) for _, units, _ in blocks_of(ff)],
        inbox(TileSlots(down_rows, down_cols)), inbox(RowSlots(vec_rows, LANES), F32),
        vmem((count // 2, width), F32), vmem((count // 2, width)), vmem((rows, width)),
        vmem((3 * count // 2, width)), vmem((3 * rows, width)),
        vmem((count, width)), vmem((rows, width), F32), vmem((rows, width)), vmem((count, part)), vmem((count, 3 * part)),
        vmem((count, LANES), F32), vmem((count, LANES), F32), vmem((8, width), F32), vmem((8, 3 * part), F32),
        vmem((slab, 2 * ff)), vmem((slab, 3 * part)), vmem((down_rows, down_cols)),
        vmem((out_rows, width)), vmem((m * vec_rows, LANES), F32), vmem((share, 3 * part * m)),
        vmem((down_rows // 2, width), F32), vmem((share, 2 * ff * m)),
    ]
    slots = (4 + len(blocks_of(ff))) * 2 * half + 3 * 2 + 2 + 2 + 3 * (m - 1) + 1
    return pl.pallas_call(
        functools.partial(backward_kernel, dims),
        out_shape=[jax.ShapeDtypeStruct(*a) for a in outputs],
        in_specs=[pl.BlockSpec(memory_space=pl.ANY)] * len(args),
        out_specs=[pl.BlockSpec(memory_space=pl.ANY)] * len(outputs),
        scratch_shapes=scratch
        + [
            pltpu.SemaphoreType.DMA((slots,)),
            pltpu.SemaphoreType.DMA((slots,)),
            pltpu.SemaphoreType.DMA((len(args) + 12,)),
            pltpu.SemaphoreType.DMA((len(outputs),)),
        ],
        compiler_params=pltpu.CompilerParams(
            collective_id=1, has_side_effects=True, vmem_limit_bytes=VMEM_BYTES
        ),
        name="backward",
    )(*args)


def rotary_lines(length):
    half = ROT // 2
    lane = np.arange(LANES) % HEAD_DIM
    angles = np.arange(length)[:, None] * (10000.0 ** (-(lane % half) * 2.0 / ROT))[None, :]
    cosine, sine = np.cos(angles), np.sin(angles)
    lines = [
        np.where(lane < ROT, cosine, 1.0),
        np.where(lane < half, -sine, 0.0),
        np.where((lane >= half) & (lane < ROT), sine, 0.0),
    ]
    return jnp.asarray(np.concatenate(lines, axis=1), F32)


def shards(tokens, cotangent, gain1, bias1, w_qkv, b_qkv, w_out, gain2, bias2, w_gate_up, w_down):
    n, m, s = lax.axis_size("dp"), lax.axis_size("seq"), lax.axis_index("seq")
    rows, width = tokens.shape
    slab = gain1.shape[0]
    inner, hidden = w_out.shape[0] * n, w_down.shape[0] * n
    part, ff = inner // m, hidden // m
    dims = (n, m, rows, width, slab, part, ff, b_qkv.shape[0] // LANES)
    parts = [gain1, bias1, gain2, bias2, b_qkv]
    total = sum(p.shape[0] for p in parts)
    length = -(-total // (TILE * LANES)) * TILE * LANES
    vec, at = jnp.zeros((length,), F32), 0
    for p in parts:
        vec = vec + jnp.pad(p.astype(F32), (at, length - at - p.shape[0]))
        at += p.shape[0]
    vec = vec.reshape(-1, LANES)
    rot = rotary_lines(rows * m)
    kept = run_forward(dims, (tokens, cotangent, w_qkv, w_gate_up, w_out, w_down, vec, rot))
    block_out, input_grad, g_gu, g_qkv, g_down, g_out, line = run_backward(dims, tuple(kept) + (rot,))
    vectors = [line[i, : size // m] for i, size in enumerate([slab] * 4 + [b_qkv.shape[0]])]
    return (
        block_out,
        input_grad,
        vectors[0],
        vectors[1],
        g_qkv.astype(F32),
        vectors[4],
        g_out.astype(F32),
        vectors[2],
        vectors[3],
        g_gu.astype(F32),
        g_down,
    )


def fits(mesh, shapes):
    n, m = mesh.shape["dp"], mesh.shape["seq"]
    (rows, width), slab = shapes[0], shapes[2][0]
    part, ff = shapes[6][0] * n // m, shapes[10][0] * n // m
    return (
        m == 4
        and n == 2 * m
        and rows % LANES == 0
        and shapes[6][0] == LANES
        and slab == 256
        and width % 512 == 0
        and shapes[5][0] % LANES == 0
        and part == 256
        and (ff // 2) + LANES - 1 <= WINDOW
        and ff // 2 + (ff // 2) % LANES <= WINDOW
        and shapes[9][1] // 2 % LANES == 0
        and 512 < ff <= 768
        and ff % 64 == 0
        and (2 * ff // n) % TILE == 0
        and 2 * ff <= width <= 4 * ff
        and 2 * 768 <= width
    )


def solution(mesh):
    rows, cols, vec = P(("dp", "seq"), None), P("dp", None), P("dp")
    flat = P(("dp", "seq"))
    def step(*args):
        body = shards if fits(mesh, [a.shape for a in args]) else shards_plain
        return body(*args)

    return jax.shard_map(
        step,
        mesh=mesh,
        in_specs=(rows, rows, vec, vec, cols, vec, cols, vec, vec, cols, cols),
        out_specs=(rows, rows, flat, flat, rows, flat, rows, flat, flat, rows, rows),
        check_vma=False,
    )
```
